32 devices in a mesh: dp: 8 (over z, core), rows: 4 (over y, x).
Axes of the slice: x: 2, y: 2, z: 4, core: 2. Of those that a mesh axis runs over, the one named last changes fastest.
Arguments:
- tokens: bfloat16 [32, 32, 32, 768], P('dp', 'rows'), may hold values from -6 to 6
- conditioning: bfloat16 [32, 768], P('dp'), may hold values from -6 to 6
- item_map: int32 [32, 32, 32], P('dp'), may hold values from 0 to 3, as said below
- ada_weight: bfloat16 [768, 4608], P(('dp', 'rows')), may hold values from -0.21875 to 0.21875
- ada_bias: bfloat16 [4608], P(('dp', 'rows')), may hold values from -3 to 3
- attn_kernel: bfloat16 [9, 768], P(None, ('dp', 'rows')), may hold values from -2 to 2
- qkv_weight: bfloat16 [768, 2304], P(('dp', 'rows')), may hold values from -0.21875 to 0.21875
- out_weight: bfloat16 [768, 768], P(('dp', 'rows')), may hold values from -2 to 2
- up_weight: bfloat16 [768, 3072], P(('dp', 'rows')), may hold values from -0.21875 to 0.21875
- ffn_kernel: bfloat16 [9, 3072], P(None, ('dp', 'rows')), may hold values from -2 to 2
- down_weight: bfloat16 [3072, 768], P(('dp', 'rows')), may hold values from -0.109375 to 0.109375
- out_cotangent: bfloat16 [32, 32, 32, 768], P('dp', 'rows'), may hold values from -6 to 6
Outputs:
- layer_out: bfloat16 [32, 32, 32, 768], P('dp', 'rows')
- token_grad: float32 [32, 32, 32, 768], P('dp', 'rows')
- derivative_of_context: float32 [32, 768], P('dp')
- ada_weight_grad: float32 [768, 4608], P(('dp', 'rows'))
- ada_bias_grad: float32 [4608], P(('dp', 'rows'))
- attn_kernel_grad: float32 [9, 768], P(None, ('dp', 'rows'))
- derivative_triple_matrix: float32 [768, 2304], P(('dp', 'rows'))
- out_weight_grad: float32 [768, 768], P(('dp', 'rows'))
- up_weight_grad: float32 [768, 3072], P(('dp', 'rows'))
- ffn_kernel_grad: float32 [9, 3072], P(None, ('dp', 'rows'))
- down_weight_grad: float32 [3072, 768], P(('dp', 'rows'))
The draws below stay inside these ranges and needn't reach their ends.
Inputs may be any that keep to these rules, and one draw needn't show every extreme that they name: `item_map`: in each canvas the labels 0 to 3 mark four latents, each a rectangle: 0 and 1 fill the first r rows, left and right of one column split; 2 and 3 fill the other rows, left and right of another split. r and both splits lie between 8 and 24, so every latent has 8 rows and columns or more.
All inputs are finite; a program needn't handle non-finite values.
Results may differ from the reference program's by a relative error of at most 0.019.
The reference program's roundings to bfloat16 on the way count: a program that leaves them out, or rounds other values in their place, can miss the bound.
Values may be sent and summed in bfloat16 or wider, within the bound.
A program may use at most 320 MiB of HBM per device.

```python
import jax
import jax.numpy as jnp
from jax import lax

D = 768
HEADS = 12
PER_GROUP_WIDTH = 64
FF = 3072
SIDE = 32
CANVASES = 32


def draw_item_map(key, part):
    first_key, second_key, third_key = jax.random.split(jax.random.fold_in(key, 7), 3)
    minimum_float = SIDE // 4
    highest = SIDE - SIDE // 4 + 1
    row_split = jax.random.randint(first_key, (CANVASES, 1, 1), minimum_float, highest)
    upper_split = jax.random.randint(second_key, (CANVASES, 1, 1), minimum_float, highest)
    lower_split = jax.random.randint(third_key, (CANVASES, 1, 1), minimum_float, highest)
    row_index = jnp.arange(SIDE, dtype=jnp.int32)[None, :, None]
    col_index = jnp.arange(SIDE, dtype=jnp.int32)[None, None, :]
    lower_half = (row_index >= row_split).astype(jnp.int32)
    col_split = jnp.where(lower_half == 1, lower_split, upper_split)
    return (2 * lower_half + (col_index >= col_split).astype(jnp.int32)).astype(jnp.int32)


def block_levels(own_key, shape, cuts, smallest, high):
    def one(position, parts):
        steps = jax.random.uniform(jax.random.fold_in(jax.random.fold_in(own_key, 6), position), (parts,), jnp.float32, smallest / len(cuts), high / len(cuts))
        return jnp.repeat(jnp.exp(steps), shape[position] // parts).reshape((-1,) + (1,) * (len(shape) - position - 1))

    factor_of = one(*cuts[0])
    for cut in cuts[1:]:
        factor_of = factor_of * one(*cut)
    return factor_of


def bell_draw(own_key, shape, spread, limit, cuts=(), kind=jnp.bfloat16):
    level = block_levels(own_key, shape, cuts, -0.22, 0.18) if cuts else 1.0
    array = jax.random.normal(own_key, shape, jnp.float32) * spread * level
    return jnp.minimum(jnp.maximum(array, -limit), limit).astype(kind)


def setup_inputs(seed: int = 0) -> dict:
    key_list = jax.random.split(jax.random.key(seed), 13)
    tokens = bell_draw(key_list[0], (CANVASES, SIDE, SIDE, D), 1.0, 6.0, ((0, 8), (1, 4)))
    conditioning = bell_draw(key_list[1], (CANVASES, D), 1.0, 6.0, ((0, 8),))
    item_map = draw_item_map(jax.random.fold_in(key_list[12], 71), 0)
    ada_weight = bell_draw(key_list[3], (D, 6 * D), D ** -0.5, 0.21875, ((0, 32),))
    ada_bias = bell_draw(key_list[4], (6 * D,), 0.5, 3.0, ((0, 32),))
    attn_kernel = bell_draw(key_list[5], (9, D), 9 ** -0.5, 2.0, ((1, 32),))
    qkv_weight = bell_draw(key_list[6], (D, 3 * D), D ** -0.5, 0.21875, ((0, 32),))
    out_weight = bell_draw(key_list[7], (D, D), (max(D // (SIDE * SIDE // 10), 1)) ** -0.5, 2.0, ((0, 32),))
    up_weight = bell_draw(key_list[8], (D, FF), D ** -0.5, 0.21875, ((0, 32),))
    ffn_kernel = bell_draw(key_list[9], (9, FF), 9 ** -0.5, 2.0, ((1, 32),))
    down_weight = bell_draw(key_list[10], (FF, D), FF ** -0.5, 0.109375, ((0, 32),))
    out_cotangent = bell_draw(key_list[11], (CANVASES, SIDE, SIDE, D), 1.0, 6.0, ((0, 8), (1, 4)))
    return dict(tokens=tokens, conditioning=conditioning, item_map=item_map, ada_weight=ada_weight, ada_bias=ada_bias, attn_kernel=attn_kernel, qkv_weight=qkv_weight, out_weight=out_weight, up_weight=up_weight, ffn_kernel=ffn_kernel, down_weight=down_weight, out_cotangent=out_cotangent)


PRECISE = lax.Precision.HIGHEST
EPSILON = 1e-06

@jax.custom_vjp
def low(v):
    return lax.optimization_barrier(v.astype(jnp.bfloat16)).astype(jnp.float32)

@jax.custom_vjp
def low_back(v):
    return v

def low_keep(v):
    return (low(v), None)

def low_pass(kept, grad):
    return (grad,)

def back_keep(v):
    return (v, None)

def back_low(kept, grad):
    return (low(grad),)
low.defvjp(low_keep, low_pass)
low_back.defvjp(back_keep, back_low)

def normalize(attended_content_array):
    average = lax.optimization_barrier(jnp.mean(attended_content_array, axis=-1, keepdims=True))
    centred = attended_content_array - average
    return centred * lax.rsqrt(lax.optimization_barrier(jnp.mean(centred * centred, axis=-1, keepdims=True)) + EPSILON)

def conv_linked(attended_content_array, labels, kernel):
    extent = attended_content_array.shape[0]
    padded_rows = jnp.pad(attended_content_array, ((1, 1), (1, 1), (0, 0)))
    labels_pad = jnp.pad(labels, 1, constant_values=-1)
    summed = jnp.zeros(attended_content_array.shape, jnp.float32)
    for row_off in range(3):
        for col_off in range(3):
            linked = labels_pad[row_off:row_off + extent, col_off:col_off + extent] == labels
            tapped = kernel[3 * row_off + col_off] * padded_rows[row_off:row_off + extent, col_off:col_off + extent]
            summed = summed + jnp.where(linked[..., None], tapped, 0.0)
    return summed

def block_forward(canvas, cond_row, labels, weights):
    ada_weight, ada_bias, attn_kernel, qkv_weight, out_weight, up_weight, ffn_kernel, down_weight = weights
    extent = canvas.shape[0]
    features = canvas.shape[-1]
    cell_count = extent * extent
    silu_low = low(jax.nn.silu(cond_row))
    modulation = low_back(jnp.dot(silu_low[None, :], ada_weight, precision=PRECISE)[0] + ada_bias)
    shift_one, scale_one, gate_one, shift_two, scale_two, gate_two = jnp.split(modulation, 6)
    modulated_one = low(normalize(canvas) * (1.0 + scale_one) + shift_one)
    local_mix = low(low_back(conv_linked(modulated_one, labels, attn_kernel)))
    projected = low(low_back(jnp.dot(local_mix.reshape(cell_count, features), qkv_weight, precision=PRECISE)))
    projected = projected.reshape(cell_count, 3, HEADS, PER_GROUP_WIDTH)
    scores = low_back(jnp.einsum('qhd,khd->hqk', projected[:, 0], projected[:, 1], precision=PRECISE) * PER_GROUP_WIDTH ** (-0.5))
    flat_labels = labels.reshape(cell_count)
    linked = flat_labels[:, None] == flat_labels[None, :]
    attention = jax.nn.softmax(jnp.where(linked[None], scores, -1e+30), axis=-1)
    attended = low(low_back(jnp.einsum('hqk,khd->qhd', low(attention), projected[:, 2], precision=PRECISE)))
    attended = attended.reshape(cell_count, features)
    attn_branch = low_back(jnp.dot(attended, out_weight, precision=PRECISE)).reshape(canvas.shape)
    middle = canvas + gate_one * attn_branch
    modulated_two = low(normalize(middle) * (1.0 + scale_two) + shift_two)
    hidden_up_projection = low(low_back(jnp.dot(modulated_two.reshape(cell_count, features), up_weight, precision=PRECISE)))
    hidden_up_projection = hidden_up_projection.reshape(extent, extent, -1)
    pre_gelu = low_back(conv_linked(hidden_up_projection, labels, ffn_kernel))
    gelu_low = low(jax.nn.gelu(pre_gelu)).reshape(cell_count, -1)
    ffn_branch = low_back(jnp.dot(gelu_low, down_weight, precision=PRECISE)).reshape(canvas.shape)
    return middle + gate_two * ffn_branch

def reference(tokens, conditioning, item_map, ada_weight, ada_bias, attn_kernel, qkv_weight, out_weight, up_weight, ffn_kernel, down_weight, out_cotangent):
    weights = tuple((entry.astype(jnp.float32) for entry in (ada_weight, ada_bias, attn_kernel, qkv_weight, out_weight, up_weight, ffn_kernel, down_weight)))

    def forward(token_values, cond_values, weight_values):

        def single_canvas(packed):
            return block_forward(packed[0], packed[1], packed[2], weight_values)
        return lax.map(jax.checkpoint(single_canvas), (token_values, cond_values, item_map))
    result, backward = jax.vjp(forward, tokens.astype(jnp.float32), conditioning.astype(jnp.float32), weights)
    token_grad, cond_grad, weight_grads = backward(out_cotangent.astype(jnp.float32))
    return (result.astype(jnp.bfloat16), token_grad, cond_grad, weight_grads[0], weight_grads[1], weight_grads[2], weight_grads[3], weight_grads[4], weight_grads[5], weight_grads[6], weight_grads[7])
```

```python
import functools

import jax
import jax.numpy as jnp
from jax import lax
from jax.experimental import pallas as pl
from jax.experimental.pallas import tpu as pltpu
from jax.sharding import PartitionSpec as P

PER_GROUP_WIDTH = 64


EPSILON = 1e-06


def padded(block, sides, width):
    for axis, dim in sides:
        count = lax.axis_size(axis)
        forward = [(i, i + 1) for i in range(count - 1)]
        backward = [(target, source) for source, target in forward]
        low = lax.ppermute(
            lax.slice_in_dim(block, block.shape[dim] - width, None, axis=dim), axis, forward
        )
        high = lax.ppermute(lax.slice_in_dim(block, 0, width, axis=dim), axis, backward)
        block = jnp.concatenate([low, block, high], axis=dim)
    return block


def normalize(attended_content_array):
    average = jnp.mean(attended_content_array, axis=-1, keepdims=True)
    centred = attended_content_array - average
    inverse = lax.rsqrt(jnp.mean(centred * centred, axis=-1, keepdims=True) + EPSILON)
    return (centred * inverse, inverse)


def normalize_back(incoming, normalized_rows, inverse):
    return inverse * (
        incoming
        - jnp.mean(incoming, axis=-1, keepdims=True)
        - normalized_rows * jnp.mean(incoming * normalized_rows, axis=-1, keepdims=True)
    )


def widen_cols(rimmed):
    return jnp.pad(rimmed, ((0, 0), (0, 0), (1, 1), (0, 0)))


def tap_mask(labels_pad, centre, row_off, col_off):
    rows_here = centre.shape[1]
    cols_here = centre.shape[2]
    return (labels_pad[:, row_off : row_off + rows_here, col_off : col_off + cols_here] == centre)[
        ..., None
    ]


def conv_forward(padded_rows, labels_pad, centre, kernel):
    rows_here = centre.shape[1]
    cols_here = centre.shape[2]
    summed = jnp.zeros(centre.shape + (kernel.shape[1],), jnp.float32)
    for row_off in range(3):
        for col_off in range(3):
            window = padded_rows[
                :, row_off : row_off + rows_here, col_off : col_off + cols_here
            ].astype(jnp.float32)
            tapped = kernel[3 * row_off + col_off].astype(jnp.float32) * window
            summed = summed + jnp.where(tap_mask(labels_pad, centre, row_off, col_off), tapped, 0.0)
    return summed


def conv_mirror(padded_rows, labels_pad, centre, kernel):
    rows_here = centre.shape[1]
    cols_here = centre.shape[2]
    summed = jnp.zeros(centre.shape + (kernel.shape[1],), jnp.float32)
    for row_off in range(3):
        for col_off in range(3):
            row_from = 2 - row_off
            col_from = 2 - col_off
            window = padded_rows[
                :, row_from : row_from + rows_here, col_from : col_from + cols_here
            ].astype(jnp.float32)
            tapped = kernel[3 * row_off + col_off].astype(jnp.float32) * window
            summed = summed + jnp.where(
                tap_mask(labels_pad, centre, row_from, col_from), tapped, 0.0
            )
    return summed


def kernel_grad(incoming, padded_rows, labels_pad, centre):
    rows_here = centre.shape[1]
    cols_here = centre.shape[2]
    incoming_values = incoming.astype(jnp.float32)
    tap_sums = []
    for row_off in range(3):
        for col_off in range(3):
            window = padded_rows[
                :, row_off : row_off + rows_here, col_off : col_off + cols_here
            ].astype(jnp.float32)
            product = jnp.where(
                tap_mask(labels_pad, centre, row_off, col_off), incoming_values * window, 0.0
            )
            tap_sums.append(jnp.sum(product, axis=(0, 1, 2)))
    return jnp.stack(tap_sums, axis=0)


def contract_rows(left, right):
    return lax.dot_general(
        left, right, (((0,), (0,)), ((), ())), preferred_element_type=jnp.float32
    )


def contract_cols(left, right):
    return lax.dot_general(
        left, right, (((1,), (1,)), ((), ())), preferred_element_type=jnp.float32
    )


def local(
    tokens,
    conditioning,
    item_map,
    ada_weight,
    ada_bias,
    attn_kernel,
    qkv_weight,
    out_weight,
    up_weight,
    ffn_kernel,
    down_weight,
    out_cotangent,
):
    canvases, rows_here, cols_here, features = tokens.shape
    cell_count = canvases * rows_here * cols_here
    position = lax.axis_index("rows")
    gathered = (
        lax.all_gather(ada_weight, ("dp", "rows"), axis=0, tiled=True),
        lax.all_gather(ada_bias, ("dp", "rows"), axis=0, tiled=True),
        lax.all_gather(attn_kernel, ("dp", "rows"), axis=1, tiled=True),
        lax.all_gather(qkv_weight, ("dp", "rows"), axis=0, tiled=True),
        lax.all_gather(out_weight, ("dp", "rows"), axis=0, tiled=True),
        lax.all_gather(up_weight, ("dp", "rows"), axis=0, tiled=True),
        lax.all_gather(ffn_kernel, ("dp", "rows"), axis=1, tiled=True),
        lax.all_gather(down_weight, ("dp", "rows"), axis=0, tiled=True),
    )
    ada_full, bias_full, kernel_attn, triple_full, out_full, up_full, kernel_ffn, down_full = (
        gathered
    )
    hidden_units = up_full.shape[1]
    head_count = features // PER_GROUP_WIDTH
    logit_divisor = PER_GROUP_WIDTH ** (-0.5)
    labels_pad = jnp.pad(item_map, ((0, 0), (1, 1), (1, 1)), constant_values=-1)
    labels_here = lax.dynamic_slice_in_dim(labels_pad, position * rows_here, rows_here + 2, 1)
    centre = labels_here[:, 1:-1, 1:-1]
    cond_values = conditioning.astype(jnp.float32)
    silu_low = jax.nn.silu(cond_values).astype(jnp.bfloat16)
    modulation = jnp.dot(silu_low, ada_full, preferred_element_type=jnp.float32) + bias_full.astype(
        jnp.float32
    )
    layer_stack = modulation.reshape(canvases, 6, 1, 1, features)
    shift_one, scale_one, gate_one, shift_two, scale_two, gate_two = (
        layer_stack[:, index] for index in range(6)
    )
    token_values = tokens.astype(jnp.float32)
    normed_one, inverse_one = normalize(token_values)
    modulated_one = (normed_one * (1.0 + scale_one) + shift_one).astype(jnp.bfloat16)
    modulated_padded = widen_cols(padded(modulated_one, (("rows", 1),), 1))
    local_mix = conv_forward(modulated_padded, labels_here, centre, kernel_attn).astype(
        jnp.bfloat16
    )
    mix_rows = local_mix.reshape(cell_count, features)
    projected = jnp.dot(mix_rows, triple_full, preferred_element_type=jnp.float32).astype(
        jnp.bfloat16
    )
    projected = projected.reshape(canvases, rows_here * cols_here, 3 * features)
    queries = projected[..., :features]
    key_rows = projected[..., features : 2 * features]
    value_rows = projected[..., 2 * features :]
    keys_all, values_all = (
        lax.all_gather(key_rows, "rows", axis=1, tiled=True),
        lax.all_gather(value_rows, "rows", axis=1, tiled=True),
    )
    query_heads = queries.reshape(canvases, -1, head_count, PER_GROUP_WIDTH)
    key_heads = keys_all.reshape(canvases, -1, head_count, PER_GROUP_WIDTH)
    value_heads = values_all.reshape(canvases, -1, head_count, PER_GROUP_WIDTH)
    scores = (
        jnp.einsum("bqhd,bkhd->bhqk", query_heads, key_heads, preferred_element_type=jnp.float32)
        * logit_divisor
    )
    label_rows = centre.reshape(canvases, -1)
    label_keys = item_map.reshape(canvases, -1)
    linked = label_rows[:, None, :, None] == label_keys[:, None, None, :]
    masked = jnp.where(linked, scores, -1e30)
    row_peak = jnp.max(masked, axis=-1, keepdims=True)
    raised = jnp.exp(masked - row_peak)
    row_total = jnp.sum(raised, axis=-1, keepdims=True)
    attention = raised / row_total
    attention_low = attention.astype(jnp.bfloat16)
    attended = jnp.einsum(
        "bhqk,bkhd->bqhd", attention_low, value_heads, preferred_element_type=jnp.float32
    ).astype(jnp.bfloat16)
    attended = attended.reshape(cell_count, features)
    attn_branch = jnp.dot(attended, out_full, preferred_element_type=jnp.float32).reshape(
        tokens.shape
    )
    middle = token_values + gate_one * attn_branch
    normed_two, inverse_two = normalize(middle)
    modulated_two = (normed_two * (1.0 + scale_two) + shift_two).astype(jnp.bfloat16)
    modulated_rows = modulated_two.reshape(cell_count, features)
    hidden_up_projection = jnp.dot(
        modulated_rows, up_full, preferred_element_type=jnp.float32
    ).astype(jnp.bfloat16)
    hidden_up_projection = hidden_up_projection.reshape(
        canvases, rows_here, cols_here, hidden_units
    )
    up_padded = widen_cols(padded(hidden_up_projection, (("rows", 1),), 1))
    pre_gelu = conv_forward(up_padded, labels_here, centre, kernel_ffn)
    activated, gelu_back = jax.vjp(jax.nn.gelu, pre_gelu)
    gelu_low = activated.astype(jnp.bfloat16).reshape(cell_count, hidden_units)
    ffn_branch = jnp.dot(gelu_low, down_full, preferred_element_type=jnp.float32).reshape(
        tokens.shape
    )
    layer_out = (middle + gate_two * ffn_branch).astype(jnp.bfloat16)
    weights_back = (
        lax.all_gather(ada_weight, ("dp", "rows"), axis=0, tiled=True),
        lax.all_gather(ada_bias, ("dp", "rows"), axis=0, tiled=True),
        lax.all_gather(attn_kernel, ("dp", "rows"), axis=1, tiled=True),
        lax.all_gather(qkv_weight, ("dp", "rows"), axis=0, tiled=True),
        lax.all_gather(out_weight, ("dp", "rows"), axis=0, tiled=True),
        lax.all_gather(up_weight, ("dp", "rows"), axis=0, tiled=True),
        lax.all_gather(ffn_kernel, ("dp", "rows"), axis=1, tiled=True),
        lax.all_gather(down_weight, ("dp", "rows"), axis=0, tiled=True),
    )
    (
        ada_back,
        bias_back,
        kernel_attn_back,
        triple_back,
        out_back,
        up_back,
        kernel_ffn_back,
        down_projection_back,
    ) = weights_back
    incoming = out_cotangent.astype(jnp.float32)
    grad_gate_two = jnp.sum(incoming * ffn_branch, axis=(1, 2))
    grad_ffn = (gate_two * incoming).astype(jnp.bfloat16).reshape(cell_count, features)
    grad_down = contract_rows(gelu_low, grad_ffn)
    grad_gelu = contract_cols(grad_ffn, down_projection_back).reshape(
        canvases, rows_here, cols_here, hidden_units
    )
    grad_pre = gelu_back(grad_gelu)[0].astype(jnp.bfloat16)
    grad_pre_padded = widen_cols(padded(grad_pre, (("rows", 1),), 1))
    grad_kernel_ffn = kernel_grad(grad_pre, up_padded, labels_here, centre)
    grad_up = (
        conv_mirror(grad_pre_padded, labels_here, centre, kernel_ffn_back)
        .astype(jnp.bfloat16)
        .reshape(cell_count, hidden_units)
    )
    grad_up_weight = contract_rows(modulated_rows, grad_up)
    grad_mod_two = contract_cols(grad_up, up_back).reshape(tokens.shape)
    grad_scale_two = jnp.sum(grad_mod_two * normed_two, axis=(1, 2))
    grad_shift_two = jnp.sum(grad_mod_two, axis=(1, 2))
    grad_middle = incoming + normalize_back(
        grad_mod_two * (1.0 + scale_two), normed_two, inverse_two
    )
    grad_gate_one = jnp.sum(grad_middle * attn_branch, axis=(1, 2))
    grad_attn = (gate_one * grad_middle).astype(jnp.bfloat16).reshape(cell_count, features)
    grad_out_weight = contract_rows(attended, grad_attn)
    grad_attended = (
        contract_cols(grad_attn, out_back)
        .astype(jnp.bfloat16)
        .reshape(canvases, -1, head_count, PER_GROUP_WIDTH)
    )
    grad_weights = jnp.einsum(
        "bqhd,bkhd->bhqk", grad_attended, value_heads, preferred_element_type=jnp.float32
    )
    row_delta = jnp.sum(attention * grad_weights, axis=-1, keepdims=True)
    grad_scores = (attention * (grad_weights - row_delta)).astype(jnp.bfloat16)
    grad_query = (
        jnp.einsum("bhqk,bkhd->bqhd", grad_scores, key_heads, preferred_element_type=jnp.float32)
        * logit_divisor
    )
    grad_key_all = (
        jnp.einsum("bhqk,bqhd->bkhd", grad_scores, query_heads, preferred_element_type=jnp.float32)
        * logit_divisor
    )
    value_gradient_full = jnp.einsum(
        "bhqk,bqhd->bkhd", attention_low, grad_attended, preferred_element_type=jnp.float32
    )
    grad_key, grad_value = (
        lax.psum_scatter(
            grad_key_all.reshape(canvases, -1, features).astype(jnp.bfloat16),
            "rows",
            scatter_dimension=1,
            tiled=True,
        ).astype(jnp.float32),
        lax.psum_scatter(
            value_gradient_full.reshape(canvases, -1, features).astype(jnp.bfloat16),
            "rows",
            scatter_dimension=1,
            tiled=True,
        ).astype(jnp.float32),
    )
    grad_projected = jnp.concatenate(
        [
            grad_query.reshape(cell_count, features),
            grad_key.reshape(cell_count, features),
            grad_value.reshape(cell_count, features),
        ],
        axis=-1,
    ).astype(jnp.bfloat16)
    grad_qkv_weight = contract_rows(mix_rows, grad_projected)
    grad_mix = contract_cols(grad_projected, triple_back).astype(jnp.bfloat16).reshape(tokens.shape)
    grad_mix_padded = widen_cols(padded(grad_mix, (("rows", 1),), 1))
    grad_kernel_attn = kernel_grad(grad_mix, modulated_padded, labels_here, centre)
    grad_mod_one = conv_mirror(grad_mix_padded, labels_here, centre, kernel_attn_back)
    grad_scale_one = jnp.sum(grad_mod_one * normed_one, axis=(1, 2))
    grad_shift_one = jnp.sum(grad_mod_one, axis=(1, 2))
    token_grad = grad_middle + normalize_back(
        grad_mod_one * (1.0 + scale_one), normed_one, inverse_one
    )
    grad_parts = jnp.concatenate(
        [
            grad_shift_one,
            grad_scale_one,
            grad_gate_one,
            grad_shift_two,
            grad_scale_two,
            grad_gate_two,
        ],
        axis=-1,
    )
    grad_modulation = lax.psum(grad_parts.astype(jnp.bfloat16), "rows")
    leader = (position == 0).astype(jnp.float32)
    grad_ada_weight = contract_rows(silu_low, grad_modulation) * leader
    grad_ada_bias = jnp.sum(grad_modulation.astype(jnp.float32), axis=0) * leader
    silu_values, silu_back = jax.vjp(jax.nn.silu, cond_values)
    derivative_of_context = silu_back(contract_cols(grad_modulation, ada_back))[0]
    summed_grads = (
        lax.psum_scatter(grad_ada_weight, ("dp", "rows"), scatter_dimension=0, tiled=True),
        lax.psum_scatter(grad_ada_bias, ("dp", "rows"), scatter_dimension=0, tiled=True),
        lax.psum_scatter(grad_kernel_attn, ("dp", "rows"), scatter_dimension=1, tiled=True),
        lax.psum_scatter(grad_qkv_weight, ("dp", "rows"), scatter_dimension=0, tiled=True),
        lax.psum_scatter(grad_out_weight, ("dp", "rows"), scatter_dimension=0, tiled=True),
        lax.psum_scatter(grad_up_weight, ("dp", "rows"), scatter_dimension=0, tiled=True),
        lax.psum_scatter(grad_kernel_ffn, ("dp", "rows"), scatter_dimension=1, tiled=True),
        lax.psum_scatter(grad_down, ("dp", "rows"), scatter_dimension=0, tiled=True),
    )
    return (layer_out, token_grad, derivative_of_context) + tuple(summed_grads)


F32=jnp.float32; BF=jnp.bfloat16
NT=(((1,),(1,)),((),()))
TN=(((0,),(0,)),((),()))

def head_masks(labels):
    cells=labels.shape[0]
    lane=lax.broadcasted_iota(jnp.int32,(cells,128),1)%64
    lab=labels[:,None]
    qm=(lane==lab).astype(BF)
    km=jnp.where((lane!=lab)&(lane<4),-1e30,0.0).astype(BF)
    return qm,km

def attn_fwd_kernel(q_ref,k_ref,v_ref,qm_ref,km_ref,o_ref,lse_ref,*,scale,qb):
    p=pl.program_id(0)
    cells=q_ref.shape[0]
    nq=cells//qb
    lane=lax.broadcasted_iota(jnp.int32,(1,128),1)
    @pl.when(p==0)
    def _():
        lse_ref[...]=jnp.zeros_like(lse_ref)
    for h in range(2):
        mine=(lane//64)==h
        k=jnp.where(mine,k_ref[...],km_ref[...])
        def body(i,c):
            rows=pl.ds(pl.multiple_of(i*qb,qb),qb)
            q=jnp.where(mine,q_ref[rows,:]*jnp.asarray(scale,BF),qm_ref[rows,:])
            s=lax.dot_general(q,k,NT,preferred_element_type=F32)
            m=jnp.max(s,axis=1,keepdims=True)
            e=jnp.exp(s-m)
            l=jnp.sum(e,axis=1,keepdims=True)
            a=(e*(1.0/l)).astype(BF)
            o=lax.dot_general(a,v_ref[...],(((1,),(0,)),((),())),preferred_element_type=F32).astype(BF)
            if h==0:
                o_ref[rows,:]=o
            else:
                o_ref[rows,:]=jnp.where(mine,o,o_ref[rows,:])
            lse_ref[rows,:]=jnp.where(lane==2*p+h,m+jnp.log(l),lse_ref[rows,:])
            return c
        lax.fori_loop(0,nq,body,0)

def attn_fwd(projected,qm,km,features,qb=256):
    cells=projected.shape[0]
    pairs=features//128
    blk=lambda off: pl.BlockSpec((cells,128),lambda p: (0,off+p))
    full=pl.BlockSpec((cells,128),lambda p:(0,0))
    return pl.pallas_call(
        functools.partial(attn_fwd_kernel,scale=0.125,qb=qb),
        grid=(pairs,),
        in_specs=[blk(0),blk(pairs),blk(2*pairs),full,full],
        out_specs=[blk(0),full],
        out_shape=[jax.ShapeDtypeStruct((cells,features),BF),jax.ShapeDtypeStruct((cells,128),F32)],
        compiler_params=pltpu.CompilerParams(dimension_semantics=("arbitrary",),vmem_limit_bytes=60<<20),
        name="attn_fwd",
    )(projected,projected,projected,qm,km)

def attn_bwd_kernel(q_ref,k_ref,v_ref,do_ref,o_ref,qm_ref,km_ref,lse_ref,dq_ref,dk_ref,dv_ref,qs,dqt,*,scale,kb):
    p=pl.program_id(0)
    cells=q_ref.shape[0]
    nk=cells//kb
    lane=lax.broadcasted_iota(jnp.int32,(1,128),1)
    sub=lax.broadcasted_iota(jnp.int32,(128,1),0)
    prod=do_ref[...].astype(F32)*o_ref[...].astype(F32)
    hi=prod.astype(BF); lo=(prod-hi.astype(F32)).astype(BF)
    srow=lax.broadcasted_iota(jnp.int32,(8,128),0)
    slane=lax.broadcasted_iota(jnp.int32,(8,128),1)
    sel=(slane//64==srow).astype(BF)
    delta=lax.dot_general(sel,hi,NT,preferred_element_type=F32)+lax.dot_general(sel,lo,NT,preferred_element_type=F32)
    qs[...]=q_ref[...]*jnp.asarray(scale,BF)
    for h in range(2):
        mine=(lane//64)==h
        q=jnp.where(mine,qs[...],qm_ref[...])
        lse=lse_ref[pl.ds(2*p+h,1),:]
        dl=delta[h:h+1,:]
        dqt[...]=jnp.zeros_like(dqt)
        def body(i,c):
            rows=pl.ds(pl.multiple_of(i*kb,kb),kb)
            kr=k_ref[rows,:]
            k=jnp.where(mine,kr,km_ref[rows,:])
            v=jnp.where(mine,v_ref[rows,:],jnp.zeros((),BF))
            st=lax.dot_general(k,q,NT,preferred_element_type=F32)
            pt=jnp.exp(st-lse)
            dpt=lax.dot_general(v,do_ref[...],NT,preferred_element_type=F32)
            ds=(pt*(dpt-dl)).astype(BF)
            dv=lax.dot_general(pt.astype(BF),do_ref[...],(((1,),(0,)),((),())),preferred_element_type=F32).astype(BF)
            dk=lax.dot_general(ds,qs[...],(((1,),(0,)),((),())),preferred_element_type=F32).astype(BF)
            dqt[...]+=lax.dot_general(kr,ds,TN,preferred_element_type=F32)
            if h==0:
                dv_ref[rows,:]=dv
                dk_ref[rows,:]=dk
            else:
                dv_ref[rows,:]=jnp.where(mine,dv,dv_ref[rows,:])
                dk_ref[rows,:]=jnp.where(mine,dk,dk_ref[rows,:])
            return c
        lax.fori_loop(0,nk,body,0)
        dq=(jnp.transpose(dqt[...])*scale).astype(BF)
        if h==0:
            dq_ref[...]=dq
        else:
            dq_ref[...]=jnp.where(mine,dq,dq_ref[...])

def attn_bwd(projected,dout,out,qm,km,lse_t,features,kb=256):
    cells=projected.shape[0]
    pairs=features//128
    blk=lambda off: pl.BlockSpec((cells,128),lambda p: (0,off+p))
    full=pl.BlockSpec((cells,128),lambda p:(0,0))
    o=jax.ShapeDtypeStruct((cells,features),BF)
    return pl.pallas_call(
        functools.partial(attn_bwd_kernel,scale=0.125,kb=kb),
        grid=(pairs,),
        in_specs=[blk(0),blk(pairs),blk(2*pairs),blk(0),blk(0),full,full,pl.BlockSpec((128,cells),lambda p:(0,0))],
        out_specs=[blk(0),blk(0),blk(0)],
        out_shape=[o,o,o],
        scratch_shapes=[pltpu.VMEM((cells,128),BF),pltpu.VMEM((128,cells),F32)],
        compiler_params=pltpu.CompilerParams(dimension_semantics=("arbitrary",),vmem_limit_bytes=60<<20),
        name="attn_bwd",
    )(projected,projected,projected,dout,out,qm,km,lse_t)

MESH=pl.DeviceIdType.MESH
NZ,NC,NR=4,2,4


def here():
    dp=lax.axis_index("dp"); rows=lax.axis_index("rows")
    return dp//NC, lax.rem(dp,NC), rows


def dev(z,core,rows):
    return (z*NC+core, rows)


def partner_xy(rows,t):
    x=lax.rem(rows,2); y=rows//2
    tx=t%2; ty=t//2
    nx=1-x if tx else x
    ny=1-y if ty else y
    return ny*2+nx


def rcopy(src,dst,ssem,rsem,target):
    return pltpu.make_async_remote_copy(src_ref=src,dst_ref=dst,send_sem=ssem,recv_sem=rsem,device_id=target,device_id_type=MESH)


def barrier_all():
    dp=lax.axis_index("dp"); rows=lax.axis_index("rows")
    me=dp*NR+rows
    total=NZ*NC*NR
    bar=pltpu.get_barrier_semaphore()
    def body(k,c):
        other=lax.rem(me+k,total)
        pl.semaphore_signal(bar,inc=1,device_id=(other//NR,lax.rem(other,NR)),device_id_type=MESH)
        return c
    lax.fori_loop(1,total,body,0)
    pl.semaphore_wait(bar,total-1)


def zmod(v):
    return lax.rem(v+NZ,NZ)


class Gather:
    SEMS=[(NZ,),(NZ,),(NZ,NR),(NZ,NR),(NZ,NR),(NZ,NR),(1,)]

    def __init__(self,shard,full,sems):
        self.shard,self.full=shard,full
        self.sz,self.rz,self.sx,self.rx,self.sc,self.rc,self.lo=sems
        self.z,self.core,self.rows=here()

    def slot(self,dz,t,core):
        rows=self.rows if t==0 else partner_xy(self.rows,t)
        return self.full.at[zmod(self.z-dz),core,rows]

    def zcopy(self,dz,receive=False):
        dst=self.slot(dz if receive else 0,0,self.core)
        return rcopy(self.shard,dst,self.sz.at[dz],self.rz.at[dz],dev(zmod(self.z+dz),self.core,self.rows))

    def piece(self,dz):
        return self.shard if dz==0 else self.slot(dz,0,self.core)

    def xcopy(self,dz,t,receive=False):
        dst=self.slot(dz,t if receive else 0,self.core)
        return rcopy(self.piece(dz),dst,self.sx.at[dz,t],self.rx.at[dz,t],dev(self.z,self.core,partner_xy(self.rows,t)))

    def ccopy(self,dz,t,receive=False):
        src=self.piece(dz) if t==0 else self.slot(dz,t,self.core)
        dst=self.slot(dz,t,1-self.core if receive else self.core)
        return rcopy(src,dst,self.sc.at[dz,t],self.rc.at[dz,t],dev(self.z,1-self.core,self.rows))

    def local(self):
        return pltpu.make_async_copy(self.shard,self.slot(0,0,self.core),self.lo.at[0])

    def start(self):
        for dz in range(1,NZ):
            self.zcopy(dz).start()
        for t in range(1,NR):
            self.xcopy(0,t).start()
        self.ccopy(0,0).start()
        self.local().start()

    def zstep(self,dz):
        self.zcopy(dz,True).wait_recv()
        for t in range(1,NR):
            self.xcopy(dz,t).start()
        self.ccopy(dz,0).start()

    def xstep(self,dz,t):
        self.xcopy(dz,t,True).wait_recv()
        self.ccopy(dz,t).start()

    def finish(self):
        for dz in range(NZ):
            for t in range(NR):
                self.ccopy(dz,t,True).wait_recv()
        for dz in range(1,NZ):
            self.zcopy(dz).wait_send()
        for dz in range(NZ):
            for t in range(NR):
                if t: self.xcopy(dz,t).wait_send()
                self.ccopy(dz,t).wait_send()
        self.local().wait()

    def run_z(self):
        for dz in range(1,NZ): self.zstep(dz)

    def run_x(self):
        for dz in range(NZ):
            for t in range(1,NR): self.xstep(dz,t)


class Scatter:
    SEMS=[(1,),(1,),(1,),(NR,),(NR,),(NZ,),(NZ,)]

    @staticmethod
    def scratch(r,c,dt):
        return [pltpu.VMEM((NZ,NR,r,c),dt),pltpu.VMEM((NZ,NR,r,c),dt),pltpu.VMEM((NR,NZ,r,c),dt),pltpu.VMEM((NZ,r,c),dt),pltpu.VMEM((NZ,r,c),dt)]

    def __init__(self,part,out,bufs,sems):
        self.part,self.out=part,out
        self.own,self.sib,self.xin,self.zout,self.zin=bufs
        self.lo,self.sc,self.rc,self.sx,self.rx,self.sz,self.rz=sems
        self.z,self.core,self.rows=here()
        self.dt=self.own.dtype

    def lcopy(self):
        return pltpu.make_async_copy(self.part.at[:,self.core],self.own,self.lo.at[0])

    def ccopy(self):
        return rcopy(self.part.at[:,1-self.core],self.sib,self.sc.at[0],self.rc.at[0],dev(self.z,1-self.core,self.rows))

    def xcopy(self,t):
        to=partner_xy(self.rows,t)
        return rcopy(self.own.at[:,to],self.xin.at[t],self.sx.at[t],self.rx.at[t],dev(self.z,self.core,to))

    def zcopy(self,dz):
        to=zmod(self.z+dz)
        return rcopy(self.zout.at[to],self.zin.at[dz],self.sz.at[dz],self.rz.at[dz],dev(to,self.core,self.rows))

    def start(self):
        self.ccopy().start(); self.lcopy().start()

    def cstep(self):
        self.lcopy().wait(); self.ccopy().wait_recv()
        def body(i,c):
            a,b=i//NR,lax.rem(i,NR)
            self.own[a,b]=(self.own[a,b].astype(F32)+self.sib[a,b].astype(F32)).astype(self.dt)
            return c
        lax.fori_loop(0,NZ*NR,body,0)
        for t in range(1,NR): self.xcopy(t).start()

    def xstep(self):
        for t in range(1,NR): self.xcopy(t).wait_recv()
        def body(a,c):
            s=self.own[a,self.rows].astype(F32)
            for t in range(1,NR): s=s+self.xin[t,a].astype(F32)
            self.zout[a]=s.astype(self.dt)
            return c
        lax.fori_loop(0,NZ,body,0)
        for dz in range(1,NZ): self.zcopy(dz).start()

    def zstep(self):
        for dz in range(1,NZ): self.zcopy(dz).wait_recv()
        s=self.zout[self.z].astype(F32)
        for dz in range(1,NZ): s=s+self.zin[dz].astype(F32)
        self.out[...]=s

    def finish(self):
        self.ccopy().wait_send()
        for t in range(1,NR): self.xcopy(t).wait_send()
        for dz in range(1,NZ): self.zcopy(dz).wait_send()


class Swap:
    SEMS=[(NR,),(NR,),(1,)]
    def __init__(self,src,dst,sems):
        self.src,self.dst=src,dst
        self.s,self.r,self.lo=sems
        self.z,self.core,self.rows=here()
    def copy(self,t,receive=False):
        to=partner_xy(self.rows,t)
        return rcopy(self.src.at[to],self.dst.at[to if receive else self.rows],self.s.at[t],self.r.at[t],dev(self.z,self.core,to))
    def local(self):
        return pltpu.make_async_copy(self.src.at[self.rows],self.dst.at[self.rows],self.lo.at[0])
    def start(self):
        for t in range(1,NR): self.copy(t).start()
        self.local().start()
    def wait(self):
        for t in range(1,NR): self.copy(t,True).wait_recv()
        self.local().wait()
    def finish(self):
        for t in range(1,NR): self.copy(t).wait_send()


class AllToAll:
    N=NZ*NC*NR
    SEMS=[(N,),(N,),(1,)]
    def __init__(self,src,dst,sems,one=False):
        self.src,self.dst,self.one=src,dst,one
        self.s,self.r,self.lo=sems
        self.me=lax.axis_index("dp")*NR+lax.axis_index("rows")
    def piece(self,n):
        return self.src if self.one else self.src.at[n]
    def copy(self,k,receive=False):
        to=lax.rem(self.me+k,self.N)
        frm=lax.rem(self.me-k+self.N,self.N)
        return rcopy(self.piece(to),self.dst.at[frm if receive else self.me],self.s.at[k],self.r.at[k],(to//NR,lax.rem(to,NR)))
    def local(self):
        return pltpu.make_async_copy(self.piece(self.me),self.dst.at[self.me],self.lo.at[0])
    def each(self,fn):
        def body(k,c):
            fn(k); return c
        lax.fori_loop(1,self.N,body,0)
    def start(self):
        self.each(lambda k:self.copy(k).start())
        self.local().start()
    def wait(self):
        self.each(lambda k:self.copy(k,True).wait_recv())
        self.local().wait()
    def finish(self):
        self.each(lambda k:self.copy(k).wait_send())


def sem_types(shapes):
    return [pltpu.SemaphoreType.DMA(s) for s in shapes]
HBM=pl.BlockSpec(memory_space=pl.ANY)
VM=pl.BlockSpec(memory_space=pltpu.VMEM)
NDEV=NZ*NC*NR


def enter_kernel(n_w,*refs):
    it=iter(refs)
    tok,cot,cond,ada,bias=[next(it) for _ in range(5)]
    shards=[next(it) for _ in range(n_w)]
    tok_o,cot_o,cond_o,mod_o=[next(it) for _ in range(4)]
    fulls=[next(it) for _ in range(n_w)]
    condv,part,modin=[next(it) for _ in range(3)]
    take=lambda cls:[next(it) for _ in cls.SEMS]
    barrier_all()
    c_all=AllToAll(cond,condv,take(AllToAll),one=True)
    swap_t=Swap(tok,tok_o,take(Swap))
    swap_c=Swap(cot,cot_o,take(Swap))
    m_all=AllToAll(part,modin,take(AllToAll))
    gathers=[Gather(s,f,take(Gather)) for s,f in zip(shards,fulls)]
    c_all.start()
    swap_t.start()
    gathers[0].start()
    c_all.wait()
    me=c_all.me
    feats=ada.shape[0]
    cv=condv[:,0,:].astype(F32)
    low=(cv/(1.0+jnp.exp(-cv))).astype(BF)
    width=cv.shape[1]
    pick=(lax.broadcasted_iota(jnp.int32,(width,feats),0)==lax.broadcasted_iota(jnp.int32,(width,feats),1)+feats*me).astype(BF)
    mine=jnp.dot(low,pick,preferred_element_type=F32).astype(BF)
    chunk=768
    for c in range(ada.shape[1]//chunk):
        pr=jnp.dot(mine,ada[:,c*chunk:(c+1)*chunk],preferred_element_type=F32)
        for l in range(chunk//128):
            i=c*(chunk//128)+l
            part[:,i,:]=pr[:,l*128:(l+1)*128]+bias[i:i+1,:]
    cond_o[...]=low
    m_all.start()
    gathers[0].run_z()
    for g in gathers[1:]: g.start()
    m_all.wait()
    s=modin[0]
    def add(i,s): return s+modin[i]
    mod_o[...]=lax.fori_loop(1,NDEV,add,s)
    swap_t.wait()
    gathers[0].run_x()
    for g in gathers[1:]:
        g.run_z()
    swap_c.start()
    for g in gathers[1:]:
        g.run_x()
    swap_c.wait()
    for g in gathers: g.finish()
    swap_t.finish(); swap_c.finish(); c_all.finish(); m_all.finish()


def enter(tok,cot,cond_row,ada,bias_rows,shards):
    n_w=len(shards)
    scr=[pltpu.VMEM((NDEV,)+cond_row.shape,cond_row.dtype),pltpu.VMEM((NDEV,)+bias_rows.shape,F32),pltpu.VMEM((NDEV,)+bias_rows.shape,F32)]
    sems=sem_types(AllToAll.SEMS)+sem_types(Swap.SEMS)*2+sem_types(AllToAll.SEMS)+sem_types(Gather.SEMS)*n_w
    outs=[jax.ShapeDtypeStruct(tok.shape,tok.dtype),jax.ShapeDtypeStruct(cot.shape,cot.dtype),
          jax.ShapeDtypeStruct((NDEV,cond_row.shape[1]),BF),jax.ShapeDtypeStruct(bias_rows.shape,F32)]
    outs+=[jax.ShapeDtypeStruct((NZ,NC,NR)+s.shape,s.dtype) for s in shards]
    return pl.pallas_call(
        functools.partial(enter_kernel,n_w),
        in_specs=[HBM,HBM,HBM,VM,VM]+[HBM]*n_w,
        out_specs=[HBM,HBM,VM,VM]+[HBM]*n_w,
        out_shape=outs,
        scratch_shapes=scr+sems,
        compiler_params=pltpu.CompilerParams(collective_id=0,has_side_effects=True,vmem_limit_bytes=48<<20),
        name="enter",
    )(tok,cot,cond_row,ada,bias_rows,*shards)


def leave_kernel(n_g,refs_spec,*refs):
    it=iter(refs)
    lay,tg,gm,low,ada=[next(it) for _ in range(5)]
    parts=[next(it) for _ in range(n_g)]
    lay_o,tg_o,ctx_o,adag_o,gm_o=[next(it) for _ in range(5)]
    gouts=[next(it) for _ in range(n_g)]
    gmv,ctxs,ctxv=[next(it) for _ in range(3)]
    bufs=[[next(it) for _ in range(5)] for _ in range(n_g)]
    take=lambda cls:[next(it) for _ in cls.SEMS]
    barrier_all()
    g_all=AllToAll(gm,gmv,take(AllToAll),one=True)
    x_all=AllToAll(ctxs,ctxv,take(AllToAll))
    sl=Swap(lay,lay_o,take(Swap)); st=Swap(tg,tg_o,take(Swap))
    sc=[Scatter(p,o,b,take(Scatter)) for p,o,b in zip(parts,gouts,bufs)]
    g_all.start()
    for s in sc: s.start()
    st.start(); sl.start()
    g_all.wait()
    me=g_all.me
    feats=ada.shape[0]
    width=low.shape[1]
    pick=(lax.broadcasted_iota(jnp.int32,(width,feats),0)==lax.broadcasted_iota(jnp.int32,(width,feats),1)+feats*me).astype(BF)
    mine=jnp.dot(low[...],pick,preferred_element_type=F32).astype(BF)
    acc=jnp.zeros((gmv.shape[0],feats),F32)
    for i in range(gmv.shape[1]):
        g=gmv[:,i,:]
        adag_o[:,i*128:(i+1)*128]=lax.dot_general(mine,g,(((0,),(0,)),((),())),preferred_element_type=F32)
        acc=acc+lax.dot_general(g,ada[:,i*128:(i+1)*128],(((1,),(1,)),((),())),preferred_element_type=F32)
    gm_o[...]=jnp.sum(gmv[...].astype(F32),axis=0)
    for n in range(NDEV):
        g0=(n//NR)*NR
        ctxs[n,0:NR,0:feats]=acc[g0:g0+NR,:]
    x_all.start()
    for s in sc: s.cstep()
    x_all.wait()
    ctx_o[...]=ctxv[...]
    for s in sc: s.xstep()
    for s in sc: s.zstep()
    st.wait(); sl.wait()
    for s in sc: s.finish()
    st.finish(); sl.finish(); g_all.finish(); x_all.finish()


def leave(lay,tg,gm,low,ada,parts):
    n_g=len(parts)
    cols=ada.shape[1]
    scr=[pltpu.VMEM((NDEV,)+gm.shape,gm.dtype),pltpu.VMEM((NDEV,8,128),F32),pltpu.VMEM((NDEV,8,128),F32)]
    for p in parts: scr+=Scatter.scratch(p.shape[3],p.shape[4],p.dtype)
    sems=sem_types(AllToAll.SEMS)*2+sem_types(Swap.SEMS)*2+sem_types(Scatter.SEMS)*n_g
    outs=[jax.ShapeDtypeStruct(lay.shape,lay.dtype),jax.ShapeDtypeStruct(tg.shape,tg.dtype),
          jax.ShapeDtypeStruct((NDEV,8,128),F32),jax.ShapeDtypeStruct(ada.shape,F32),jax.ShapeDtypeStruct(gm.shape,F32)]
    outs+=[jax.ShapeDtypeStruct(p.shape[3:],F32) for p in parts]
    return pl.pallas_call(
        functools.partial(leave_kernel,n_g,None),
        in_specs=[HBM,HBM,HBM,VM,VM]+[HBM]*n_g,
        out_specs=[HBM,HBM,VM,VM,VM]+[VM]*n_g,
        out_shape=outs,
        scratch_shapes=scr+sems,
        compiler_params=pltpu.CompilerParams(collective_id=1,has_side_effects=True,vmem_limit_bytes=60<<20),
        name="leave",
    )(lay,tg,gm,low,ada,*parts)


def own_rows(padded_cells):
    return jnp.pad(padded_cells,((0,0),(1,1),(1,1),(0,0)))


def fast(tokens,conditioning,item_map,ada_weight,ada_bias,attn_kernel,qkv_weight,out_weight,up_weight,ffn_kernel,down_weight,out_cotangent):
    canvases,rows_here,cols,features=tokens.shape
    side=rows_here*NR
    cells=side*cols
    rows=lax.axis_index("rows"); dp=lax.axis_index("dp"); me=dp*NR+rows
    hidden=up_weight.shape[1]
    cond_row=lax.dynamic_slice_in_dim(conditioning,rows,1,0)
    cond_row8=jnp.pad(cond_row,((0,7),(0,0)))
    mod_cols=ada_weight.shape[1]
    bshard=ada_bias.shape[0]
    bias_rows=lax.dynamic_update_slice_in_dim(jnp.zeros((mod_cols,),F32),ada_bias.astype(F32),me*bshard,0).reshape(mod_cols//128,128)
    pad8=(-(mod_cols//128))%8
    taps=jnp.pad(jnp.concatenate([attn_kernel,ffn_kernel],axis=1),((0,7),(0,128-attn_kernel.shape[1]-ffn_kernel.shape[1])))
    ta,tf=attn_kernel.shape[1],ffn_kernel.shape[1]
    tok,cot,low_all,mod,qkv_f,taps_f,out_f,up_f,down_f=enter(
        tokens.reshape(NR,rows_here*cols,features),out_cotangent.reshape(NR,rows_here*cols,features),
        cond_row8,ada_weight,bias_rows,[qkv_weight,taps,out_weight,up_weight,down_weight])
    full2=lambda a:a.reshape(-1,a.shape[-1])
    triple_full,out_full,up_full,down_full=full2(qkv_f),full2(out_f),full2(up_f),full2(down_f)
    taps_f=taps_f.reshape(NDEV,16,128)[:,:9]
    kernel_attn=taps_f[:,:,:ta].transpose(1,0,2).reshape(9,features)
    kernel_ffn=taps_f[:,:,ta:ta+tf].transpose(1,0,2).reshape(9,hidden)
    labels=lax.dynamic_slice_in_dim(item_map,rows,1,0)
    labels_pad=jnp.pad(labels,((0,0),(1,1),(1,1)),constant_values=-1)
    shift1,scale1,gate1,shift2,scale2,gate2=(mod.reshape(6,features)[i][None,None,None] for i in range(6))
    x=tok.reshape(1,side,cols,features).astype(F32)
    incoming=cot.reshape(1,side,cols,features).astype(F32)
    n1,i1=normalize(x)
    m1=(n1*(1.0+scale1)+shift1).astype(BF)
    m1p=own_rows(m1)
    mix=conv_forward(m1p,labels_pad,labels,kernel_attn).astype(BF).reshape(cells,features)
    projected=jnp.dot(mix,triple_full,preferred_element_type=F32).astype(BF)
    qm,km=head_masks(labels.reshape(cells))
    attended,lse=attn_fwd(projected,qm,km,features)
    branch=jnp.dot(attended,out_full,preferred_element_type=F32).reshape(x.shape)
    middle=x+gate1*branch
    n2,i2=normalize(middle)
    m2=(n2*(1.0+scale2)+shift2).astype(BF)
    m2r=m2.reshape(cells,features)
    hid=jnp.dot(m2r,up_full,preferred_element_type=F32).astype(BF).reshape(1,side,cols,hidden)
    hidp=own_rows(hid)
    pre=conv_forward(hidp,labels_pad,labels,kernel_ffn)
    act,gback=jax.vjp(jax.nn.gelu,pre)
    glow=act.astype(BF).reshape(cells,hidden)
    fbranch=jnp.dot(glow,down_full,preferred_element_type=F32).reshape(x.shape)
    layer_out=(middle+gate2*fbranch).astype(BF)
    g_gate2=jnp.sum(incoming*fbranch,axis=(1,2))
    gffn=(gate2*incoming).astype(BF).reshape(cells,features)
    g_down=contract_rows(glow,gffn)
    ggelu=contract_cols(gffn,down_full).reshape(1,side,cols,hidden)
    gpre=gback(ggelu)[0].astype(BF)
    gprep=own_rows(gpre)
    g_kffn=kernel_grad(gpre,hidp,labels_pad,labels)
    gup=conv_mirror(gprep,labels_pad,labels,kernel_ffn).astype(BF).reshape(cells,hidden)
    g_up=contract_rows(m2r,gup)
    gm2=contract_cols(gup,up_full).reshape(x.shape)
    g_scale2=jnp.sum(gm2*n2,axis=(1,2)); g_shift2=jnp.sum(gm2,axis=(1,2))
    gmid=incoming+normalize_back(gm2*(1.0+scale2),n2,i2)
    g_gate1=jnp.sum(gmid*branch,axis=(1,2))
    gattn=(gate1*gmid).astype(BF).reshape(cells,features)
    g_out=contract_rows(attended,gattn)
    gatt=contract_cols(gattn,out_full).astype(BF)
    dq,dk,dv=attn_bwd(projected,gatt,attended,qm,km,lse.T,features)
    gproj=jnp.concatenate([dq,dk,dv],axis=1)
    g_qkv=contract_rows(mix,gproj)
    gmix=contract_cols(gproj,triple_full).astype(BF).reshape(x.shape)
    g_kattn=kernel_grad(gmix,m1p,labels_pad,labels)
    gm1=conv_mirror(own_rows(gmix),labels_pad,labels,kernel_attn)
    g_scale1=jnp.sum(gm1*n1,axis=(1,2)); g_shift1=jnp.sum(gm1,axis=(1,2))
    tgrad=gmid+normalize_back(gm1*(1.0+scale1),n1,i1)
    gmod=jnp.concatenate([g_shift1,g_scale1,g_gate1,g_shift2,g_scale2,g_gate2],axis=-1).astype(BF)
    gtaps=jnp.concatenate([g_kattn.reshape(9,NDEV,ta),g_kffn.reshape(9,NDEV,tf)],axis=2).transpose(1,0,2)
    gtaps=jnp.pad(gtaps,((0,0),(0,7),(0,128-ta-tf))).reshape(NZ,NC,NR,16,128)
    sp=lambda g:g.astype(BF).reshape(NZ,NC,NR,g.shape[0]//NDEV,g.shape[1])
    lay,tg,ctx,adag,gmsum,q_o,t_o,o_o,u_o,d_o=leave(
        layer_out.reshape(NR,rows_here*cols,features),tgrad.astype(BF).reshape(NR,rows_here*cols,features),
        gmod.reshape(mod_cols//128,128),low_all,ada_weight,[sp(g_qkv),gtaps,sp(g_out),sp(g_up),sp(g_down)])
    shape4=(NR,rows_here,cols,features)
    feats=ada_weight.shape[0]
    dsilu=ctx[:,:NR,:feats].transpose(1,0,2).reshape(NR,features)
    cv=conditioning.astype(F32)
    _,sback=jax.vjp(jax.nn.silu,cv)
    dctx=sback(dsilu)[0]
    gbias=lax.dynamic_slice_in_dim(gmsum.reshape(mod_cols),me*bshard,bshard,0)
    return (lay.reshape(shape4),tg.reshape(shape4).astype(F32),dctx,adag,gbias,t_o[:9,:ta],q_o,o_o,u_o,t_o[:9,ta:ta+tf],d_o)


def solution(mesh):
    quick=dict(mesh.shape)=={"dp":NZ*NC,"rows":NR}
    return jax.shard_map(
        fast if quick else local,
        mesh=mesh,
        in_specs=(
            P("dp", "rows", None, None),
            P("dp", None),
            P("dp", None, None),
            P(("dp", "rows"), None),
            P(("dp", "rows")),
            P(None, ("dp", "rows")),
            P(("dp", "rows"), None),
            P(("dp", "rows"), None),
            P(("dp", "rows"), None),
            P(None, ("dp", "rows")),
            P(("dp", "rows"), None),
            P("dp", "rows", None, None),
        ),
        out_specs=(
            P("dp", "rows", None, None),
            P("dp", "rows", None, None),
            P("dp", None),
            P(("dp", "rows"), None),
            P(("dp", "rows")),
            P(None, ("dp", "rows")),
            P(("dp", "rows"), None),
            P(("dp", "rows"), None),
            P(("dp", "rows"), None),
            P(None, ("dp", "rows")),
            P(("dp", "rows"), None),
        ),
        check_vma=False,
    )
```

```python
import functools

import jax
import jax.numpy as jnp
from jax import lax
from jax.experimental import pallas as pl
from jax.experimental.pallas import tpu as pltpu
from jax.sharding import PartitionSpec as P

PER_GROUP_WIDTH = 64


EPSILON = 1e-06


def padded(block, sides, width):
    for axis, dim in sides:
        count = lax.axis_size(axis)
        forward = [(i, i + 1) for i in range(count - 1)]
        backward = [(target, source) for source, target in forward]
        low = lax.ppermute(
            lax.slice_in_dim(block, block.shape[dim] - width, None, axis=dim), axis, forward
        )
        high = lax.ppermute(lax.slice_in_dim(block, 0, width, axis=dim), axis, backward)
        block = jnp.concatenate([low, block, high], axis=dim)
    return block


def normalize(attended_content_array):
    average = jnp.mean(attended_content_array, axis=-1, keepdims=True)
    centred = attended_content_array - average
    inverse = lax.rsqrt(jnp.mean(centred * centred, axis=-1, keepdims=True) + EPSILON)
    return (centred * inverse, inverse)


def normalize_back(incoming, normalized_rows, inverse):
    return inverse * (
        incoming
        - jnp.mean(incoming, axis=-1, keepdims=True)
        - normalized_rows * jnp.mean(incoming * normalized_rows, axis=-1, keepdims=True)
    )


def widen_cols(rimmed):
    return jnp.pad(rimmed, ((0, 0), (0, 0), (1, 1), (0, 0)))


def tap_mask(labels_pad, centre, row_off, col_off):
    rows_here = centre.shape[1]
    cols_here = centre.shape[2]
    return (labels_pad[:, row_off : row_off + rows_here, col_off : col_off + cols_here] == centre)[
        ..., None
    ]


def conv_forward(padded_rows, labels_pad, centre, kernel):
    rows_here = centre.shape[1]
    cols_here = centre.shape[2]
    summed = jnp.zeros(centre.shape + (kernel.shape[1],), jnp.float32)
    for row_off in range(3):
        for col_off in range(3):
            window = padded_rows[
                :, row_off : row_off + rows_here, col_off : col_off + cols_here
            ].astype(jnp.float32)
            tapped = kernel[3 * row_off + col_off].astype(jnp.float32) * window
            summed = summed + jnp.where(tap_mask(labels_pad, centre, row_off, col_off), tapped, 0.0)
    return summed


def conv_mirror(padded_rows, labels_pad, centre, kernel):
    rows_here = centre.shape[1]
    cols_here = centre.shape[2]
    summed = jnp.zeros(centre.shape + (kernel.shape[1],), jnp.float32)
    for row_off in range(3):
        for col_off in range(3):
            row_from = 2 - row_off
            col_from = 2 - col_off
            window = padded_rows[
                :, row_from : row_from + rows_here, col_from : col_from + cols_here
            ].astype(jnp.float32)
            tapped = kernel[3 * row_off + col_off].astype(jnp.float32) * window
            summed = summed + jnp.where(
                tap_mask(labels_pad, centre, row_from, col_from), tapped, 0.0
            )
    return summed


def kernel_grad(incoming, padded_rows, labels_pad, centre):
    rows_here = centre.shape[1]
    cols_here = centre.shape[2]
    incoming_values = incoming.astype(jnp.float32)
    tap_sums = []
    for row_off in range(3):
        for col_off in range(3):
            window = padded_rows[
                :, row_off : row_off + rows_here, col_off : col_off + cols_here
            ].astype(jnp.float32)
            product = jnp.where(
                tap_mask(labels_pad, centre, row_off, col_off), incoming_values * window, 0.0
            )
            tap_sums.append(jnp.sum(product, axis=(0, 1, 2)))
    return jnp.stack(tap_sums, axis=0)


def contract_rows(left, right):
    return lax.dot_general(
        left, right, (((0,), (0,)), ((), ())), preferred_element_type=jnp.float32
    )


def contract_cols(left, right):
    return lax.dot_general(
        left, right, (((1,), (1,)), ((), ())), preferred_element_type=jnp.float32
    )


def local(
    tokens,
    conditioning,
    item_map,
    ada_weight,
    ada_bias,
    attn_kernel,
    qkv_weight,
    out_weight,
    up_weight,
    ffn_kernel,
    down_weight,
    out_cotangent,
):
    canvases, rows_here, cols_here, features = tokens.shape
    cell_count = canvases * rows_here * cols_here
    position = lax.axis_index("rows")
    gathered = (
        lax.all_gather(ada_weight, ("dp", "rows"), axis=0, tiled=True),
        lax.all_gather(ada_bias, ("dp", "rows"), axis=0, tiled=True),
        lax.all_gather(attn_kernel, ("dp", "rows"), axis=1, tiled=True),
        lax.all_gather(qkv_weight, ("dp", "rows"), axis=0, tiled=True),
        lax.all_gather(out_weight, ("dp", "rows"), axis=0, tiled=True),
        lax.all_gather(up_weight, ("dp", "rows"), axis=0, tiled=True),
        lax.all_gather(ffn_kernel, ("dp", "rows"), axis=1, tiled=True),
        lax.all_gather(down_weight, ("dp", "rows"), axis=0, tiled=True),
    )
    ada_full, bias_full, kernel_attn, triple_full, out_full, up_full, kernel_ffn, down_full = (
        gathered
    )
    hidden_units = up_full.shape[1]
    head_count = features // PER_GROUP_WIDTH
    logit_divisor = PER_GROUP_WIDTH ** (-0.5)
    labels_pad = jnp.pad(item_map, ((0, 0), (1, 1), (1, 1)), constant_values=-1)
    labels_here = lax.dynamic_slice_in_dim(labels_pad, position * rows_here, rows_here + 2, 1)
    centre = labels_here[:, 1:-1, 1:-1]
    cond_values = conditioning.astype(jnp.float32)
    silu_low = jax.nn.silu(cond_values).astype(jnp.bfloat16)
    modulation = jnp.dot(silu_low, ada_full, preferred_element_type=jnp.float32) + bias_full.astype(
        jnp.float32
    )
    layer_stack = modulation.reshape(canvases, 6, 1, 1, features)
    shift_one, scale_one, gate_one, shift_two, scale_two, gate_two = (
        layer_stack[:, index] for index in range(6)
    )
    token_values = tokens.astype(jnp.float32)
    normed_one, inverse_one = normalize(token_values)
    modulated_one = (normed_one * (1.0 + scale_one) + shift_one).astype(jnp.bfloat16)
    modulated_padded = widen_cols(padded(modulated_one, (("rows", 1),), 1))
    local_mix = conv_forward(modulated_padded, labels_here, centre, kernel_attn).astype(
        jnp.bfloat16
    )
    mix_rows = local_mix.reshape(cell_count, features)
    projected = jnp.dot(mix_rows, triple_full, preferred_element_type=jnp.float32).astype(
        jnp.bfloat16
    )
    projected = projected.reshape(canvases, rows_here * cols_here, 3 * features)
    queries = projected[..., :features]
    key_rows = projected[..., features : 2 * features]
    value_rows = projected[..., 2 * features :]
    keys_all, values_all = (
        lax.all_gather(key_rows, "rows", axis=1, tiled=True),
        lax.all_gather(value_rows, "rows", axis=1, tiled=True),
    )
    query_heads = queries.reshape(canvases, -1, head_count, PER_GROUP_WIDTH)
    key_heads = keys_all.reshape(canvases, -1, head_count, PER_GROUP_WIDTH)
    value_heads = values_all.reshape(canvases, -1, head_count, PER_GROUP_WIDTH)
    scores = (
        jnp.einsum("bqhd,bkhd->bhqk", query_heads, key_heads, preferred_element_type=jnp.float32)
        * logit_divisor
    )
    label_rows = centre.reshape(canvases, -1)
    label_keys = item_map.reshape(canvases, -1)
    linked = label_rows[:, None, :, None] == label_keys[:, None, None, :]
    masked = jnp.where(linked, scores, -1e30)
    row_peak = jnp.max(masked, axis=-1, keepdims=True)
    raised = jnp.exp(masked - row_peak)
    row_total = jnp.sum(raised, axis=-1, keepdims=True)
    attention = raised / row_total
    attention_low = attention.astype(jnp.bfloat16)
    attended = jnp.einsum(
        "bhqk,bkhd->bqhd", attention_low, value_heads, preferred_element_type=jnp.float32
    ).astype(jnp.bfloat16)
    attended = attended.reshape(cell_count, features)
    attn_branch = jnp.dot(attended, out_full, preferred_element_type=jnp.float32).reshape(
        tokens.shape
    )
    middle = token_values + gate_one * attn_branch
    normed_two, inverse_two = normalize(middle)
    modulated_two = (normed_two * (1.0 + scale_two) + shift_two).astype(jnp.bfloat16)
    modulated_rows = modulated_two.reshape(cell_count, features)
    hidden_up_projection = jnp.dot(
        modulated_rows, up_full, preferred_element_type=jnp.float32
    ).astype(jnp.bfloat16)
    hidden_up_projection = hidden_up_projection.reshape(
        canvases, rows_here, cols_here, hidden_units
    )
    up_padded = widen_cols(padded(hidden_up_projection, (("rows", 1),), 1))
    pre_gelu = conv_forward(up_padded, labels_here, centre, kernel_ffn)
    activated, gelu_back = jax.vjp(jax.nn.gelu, pre_gelu)
    gelu_low = activated.astype(jnp.bfloat16).reshape(cell_count, hidden_units)
    ffn_branch = jnp.dot(gelu_low, down_full, preferred_element_type=jnp.float32).reshape(
        tokens.shape
    )
    layer_out = (middle + gate_two * ffn_branch).astype(jnp.bfloat16)
    weights_back = (
        lax.all_gather(ada_weight, ("dp", "rows"), axis=0, tiled=True),
        lax.all_gather(ada_bias, ("dp", "rows"), axis=0, tiled=True),
        lax.all_gather(attn_kernel, ("dp", "rows"), axis=1, tiled=True),
        lax.all_gather(qkv_weight, ("dp", "rows"), axis=0, tiled=True),
        lax.all_gather(out_weight, ("dp", "rows"), axis=0, tiled=True),
        lax.all_gather(up_weight, ("dp", "rows"), axis=0, tiled=True),
        lax.all_gather(ffn_kernel, ("dp", "rows"), axis=1, tiled=True),
        lax.all_gather(down_weight, ("dp", "rows"), axis=0, tiled=True),
    )
    (
        ada_back,
        bias_back,
        kernel_attn_back,
        triple_back,
        out_back,
        up_back,
        kernel_ffn_back,
        down_projection_back,
    ) = weights_back
    incoming = out_cotangent.astype(jnp.float32)
    grad_gate_two = jnp.sum(incoming * ffn_branch, axis=(1, 2))
    grad_ffn = (gate_two * incoming).astype(jnp.bfloat16).reshape(cell_count, features)
    grad_down = contract_rows(gelu_low, grad_ffn)
    grad_gelu = contract_cols(grad_ffn, down_projection_back).reshape(
        canvases, rows_here, cols_here, hidden_units
    )
    grad_pre = gelu_back(grad_gelu)[0].astype(jnp.bfloat16)
    grad_pre_padded = widen_cols(padded(grad_pre, (("rows", 1),), 1))
    grad_kernel_ffn = kernel_grad(grad_pre, up_padded, labels_here, centre)
    grad_up = (
        conv_mirror(grad_pre_padded, labels_here, centre, kernel_ffn_back)
        .astype(jnp.bfloat16)
        .reshape(cell_count, hidden_units)
    )
    grad_up_weight = contract_rows(modulated_rows, grad_up)
    grad_mod_two = contract_cols(grad_up, up_back).reshape(tokens.shape)
    grad_scale_two = jnp.sum(grad_mod_two * normed_two, axis=(1, 2))
    grad_shift_two = jnp.sum(grad_mod_two, axis=(1, 2))
    grad_middle = incoming + normalize_back(
        grad_mod_two * (1.0 + scale_two), normed_two, inverse_two
    )
    grad_gate_one = jnp.sum(grad_middle * attn_branch, axis=(1, 2))
    grad_attn = (gate_one * grad_middle).astype(jnp.bfloat16).reshape(cell_count, features)
    grad_out_weight = contract_rows(attended, grad_attn)
    grad_attended = (
        contract_cols(grad_attn, out_back)
        .astype(jnp.bfloat16)
        .reshape(canvases, -1, head_count, PER_GROUP_WIDTH)
    )
    grad_weights = jnp.einsum(
        "bqhd,bkhd->bhqk", grad_attended, value_heads, preferred_element_type=jnp.float32
    )
    row_delta = jnp.sum(attention * grad_weights, axis=-1, keepdims=True)
    grad_scores = (attention * (grad_weights - row_delta)).astype(jnp.bfloat16)
    grad_query = (
        jnp.einsum("bhqk,bkhd->bqhd", grad_scores, key_heads, preferred_element_type=jnp.float32)
        * logit_divisor
    )
    grad_key_all = (
        jnp.einsum("bhqk,bqhd->bkhd", grad_scores, query_heads, preferred_element_type=jnp.float32)
        * logit_divisor
    )
    value_gradient_full = jnp.einsum(
        "bhqk,bqhd->bkhd", attention_low, grad_attended, preferred_element_type=jnp.float32
    )
    grad_key, grad_value = (
        lax.psum_scatter(
            grad_key_all.reshape(canvases, -1, features).astype(jnp.bfloat16),
            "rows",
            scatter_dimension=1,
            tiled=True,
        ).astype(jnp.float32),
        lax.psum_scatter(
            value_gradient_full.reshape(canvases, -1, features).astype(jnp.bfloat16),
            "rows",
            scatter_dimension=1,
            tiled=True,
        ).astype(jnp.float32),
    )
    grad_projected = jnp.concatenate(
        [
            grad_query.reshape(cell_count, features),
            grad_key.reshape(cell_count, features),
            grad_value.reshape(cell_count, features),
        ],
        axis=-1,
    ).astype(jnp.bfloat16)
    grad_qkv_weight = contract_rows(mix_rows, grad_projected)
    grad_mix = contract_cols(grad_projected, triple_back).astype(jnp.bfloat16).reshape(tokens.shape)
    grad_mix_padded = widen_cols(padded(grad_mix, (("rows", 1),), 1))
    grad_kernel_attn = kernel_grad(grad_mix, modulated_padded, labels_here, centre)
    grad_mod_one = conv_mirror(grad_mix_padded, labels_here, centre, kernel_attn_back)
    grad_scale_one = jnp.sum(grad_mod_one * normed_one, axis=(1, 2))
    grad_shift_one = jnp.sum(grad_mod_one, axis=(1, 2))
    token_grad = grad_middle + normalize_back(
        grad_mod_one * (1.0 + scale_one), normed_one, inverse_one
    )
    grad_parts = jnp.concatenate(
        [
            grad_shift_one,
            grad_scale_one,
            grad_gate_one,
            grad_shift_two,
            grad_scale_two,
            grad_gate_two,
        ],
        axis=-1,
    )
    grad_modulation = lax.psum(grad_parts.astype(jnp.bfloat16), "rows")
    leader = (position == 0).astype(jnp.float32)
    grad_ada_weight = contract_rows(silu_low, grad_modulation) * leader
    grad_ada_bias = jnp.sum(grad_modulation.astype(jnp.float32), axis=0) * leader
    silu_values, silu_back = jax.vjp(jax.nn.silu, cond_values)
    derivative_of_context = silu_back(contract_cols(grad_modulation, ada_back))[0]
    summed_grads = (
        lax.psum_scatter(grad_ada_weight, ("dp", "rows"), scatter_dimension=0, tiled=True),
        lax.psum_scatter(grad_ada_bias, ("dp", "rows"), scatter_dimension=0, tiled=True),
        lax.psum_scatter(grad_kernel_attn, ("dp", "rows"), scatter_dimension=1, tiled=True),
        lax.psum_scatter(grad_qkv_weight, ("dp", "rows"), scatter_dimension=0, tiled=True),
        lax.psum_scatter(grad_out_weight, ("dp", "rows"), scatter_dimension=0, tiled=True),
        lax.psum_scatter(grad_up_weight, ("dp", "rows"), scatter_dimension=0, tiled=True),
        lax.psum_scatter(grad_kernel_ffn, ("dp", "rows"), scatter_dimension=1, tiled=True),
        lax.psum_scatter(grad_down, ("dp", "rows"), scatter_dimension=0, tiled=True),
    )
    return (layer_out, token_grad, derivative_of_context) + tuple(summed_grads)


F32=jnp.float32; BF=jnp.bfloat16
NT=(((1,),(1,)),((),()))
TN=(((0,),(0,)),((),()))

def head_masks(labels):
    cells=labels.shape[0]
    lane=lax.broadcasted_iota(jnp.int32,(cells,128),1)%64
    lab=labels[:,None]
    qm=(lane==lab).astype(BF)
    km=jnp.where((lane!=lab)&(lane<4),-1e30,0.0).astype(BF)
    return qm,km

MESH=pl.DeviceIdType.MESH
NZ,NC,NR=4,2,4


def here():
    dp=lax.axis_index("dp"); rows=lax.axis_index("rows")
    return dp//NC, lax.rem(dp,NC), rows


def dev(z,core,rows):
    return (z*NC+core, rows)


def partner_xy(rows,t):
    x=lax.rem(rows,2); y=rows//2
    tx=t%2; ty=t//2
    nx=1-x if tx else x
    ny=1-y if ty else y
    return ny*2+nx


def rcopy(src,dst,ssem,rsem,target):
    return pltpu.make_async_remote_copy(src_ref=src,dst_ref=dst,send_sem=ssem,recv_sem=rsem,device_id=target,device_id_type=MESH)


def barrier_all():
    dp=lax.axis_index("dp"); rows=lax.axis_index("rows")
    me=dp*NR+rows
    total=NZ*NC*NR
    bar=pltpu.get_barrier_semaphore()
    def body(k,c):
        other=lax.rem(me+k,total)
        pl.semaphore_signal(bar,inc=1,device_id=(other//NR,lax.rem(other,NR)),device_id_type=MESH)
        return c
    lax.fori_loop(1,total,body,0)
    pl.semaphore_wait(bar,total-1)


def zmod(v):
    return lax.rem(v+NZ,NZ)


class Gather:
    SEMS=[(NZ,),(NZ,),(NZ,NR),(NZ,NR),(NZ,NR),(NZ,NR),(1,)]

    def __init__(self,shard,full,sems):
        self.shard,self.full=shard,full
        self.sz,self.rz,self.sx,self.rx,self.sc,self.rc,self.lo=sems
        self.z,self.core,self.rows=here()

    def slot(self,dz,t,core):
        rows=self.rows if t==0 else partner_xy(self.rows,t)
        return self.full.at[zmod(self.z-dz),core,rows]

    def zcopy(self,dz,receive=False):
        dst=self.slot(dz if receive else 0,0,self.core)
        return rcopy(self.shard,dst,self.sz.at[dz],self.rz.at[dz],dev(zmod(self.z+dz),self.core,self.rows))

    def piece(self,dz):
        return self.shard if dz==0 else self.slot(dz,0,self.core)

    def xcopy(self,dz,t,receive=False):
        dst=self.slot(dz,t if receive else 0,self.core)
        return rcopy(self.piece(dz),dst,self.sx.at[dz,t],self.rx.at[dz,t],dev(self.z,self.core,partner_xy(self.rows,t)))

    def ccopy(self,dz,t,receive=False):
        src=self.piece(dz) if t==0 else self.slot(dz,t,self.core)
        dst=self.slot(dz,t,1-self.core if receive else self.core)
        return rcopy(src,dst,self.sc.at[dz,t],self.rc.at[dz,t],dev(self.z,1-self.core,self.rows))

    def local(self):
        return pltpu.make_async_copy(self.shard,self.slot(0,0,self.core),self.lo.at[0])

    def start(self):
        for dz in range(1,NZ):
            self.zcopy(dz).start()
        for t in range(1,NR):
            self.xcopy(0,t).start()
        self.ccopy(0,0).start()
        self.local().start()

    def zstep(self,dz):
        self.zcopy(dz,True).wait_recv()
        for t in range(1,NR):
            self.xcopy(dz,t).start()
        self.ccopy(dz,0).start()

    def xstep(self,dz,t):
        self.xcopy(dz,t,True).wait_recv()
        self.ccopy(dz,t).start()

    def finish(self):
        for dz in range(NZ):
            for t in range(NR):
                self.ccopy(dz,t,True).wait_recv()
        for dz in range(1,NZ):
            self.zcopy(dz).wait_send()
        for dz in range(NZ):
            for t in range(NR):
                if t: self.xcopy(dz,t).wait_send()
                self.ccopy(dz,t).wait_send()
        self.local().wait()

    def run_z(self):
        for dz in range(1,NZ): self.zstep(dz)

    def run_x(self):
        for dz in range(NZ):
            for t in range(1,NR): self.xstep(dz,t)


class Scatter:
    SEMS=[(1,),(1,),(1,),(NR,),(NR,),(NZ,),(NZ,)]

    @staticmethod
    def scratch(r,c,dt):
        return [pltpu.VMEM((NZ,NR,r,c),dt),pltpu.VMEM((NZ,NR,r,c),dt),pltpu.VMEM((NR,NZ,r,c),dt),pltpu.VMEM((NZ,r,c),dt),pltpu.VMEM((NZ,r,c),dt)]

    def __init__(self,part,out,bufs,sems):
        self.part,self.out=part,out
        self.own,self.sib,self.xin,self.zout,self.zin=bufs
        self.lo,self.sc,self.rc,self.sx,self.rx,self.sz,self.rz=sems
        self.z,self.core,self.rows=here()
        self.dt=self.own.dtype

    def lcopy(self):
        return pltpu.make_async_copy(self.part.at[:,self.core],self.own,self.lo.at[0])

    def ccopy(self):
        return rcopy(self.part.at[:,1-self.core],self.sib,self.sc.at[0],self.rc.at[0],dev(self.z,1-self.core,self.rows))

    def xcopy(self,t):
        to=partner_xy(self.rows,t)
        return rcopy(self.own.at[:,to],self.xin.at[t],self.sx.at[t],self.rx.at[t],dev(self.z,self.core,to))

    def zcopy(self,dz):
        to=zmod(self.z+dz)
        return rcopy(self.zout.at[to],self.zin.at[dz],self.sz.at[dz],self.rz.at[dz],dev(to,self.core,self.rows))

    def start(self):
        self.ccopy().start(); self.lcopy().start()

    def cstep(self):
        self.lcopy().wait(); self.ccopy().wait_recv()
        def body(i,c):
            a,b=i//NR,lax.rem(i,NR)
            self.own[a,b]=(self.own[a,b].astype(F32)+self.sib[a,b].astype(F32)).astype(self.dt)
            return c
        lax.fori_loop(0,NZ*NR,body,0)
        for t in range(1,NR): self.xcopy(t).start()

    def xstep(self):
        for t in range(1,NR): self.xcopy(t).wait_recv()
        def body(a,c):
            s=self.own[a,self.rows].astype(F32)
            for t in range(1,NR): s=s+self.xin[t,a].astype(F32)
            self.zout[a]=s.astype(self.dt)
            return c
        lax.fori_loop(0,NZ,body,0)
        for dz in range(1,NZ): self.zcopy(dz).start()

    def zstep(self):
        for dz in range(1,NZ): self.zcopy(dz).wait_recv()
        s=self.zout[self.z].astype(F32)
        for dz in range(1,NZ): s=s+self.zin[dz].astype(F32)
        self.out[...]=s

    def finish(self):
        self.ccopy().wait_send()
        for t in range(1,NR): self.xcopy(t).wait_send()
        for dz in range(1,NZ): self.zcopy(dz).wait_send()


class Swap:
    SEMS=[(NR,),(NR,),(1,)]
    def __init__(self,src,dst,sems):
        self.src,self.dst=src,dst
        self.s,self.r,self.lo=sems
        self.z,self.core,self.rows=here()
    def copy(self,t,receive=False):
        to=partner_xy(self.rows,t)
        return rcopy(self.src.at[to],self.dst.at[to if receive else self.rows],self.s.at[t],self.r.at[t],dev(self.z,self.core,to))
    def local(self):
        return pltpu.make_async_copy(self.src.at[self.rows],self.dst.at[self.rows],self.lo.at[0])
    def start(self):
        for t in range(1,NR): self.copy(t).start()
        self.local().start()
    def wait(self):
        for t in range(1,NR): self.copy(t,True).wait_recv()
        self.local().wait()
    def finish(self):
        for t in range(1,NR): self.copy(t).wait_send()


class AllToAll:
    N=NZ*NC*NR
    SEMS=[(N,),(N,),(1,)]
    def __init__(self,src,dst,sems,one=False):
        self.src,self.dst,self.one=src,dst,one
        self.s,self.r,self.lo=sems
        self.me=lax.axis_index("dp")*NR+lax.axis_index("rows")
    def piece(self,n):
        return self.src if self.one else self.src.at[n]
    def copy(self,k,receive=False):
        to=lax.rem(self.me+k,self.N)
        frm=lax.rem(self.me-k+self.N,self.N)
        return rcopy(self.piece(to),self.dst.at[frm if receive else self.me],self.s.at[k],self.r.at[k],(to//NR,lax.rem(to,NR)))
    def local(self):
        return pltpu.make_async_copy(self.piece(self.me),self.dst.at[self.me],self.lo.at[0])
    def each(self,fn):
        def body(k,c):
            fn(k); return c
        lax.fori_loop(1,self.N,body,0)
    def start(self):
        self.each(lambda k:self.copy(k).start())
        self.local().start()
    def wait(self):
        self.each(lambda k:self.copy(k,True).wait_recv())
        self.local().wait()
    def finish(self):
        self.each(lambda k:self.copy(k).wait_send())


def sem_types(shapes):
    return [pltpu.SemaphoreType.DMA(s) for s in shapes]
class GatherZ:
    SEMS=[(NZ,),(NZ,),(1,)]
    def __init__(self,shard,zp,sems):
        self.shard,self.zp=shard,zp
        self.s,self.r,self.lo=sems
        self.z,self.core,self.rows=here()
    def copy(self,dz,receive=False):
        to=zmod(self.z+dz)
        frm=zmod(self.z-dz)
        return rcopy(self.shard,self.zp.at[frm if receive else self.z],self.s.at[dz],self.r.at[dz],dev(to,self.core,self.rows))
    def local(self):
        return pltpu.make_async_copy(self.shard,self.zp.at[self.z],self.lo.at[0])
    def start(self):
        for dz in range(1,NZ): self.copy(dz).start()
        self.local().start()
    def wait(self):
        for dz in range(1,NZ): self.copy(dz,True).wait_recv()
    def finish(self):
        for dz in range(1,NZ): self.copy(dz).wait_send()
        self.local().wait()


class GatherXY:
    SEMS=[(NZ,NR),(NZ,NR),(NZ,NR),(NZ,NR),(1,)]
    def __init__(self,zp,full,sems):
        self.zp,self.full=zp,full
        self.sx,self.rx,self.sc,self.rc,self.lo=sems
        self.z,self.core,self.rows=here()
    def place(self,t):
        return self.rows if t==0 else partner_xy(self.rows,t)
    def xcopy(self,k,t,receive=False):
        return rcopy(self.zp.at[k],self.full.at[k,self.core,self.place(t) if receive else self.rows],self.sx.at[k,t],self.rx.at[k,t],dev(self.z,self.core,self.place(t)))
    def ccopy(self,k,t,receive=False):
        src=self.zp.at[k] if t==0 else self.full.at[k,self.core,self.place(t)]
        dst=self.full.at[k,1-self.core if receive else self.core,self.place(t)]
        return rcopy(src,dst,self.sc.at[k,t],self.rc.at[k,t],dev(self.z,1-self.core,self.rows))
    def local(self):
        return pltpu.make_async_copy(self.zp,self.full.at[:,self.core,self.rows],self.lo.at[0])
    def start(self,ks=range(NZ)):
        for k in ks:
            for t in range(1,NR): self.xcopy(k,t).start()
            self.ccopy(k,0).start()
    def start_local(self):
        self.local().start()
    def step(self,k):
        for t in range(1,NR):
            self.xcopy(k,t,True).wait_recv()
            self.ccopy(k,t).start()
    def arrive(self,k):
        for t in range(NR): self.ccopy(k,t,True).wait_recv()
    def finish(self):
        for k in range(NZ):
            for t in range(NR):
                if t: self.xcopy(k,t).wait_send()
                self.ccopy(k,t).wait_send()
        self.local().wait()
    def finish_remote(self):
        for k in range(NZ):
            for t in range(NR):
                if t: self.xcopy(k,t).wait_send()
                self.ccopy(k,t).wait_send()


class ScatterZ:
    SEMS=[(NZ,),(NZ,)]
    @staticmethod
    def scratch(r,c,dt):
        return [pltpu.VMEM((NZ,r,c),dt)]
    def __init__(self,zout,out,bufs,sems):
        self.zout,self.out=zout,out
        self.zin,=bufs
        self.s,self.r=sems
        self.z,self.core,self.rows=here()
    def copy(self,dz):
        to=zmod(self.z+dz)
        return rcopy(self.zout.at[to],self.zin.at[dz],self.s.at[dz],self.r.at[dz],dev(to,self.core,self.rows))
    def start(self):
        for dz in range(1,NZ): self.copy(dz).start()
    def step(self):
        for dz in range(1,NZ): self.copy(dz).wait_recv()
        v=self.zout[self.z].astype(F32)
        for dz in range(1,NZ): v=v+self.zin[dz].astype(F32)
        self.out[...]=v
    def finish(self):
        for dz in range(1,NZ): self.copy(dz).wait_send()


class Events:
    def __init__(self): self.at={}
    def add(self,slot,fn): self.at.setdefault(slot,[]).append(fn)
    def run(self,outer,inner,width):
        for slot,fns in self.at.items():
            if slot%width==inner:
                @pl.when(outer==slot//width)
                def _(fns=fns):
                    for fn in fns: fn()
NN=(((1,),(0,)),((),()))
C0=0.7978845608028654
C1=0.044715


def dotf(a,b,dims=NN):
    return lax.dot_general(a,b,dims,preferred_element_type=F32)


def loop(n,fn,unroll=1):
    def body(i,c):
        fn(i); return c
    lax.fori_loop(0,n,body,0,unroll=unroll)


def rows_of(i,n):
    return pl.ds(pl.multiple_of(i*n,n),n)


def normal_rows(v):
    d=1.0/v.shape[1]
    c=v-jnp.sum(v,axis=1,keepdims=True)*d
    inv=lax.rsqrt(jnp.sum(c*c,axis=1,keepdims=True)*d+EPSILON)
    return c*inv,inv


def normal_back_rows(g,n,inv):
    d=1.0/g.shape[1]
    return inv*(g-jnp.sum(g,axis=1,keepdims=True)*d-n*(jnp.sum(g*n,axis=1,keepdims=True)*d))


def fold8(v):
    s=v[0:8]
    for k in range(1,v.shape[0]//8): s=s+v[8*k:8*k+8]
    return s


def conv_loops(side,lanes_n,width,forward,finish):
    pass


def shifts(f,ml,mr):
    n=f.shape[0]
    return pltpu.roll(f,1,0)*ml, pltpu.roll(f,n-1,0)*mr


def conv_rows(src,dst_fn,taps,ml_ref,mr_ref,rl_ref,lane,side,cols):
    sl=pl.ds(lane*128,128)
    k=[taps[q:q+1,lane*128:(lane+1)*128] for q in range(9)]
    zero=jnp.zeros((cols,128),F32)
    def body(i,c):
        hm,part=c
        f=src[rows_of(i,cols),lane*128:(lane+1)*128]
        fm,fp=shifts(f,ml_ref[rows_of(i,cols),:],mr_ref[rows_of(i,cols),:])
        h=[k[3*a]*fm+k[3*a+1]*f+k[3*a+2]*fp for a in range(3)]
        done=part+rl_ref[i]*h[2]
        @pl.when(i>0)
        def _(): dst_fn(i-1,done)
        return h[0],h[1]+rl_ref[i]*hm
    hm,part=lax.fori_loop(0,side,body,(zero,zero),unroll=4)
    dst_fn(side-1,part)


def back_rows(g_ref,f_ref,dst_fn,taps,ml_ref,mr_ref,rl_ref,lane,side,cols):
    ls=slice(lane*128,(lane+1)*128)
    k=[taps[q:q+1,ls] for q in range(9)]
    zero=jnp.zeros((cols,128),F32)
    z8=jnp.zeros((8,128),F32)
    def body(i,c):
        hp,part,fprev,acc=c
        g=g_ref[rows_of(i,cols),ls]
        gm,gp=shifts(g,ml_ref[rows_of(i,cols),:],mr_ref[rows_of(i,cols),:])
        gs=(gp,g,gm)
        q=[k[3*a]*gp+k[3*a+1]*g+k[3*a+2]*gm for a in range(3)]
        done=part+rl_ref[i]*q[0]
        @pl.when(i>0)
        def _(): dst_fn(i-1,done)
        f=f_ref[rows_of(i,cols),ls]
        nxt=f_ref[pl.ds(pl.multiple_of(jnp.minimum(i+1,side-1)*cols,cols),cols),ls]
        fs=(fprev*rl_ref[i],f,nxt*rl_ref[i+1])
        acc=tuple(acc[3*a+b]+fold8(fs[a]*gs[b]) for a in range(3) for b in range(3))
        return q[2],q[1]+rl_ref[i]*hp,f,acc
    hp,part,_,acc=lax.fori_loop(0,side,body,(zero,zero,zero,(z8,)*9),unroll=4)
    dst_fn(side-1,part)
    return acc


def link_masks(labels):
    side,cols=labels.shape
    left=jnp.pad(labels[:,1:]==labels[:,:-1],((0,0),(1,0)))
    right=jnp.pad(labels[:,1:]==labels[:,:-1],((0,0),(0,1)))
    wide=lambda m: jnp.broadcast_to(m.reshape(side*cols,1).astype(F32),(side*cols,128))
    top=labels[:,0]//2
    rl=jnp.pad((top[1:]==top[:-1]).astype(F32),(1,1))
    return wide(left),wide(right),rl
HBM=pl.BlockSpec(memory_space=pl.ANY)
VM=pl.BlockSpec(memory_space=pltpu.VMEM)
SM=pl.BlockSpec(memory_space=pltpu.SMEM)
NDEV=NZ*NC*NR
S_=jax.ShapeDtypeStruct


def taker(it):
    return lambda cls:[next(it) for _ in cls.SEMS]


def enter_kernel(n_z,*refs):
    it=iter(refs)
    tok,cond,ada,bias,qkv,taps=[next(it) for _ in range(6)]
    shards=[next(it) for _ in range(n_z)]
    tok_o,cond_o,mod_o,qkv_o,taps_o=[next(it) for _ in range(5)]
    zps=[next(it) for _ in range(n_z)]
    condv,part=[next(it) for _ in range(2)]
    mbufs=[next(it) for _ in range(5)]
    take=taker(it)
    barrier_all()
    c_all=AllToAll(cond,condv,take(AllToAll),one=True)
    swap_t=Swap(tok,tok_o,take(Swap))
    m_all=Scatter(part,mod_o,mbufs,take(Scatter))
    g_taps=Gather(taps,taps_o,take(Gather))
    g_qkv=Gather(qkv,qkv_o,take(Gather))
    gz=[GatherZ(s,z,take(GatherZ)) for s,z in zip(shards,zps)]
    c_all.start()
    swap_t.start()
    g_taps.start()
    g_qkv.start()
    c_all.wait()
    me=c_all.me
    feats=ada.shape[0]
    cv=condv[:,0,:].astype(F32)
    low=(cv/(1.0+jnp.exp(-cv))).astype(BF)
    width=cv.shape[1]
    pick=(lax.broadcasted_iota(jnp.int32,(width,feats),0)==lax.broadcasted_iota(jnp.int32,(width,feats),1)+feats*me).astype(BF)
    mine=jnp.dot(low,pick,preferred_element_type=F32).astype(BF)
    chunk=768
    for c in range(ada.shape[1]//chunk):
        pr=jnp.dot(mine,ada[:,c*chunk:(c+1)*chunk],preferred_element_type=F32)
        for l in range(chunk//128):
            i=c*(chunk//128)+l
            part[:,:,:,i,:]=(pr[:,l*128:(l+1)*128]+bias[i:i+1,:]).reshape(NZ,NC,NR,128)
    cond_o[...]=low
    m_all.start()
    m_all.cstep()
    g_taps.run_z(); g_qkv.run_z()
    m_all.xstep()
    for g in gz: g.start()
    m_all.zstep()
    swap_t.wait()
    g_taps.run_x(); g_qkv.run_x()
    for g in gz: g.wait()
    for g in [g_taps,g_qkv,swap_t,c_all,m_all]+gz: g.finish()


def enter(tok,cond_row,ada,bias_rows,qkv,taps,shards):
    n=len(shards)
    scr=[pltpu.VMEM((NDEV,)+cond_row.shape,cond_row.dtype),pltpu.VMEM((NZ,NC,NR)+bias_rows.shape,F32)]+Scatter.scratch(bias_rows.shape[0],128,F32)
    sems=sem_types(AllToAll.SEMS)+sem_types(Swap.SEMS)+sem_types(Scatter.SEMS)+sem_types(Gather.SEMS)*2+sem_types(GatherZ.SEMS)*n
    outs=[S_(tok.shape,tok.dtype),S_((NDEV,cond_row.shape[1]),BF),S_(bias_rows.shape,F32),
          S_((NZ,NC,NR)+qkv.shape,qkv.dtype),S_((NZ,NC,NR)+taps.shape,taps.dtype)]
    outs+=[S_((NZ,)+s.shape,s.dtype) for s in shards]
    return pl.pallas_call(
        functools.partial(enter_kernel,n),
        in_specs=[HBM,HBM,VM,VM,HBM,HBM]+[HBM]*n,
        out_specs=[HBM,VM,VM,HBM,HBM]+[HBM]*n,
        out_shape=outs,
        scratch_shapes=scr+sems,
        compiler_params=pltpu.CompilerParams(collective_id=0,has_side_effects=True,vmem_limit_bytes=48<<20),
        name="enter",
    )(tok,cond_row,ada,bias_rows,qkv,taps,*shards)


def forward_kernel(n_w,qb,*refs):
    it=iter(refs)
    mix,qkv,qm,km,cot,late=[next(it) for _ in range(6)]
    zps=[next(it) for _ in range(n_w)]
    proj,att,lse_t,cot_o,late_o=[next(it) for _ in range(5)]
    fulls=[next(it) for _ in range(n_w)]
    lse=next(it)
    take=taker(it)
    barrier_all()
    swap_c=Swap(cot,cot_o,take(Swap))
    gs=[GatherXY(a,b,take(GatherXY)) for a,b in zip(zps,fulls)]
    gl=GatherZ(late,late_o,take(GatherZ))
    gl.start()
    gs[0].start(); swap_c.start(); gs[1].start()
    for g in gs: g.start_local()
    ev=Events()
    for k in range(NZ):
        ev.add(1,lambda k=k: gs[0].step(k))
        ev.add(8+k,lambda k=k: gs[1].step(k))
    cells,feat=att.shape
    CH=256
    def pr(i):
        proj[rows_of(i,CH),:]=dotf(mix[rows_of(i,CH),:],qkv[...]).astype(BF)
    loop(cells//CH,pr)
    pairs=feat//128
    lane=lax.broadcasted_iota(jnp.int32,(1,128),1)
    lse[...]=jnp.zeros_like(lse)
    def pair(p):
        cq=pl.ds(pl.multiple_of(p*128,128),128)
        ck=pl.ds(pl.multiple_of(feat+p*128,128),128)
        cv=pl.ds(pl.multiple_of(2*feat+p*128,128),128)
        for h in range(2):
            ev.run(p,h,2)
            mine=(lane//64)==h
            k=jnp.where(mine,proj[:,ck],km[...])
            def body(i):
                r=rows_of(i,qb)
                q=jnp.where(mine,proj[r,cq]*jnp.asarray(0.125,BF),qm[r,:])
                s=dotf(q,k,NT)
                m=jnp.max(s,axis=1,keepdims=True)
                e=jnp.exp(s-m)
                l=jnp.sum(e,axis=1,keepdims=True)
                a=(e*(1.0/l)).astype(BF)
                o=dotf(a,proj[:,cv]).astype(BF)
                if h==0:
                    att[r,cq]=o
                else:
                    att[r,cq]=jnp.where(mine,o,att[r,cq])
                lse[r,:]=jnp.where(lane==2*p+h,m+jnp.log(l),lse[r,:])
            loop(cells//qb,body)
    loop(pairs,pair)
    lse_t[...]=jnp.transpose(lse[...])
    for g in gs:
        for k in range(NZ): g.arrive(k)
    swap_c.wait()
    gl.wait()
    for g in gs+[swap_c,gl]: g.finish()


def forward(mix,qkv,qm,km,cot,late,zps):
    n=len(zps)
    cells,feat=mix.shape
    outs=[S_((cells,3*feat),BF),S_((cells,feat),BF),S_((128,cells),F32),S_(cot.shape,cot.dtype),S_((NZ,)+late.shape,late.dtype)]
    outs+=[S_((NZ,NC,NR)+z.shape[1:],z.dtype) for z in zps]
    return pl.pallas_call(
        functools.partial(forward_kernel,n,256),
        in_specs=[VM,VM,VM,VM,HBM,HBM]+[HBM]*n,
        out_specs=[VM,VM,VM,HBM,HBM]+[HBM]*n,
        out_shape=outs,
        scratch_shapes=[pltpu.VMEM((cells,128),F32)]+sem_types(Swap.SEMS)+sem_types(GatherXY.SEMS)*n+sem_types(GatherZ.SEMS),
        compiler_params=pltpu.CompilerParams(collective_id=1,has_side_effects=True,vmem_limit_bytes=60<<20),
        name="attn_fwd",
    )(mix,qkv,qm,km,cot,late,*zps)


def backward_kernel(n_g,kb,*refs):
    it=iter(refs)
    proj,do,o,qm,km,lse_t,lay,gout=[next(it) for _ in range(8)]
    parts=[next(it) for _ in range(n_g)]
    gp,lay_o,gout_o=[next(it) for _ in range(3)]
    gouts=[next(it) for _ in range(n_g)]
    qs,dqt=[next(it) for _ in range(2)]
    obufs=[next(it) for _ in range(5)]
    bufs=[[next(it) for _ in range(1)] for _ in range(n_g)]
    take=taker(it)
    barrier_all()
    sl=Swap(lay,lay_o,take(Swap))
    so=Scatter(gout,gout_o,obufs,take(Scatter))
    sc=[ScatterZ(p,g,b,take(ScatterZ)) for p,g,b in zip(parts,gouts,bufs)]
    ev=Events()
    so.start()
    for s in sc: s.start()
    sl.start()
    ev.add(1,so.cstep)
    ev.add(6,so.xstep)
    for s in sc: ev.add(8,s.step)
    ev.add(11,so.zstep)
    cells,feat=do.shape
    pairs=feat//128
    lane=lax.broadcasted_iota(jnp.int32,(1,128),1)
    srow=lax.broadcasted_iota(jnp.int32,(8,128),0)
    slane=lax.broadcasted_iota(jnp.int32,(8,128),1)
    sel=(slane//64==srow).astype(BF)
    def pair(p):
        cq=pl.ds(pl.multiple_of(p*128,128),128)
        ck=pl.ds(pl.multiple_of(feat+p*128,128),128)
        cv=pl.ds(pl.multiple_of(2*feat+p*128,128),128)
        prod=do[:,cq].astype(F32)*o[:,cq].astype(F32)
        hi=prod.astype(BF); lo=(prod-hi.astype(F32)).astype(BF)
        delta=dotf(sel,hi,NT)+dotf(sel,lo,NT)
        qs[...]=proj[:,cq]*jnp.asarray(0.125,BF)
        for h in range(2):
            ev.run(p,h,2)
            mine=(lane//64)==h
            q=jnp.where(mine,qs[...],qm[...])
            ls=lse_t[pl.ds(2*p+h,1),:]
            dl=delta[h:h+1,:]
            dqt[...]=jnp.zeros_like(dqt)
            def body(i):
                r=rows_of(i,kb)
                kr=proj[r,ck]
                k=jnp.where(mine,kr,km[r,:])
                v=jnp.where(mine,proj[r,cv],jnp.zeros((),BF))
                st=dotf(k,q,NT)
                pt=jnp.exp(st-ls)
                dpt=dotf(v,do[:,cq],NT)
                ds=(pt*(dpt-dl)).astype(BF)
                dv=dotf(pt.astype(BF),do[:,cq]).astype(BF)
                dk=dotf(ds,qs[...]).astype(BF)
                dqt[...]+=dotf(kr,ds,TN)
                if h==0:
                    gp[r,cv]=dv
                    gp[r,ck]=dk
                else:
                    gp[r,cv]=jnp.where(mine,dv,gp[r,cv])
                    gp[r,ck]=jnp.where(mine,dk,gp[r,ck])
            loop(cells//kb,body)
            dq=(jnp.transpose(dqt[...])*0.125).astype(BF)
            if h==0:
                gp[:,cq]=dq
            else:
                gp[:,cq]=jnp.where(mine,dq,gp[:,cq])
    loop(pairs,pair)
    sl.wait()
    for s in sc+[sl,so]: s.finish()


def backward(proj,do,o,qm,km,lse_t,lay,gout,parts):
    n=len(parts)
    cells,feat=do.shape
    outs=[S_((cells,3*feat),BF),S_(lay.shape,lay.dtype),S_(gout.shape[3:],F32)]+[S_(p.shape[1:],F32) for p in parts]
    scr=[pltpu.VMEM((cells,128),BF),pltpu.VMEM((128,cells),F32)]+Scatter.scratch(gout.shape[3],gout.shape[4],gout.dtype)
    for p in parts: scr+=ScatterZ.scratch(p.shape[1],p.shape[2],p.dtype)
    return pl.pallas_call(
        functools.partial(backward_kernel,n,256),
        in_specs=[VM,VM,VM,VM,VM,VM,HBM,HBM]+[VM]*n,
        out_specs=[VM,HBM,VM]+[VM]*n,
        out_shape=outs,
        scratch_shapes=scr+sem_types(Swap.SEMS)+sem_types(Scatter.SEMS)+sem_types(ScatterZ.SEMS)*n,
        compiler_params=pltpu.CompilerParams(collective_id=2,has_side_effects=True,vmem_limit_bytes=62<<20),
        name="attn_bwd",
    )(proj,do,o,qm,km,lse_t,lay,gout,*parts)


def leave_kernel(n_g,*refs):
    it=iter(refs)
    tg,gm,low,ada=[next(it) for _ in range(4)]
    parts=[next(it) for _ in range(n_g)]
    tg_o,ctx_o,adag_o,gm_o=[next(it) for _ in range(4)]
    gouts=[next(it) for _ in range(n_g)]
    gmv,ctxs,ctxv=[next(it) for _ in range(3)]
    bufs=[[next(it) for _ in range(5)] for _ in range(n_g)]
    take=taker(it)
    barrier_all()
    g_all=AllToAll(gm,gmv,take(AllToAll),one=True)
    x_all=AllToAll(ctxs,ctxv,take(AllToAll))
    st=Swap(tg,tg_o,take(Swap))
    sc=[Scatter(p,o,b,take(Scatter)) for p,o,b in zip(parts,gouts,bufs)]
    g_all.start()
    for s in sc: s.start()
    st.start()
    g_all.wait()
    me=g_all.me
    feats=ada.shape[0]
    width=low.shape[1]
    pick=(lax.broadcasted_iota(jnp.int32,(width,feats),0)==lax.broadcasted_iota(jnp.int32,(width,feats),1)+feats*me).astype(BF)
    mine=jnp.dot(low[...],pick,preferred_element_type=F32).astype(BF)
    acc=jnp.zeros((gmv.shape[0],feats),F32)
    for i in range(gmv.shape[1]):
        g=gmv[:,i,:]
        adag_o[:,i*128:(i+1)*128]=lax.dot_general(mine,g,(((0,),(0,)),((),())),preferred_element_type=F32)
        acc=acc+lax.dot_general(g,ada[:,i*128:(i+1)*128],(((1,),(1,)),((),())),preferred_element_type=F32)
    gm_o[...]=jnp.sum(gmv[...].astype(F32),axis=0)
    for n in range(NDEV):
        g0=(n//NR)*NR
        ctxs[n,0:NR,0:feats]=acc[g0:g0+NR,:]
    x_all.start()
    for s in sc: s.cstep()
    x_all.wait()
    ctx_o[...]=ctxv[...]
    for s in sc: s.xstep()
    for s in sc: s.zstep()
    st.wait()
    for s in sc: s.finish()
    st.finish(); g_all.finish(); x_all.finish()


def leave(tg,gm,low,ada,parts):
    n_g=len(parts)
    scr=[pltpu.VMEM((NDEV,)+gm.shape,gm.dtype),pltpu.VMEM((NDEV,8,128),F32),pltpu.VMEM((NDEV,8,128),F32)]
    for p in parts: scr+=Scatter.scratch(p.shape[3],p.shape[4],p.dtype)
    sems=sem_types(AllToAll.SEMS)*2+sem_types(Swap.SEMS)+sem_types(Scatter.SEMS)*n_g
    outs=[S_(tg.shape,tg.dtype),S_((NDEV,8,128),F32),S_(ada.shape,F32),S_(gm.shape,F32)]
    outs+=[S_(p.shape[3:],F32) for p in parts]
    return pl.pallas_call(
        functools.partial(leave_kernel,n_g),
        in_specs=[HBM,HBM,VM,VM]+[HBM]*n_g,
        out_specs=[HBM,VM,VM,VM]+[VM]*n_g,
        out_shape=outs,
        scratch_shapes=scr+sems,
        compiler_params=pltpu.CompilerParams(collective_id=3,has_side_effects=True,vmem_limit_bytes=60<<20),
        name="leave",
    )(tg,gm,low,ada,*parts)
def greet(targets):
    bar=pltpu.get_barrier_semaphore()
    for d in targets:
        pl.semaphore_signal(bar,inc=1,device_id=d,device_id_type=MESH)
    pl.semaphore_wait(bar,len(targets))


def near():
    z,core,rows=here()
    return [dev(z,1-core,rows)]+[dev(z,core,partner_xy(rows,t)) for t in range(1,NR)]


class PipeScatter:
    SEMS=[(2,),(2,),(2,NR),(2,NR)]
    @staticmethod
    def scratch(r,c):
        return [pltpu.VMEM((2,NZ,NC,NR,r,c),BF),pltpu.VMEM((2,NZ,NR,r,c),BF),pltpu.VMEM((2,NZ,NR,r,c),BF),pltpu.VMEM((2,NR,NZ,r,c),BF)]
    def __init__(self,bufs,sems):
        self.part,self.sib,self.own,self.xin=bufs
        self.sc,self.rc,self.sx,self.rx=sems
        self.z,self.core,self.rows=here()
    def ccopy(self,s):
        return rcopy(self.part.at[s,:,1-self.core],self.sib.at[s],self.sc.at[s],self.rc.at[s],dev(self.z,1-self.core,self.rows))
    def xcopy(self,s,t):
        to=partner_xy(self.rows,t)
        return rcopy(self.own.at[s,:,to],self.xin.at[s,t],self.sx.at[s,t],self.rx.at[s,t],dev(self.z,self.core,to))
    def send_core(self,s):
        self.ccopy(s).start()
    def send_square(self,s):
        self.ccopy(s).wait()
        def body(i):
            a,b=i//NR,lax.rem(i,NR)
            self.own[s,a,b]=(self.part[s,a,self.core,b].astype(F32)+self.sib[s,a,b].astype(F32)).astype(BF)
        loop(NZ*NR,body)
        for t in range(1,NR): self.xcopy(s,t).start()
    def collect(self,s,put):
        for t in range(1,NR): self.xcopy(s,t).wait()
        def body(a):
            v=self.own[s,a,self.rows].astype(F32)
            for t in range(1,NR): v=v+self.xin[s,t,a].astype(F32)
            put(a,v.astype(BF))
        loop(NZ,body)


class RowScatter:
    SEMS=[(2,),(2,),(2,NR),(2,NR)]
    @staticmethod
    def scratch(r,c):
        return [pltpu.VMEM((2,NR,r,c),BF),pltpu.VMEM((2,NR,r,c),BF),pltpu.VMEM((2,NR,r,c),BF)]
    def __init__(self,part,zout,bufs,sems):
        self.part,self.zout=part,zout
        self.sib,self.own,self.xin=bufs
        self.sc,self.rc,self.sx,self.rx=sems
        self.z,self.core,self.rows=here()
    def ccopy(self,k):
        s=k%2
        return rcopy(self.part.at[k,1-self.core],self.sib.at[s],self.sc.at[s],self.rc.at[s],dev(self.z,1-self.core,self.rows))
    def xcopy(self,k,t):
        s=k%2
        to=partner_xy(self.rows,t)
        return rcopy(self.own.at[s,to],self.xin.at[s,t],self.sx.at[s,t],self.rx.at[s,t],dev(self.z,self.core,to))
    def send_core(self,k):
        self.ccopy(k).start()
    def send_square(self,k):
        self.ccopy(k).wait()
        s=k%2
        def body(b):
            self.own[s,b]=(self.part[k,self.core,b].astype(F32)+self.sib[s,b].astype(F32)).astype(BF)
        loop(NR,body)
        for t in range(1,NR): self.xcopy(k,t).start()
    def collect(self,k):
        s=k%2
        for t in range(1,NR): self.xcopy(k,t).wait()
        v=self.own[s,self.rows].astype(F32)
        for t in range(1,NR): v=v+self.xin[s,t].astype(F32)
        self.zout[k]=v.astype(BF)


def ffn_kernel_body(*refs,side,cols):
    it=iter(refs)
    nx=lambda n:[next(it) for _ in range(n)]
    x_ref,att_ref,cot_ref,mod_ref,outw_ref,up_ref,zpd,tap_ref,ml_ref,mr_ref,rl_ref=nx(11)
    lay_ref,gmid_ref,gatt_ref,gout_ref,zup,zdown,gtap_ref,sums_ref=nx(8)
    m2,m2t,gffn,branch,middle,fb,gm2,F,G,glow,gub,dfull,gd=nx(13)
    ubufs=nx(4); dbufs=nx(3)
    take=taker(it)
    ga=GatherXY(zpd,dfull,take(GatherXY))
    us=PipeScatter(ubufs,take(PipeScatter))
    ds=RowScatter(gd,zdown,dbufs,take(RowScatter))
    t=pl.program_id(0)
    cells,feat=x_ref.shape
    T=up_ref.shape[1]
    hidden=NDEV*zpd.shape[1]
    steps=hidden//T; last=steps-1
    block=hidden//NZ
    CH=256; EC=32
    shift2=mod_ref[3:4,:]; scale2=mod_ref[4:5,:]; gate2=mod_ref[5:6,:]; gate1=mod_ref[2:3,:]
    slot=lax.rem(t,2); other=lax.rem(t+1,2)
    ready={}
    for k in range(NZ): ready[k]=-(-((k+1)*block)//T)-1
    need={}
    for k in range(NZ): need[k]=(k*block)//T
    def put_up(tile):
        def put(a,v): zup[a,:,pl.ds(pl.multiple_of(tile*T,128),T)]=v
        return put

    @pl.when(t==0)
    def _():
        greet(near())
        ga.start(); ga.start_local()
        def a(i):
            branch[rows_of(i,CH),:]=dotf(att_ref[rows_of(i,CH),:],outw_ref[...])
        loop(cells//CH,a)
        def b(i):
            r=rows_of(i,EC)
            mid=x_ref[r,:].astype(F32)+gate1*branch[r,:]
            middle[r,:]=mid
            n,_=normal_rows(mid)
            m2[r,:]=(n*(1.0+scale2)+shift2).astype(BF)
            gffn[r,:]=(gate2*cot_ref[r,:].astype(F32)).astype(BF)
        loop(cells//EC,b)
        ga.step(0)
        def c(i):
            r=rows_of(i,CH)
            m2t[:,pl.ds(pl.multiple_of(i*CH,CH),CH)]=jnp.transpose(m2[r,:])
            fb[r,:]=jnp.zeros((CH,feat),F32)
            gm2[r,:]=jnp.zeros((CH,feat),F32)
        loop(cells//CH,c)
        ga.local().wait()
    for k in range(NZ):
        @pl.when(t==need[k])
        def _(k=k):
            if k: ga.step(k)
            ga.arrive(k)
    @pl.when(t>=2)
    def _():
        us.collect(slot,put_up(t-2))
    for k in range(NZ):
        if ready[k]+2<=last:
            @pl.when(t==ready[k]+2)
            def _(k=k): ds.collect(k)

    dw=dfull.reshape(hidden,feat)
    gdw=gd.reshape(hidden,feat)
    tr=pl.ds(pl.multiple_of(t*T,T),T)
    def first(i):
        r=rows_of(i,CH)
        F[r,:]=dotf(m2[r,:],up_ref[...]).astype(BF).astype(F32)
        G[r,:]=dotf(gffn[r,:],dw[tr,:],NT)
    loop(cells//CH,first)

    taps=tap_ref[...].astype(F32)
    for lane in range(T//128):
        ls=slice(lane*128,(lane+1)*128)
        def put(i,u):
            r=rows_of(i,cols)
            u2=u*u
            th=jnp.tanh(C0*(u+C1*(u2*u)))
            half=0.5*(1.0+th)
            glow[r,ls]=(u*half).astype(BF)
            d=half+(0.5*u)*(1.0-th*th)*(C0*(1.0+(3.0*C1)*u2))
            G[r,ls]=(G[r,ls]*d).astype(BF).astype(F32)
        conv_rows(F,put,taps,ml_ref,mr_ref,rl_ref,lane,side,cols)
    @pl.when(t>=1)
    def _():
        us.send_square(other)
    for k in range(NZ):
        if ready[k]+1<=last:
            @pl.when(t==ready[k]+1)
            def _(k=k): ds.send_square(k)
    for lane in range(T//128):
        ls=slice(lane*128,(lane+1)*128)
        def put2(i,u):
            gub[rows_of(i,cols),ls]=u.astype(BF)
        acc=back_rows(G,F,put2,taps,ml_ref,mr_ref,rl_ref,lane,side,cols)
        for q in range(9):
            gtap_ref[q:q+1,ls]=jnp.sum(acc[q],axis=0,keepdims=True)
    gtap_ref[9:16,:]=jnp.zeros((7,T),F32)

    r_=feat//NDEV
    def third(i):
        n=NC*NR*r_
        us.part[slot,i]=dotf(m2t[rows_of(i,n),:],gub[...]).astype(BF).reshape(NC,NR,r_,T)
    loop(NZ,third)
    us.send_core(slot)
    for i in range(T//256):
        gdw[pl.ds(pl.multiple_of(t*T+i*256,256),256),:]=dotf(glow[:,i*256:(i+1)*256],gffn[...],TN).astype(BF)
    for k in range(NZ):
        @pl.when(t==ready[k])
        def _(k=k): ds.send_core(k)
    def second(i):
        r=rows_of(i,CH)
        fb[r,:]+=dotf(glow[r,:],dw[tr,:])
        gm2[r,:]+=dotf(gub[r,:],up_ref[...],NT)
    loop(cells//CH,second)

    @pl.when(t==last)
    def _():
        us.collect(other,put_up(last-1))
        late=[k for k in range(NZ) if ready[k]+1>last]
        mid_=[k for k in range(NZ) if ready[k]+1==last]
        for k in mid_: ds.collect(k)
        us.send_square(slot)
        for k in late: ds.send_square(k)
        z=jnp.zeros((8,feat),F32)
        def body(i,c):
            sg2,ss2,sc2,sg1=c
            r=rows_of(i,EC)
            inc=cot_ref[r,:].astype(F32)
            mid=middle[r,:]
            n,inv=normal_rows(mid)
            lay_ref[r,:]=(mid+gate2*fb[r,:]).astype(BF)
            gm=gm2[r,:]
            gmid=inc+normal_back_rows(gm*(1.0+scale2),n,inv)
            gmid_ref[r,:]=gmid
            gffn[r,:]=(gate1*gmid).astype(BF)
            return (sg2+fold8(inc*fb[r,:]),ss2+fold8(gm),sc2+fold8(gm*n),sg1+fold8(gmid*branch[r,:]))
        res=lax.fori_loop(0,cells//EC,body,(z,z,z,z))
        for q in range(4):
            sums_ref[q:q+1,:]=jnp.sum(res[q],axis=0,keepdims=True)
        sums_ref[4:8,:]=jnp.zeros((4,feat),F32)
        def b(i):
            r=rows_of(i,CH)
            gatt_ref[r,:]=dotf(gffn[r,:],outw_ref[...],NT).astype(BF)
        loop(cells//CH,b)
        for i in range(feat//256):
            gout_ref[i*256:(i+1)*256,:]=dotf(att_ref[:,i*256:(i+1)*256],gffn[...],TN).astype(BF)
        us.collect(slot,put_up(last))
        for k in late: ds.collect(k)
        ga.finish_remote()


def ffn(x,att,cot,mod6,outw,up,zpd,taps,ml,mr,rl,side,cols,T=512):
    cells,feat=x.shape
    hidden=up.shape[1]
    vm=lambda shape: pl.BlockSpec(shape,lambda t:(0,)*len(shape),pipeline_mode=pl.Buffered(1))
    r_,d_=feat//NDEV,hidden//NDEV
    return pl.pallas_call(
        functools.partial(ffn_kernel_body,side=side,cols=cols),
        grid=(hidden//T,),
        in_specs=[vm((cells,feat)),vm((cells,feat)),vm((cells,feat)),vm((8,feat)),vm((feat,feat)),
                  pl.BlockSpec((feat,T),lambda t:(0,t)),HBM,pl.BlockSpec((16,T),lambda t:(0,t)),
                  vm((cells,128)),vm((cells,128)),SM],
        out_specs=[vm((cells,feat)),vm((cells,feat)),vm((cells,feat)),vm((feat,feat)),
                   vm((NZ,r_,hidden)),vm((NZ,d_,feat)),pl.BlockSpec((16,T),lambda t:(0,t)),vm((8,feat))],
        out_shape=[S_((cells,feat),BF),S_((cells,feat),F32),S_((cells,feat),BF),S_((feat,feat),BF),S_((NZ,r_,hidden),BF),S_((NZ,d_,feat),BF),S_((16,hidden),F32),S_((8,feat),F32)],
        scratch_shapes=[pltpu.VMEM((cells,feat),BF),pltpu.VMEM((feat,cells),BF),pltpu.VMEM((cells,feat),BF),
                        pltpu.VMEM((cells,feat),F32),pltpu.VMEM((cells,feat),F32),pltpu.VMEM((cells,feat),F32),pltpu.VMEM((cells,feat),F32),
                        pltpu.VMEM((cells,T),F32),pltpu.VMEM((cells,T),F32),pltpu.VMEM((cells,T),BF),pltpu.VMEM((cells,T),BF),
                        pltpu.VMEM((NZ,NC,NR,d_,feat),BF),pltpu.VMEM((NZ,NC,NR,d_,feat),BF)]
                       +PipeScatter.scratch(r_,T)+RowScatter.scratch(d_,feat)
                       +sem_types(GatherXY.SEMS)+sem_types(PipeScatter.SEMS)+sem_types(RowScatter.SEMS),
        compiler_params=pltpu.CompilerParams(dimension_semantics=("arbitrary",),vmem_limit_bytes=63<<20,collective_id=4,has_side_effects=True),
        name="ffn",
    )(x,att,cot,mod6,outw,up,zpd,taps,ml,mr,rl)
def own_rows(padded_cells):
    return jnp.pad(padded_cells,((0,0),(1,1),(1,1),(0,0)))


def fast(tokens,conditioning,item_map,ada_weight,ada_bias,attn_kernel,qkv_weight,out_weight,up_weight,ffn_kernel,down_weight,out_cotangent):
    canvases,rows_here,cols,features=tokens.shape
    side=rows_here*NR
    cells=side*cols
    rows=lax.axis_index("rows"); dp=lax.axis_index("dp"); me=dp*NR+rows
    hidden=up_weight.shape[1]
    cond_row=jnp.pad(lax.dynamic_slice_in_dim(conditioning,rows,1,0),((0,7),(0,0)))
    mod_cols=ada_weight.shape[1]
    bshard=ada_bias.shape[0]
    bias_rows=lax.dynamic_update_slice_in_dim(jnp.zeros((mod_cols,),F32),ada_bias.astype(F32),me*bshard,0).reshape(mod_cols//128,128)
    ta,tf=attn_kernel.shape[1],ffn_kernel.shape[1]
    taps=jnp.pad(jnp.concatenate([attn_kernel,ffn_kernel],axis=1),((0,7),(0,128-ta-tf)))
    blocks=(NR,rows_here*cols,features)
    tok,low_all,mod,qkv_f,taps_f,*zps=enter(tokens.reshape(blocks),cond_row,ada_weight,bias_rows,qkv_weight,taps,[out_weight,up_weight])
    full2=lambda a:a.reshape(-1,a.shape[-1])
    triple_full=full2(qkv_f)
    taps_f=taps_f.reshape(NDEV,16,128)[:,:9]
    kernel_attn=taps_f[:,:,:ta].transpose(1,0,2).reshape(9,features)
    kernel_ffn=taps_f[:,:,ta:ta+tf].transpose(1,0,2).reshape(9,hidden)
    labels=lax.dynamic_slice_in_dim(item_map,rows,1,0)
    labels_pad=jnp.pad(labels,((0,0),(1,1),(1,1)),constant_values=-1)
    qm,km=head_masks(labels.reshape(cells))
    ml,mr,rl=link_masks(labels[0])
    mod6=mod.reshape(6,features)
    shift1,scale1,gate1,shift2,scale2,gate2=(mod6[i][None,None,None] for i in range(6))
    x=tok.reshape(1,side,cols,features).astype(F32)
    n1,i1=normalize(x)
    m1=(n1*(1.0+scale1)+shift1).astype(BF)
    m1p=own_rows(m1)
    mix=conv_forward(m1p,labels_pad,labels,kernel_attn).astype(BF).reshape(cells,features)
    proj,attended,lse_t,cot,zp_down,out_f,up_f=forward(mix,triple_full,qm,km,out_cotangent.reshape(blocks),down_weight,zps)
    lay,gmid,gatt,g_out,z_up,z_down,g_kffn,sums=ffn(
        tok.reshape(cells,features),attended,cot.reshape(cells,features),jnp.pad(mod6,((0,2),(0,0))),
        full2(out_f),full2(up_f),zp_down,jnp.pad(kernel_ffn,((0,7),(0,0))),ml,mr,rl,side,cols)
    sp=lambda g:g.reshape(NZ,NC,NR,g.shape[0]//NDEV,g.shape[1])
    gproj,lay_o,o_o,u_o,d_o=backward(proj,gatt,attended,qm,km,lse_t,lay.reshape(blocks),sp(g_out),[z_up,z_down])
    g_gate2,g_shift2,g_scale2,g_gate1=(sums[i:i+1] for i in range(4))
    gmid=gmid.reshape(x.shape)
    g_qkv=contract_rows(mix,gproj).astype(BF)
    gmix=contract_cols(gproj,triple_full).astype(BF).reshape(x.shape)
    g_kattn=kernel_grad(gmix,m1p,labels_pad,labels)
    gm1=conv_mirror(own_rows(gmix),labels_pad,labels,kernel_attn)
    g_scale1=jnp.sum(gm1*n1,axis=(1,2)); g_shift1=jnp.sum(gm1,axis=(1,2))
    tgrad=gmid+normalize_back(gm1*(1.0+scale1),n1,i1)
    gmod=jnp.concatenate([g_shift1,g_scale1,g_gate1,g_shift2,g_scale2,g_gate2],axis=-1).astype(BF)
    gtaps=jnp.concatenate([g_kattn.reshape(9,NDEV,ta),g_kffn[:9].reshape(9,NDEV,tf)],axis=2).transpose(1,0,2)
    gtaps=jnp.pad(gtaps,((0,0),(0,7),(0,128-ta-tf))).reshape(NZ,NC,NR,16,128)
    tg,ctx,adag,gmsum,q_o,t_o=leave(tgrad.astype(BF).reshape(blocks),gmod.reshape(mod_cols//128,128),low_all,ada_weight,[sp(g_qkv),gtaps])
    shape4=(NR,rows_here,cols,features)
    feats=ada_weight.shape[0]
    dsilu=ctx[:,:NR,:feats].transpose(1,0,2).reshape(NR,features)
    cv=conditioning.astype(F32)
    _,sback=jax.vjp(jax.nn.silu,cv)
    dctx=sback(dsilu)[0]
    gbias=lax.dynamic_slice_in_dim(gmsum.reshape(mod_cols),me*bshard,bshard,0)
    return (lay_o.reshape(shape4),tg.reshape(shape4).astype(F32),dctx,adag,gbias,t_o[:9,:ta],q_o,o_o,u_o,t_o[:9,ta:ta+tf],d_o)


def solution(mesh):
    quick=dict(mesh.shape)=={"dp":NZ*NC,"rows":NR}
    return jax.shard_map(
        fast if quick else local,
        mesh=mesh,
        in_specs=(
            P("dp", "rows", None, None),
            P("dp", None),
            P("dp", None, None),
            P(("dp", "rows"), None),
            P(("dp", "rows")),
            P(None, ("dp", "rows")),
            P(("dp", "rows"), None),
            P(("dp", "rows"), None),
            P(("dp", "rows"), None),
            P(None, ("dp", "rows")),
            P(("dp", "rows"), None),
            P("dp", "rows", None, None),
        ),
        out_specs=(
            P("dp", "rows", None, None),
            P("dp", "rows", None, None),
            P("dp", None),
            P(("dp", "rows"), None),
            P(("dp", "rows")),
            P(None, ("dp", "rows")),
            P(("dp", "rows"), None),
            P(("dp", "rows"), None),
            P(("dp", "rows"), None),
            P(None, ("dp", "rows")),
            P(("dp", "rows"), None),
        ),
        check_vma=False,
    )
```

```python
import functools

import jax
import jax.numpy as jnp
from jax import lax
from jax.experimental import pallas as pl
from jax.experimental.pallas import tpu as pltpu
from jax.sharding import PartitionSpec as P

PER_GROUP_WIDTH = 64


EPSILON = 1e-06


def padded(block, sides, width):
    for axis, dim in sides:
        count = lax.axis_size(axis)
        forward = [(i, i + 1) for i in range(count - 1)]
        backward = [(target, source) for source, target in forward]
        low = lax.ppermute(
            lax.slice_in_dim(block, block.shape[dim] - width, None, axis=dim), axis, forward
        )
        high = lax.ppermute(lax.slice_in_dim(block, 0, width, axis=dim), axis, backward)
        block = jnp.concatenate([low, block, high], axis=dim)
    return block


def normalize(attended_content_array):
    average = jnp.mean(attended_content_array, axis=-1, keepdims=True)
    centred = attended_content_array - average
    inverse = lax.rsqrt(jnp.mean(centred * centred, axis=-1, keepdims=True) + EPSILON)
    return (centred * inverse, inverse)


def normalize_back(incoming, normalized_rows, inverse):
    return inverse * (
        incoming
        - jnp.mean(incoming, axis=-1, keepdims=True)
        - normalized_rows * jnp.mean(incoming * normalized_rows, axis=-1, keepdims=True)
    )


def widen_cols(rimmed):
    return jnp.pad(rimmed, ((0, 0), (0, 0), (1, 1), (0, 0)))


def tap_mask(labels_pad, centre, row_off, col_off):
    rows_here = centre.shape[1]
    cols_here = centre.shape[2]
    return (labels_pad[:, row_off : row_off + rows_here, col_off : col_off + cols_here] == centre)[
        ..., None
    ]


def conv_forward(padded_rows, labels_pad, centre, kernel):
    rows_here = centre.shape[1]
    cols_here = centre.shape[2]
    summed = jnp.zeros(centre.shape + (kernel.shape[1],), jnp.float32)
    for row_off in range(3):
        for col_off in range(3):
            window = padded_rows[
                :, row_off : row_off + rows_here, col_off : col_off + cols_here
            ].astype(jnp.float32)
            tapped = kernel[3 * row_off + col_off].astype(jnp.float32) * window
            summed = summed + jnp.where(tap_mask(labels_pad, centre, row_off, col_off), tapped, 0.0)
    return summed


def conv_mirror(padded_rows, labels_pad, centre, kernel):
    rows_here = centre.shape[1]
    cols_here = centre.shape[2]
    summed = jnp.zeros(centre.shape + (kernel.shape[1],), jnp.float32)
    for row_off in range(3):
        for col_off in range(3):
            row_from = 2 - row_off
            col_from = 2 - col_off
            window = padded_rows[
                :, row_from : row_from + rows_here, col_from : col_from + cols_here
            ].astype(jnp.float32)
            tapped = kernel[3 * row_off + col_off].astype(jnp.float32) * window
            summed = summed + jnp.where(
                tap_mask(labels_pad, centre, row_from, col_from), tapped, 0.0
            )
    return summed


def kernel_grad(incoming, padded_rows, labels_pad, centre):
    rows_here = centre.shape[1]
    cols_here = centre.shape[2]
    incoming_values = incoming.astype(jnp.float32)
    tap_sums = []
    for row_off in range(3):
        for col_off in range(3):
            window = padded_rows[
                :, row_off : row_off + rows_here, col_off : col_off + cols_here
            ].astype(jnp.float32)
            product = jnp.where(
                tap_mask(labels_pad, centre, row_off, col_off), incoming_values * window, 0.0
            )
            tap_sums.append(jnp.sum(product, axis=(0, 1, 2)))
    return jnp.stack(tap_sums, axis=0)


def contract_rows(left, right):
    return lax.dot_general(
        left, right, (((0,), (0,)), ((), ())), preferred_element_type=jnp.float32
    )


def contract_cols(left, right):
    return lax.dot_general(
        left, right, (((1,), (1,)), ((), ())), preferred_element_type=jnp.float32
    )


def local(
    tokens,
    conditioning,
    item_map,
    ada_weight,
    ada_bias,
    attn_kernel,
    qkv_weight,
    out_weight,
    up_weight,
    ffn_kernel,
    down_weight,
    out_cotangent,
):
    canvases, rows_here, cols_here, features = tokens.shape
    cell_count = canvases * rows_here * cols_here
    position = lax.axis_index("rows")
    gathered = (
        lax.all_gather(ada_weight, ("dp", "rows"), axis=0, tiled=True),
        lax.all_gather(ada_bias, ("dp", "rows"), axis=0, tiled=True),
        lax.all_gather(attn_kernel, ("dp", "rows"), axis=1, tiled=True),
        lax.all_gather(qkv_weight, ("dp", "rows"), axis=0, tiled=True),
        lax.all_gather(out_weight, ("dp", "rows"), axis=0, tiled=True),
        lax.all_gather(up_weight, ("dp", "rows"), axis=0, tiled=True),
        lax.all_gather(ffn_kernel, ("dp", "rows"), axis=1, tiled=True),
        lax.all_gather(down_weight, ("dp", "rows"), axis=0, tiled=True),
    )
    ada_full, bias_full, kernel_attn, triple_full, out_full, up_full, kernel_ffn, down_full = (
        gathered
    )
    hidden_units = up_full.shape[1]
    head_count = features // PER_GROUP_WIDTH
    logit_divisor = PER_GROUP_WIDTH ** (-0.5)
    labels_pad = jnp.pad(item_map, ((0, 0), (1, 1), (1, 1)), constant_values=-1)
    labels_here = lax.dynamic_slice_in_dim(labels_pad, position * rows_here, rows_here + 2, 1)
    centre = labels_here[:, 1:-1, 1:-1]
    cond_values = conditioning.astype(jnp.float32)
    silu_low = jax.nn.silu(cond_values).astype(jnp.bfloat16)
    modulation = jnp.dot(silu_low, ada_full, preferred_element_type=jnp.float32) + bias_full.astype(
        jnp.float32
    )
    layer_stack = modulation.reshape(canvases, 6, 1, 1, features)
    shift_one, scale_one, gate_one, shift_two, scale_two, gate_two = (
        layer_stack[:, index] for index in range(6)
    )
    token_values = tokens.astype(jnp.float32)
    normed_one, inverse_one = normalize(token_values)
    modulated_one = (normed_one * (1.0 + scale_one) + shift_one).astype(jnp.bfloat16)
    modulated_padded = widen_cols(padded(modulated_one, (("rows", 1),), 1))
    local_mix = conv_forward(modulated_padded, labels_here, centre, kernel_attn).astype(
        jnp.bfloat16
    )
    mix_rows = local_mix.reshape(cell_count, features)
    projected = jnp.dot(mix_rows, triple_full, preferred_element_type=jnp.float32).astype(
        jnp.bfloat16
    )
    projected = projected.reshape(canvases, rows_here * cols_here, 3 * features)
    queries = projected[..., :features]
    key_rows = projected[..., features : 2 * features]
    value_rows = projected[..., 2 * features :]
    keys_all, values_all = (
        lax.all_gather(key_rows, "rows", axis=1, tiled=True),
        lax.all_gather(value_rows, "rows", axis=1, tiled=True),
    )
    query_heads = queries.reshape(canvases, -1, head_count, PER_GROUP_WIDTH)
    key_heads = keys_all.reshape(canvases, -1, head_count, PER_GROUP_WIDTH)
    value_heads = values_all.reshape(canvases, -1, head_count, PER_GROUP_WIDTH)
    scores = (
        jnp.einsum("bqhd,bkhd->bhqk", query_heads, key_heads, preferred_element_type=jnp.float32)
        * logit_divisor
    )
    label_rows = centre.reshape(canvases, -1)
    label_keys = item_map.reshape(canvases, -1)
    linked = label_rows[:, None, :, None] == label_keys[:, None, None, :]
    masked = jnp.where(linked, scores, -1e30)
    row_peak = jnp.max(masked, axis=-1, keepdims=True)
    raised = jnp.exp(masked - row_peak)
    row_total = jnp.sum(raised, axis=-1, keepdims=True)
    attention = raised / row_total
    attention_low = attention.astype(jnp.bfloat16)
    attended = jnp.einsum(
        "bhqk,bkhd->bqhd", attention_low, value_heads, preferred_element_type=jnp.float32
    ).astype(jnp.bfloat16)
    attended = attended.reshape(cell_count, features)
    attn_branch = jnp.dot(attended, out_full, preferred_element_type=jnp.float32).reshape(
        tokens.shape
    )
    middle = token_values + gate_one * attn_branch
    normed_two, inverse_two = normalize(middle)
    modulated_two = (normed_two * (1.0 + scale_two) + shift_two).astype(jnp.bfloat16)
    modulated_rows = modulated_two.reshape(cell_count, features)
    hidden_up_projection = jnp.dot(
        modulated_rows, up_full, preferred_element_type=jnp.float32
    ).astype(jnp.bfloat16)
    hidden_up_projection = hidden_up_projection.reshape(
        canvases, rows_here, cols_here, hidden_units
    )
    up_padded = widen_cols(padded(hidden_up_projection, (("rows", 1),), 1))
    pre_gelu = conv_forward(up_padded, labels_here, centre, kernel_ffn)
    activated, gelu_back = jax.vjp(jax.nn.gelu, pre_gelu)
    gelu_low = activated.astype(jnp.bfloat16).reshape(cell_count, hidden_units)
    ffn_branch = jnp.dot(gelu_low, down_full, preferred_element_type=jnp.float32).reshape(
        tokens.shape
    )
    layer_out = (middle + gate_two * ffn_branch).astype(jnp.bfloat16)
    weights_back = (
        lax.all_gather(ada_weight, ("dp", "rows"), axis=0, tiled=True),
        lax.all_gather(ada_bias, ("dp", "rows"), axis=0, tiled=True),
        lax.all_gather(attn_kernel, ("dp", "rows"), axis=1, tiled=True),
        lax.all_gather(qkv_weight, ("dp", "rows"), axis=0, tiled=True),
        lax.all_gather(out_weight, ("dp", "rows"), axis=0, tiled=True),
        lax.all_gather(up_weight, ("dp", "rows"), axis=0, tiled=True),
        lax.all_gather(ffn_kernel, ("dp", "rows"), axis=1, tiled=True),
        lax.all_gather(down_weight, ("dp", "rows"), axis=0, tiled=True),
    )
    (
        ada_back,
        bias_back,
        kernel_attn_back,
        triple_back,
        out_back,
        up_back,
        kernel_ffn_back,
        down_projection_back,
    ) = weights_back
    incoming = out_cotangent.astype(jnp.float32)
    grad_gate_two = jnp.sum(incoming * ffn_branch, axis=(1, 2))
    grad_ffn = (gate_two * incoming).astype(jnp.bfloat16).reshape(cell_count, features)
    grad_down = contract_rows(gelu_low, grad_ffn)
    grad_gelu = contract_cols(grad_ffn, down_projection_back).reshape(
        canvases, rows_here, cols_here, hidden_units
    )
    grad_pre = gelu_back(grad_gelu)[0].astype(jnp.bfloat16)
    grad_pre_padded = widen_cols(padded(grad_pre, (("rows", 1),), 1))
    grad_kernel_ffn = kernel_grad(grad_pre, up_padded, labels_here, centre)
    grad_up = (
        conv_mirror(grad_pre_padded, labels_here, centre, kernel_ffn_back)
        .astype(jnp.bfloat16)
        .reshape(cell_count, hidden_units)
    )
    grad_up_weight = contract_rows(modulated_rows, grad_up)
    grad_mod_two = contract_cols(grad_up, up_back).reshape(tokens.shape)
    grad_scale_two = jnp.sum(grad_mod_two * normed_two, axis=(1, 2))
    grad_shift_two = jnp.sum(grad_mod_two, axis=(1, 2))
    grad_middle = incoming + normalize_back(
        grad_mod_two * (1.0 + scale_two), normed_two, inverse_two
    )
    grad_gate_one = jnp.sum(grad_middle * attn_branch, axis=(1, 2))
    grad_attn = (gate_one * grad_middle).astype(jnp.bfloat16).reshape(cell_count, features)
    grad_out_weight = contract_rows(attended, grad_attn)
    grad_attended = (
        contract_cols(grad_attn, out_back)
        .astype(jnp.bfloat16)
        .reshape(canvases, -1, head_count, PER_GROUP_WIDTH)
    )
    grad_weights = jnp.einsum(
        "bqhd,bkhd->bhqk", grad_attended, value_heads, preferred_element_type=jnp.float32
    )
    row_delta = jnp.sum(attention * grad_weights, axis=-1, keepdims=True)
    grad_scores = (attention * (grad_weights - row_delta)).astype(jnp.bfloat16)
    grad_query = (
        jnp.einsum("bhqk,bkhd->bqhd", grad_scores, key_heads, preferred_element_type=jnp.float32)
        * logit_divisor
    )
    grad_key_all = (
        jnp.einsum("bhqk,bqhd->bkhd", grad_scores, query_heads, preferred_element_type=jnp.float32)
        * logit_divisor
    )
    value_gradient_full = jnp.einsum(
        "bhqk,bqhd->bkhd", attention_low, grad_attended, preferred_element_type=jnp.float32
    )
    grad_key, grad_value = (
        lax.psum_scatter(
            grad_key_all.reshape(canvases, -1, features).astype(jnp.bfloat16),
            "rows",
            scatter_dimension=1,
            tiled=True,
        ).astype(jnp.float32),
        lax.psum_scatter(
            value_gradient_full.reshape(canvases, -1, features).astype(jnp.bfloat16),
            "rows",
            scatter_dimension=1,
            tiled=True,
        ).astype(jnp.float32),
    )
    grad_projected = jnp.concatenate(
        [
            grad_query.reshape(cell_count, features),
            grad_key.reshape(cell_count, features),
            grad_value.reshape(cell_count, features),
        ],
        axis=-1,
    ).astype(jnp.bfloat16)
    grad_qkv_weight = contract_rows(mix_rows, grad_projected)
    grad_mix = contract_cols(grad_projected, triple_back).astype(jnp.bfloat16).reshape(tokens.shape)
    grad_mix_padded = widen_cols(padded(grad_mix, (("rows", 1),), 1))
    grad_kernel_attn = kernel_grad(grad_mix, modulated_padded, labels_here, centre)
    grad_mod_one = conv_mirror(grad_mix_padded, labels_here, centre, kernel_attn_back)
    grad_scale_one = jnp.sum(grad_mod_one * normed_one, axis=(1, 2))
    grad_shift_one = jnp.sum(grad_mod_one, axis=(1, 2))
    token_grad = grad_middle + normalize_back(
        grad_mod_one * (1.0 + scale_one), normed_one, inverse_one
    )
    grad_parts = jnp.concatenate(
        [
            grad_shift_one,
            grad_scale_one,
            grad_gate_one,
            grad_shift_two,
            grad_scale_two,
            grad_gate_two,
        ],
        axis=-1,
    )
    grad_modulation = lax.psum(grad_parts.astype(jnp.bfloat16), "rows")
    leader = (position == 0).astype(jnp.float32)
    grad_ada_weight = contract_rows(silu_low, grad_modulation) * leader
    grad_ada_bias = jnp.sum(grad_modulation.astype(jnp.float32), axis=0) * leader
    silu_values, silu_back = jax.vjp(jax.nn.silu, cond_values)
    derivative_of_context = silu_back(contract_cols(grad_modulation, ada_back))[0]
    summed_grads = (
        lax.psum_scatter(grad_ada_weight, ("dp", "rows"), scatter_dimension=0, tiled=True),
        lax.psum_scatter(grad_ada_bias, ("dp", "rows"), scatter_dimension=0, tiled=True),
        lax.psum_scatter(grad_kernel_attn, ("dp", "rows"), scatter_dimension=1, tiled=True),
        lax.psum_scatter(grad_qkv_weight, ("dp", "rows"), scatter_dimension=0, tiled=True),
        lax.psum_scatter(grad_out_weight, ("dp", "rows"), scatter_dimension=0, tiled=True),
        lax.psum_scatter(grad_up_weight, ("dp", "rows"), scatter_dimension=0, tiled=True),
        lax.psum_scatter(grad_kernel_ffn, ("dp", "rows"), scatter_dimension=1, tiled=True),
        lax.psum_scatter(grad_down, ("dp", "rows"), scatter_dimension=0, tiled=True),
    )
    return (layer_out, token_grad, derivative_of_context) + tuple(summed_grads)


F32=jnp.float32; BF=jnp.bfloat16
NT=(((1,),(1,)),((),()))
TN=(((0,),(0,)),((),()))

def head_masks(labels):
    cells=labels.shape[0]
    lane=lax.broadcasted_iota(jnp.int32,(cells,128),1)%64
    lab=labels[:,None]
    qm=(lane==lab).astype(BF)
    km=jnp.where((lane!=lab)&(lane<4),-1e30,0.0).astype(BF)
    return qm,km

MESH=pl.DeviceIdType.MESH
NZ,NC,NR=4,2,4


def here():
    dp=lax.axis_index("dp"); rows=lax.axis_index("rows")
    return dp//NC, lax.rem(dp,NC), rows


def dev(z,core,rows):
    return (z*NC+core, rows)


def partner_xy(rows,t):
    x=lax.rem(rows,2); y=rows//2
    tx=t%2; ty=t//2
    nx=1-x if tx else x
    ny=1-y if ty else y
    return ny*2+nx


def rcopy(src,dst,ssem,rsem,target):
    return pltpu.make_async_remote_copy(src_ref=src,dst_ref=dst,send_sem=ssem,recv_sem=rsem,device_id=target,device_id_type=MESH)


def barrier_all():
    dp=lax.axis_index("dp"); rows=lax.axis_index("rows")
    me=dp*NR+rows
    total=NZ*NC*NR
    bar=pltpu.get_barrier_semaphore()
    def body(k,c):
        other=lax.rem(me+k,total)
        pl.semaphore_signal(bar,inc=1,device_id=(other//NR,lax.rem(other,NR)),device_id_type=MESH)
        return c
    lax.fori_loop(1,total,body,0)
    pl.semaphore_wait(bar,total-1)


def zmod(v):
    return lax.rem(v+NZ,NZ)


class Gather:
    SEMS=[(NZ,),(NZ,),(NZ,NR),(NZ,NR),(NZ,NR),(NZ,NR),(1,)]

    def __init__(self,shard,full,sems):
        self.shard,self.full=shard,full
        self.sz,self.rz,self.sx,self.rx,self.sc,self.rc,self.lo=sems
        self.z,self.core,self.rows=here()

    def slot(self,dz,t,core):
        rows=self.rows if t==0 else partner_xy(self.rows,t)
        return self.full.at[zmod(self.z-dz),core,rows]

    def zcopy(self,dz,receive=False):
        dst=self.slot(dz if receive else 0,0,self.core)
        return rcopy(self.shard,dst,self.sz.at[dz],self.rz.at[dz],dev(zmod(self.z+dz),self.core,self.rows))

    def piece(self,dz):
        return self.shard if dz==0 else self.slot(dz,0,self.core)

    def xcopy(self,dz,t,receive=False):
        dst=self.slot(dz,t if receive else 0,self.core)
        return rcopy(self.piece(dz),dst,self.sx.at[dz,t],self.rx.at[dz,t],dev(self.z,self.core,partner_xy(self.rows,t)))

    def ccopy(self,dz,t,receive=False):
        src=self.piece(dz) if t==0 else self.slot(dz,t,self.core)
        dst=self.slot(dz,t,1-self.core if receive else self.core)
        return rcopy(src,dst,self.sc.at[dz,t],self.rc.at[dz,t],dev(self.z,1-self.core,self.rows))

    def local(self):
        return pltpu.make_async_copy(self.shard,self.slot(0,0,self.core),self.lo.at[0])

    def start(self):
        for dz in range(1,NZ):
            self.zcopy(dz).start()
        for t in range(1,NR):
            self.xcopy(0,t).start()
        self.ccopy(0,0).start()
        self.local().start()

    def zstep(self,dz):
        self.zcopy(dz,True).wait_recv()
        for t in range(1,NR):
            self.xcopy(dz,t).start()
        self.ccopy(dz,0).start()

    def xstep(self,dz,t):
        self.xcopy(dz,t,True).wait_recv()
        self.ccopy(dz,t).start()

    def finish(self):
        for dz in range(NZ):
            for t in range(NR):
                self.ccopy(dz,t,True).wait_recv()
        for dz in range(1,NZ):
            self.zcopy(dz).wait_send()
        for dz in range(NZ):
            for t in range(NR):
                if t: self.xcopy(dz,t).wait_send()
                self.ccopy(dz,t).wait_send()
        self.local().wait()

    def run_z(self):
        for dz in range(1,NZ): self.zstep(dz)

    def run_x(self):
        for dz in range(NZ):
            for t in range(1,NR): self.xstep(dz,t)


class Scatter:
    SEMS=[(1,),(1,),(1,),(NR,),(NR,),(NZ,),(NZ,)]

    @staticmethod
    def scratch(r,c,dt):
        return [pltpu.VMEM((NZ,NR,r,c),dt),pltpu.VMEM((NZ,NR,r,c),dt),pltpu.VMEM((NR,NZ,r,c),dt),pltpu.VMEM((NZ,r,c),dt),pltpu.VMEM((NZ,r,c),dt)]

    def __init__(self,part,out,bufs,sems):
        self.part,self.out=part,out
        self.own,self.sib,self.xin,self.zout,self.zin=bufs
        self.lo,self.sc,self.rc,self.sx,self.rx,self.sz,self.rz=sems
        self.z,self.core,self.rows=here()
        self.dt=self.own.dtype

    def lcopy(self):
        return pltpu.make_async_copy(self.part.at[:,self.core],self.own,self.lo.at[0])

    def ccopy(self):
        return rcopy(self.part.at[:,1-self.core],self.sib,self.sc.at[0],self.rc.at[0],dev(self.z,1-self.core,self.rows))

    def xcopy(self,t):
        to=partner_xy(self.rows,t)
        return rcopy(self.own.at[:,to],self.xin.at[t],self.sx.at[t],self.rx.at[t],dev(self.z,self.core,to))

    def zcopy(self,dz):
        to=zmod(self.z+dz)
        return rcopy(self.zout.at[to],self.zin.at[dz],self.sz.at[dz],self.rz.at[dz],dev(to,self.core,self.rows))

    def start(self):
        self.ccopy().start(); self.lcopy().start()

    def cstep(self):
        self.lcopy().wait(); self.ccopy().wait_recv()
        def body(i,c):
            a,b=i//NR,lax.rem(i,NR)
            self.own[a,b]=(self.own[a,b].astype(F32)+self.sib[a,b].astype(F32)).astype(self.dt)
            return c
        lax.fori_loop(0,NZ*NR,body,0)
        for t in range(1,NR): self.xcopy(t).start()

    def xstep(self):
        for t in range(1,NR): self.xcopy(t).wait_recv()
        def body(a,c):
            s=self.own[a,self.rows].astype(F32)
            for t in range(1,NR): s=s+self.xin[t,a].astype(F32)
            self.zout[a]=s.astype(self.dt)
            return c
        lax.fori_loop(0,NZ,body,0)
        for dz in range(1,NZ): self.zcopy(dz).start()

    def zstep(self):
        for dz in range(1,NZ): self.zcopy(dz).wait_recv()
        s=self.zout[self.z].astype(F32)
        for dz in range(1,NZ): s=s+self.zin[dz].astype(F32)
        self.out[...]=s

    def finish(self):
        self.ccopy().wait_send()
        for t in range(1,NR): self.xcopy(t).wait_send()
        for dz in range(1,NZ): self.zcopy(dz).wait_send()


class Swap:
    SEMS=[(NR,),(NR,),(1,)]
    def __init__(self,src,dst,sems):
        self.src,self.dst=src,dst
        self.s,self.r,self.lo=sems
        self.z,self.core,self.rows=here()
    def copy(self,t,receive=False):
        to=partner_xy(self.rows,t)
        return rcopy(self.src.at[to],self.dst.at[to if receive else self.rows],self.s.at[t],self.r.at[t],dev(self.z,self.core,to))
    def local(self):
        return pltpu.make_async_copy(self.src.at[self.rows],self.dst.at[self.rows],self.lo.at[0])
    def start(self):
        for t in range(1,NR): self.copy(t).start()
        self.local().start()
    def wait(self):
        for t in range(1,NR): self.copy(t,True).wait_recv()
        self.local().wait()
    def finish(self):
        for t in range(1,NR): self.copy(t).wait_send()


class AllToAll:
    N=NZ*NC*NR
    SEMS=[(N,),(N,),(1,)]
    def __init__(self,src,dst,sems,one=False):
        self.src,self.dst,self.one=src,dst,one
        self.s,self.r,self.lo=sems
        self.me=lax.axis_index("dp")*NR+lax.axis_index("rows")
    def piece(self,n):
        return self.src if self.one else self.src.at[n]
    def copy(self,k,receive=False):
        to=lax.rem(self.me+k,self.N)
        frm=lax.rem(self.me-k+self.N,self.N)
        return rcopy(self.piece(to),self.dst.at[frm if receive else self.me],self.s.at[k],self.r.at[k],(to//NR,lax.rem(to,NR)))
    def local(self):
        return pltpu.make_async_copy(self.piece(self.me),self.dst.at[self.me],self.lo.at[0])
    def each(self,fn):
        def body(k,c):
            fn(k); return c
        lax.fori_loop(1,self.N,body,0)
    def start(self):
        self.each(lambda k:self.copy(k).start())
        self.local().start()
    def wait(self):
        self.each(lambda k:self.copy(k,True).wait_recv())
        self.local().wait()
    def finish(self):
        self.each(lambda k:self.copy(k).wait_send())


def sem_types(shapes):
    return [pltpu.SemaphoreType.DMA(s) for s in shapes]
class GatherZ:
    SEMS=[(NZ,),(NZ,),(1,)]
    def __init__(self,shard,zp,sems):
        self.shard,self.zp=shard,zp
        self.s,self.r,self.lo=sems
        self.z,self.core,self.rows=here()
    def copy(self,dz,receive=False):
        to=zmod(self.z+dz)
        frm=zmod(self.z-dz)
        return rcopy(self.shard,self.zp.at[frm if receive else self.z],self.s.at[dz],self.r.at[dz],dev(to,self.core,self.rows))
    def local(self):
        return pltpu.make_async_copy(self.shard,self.zp.at[self.z],self.lo.at[0])
    def start(self):
        for dz in range(1,NZ): self.copy(dz).start()
        self.local().start()
    def wait(self):
        for dz in range(1,NZ): self.copy(dz,True).wait_recv()
    def finish(self):
        for dz in range(1,NZ): self.copy(dz).wait_send()
        self.local().wait()


class GatherXY:
    SEMS=[(NZ,NR),(NZ,NR),(NZ,NR),(NZ,NR),(1,)]
    def __init__(self,zp,full,sems):
        self.zp,self.full=zp,full
        self.sx,self.rx,self.sc,self.rc,self.lo=sems
        self.z,self.core,self.rows=here()
    def place(self,t):
        return self.rows if t==0 else partner_xy(self.rows,t)
    def xcopy(self,k,t,receive=False):
        return rcopy(self.zp.at[k],self.full.at[k,self.core,self.place(t) if receive else self.rows],self.sx.at[k,t],self.rx.at[k,t],dev(self.z,self.core,self.place(t)))
    def ccopy(self,k,t,receive=False):
        src=self.zp.at[k] if t==0 else self.full.at[k,self.core,self.place(t)]
        dst=self.full.at[k,1-self.core if receive else self.core,self.place(t)]
        return rcopy(src,dst,self.sc.at[k,t],self.rc.at[k,t],dev(self.z,1-self.core,self.rows))
    def local(self):
        return pltpu.make_async_copy(self.zp,self.full.at[:,self.core,self.rows],self.lo.at[0])
    def start(self,ks=range(NZ)):
        for k in ks:
            for t in range(1,NR): self.xcopy(k,t).start()
            self.ccopy(k,0).start()
    def start_local(self):
        self.local().start()
    def step(self,k):
        for t in range(1,NR):
            self.xcopy(k,t,True).wait_recv()
            self.ccopy(k,t).start()
    def arrive(self,k):
        for t in range(NR): self.ccopy(k,t,True).wait_recv()
    def finish(self):
        for k in range(NZ):
            for t in range(NR):
                if t: self.xcopy(k,t).wait_send()
                self.ccopy(k,t).wait_send()
        self.local().wait()
    def finish_remote(self):
        for k in range(NZ):
            for t in range(NR):
                if t: self.xcopy(k,t).wait_send()
                self.ccopy(k,t).wait_send()


class ScatterZ:
    SEMS=[(NZ,),(NZ,)]
    @staticmethod
    def scratch(r,c,dt):
        return [pltpu.VMEM((NZ,r,c),dt)]
    def __init__(self,zout,out,bufs,sems):
        self.zout,self.out=zout,out
        self.zin,=bufs
        self.s,self.r=sems
        self.z,self.core,self.rows=here()
    def copy(self,dz):
        to=zmod(self.z+dz)
        return rcopy(self.zout.at[to],self.zin.at[dz],self.s.at[dz],self.r.at[dz],dev(to,self.core,self.rows))
    def start(self):
        for dz in range(1,NZ): self.copy(dz).start()
    def step(self):
        for dz in range(1,NZ): self.copy(dz).wait_recv()
        v=self.zout[self.z].astype(F32)
        for dz in range(1,NZ): v=v+self.zin[dz].astype(F32)
        self.out[...]=v
    def finish(self):
        for dz in range(1,NZ): self.copy(dz).wait_send()


class Events:
    def __init__(self): self.at={}
    def add(self,slot,fn): self.at.setdefault(slot,[]).append(fn)
    def run(self,outer,inner,width):
        for slot,fns in self.at.items():
            if slot%width==inner:
                @pl.when(outer==slot//width)
                def _(fns=fns):
                    for fn in fns: fn()
NN=(((1,),(0,)),((),()))
C0=0.7978845608028654
C1=0.044715


def dotf(a,b,dims=NN):
    return lax.dot_general(a,b,dims,preferred_element_type=F32)


def loop(n,fn,unroll=1):
    def body(i,c):
        fn(i); return c
    lax.fori_loop(0,n,body,0,unroll=unroll)


def rows_of(i,n):
    return pl.ds(pl.multiple_of(i*n,n),n)


def normal_rows(v):
    d=1.0/v.shape[1]
    c=v-jnp.sum(v,axis=1,keepdims=True)*d
    inv=lax.rsqrt(jnp.sum(c*c,axis=1,keepdims=True)*d+EPSILON)
    return c*inv,inv


def normal_back_rows(g,n,inv):
    d=1.0/g.shape[1]
    return inv*(g-jnp.sum(g,axis=1,keepdims=True)*d-n*(jnp.sum(g*n,axis=1,keepdims=True)*d))


def fold8(v):
    s=v[0:8]
    for k in range(1,v.shape[0]//8): s=s+v[8*k:8*k+8]
    return s


def conv_loops(side,lanes_n,width,forward,finish):
    pass


def shifts(f,ml,mr):
    n=f.shape[0]
    return pltpu.roll(f,1,0)*ml, pltpu.roll(f,n-1,0)*mr


def conv_rows(src,dst_fn,taps,ml_ref,mr_ref,rl_ref,lane,side,cols):
    sl=pl.ds(lane*128,128)
    k=[taps[q:q+1,lane*128:(lane+1)*128] for q in range(9)]
    zero=jnp.zeros((cols,128),F32)
    def body(i,c):
        hm,part=c
        f=src[rows_of(i,cols),lane*128:(lane+1)*128]
        fm,fp=shifts(f,ml_ref[rows_of(i,cols),:],mr_ref[rows_of(i,cols),:])
        h=[k[3*a]*fm+k[3*a+1]*f+k[3*a+2]*fp for a in range(3)]
        done=part+rl_ref[i]*h[2]
        @pl.when(i>0)
        def _(): dst_fn(i-1,done)
        return h[0],h[1]+rl_ref[i]*hm
    hm,part=lax.fori_loop(0,side,body,(zero,zero),unroll=8)
    dst_fn(side-1,part)


def back_rows(g_ref,f_ref,dst_fn,taps,ml_ref,mr_ref,rl_ref,lane,side,cols):
    ls=slice(lane*128,(lane+1)*128)
    k=[taps[q:q+1,ls] for q in range(9)]
    zero=jnp.zeros((cols,128),F32)
    z8=jnp.zeros((8,128),F32)
    def body(i,c):
        hp,part,fprev,acc=c
        g=g_ref[rows_of(i,cols),ls]
        gm,gp=shifts(g,ml_ref[rows_of(i,cols),:],mr_ref[rows_of(i,cols),:])
        gs=(gp,g,gm)
        q=[k[3*a]*gp+k[3*a+1]*g+k[3*a+2]*gm for a in range(3)]
        done=part+rl_ref[i]*q[0]
        @pl.when(i>0)
        def _(): dst_fn(i-1,done)
        f=f_ref[rows_of(i,cols),ls].astype(F32)
        nxt=f_ref[pl.ds(pl.multiple_of(jnp.minimum(i+1,side-1)*cols,cols),cols),ls].astype(F32)
        fs=(fprev*rl_ref[i],f,nxt*rl_ref[i+1])
        acc=tuple(acc[3*a+b]+fold8(fs[a]*gs[b]) for a in range(3) for b in range(3))
        return q[2],q[1]+rl_ref[i]*hp,f,acc
    hp,part,_,acc=lax.fori_loop(0,side,body,(zero,zero,zero,(z8,)*9),unroll=8)
    dst_fn(side-1,part)
    return acc


def link_masks(labels):
    side,cols=labels.shape
    left=jnp.pad(labels[:,1:]==labels[:,:-1],((0,0),(1,0)))
    right=jnp.pad(labels[:,1:]==labels[:,:-1],((0,0),(0,1)))
    wide=lambda m: jnp.broadcast_to(m.reshape(side*cols,1).astype(F32),(side*cols,128))
    top=labels[:,0]//2
    rl=jnp.pad((top[1:]==top[:-1]).astype(F32),(1,1))
    return wide(left),wide(right),rl
HBM=pl.BlockSpec(memory_space=pl.ANY)
VM=pl.BlockSpec(memory_space=pltpu.VMEM)
SM=pl.BlockSpec(memory_space=pltpu.SMEM)
NDEV=NZ*NC*NR
S_=jax.ShapeDtypeStruct


def taker(it):
    return lambda cls:[next(it) for _ in cls.SEMS]


def enter_kernel(n_z,*refs):
    it=iter(refs)
    tok,cond,ada,bias,qkv,taps=[next(it) for _ in range(6)]
    shards=[next(it) for _ in range(n_z)]
    tok_o,cond_o,mod_o,qkv_o,taps_o=[next(it) for _ in range(5)]
    zps=[next(it) for _ in range(n_z)]
    condv,part=[next(it) for _ in range(2)]
    mbufs=[next(it) for _ in range(5)]
    take=taker(it)
    barrier_all()
    c_all=AllToAll(cond,condv,take(AllToAll),one=True)
    swap_t=Swap(tok,tok_o,take(Swap))
    m_all=Scatter(part,mod_o,mbufs,take(Scatter))
    g_taps=Gather(taps,taps_o,take(Gather))
    g_qkv=Gather(qkv,qkv_o,take(Gather))
    gz=[GatherZ(s,z,take(GatherZ)) for s,z in zip(shards,zps)]
    c_all.start()
    swap_t.start()
    g_taps.start()
    g_qkv.start()
    c_all.wait()
    me=c_all.me
    feats=ada.shape[0]
    cv=condv[:,0,:].astype(F32)
    low=(cv/(1.0+jnp.exp(-cv))).astype(BF)
    width=cv.shape[1]
    pick=(lax.broadcasted_iota(jnp.int32,(width,feats),0)==lax.broadcasted_iota(jnp.int32,(width,feats),1)+feats*me).astype(BF)
    mine=jnp.dot(low,pick,preferred_element_type=F32).astype(BF)
    chunk=768
    for c in range(ada.shape[1]//chunk):
        pr=jnp.dot(mine,ada[:,c*chunk:(c+1)*chunk],preferred_element_type=F32)
        for l in range(chunk//128):
            i=c*(chunk//128)+l
            part[:,:,:,i,:]=(pr[:,l*128:(l+1)*128]+bias[i:i+1,:]).reshape(NZ,NC,NR,128)
    cond_o[...]=low
    m_all.start()
    m_all.cstep()
    g_taps.run_z(); g_qkv.run_z()
    m_all.xstep()
    for g in gz: g.start()
    m_all.zstep()
    swap_t.wait()
    g_taps.run_x(); g_qkv.run_x()
    for g in gz: g.wait()
    for g in [g_taps,g_qkv,swap_t,c_all,m_all]+gz: g.finish()


def enter(tok,cond_row,ada,bias_rows,qkv,taps,shards):
    n=len(shards)
    scr=[pltpu.VMEM((NDEV,)+cond_row.shape,cond_row.dtype),pltpu.VMEM((NZ,NC,NR)+bias_rows.shape,F32)]+Scatter.scratch(bias_rows.shape[0],128,F32)
    sems=sem_types(AllToAll.SEMS)+sem_types(Swap.SEMS)+sem_types(Scatter.SEMS)+sem_types(Gather.SEMS)*2+sem_types(GatherZ.SEMS)*n
    outs=[S_(tok.shape,tok.dtype),S_((NDEV,cond_row.shape[1]),BF),S_(bias_rows.shape,F32),
          S_((NZ,NC,NR)+qkv.shape,qkv.dtype),S_((NZ,NC,NR)+taps.shape,taps.dtype)]
    outs+=[S_((NZ,)+s.shape,s.dtype) for s in shards]
    return pl.pallas_call(
        functools.partial(enter_kernel,n),
        in_specs=[VM,HBM,VM,VM,VM,VM]+[VM]*n,
        out_specs=[HBM,VM,VM,HBM,HBM]+[HBM]*n,
        out_shape=outs,
        scratch_shapes=scr+sems,
        compiler_params=pltpu.CompilerParams(collective_id=0,has_side_effects=True,vmem_limit_bytes=63<<20),
        name="enter",
    )(tok,cond_row,ada,bias_rows,qkv,taps,*shards)


def forward_kernel(n_w,qb,*refs):
    it=iter(refs)
    mix,qkv,qm,km,cot,late=[next(it) for _ in range(6)]
    zps=[next(it) for _ in range(n_w)]
    proj,att,lse_t,cot_o,late_o=[next(it) for _ in range(5)]
    fulls=[next(it) for _ in range(n_w)]
    lse=next(it)
    take=taker(it)
    barrier_all()
    swap_c=Swap(cot,cot_o,take(Swap))
    gs=[GatherXY(a,b,take(GatherXY)) for a,b in zip(zps,fulls)]
    gl=GatherZ(late,late_o,take(GatherZ))
    gl.start()
    gs[0].start(); swap_c.start(); gs[1].start()
    for g in gs: g.start_local()
    ev=Events()
    for k in range(NZ):
        ev.add(1,lambda k=k: gs[0].step(k))
        ev.add(8+k,lambda k=k: gs[1].step(k))
    cells,feat=att.shape
    CH=256
    def pr(i):
        proj[rows_of(i,CH),:]=dotf(mix[rows_of(i,CH),:],qkv[...]).astype(BF)
    loop(cells//CH,pr)
    pairs=feat//128
    lane=lax.broadcasted_iota(jnp.int32,(1,128),1)
    lse[...]=jnp.zeros_like(lse)
    def pair(p):
        cq=pl.ds(pl.multiple_of(p*128,128),128)
        ck=pl.ds(pl.multiple_of(feat+p*128,128),128)
        cv=pl.ds(pl.multiple_of(2*feat+p*128,128),128)
        for h in range(2):
            ev.run(p,h,2)
            mine=(lane//64)==h
            k=jnp.where(mine,proj[:,ck],km[...])
            def body(i):
                r=rows_of(i,qb)
                q=jnp.where(mine,proj[r,cq]*jnp.asarray(0.125,BF),qm[r,:])
                s=dotf(q,k,NT)
                m=jnp.max(s,axis=1,keepdims=True)
                e=jnp.exp(s-m)
                l=jnp.sum(e,axis=1,keepdims=True)
                a=(e*(1.0/l)).astype(BF)
                o=dotf(a,proj[:,cv]).astype(BF)
                if h==0:
                    att[r,cq]=o
                else:
                    att[r,cq]=jnp.where(mine,o,att[r,cq])
                lse[r,:]=jnp.where(lane==2*p+h,m+jnp.log(l),lse[r,:])
            loop(cells//qb,body,2)
    loop(pairs,pair)
    lse_t[...]=jnp.transpose(lse[...])
    for g in gs:
        for k in range(NZ): g.arrive(k)
    swap_c.wait()
    gl.wait()
    for g in gs+[swap_c,gl]: g.finish()


def forward(mix,qkv,qm,km,cot,late,zps):
    n=len(zps)
    cells,feat=mix.shape
    outs=[S_((cells,3*feat),BF),S_((cells,feat),BF),S_((128,cells),F32),S_(cot.shape,cot.dtype),S_((NZ,)+late.shape,late.dtype)]
    outs+=[S_((NZ,NC,NR)+z.shape[1:],z.dtype) for z in zps]
    return pl.pallas_call(
        functools.partial(forward_kernel,n,512),
        in_specs=[VM,VM,VM,VM,VM,VM]+[VM]*n,
        out_specs=[VM,VM,VM,HBM,HBM]+[HBM]*n,
        out_shape=outs,
        scratch_shapes=[pltpu.VMEM((cells,128),F32)]+sem_types(Swap.SEMS)+sem_types(GatherXY.SEMS)*n+sem_types(GatherZ.SEMS),
        compiler_params=pltpu.CompilerParams(collective_id=1,has_side_effects=True,vmem_limit_bytes=63<<20),
        name="attn_fwd",
    )(mix,qkv,qm,km,cot,late,*zps)


def backward_kernel(n_g,kb,*refs):
    it=iter(refs)
    nx=lambda n:[next(it) for _ in range(n)]
    proj,do,o,qm,km,lse_t,mix,lay,gout=nx(9)
    parts=nx(n_g)
    gp,lay_o,gout_o,zq,lastq=nx(5)
    gouts=nx(n_g)
    qs,dqt,mixt=nx(3)
    obufs=nx(5)
    qbufs=nx(4)
    bufs=[nx(1) for _ in range(n_g)]
    take=taker(it)
    barrier_all()
    sl=Swap(lay,lay_o,take(Swap))
    so=Scatter(gout,gout_o,obufs,take(Scatter))
    uq=PipeScatter(qbufs,take(PipeScatter))
    sc=[ScatterZ(p,g,b,take(ScatterZ)) for p,g,b in zip(parts,gouts,bufs)]
    cells,feat=do.shape
    pairs=feat//128
    W=256
    tiles=pairs//2
    r_=feat//NDEV
    def put_q(m):
        def put(a,v):
            for s in range(3):
                zq[a,:,(s*(tiles-1)+m)*W:(s*(tiles-1)+m+1)*W]=v[:,s*W:(s+1)*W]
        return put
    ev=Events()
    so.start()
    for s in sc: s.start()
    ev.add(1,so.cstep)
    ev.add(2,sl.start)
    ev.add(5,lambda: uq.send_square(0))
    ev.add(6,so.xstep)
    for s in sc: ev.add(7,s.step)
    ev.add(8,lambda: uq.collect(0,put_q(0)))
    ev.add(9,lambda: uq.send_square(1))
    ev.add(11,so.zstep)
    lane=lax.broadcasted_iota(jnp.int32,(1,128),1)
    srow=lax.broadcasted_iota(jnp.int32,(8,128),0)
    slane=lax.broadcasted_iota(jnp.int32,(8,128),1)
    sel=(slane//64==srow).astype(BF)
    def tr(i):
        mixt[:,pl.ds(pl.multiple_of(i*256,256),256)]=jnp.transpose(mix[rows_of(i,256),:])
    loop(cells//256,tr)
    def pair(p):
        cq=pl.ds(pl.multiple_of(p*128,128),128)
        ck=pl.ds(pl.multiple_of(feat+p*128,128),128)
        cv=pl.ds(pl.multiple_of(2*feat+p*128,128),128)
        prod=do[:,cq].astype(F32)*o[:,cq].astype(F32)
        hi=prod.astype(BF); lo=(prod-hi.astype(F32)).astype(BF)
        delta=dotf(sel,hi,NT)+dotf(sel,lo,NT)
        qs[...]=proj[:,cq]*jnp.asarray(0.125,BF)
        for h in range(2):
            ev.run(p,h,2)
            mine=(lane//64)==h
            q=jnp.where(mine,qs[...],qm[...])
            ls=lse_t[pl.ds(2*p+h,1),:]
            dl=delta[h:h+1,:]
            dqt[...]=jnp.zeros_like(dqt)
            def body(i):
                r=rows_of(i,kb)
                kr=proj[r,ck]
                k=jnp.where(mine,kr,km[r,:])
                v=jnp.where(mine,proj[r,cv],jnp.zeros((),BF))
                st=dotf(k,q,NT)
                pt=jnp.exp(st-ls)
                dpt=dotf(v,do[:,cq],NT)
                ds=(pt*(dpt-dl)).astype(BF)
                dv=dotf(pt.astype(BF),do[:,cq]).astype(BF)
                dk=dotf(ds,qs[...]).astype(BF)
                dqt[...]+=dotf(kr,ds,TN)
                if h==0:
                    gp[r,cv]=dv
                    gp[r,ck]=dk
                else:
                    gp[r,cv]=jnp.where(mine,dv,gp[r,cv])
                    gp[r,ck]=jnp.where(mine,dk,gp[r,ck])
            loop(cells//kb,body,2)
            dq=(jnp.transpose(dqt[...])*0.125).astype(BF)
            if h==0:
                gp[:,cq]=dq
            else:
                gp[:,cq]=jnp.where(mine,dq,gp[:,cq])
        @pl.when(lax.rem(p,2)==1)
        def _():
            m=p//2
            s=lax.rem(m,2)
            n=NC*NR*r_
            def tile(i):
                for c in range(3):
                    cols=pl.ds(pl.multiple_of(c*feat+m*W,W),W)
                    uq.part[s,i,:,:,:,c*W:(c+1)*W]=dotf(mixt[rows_of(i,n),:],gp[:,cols]).astype(BF).reshape(NC,NR,r_,W)
            loop(NZ,tile)
            @pl.when(m<tiles-1)
            def _(): uq.send_core(s)
    loop(pairs,pair)
    uq.collect(1,put_q(1))
    lastq[...]=uq.part[0]
    sl.wait()
    for s in sc+[sl,so]: s.finish()


def backward(proj,do,o,qm,km,lse_t,mix,lay,gout,parts):
    n=len(parts)
    cells,feat=do.shape
    r_=feat//NDEV
    outs=[S_((cells,3*feat),BF),S_(lay.shape,lay.dtype),S_(gout.shape[3:],F32),S_((NZ,r_,2*feat),BF),S_((NZ,NC,NR,r_,feat),BF)]+[S_(p.shape[1:],F32) for p in parts]
    scr=[pltpu.VMEM((cells,128),BF),pltpu.VMEM((128,cells),F32),pltpu.VMEM((feat,cells),BF)]
    scr+=Scatter.scratch(gout.shape[3],gout.shape[4],gout.dtype)+PipeScatter.scratch(r_,feat)
    for p in parts: scr+=ScatterZ.scratch(p.shape[1],p.shape[2],p.dtype)
    return pl.pallas_call(
        functools.partial(backward_kernel,n,512),
        in_specs=[VM,VM,VM,VM,VM,VM,VM,VM,HBM]+[VM]*n,
        out_specs=[VM,HBM,VM,VM,VM]+[VM]*n,
        out_shape=outs,
        scratch_shapes=scr+sem_types(Swap.SEMS)+sem_types(Scatter.SEMS)+sem_types(PipeScatter.SEMS)+sem_types(ScatterZ.SEMS)*n,
        compiler_params=pltpu.CompilerParams(collective_id=2,has_side_effects=True,vmem_limit_bytes=63<<20),
        name="attn_bwd",
    )(proj,do,o,qm,km,lse_t,mix,lay,gout,*parts)


def spread(dst,src_ref,width,at):
    lane=lax.broadcasted_iota(jnp.int32,(1,128),1)
    for n in range(NDEV):
        lo=n*width
        c,off=lo//128,lo%128
        sh=(at-off)%128
        v=src_ref[:,c*128:(c+1)*128]
        v=pltpu.roll(v,sh,1) if sh else v
        if off+width>128:
            w=src_ref[:,(c+1)*128:(c+2)*128]
            w=pltpu.roll(w,sh,1) if sh else w
            v=jnp.where(lane<at+128-off,v,w)
        keep=(lane>=at)&(lane<at+width)
        i=(n//(NC*NR),(n//NR)%NC,n%NR)
        if at==0: dst[i]=jnp.where(keep,v,0.0)
        else: dst[i]=jnp.where(keep,v,dst[i])


def tail_kernel(side,cols,ta,tf,*refs):
    it=iter(refs)
    nx=lambda n:[next(it) for _ in range(n)]
    gproj,qkv,m1,x_ref,gmid,mod,tap_ref,ml_ref,mr_ref,rl_ref,sums,gkf,low,ada,zq,lastq=nx(16)
    tg_o,ctx_o,adag_o,gm_o,q_o,ql_o,tap_o=nx(7)
    G,gm1,tgb,tgin,ktap,gme,gml,gmev,gmlv,ctxs,ctxv,tpart=nx(12)
    zbufs=nx(1); lbufs=nx(5); tbufs=nx(5)
    take=taker(it)
    barrier_all()
    sz=ScatterZ(zq,q_o,zbufs,take(ScatterZ))
    slq=Scatter(lastq,ql_o,lbufs,take(Scatter))
    stp=Scatter(tpart,tap_o,tbufs,take(Scatter))
    st=Swap(tgb,tgin,take(Swap))
    ge=AllToAll(gme,gmev,take(AllToAll),one=True)
    gl=AllToAll(gml,gmlv,take(AllToAll),one=True)
    xa=AllToAll(ctxs,ctxv,take(AllToAll))
    slq.start(); sz.start()
    cells,feat=x_ref.shape
    L=feat//128
    for i,q in enumerate((3,1,2,0)):
        for l in range(L):
            gme[i*L+l:i*L+l+1,:]=sums[q:q+1,l*128:(l+1)*128].astype(BF)
    ge.start()
    CH=1024; EC=256
    def a(i):
        r=rows_of(i,CH)
        G[r,:]=dotf(gproj[r,:],qkv[...],NT).astype(BF).astype(F32)
    loop(cells//CH,a)
    slq.cstep()
    taps=tap_ref[...].astype(F32)
    for lane in range(L):
        ls=slice(lane*128,(lane+1)*128)
        def put(i,u):
            gm1[rows_of(i,cols),ls]=u
        acc=back_rows(G,m1,put,taps,ml_ref,mr_ref,rl_ref,lane,side,cols)
        for q in range(9):
            ktap[q:q+1,ls]=jnp.sum(acc[q],axis=0,keepdims=True)
    ktap[9:16,:]=jnp.zeros((7,feat),F32)
    spread(tpart,ktap,ta,0)
    spread(tpart,gkf,tf,ta)
    stp.start()
    slq.xstep()
    shift1=mod[0:1,:]; scale1=mod[1:2,:]
    z8=jnp.zeros((8,feat),F32)
    block=cells//NR
    c=(z8,z8)
    for t in (3,1,2,0):
        to=partner_xy(st.rows,t) if t else st.rows
        def body(i,c,to=to):
            ss,sc=c
            rl_=pl.ds(pl.multiple_of(i*EC,EC),EC)
            r=pl.ds(pl.multiple_of(to*block+i*EC,EC),EC)
            n,inv=normal_rows(x_ref[r,:].astype(F32))
            g=gm1[r,:]
            tgb[to,rl_,:]=(gmid[r,:]+normal_back_rows(g*(1.0+scale1),n,inv)).astype(BF)
            return ss+fold8(g),sc+fold8(g*n)
        c=lax.fori_loop(0,block//EC,body,c)
        if t: st.copy(t).start()
        else: st.local().start()
        if t==3: stp.cstep()
        if t==1: stp.xstep()
    for i,v in enumerate(c):
        v=jnp.sum(v,axis=0,keepdims=True)
        for l in range(L): gml[i*L+l:i*L+l+1,:]=v[:,l*128:(l+1)*128].astype(BF)
    gml[2*L:16,:]=jnp.zeros((16-2*L,128),BF)
    gl.start()
    me=gl.me
    feats=ada.shape[0]
    width=low.shape[1]
    pick=(lax.broadcasted_iota(jnp.int32,(width,feats),0)==lax.broadcasted_iota(jnp.int32,(width,feats),1)+feats*me).astype(BF)
    mine=jnp.dot(low[...],pick,preferred_element_type=F32).astype(BF)
    acc=jnp.zeros((NDEV,feats),F32)
    ge.wait()
    def use(src,n,base,acc):
        for i in range(n):
            g=src[:,i,:]
            j=base+i
            adag_o[:,j*128:(j+1)*128]=lax.dot_general(mine,g,TN,preferred_element_type=F32)
            gm_o[j:j+1,:]=jnp.sum(g.astype(F32),axis=0,keepdims=True)
            acc=acc+lax.dot_general(g,ada[:,j*128:(j+1)*128],NT,preferred_element_type=F32)
        return acc
    acc=use(gmev,4*L,2*L,acc)
    gl.wait()
    acc=use(gmlv,2*L,0,acc)
    for n in range(NDEV):
        g0=(n//NR)*NR
        ctxs[n,0:NR,0:feats]=acc[g0:g0+NR,:]
    xa.start()
    sz.step()
    slq.zstep()
    stp.zstep()
    st.wait()
    def up(i):
        for b in range(NR):
            tg_o[b,rows_of(i,EC),:]=tgin[b,rows_of(i,EC),:].astype(F32)
    loop(block//EC,up)
    xa.wait()
    ctx_o[...]=ctxv[...]
    for s in (sz,slq,stp,st,ge,gl,xa): s.finish()


def tail(gproj,qkv,m1,x,gmid,mod,taps,ml,mr,rl,sums,gkf,low,ada,zq,lastq,side,cols,ta,tf):
    cells,feat=x.shape
    block=cells//NR
    r_=feat//NDEV
    V=pltpu.VMEM
    L=feat//128
    outs=[S_((NR,block,feat),F32),S_((NDEV,8,128),F32),S_(ada.shape,F32),S_((6*L,128),F32),S_(zq.shape[1:],F32),S_(lastq.shape[3:],F32),S_((16,128),F32)]
    scr=[V((cells,feat),F32),V((cells,feat),F32),V((NR,block,feat),BF),V((NR,block,feat),BF),V((16,feat),F32),
         V((4*L,128),BF),V((16,128),BF),V((NDEV,4*L,128),BF),V((NDEV,16,128),BF),V((NDEV,8,128),F32),V((NDEV,8,128),F32),V((NZ,NC,NR,16,128),F32)]
    scr+=ScatterZ.scratch(r_,zq.shape[2],BF)+Scatter.scratch(r_,feat,BF)+Scatter.scratch(16,128,F32)
    sems=sem_types(ScatterZ.SEMS)+sem_types(Scatter.SEMS)*2+sem_types(Swap.SEMS)+sem_types(AllToAll.SEMS)*3
    return pl.pallas_call(
        functools.partial(tail_kernel,side,cols,ta,tf),
        in_specs=[VM]*9+[SM]+[VM]*6,
        out_specs=[VM]*7,
        out_shape=outs,
        scratch_shapes=scr+sems,
        compiler_params=pltpu.CompilerParams(collective_id=3,has_side_effects=True,vmem_limit_bytes=63<<20),
        name="tail",
    )(gproj,qkv,m1,x,gmid,mod,taps,ml,mr,rl,sums,gkf,low,ada,zq,lastq)


def greet(targets):
    bar=pltpu.get_barrier_semaphore()
    for d in targets:
        pl.semaphore_signal(bar,inc=1,device_id=d,device_id_type=MESH)
    pl.semaphore_wait(bar,len(targets))


def near():
    z,core,rows=here()
    return [dev(z,1-core,rows)]+[dev(z,core,partner_xy(rows,t)) for t in range(1,NR)]


class PipeScatter:
    SEMS=[(2,),(2,),(2,NR),(2,NR)]
    @staticmethod
    def scratch(r,c):
        return [pltpu.VMEM((2,NZ,NC,NR,r,c),BF),pltpu.VMEM((2,NZ,NR,r,c),BF),pltpu.VMEM((2,NZ,NR,r,c),BF),pltpu.VMEM((2,NR,NZ,r,c),BF)]
    def __init__(self,bufs,sems):
        self.part,self.sib,self.own,self.xin=bufs
        self.sc,self.rc,self.sx,self.rx=sems
        self.z,self.core,self.rows=here()
    def ccopy(self,s):
        return rcopy(self.part.at[s,:,1-self.core],self.sib.at[s],self.sc.at[s],self.rc.at[s],dev(self.z,1-self.core,self.rows))
    def xcopy(self,s,t):
        to=partner_xy(self.rows,t)
        return rcopy(self.own.at[s,:,to],self.xin.at[s,t],self.sx.at[s,t],self.rx.at[s,t],dev(self.z,self.core,to))
    def send_core(self,s):
        self.ccopy(s).start()
    def send_square(self,s):
        self.ccopy(s).wait()
        def body(i):
            a,b=i//NR,lax.rem(i,NR)
            self.own[s,a,b]=(self.part[s,a,self.core,b].astype(F32)+self.sib[s,a,b].astype(F32)).astype(BF)
        loop(NZ*NR,body)
        for t in range(1,NR): self.xcopy(s,t).start()
    def collect(self,s,put):
        for t in range(1,NR): self.xcopy(s,t).wait()
        def body(a):
            v=self.own[s,a,self.rows].astype(F32)
            for t in range(1,NR): v=v+self.xin[s,t,a].astype(F32)
            put(a,v.astype(BF))
        loop(NZ,body)


class RowScatter:
    SEMS=[(2,),(2,),(2,NR),(2,NR)]
    @staticmethod
    def scratch(r,c):
        return [pltpu.VMEM((2,NR,r,c),BF),pltpu.VMEM((2,NR,r,c),BF),pltpu.VMEM((2,NR,r,c),BF)]
    def __init__(self,part,zout,bufs,sems):
        self.part,self.zout=part,zout
        self.sib,self.own,self.xin=bufs
        self.sc,self.rc,self.sx,self.rx=sems
        self.z,self.core,self.rows=here()
    def ccopy(self,k):
        s=k%2
        return rcopy(self.part.at[k,1-self.core],self.sib.at[s],self.sc.at[s],self.rc.at[s],dev(self.z,1-self.core,self.rows))
    def xcopy(self,k,t):
        s=k%2
        to=partner_xy(self.rows,t)
        return rcopy(self.own.at[s,to],self.xin.at[s,t],self.sx.at[s,t],self.rx.at[s,t],dev(self.z,self.core,to))
    def send_core(self,k):
        self.ccopy(k).start()
    def send_square(self,k):
        self.ccopy(k).wait()
        s=k%2
        def body(b):
            self.own[s,b]=(self.part[k,self.core,b].astype(F32)+self.sib[s,b].astype(F32)).astype(BF)
        loop(NR,body)
        for t in range(1,NR): self.xcopy(k,t).start()
    def collect(self,k):
        s=k%2
        for t in range(1,NR): self.xcopy(k,t).wait()
        v=self.own[s,self.rows].astype(F32)
        for t in range(1,NR): v=v+self.xin[s,t].astype(F32)
        self.zout[k]=v.astype(BF)


def ffn_kernel_body(*refs,side,cols):
    it=iter(refs)
    nx=lambda n:[next(it) for _ in range(n)]
    x_ref,att_ref,cot_ref,mod_ref,outw_ref,up_ref,zpd,tap_ref,ml_ref,mr_ref,rl_ref=nx(11)
    lay_ref,gmid_ref,gatt_ref,gout_ref,zup,zdown,gtap_ref,sums_ref=nx(8)
    m2,m2t,gffn,branch,middle,fb,gm2,F,G,glow,gub,dfull,gd=nx(13)
    ubufs=nx(4); dbufs=nx(3)
    take=taker(it)
    ga=GatherXY(zpd,dfull,take(GatherXY))
    us=PipeScatter(ubufs,take(PipeScatter))
    ds=RowScatter(gd,zdown,dbufs,take(RowScatter))
    t=pl.program_id(0)
    cells,feat=x_ref.shape
    T=up_ref.shape[1]
    hidden=NDEV*zpd.shape[1]
    steps=hidden//T; last=steps-1
    block=hidden//NZ
    CH=1024; EC=256
    shift2=mod_ref[3:4,:]; scale2=mod_ref[4:5,:]; gate2=mod_ref[5:6,:]; gate1=mod_ref[2:3,:]
    slot=lax.rem(t,2); other=lax.rem(t+1,2)
    ready={}
    for k in range(NZ): ready[k]=-(-((k+1)*block)//T)-1
    need={}
    for k in range(NZ): need[k]=(k*block)//T
    def put_up(tile):
        def put(a,v): zup[a,:,pl.ds(pl.multiple_of(tile*T,128),T)]=v
        return put

    @pl.when(t==0)
    def _():
        greet(near())
        ga.start(); ga.start_local()
        def a(i):
            branch[rows_of(i,CH),:]=dotf(att_ref[rows_of(i,CH),:],outw_ref[...])
        loop(cells//CH,a)
        def b(i):
            r=rows_of(i,EC)
            mid=x_ref[r,:].astype(F32)+gate1*branch[r,:]
            middle[r,:]=mid
            n,_=normal_rows(mid)
            m2[r,:]=(n*(1.0+scale2)+shift2).astype(BF)
            gffn[r,:]=(gate2*cot_ref[r,:].astype(F32)).astype(BF)
        loop(cells//EC,b)
        ga.step(0)
        def c(i):
            r=rows_of(i,CH)
            m2t[:,pl.ds(pl.multiple_of(i*CH,CH),CH)]=jnp.transpose(m2[r,:])
            fb[r,:]=jnp.zeros((CH,feat),F32)
            gm2[r,:]=jnp.zeros((CH,feat),F32)
        loop(cells//CH,c)
        ga.local().wait()
    for k in range(NZ):
        @pl.when(t==need[k])
        def _(k=k):
            if k: ga.step(k)
            ga.arrive(k)
    @pl.when(t>=2)
    def _():
        us.collect(slot,put_up(t-2))
    for k in range(NZ):
        if ready[k]+2<=last:
            @pl.when(t==ready[k]+2)
            def _(k=k): ds.collect(k)

    dw=dfull.reshape(hidden,feat)
    gdw=gd.reshape(hidden,feat)
    tr=pl.ds(pl.multiple_of(t*T,T),T)
    def first(i):
        r=rows_of(i,CH)
        F[r,:]=dotf(m2[r,:],up_ref[...]).astype(BF).astype(F32)
        G[r,:]=dotf(gffn[r,:],dw[tr,:],NT)
    loop(cells//CH,first)

    taps=tap_ref[...].astype(F32)
    for lane in range(T//128):
        ls=slice(lane*128,(lane+1)*128)
        def put(i,u):
            r=rows_of(i,cols)
            u2=u*u
            th=jnp.tanh(C0*(u+C1*(u2*u)))
            half=0.5*(1.0+th)
            glow[r,ls]=(u*half).astype(BF)
            d=half+(0.5*u)*(1.0-th*th)*(C0*(1.0+(3.0*C1)*u2))
            G[r,ls]=(G[r,ls]*d).astype(BF).astype(F32)
        conv_rows(F,put,taps,ml_ref,mr_ref,rl_ref,lane,side,cols)
    @pl.when(t>=1)
    def _():
        us.send_square(other)
    for k in range(NZ):
        if ready[k]+1<=last:
            @pl.when(t==ready[k]+1)
            def _(k=k): ds.send_square(k)
    for lane in range(T//128):
        ls=slice(lane*128,(lane+1)*128)
        def put2(i,u):
            gub[rows_of(i,cols),ls]=u.astype(BF)
        acc=back_rows(G,F,put2,taps,ml_ref,mr_ref,rl_ref,lane,side,cols)
        for q in range(9):
            gtap_ref[q:q+1,ls]=jnp.sum(acc[q],axis=0,keepdims=True)
    gtap_ref[9:16,:]=jnp.zeros((7,T),F32)

    r_=feat//NDEV
    def third(i):
        n=NC*NR*r_
        us.part[slot,i]=dotf(m2t[rows_of(i,n),:],gub[...]).astype(BF).reshape(NC,NR,r_,T)
    loop(NZ,third)
    us.send_core(slot)
    for i in range(T//256):
        gdw[pl.ds(pl.multiple_of(t*T+i*256,256),256),:]=dotf(glow[:,i*256:(i+1)*256],gffn[...],TN).astype(BF)
    for k in range(NZ):
        @pl.when(t==ready[k])
        def _(k=k): ds.send_core(k)
    def second(i):
        r=rows_of(i,CH)
        fb[r,:]+=dotf(glow[r,:],dw[tr,:])
        gm2[r,:]+=dotf(gub[r,:],up_ref[...],NT)
    loop(cells//CH,second)

    @pl.when(t==last)
    def _():
        us.collect(other,put_up(last-1))
        late=[k for k in range(NZ) if ready[k]+1>last]
        mid_=[k for k in range(NZ) if ready[k]+1==last]
        for k in mid_: ds.collect(k)
        us.send_square(slot)
        for k in late: ds.send_square(k)
        z=jnp.zeros((8,feat),F32)
        def body(i,c):
            sg2,ss2,sc2,sg1=c
            r=rows_of(i,EC)
            inc=cot_ref[r,:].astype(F32)
            mid=middle[r,:]
            n,inv=normal_rows(mid)
            lay_ref[r,:]=(mid+gate2*fb[r,:]).astype(BF)
            gm=gm2[r,:]
            gmid=inc+normal_back_rows(gm*(1.0+scale2),n,inv)
            gmid_ref[r,:]=gmid
            gffn[r,:]=(gate1*gmid).astype(BF)
            return (sg2+fold8(inc*fb[r,:]),ss2+fold8(gm),sc2+fold8(gm*n),sg1+fold8(gmid*branch[r,:]))
        res=lax.fori_loop(0,cells//EC,body,(z,z,z,z))
        for q in range(4):
            sums_ref[q:q+1,:]=jnp.sum(res[q],axis=0,keepdims=True)
        sums_ref[4:8,:]=jnp.zeros((4,feat),F32)
        def b(i):
            r=rows_of(i,CH)
            gatt_ref[r,:]=dotf(gffn[r,:],outw_ref[...],NT).astype(BF)
        loop(cells//CH,b)
        for i in range(feat//256):
            gout_ref[i*256:(i+1)*256,:]=dotf(att_ref[:,i*256:(i+1)*256],gffn[...],TN).astype(BF)
        us.collect(slot,put_up(last))
        for k in late: ds.collect(k)
        ga.finish_remote()


def ffn(x,att,cot,mod6,outw,up,zpd,taps,ml,mr,rl,side,cols,T=512):
    cells,feat=x.shape
    hidden=up.shape[1]
    vm=lambda shape: pl.BlockSpec(shape,lambda t:(0,)*len(shape),pipeline_mode=pl.Buffered(1))
    r_,d_=feat//NDEV,hidden//NDEV
    return pl.pallas_call(
        functools.partial(ffn_kernel_body,side=side,cols=cols),
        grid=(hidden//T,),
        in_specs=[vm((cells,feat)),vm((cells,feat)),vm((cells,feat)),vm((8,feat)),vm((feat,feat)),
                  pl.BlockSpec((feat,T),lambda t:(0,t)),HBM,pl.BlockSpec((16,T),lambda t:(0,t)),
                  vm((cells,128)),vm((cells,128)),SM],
        out_specs=[vm((cells,feat)),vm((cells,feat)),vm((cells,feat)),vm((feat,feat)),
                   vm((NZ,r_,hidden)),vm((NZ,d_,feat)),pl.BlockSpec((16,T),lambda t:(0,t)),vm((8,feat))],
        out_shape=[S_((cells,feat),BF),S_((cells,feat),F32),S_((cells,feat),BF),S_((feat,feat),BF),S_((NZ,r_,hidden),BF),S_((NZ,d_,feat),BF),S_((16,hidden),F32),S_((8,feat),F32)],
        scratch_shapes=[pltpu.VMEM((cells,feat),BF),pltpu.VMEM((feat,cells),BF),pltpu.VMEM((cells,feat),BF),
                        pltpu.VMEM((cells,feat),F32),pltpu.VMEM((cells,feat),F32),pltpu.VMEM((cells,feat),F32),pltpu.VMEM((cells,feat),F32),
                        pltpu.VMEM((cells,T),F32),pltpu.VMEM((cells,T),F32),pltpu.VMEM((cells,T),BF),pltpu.VMEM((cells,T),BF),
                        pltpu.VMEM((NZ,NC,NR,d_,feat),BF),pltpu.VMEM((NZ,NC,NR,d_,feat),BF)]
                       +PipeScatter.scratch(r_,T)+RowScatter.scratch(d_,feat)
                       +sem_types(GatherXY.SEMS)+sem_types(PipeScatter.SEMS)+sem_types(RowScatter.SEMS),
        compiler_params=pltpu.CompilerParams(dimension_semantics=("arbitrary",),vmem_limit_bytes=63<<20,collective_id=4,has_side_effects=True),
        name="ffn",
    )(x,att,cot,mod6,outw,up,zpd,taps,ml,mr,rl)
def own_rows(padded_cells):
    return jnp.pad(padded_cells,((0,0),(1,1),(1,1),(0,0)))


def fast(tokens,conditioning,item_map,ada_weight,ada_bias,attn_kernel,qkv_weight,out_weight,up_weight,ffn_kernel,down_weight,out_cotangent):
    canvases,rows_here,cols,features=tokens.shape
    side=rows_here*NR
    cells=side*cols
    rows=lax.axis_index("rows"); dp=lax.axis_index("dp"); me=dp*NR+rows
    hidden=up_weight.shape[1]
    cond_row=jnp.pad(lax.dynamic_slice_in_dim(conditioning,rows,1,0),((0,7),(0,0)))
    mod_cols=ada_weight.shape[1]
    bshard=ada_bias.shape[0]
    bias_rows=lax.dynamic_update_slice_in_dim(jnp.zeros((mod_cols,),F32),ada_bias.astype(F32),me*bshard,0).reshape(mod_cols//128,128)
    ta,tf=attn_kernel.shape[1],ffn_kernel.shape[1]
    taps=jnp.pad(jnp.concatenate([attn_kernel,ffn_kernel],axis=1),((0,7),(0,128-ta-tf)))
    blocks=(NR,rows_here*cols,features)
    tok,low_all,mod,qkv_f,taps_f,*zps=enter(tokens.reshape(blocks),cond_row,ada_weight,bias_rows,qkv_weight,taps,[out_weight,up_weight])
    full2=lambda a:a.reshape(-1,a.shape[-1])
    triple_full=full2(qkv_f)
    taps_f=taps_f.reshape(NDEV,16,128)[:,:9]
    kernel_attn=taps_f[:,:,:ta].transpose(1,0,2).reshape(9,features)
    kernel_ffn=taps_f[:,:,ta:ta+tf].transpose(1,0,2).reshape(9,hidden)
    labels=lax.dynamic_slice_in_dim(item_map,rows,1,0)
    labels_pad=jnp.pad(labels,((0,0),(1,1),(1,1)),constant_values=-1)
    qm,km=head_masks(labels.reshape(cells))
    ml,mr,rl=link_masks(labels[0])
    mod6=mod.reshape(6,features)
    shift1,scale1,gate1,shift2,scale2,gate2=(mod6[i][None,None,None] for i in range(6))
    x=tok.reshape(1,side,cols,features).astype(F32)
    n1,i1=normalize(x)
    m1=(n1*(1.0+scale1)+shift1).astype(BF)
    m1p=own_rows(m1)
    mix=conv_forward(m1p,labels_pad,labels,kernel_attn).astype(BF).reshape(cells,features)
    proj,attended,lse_t,cot,zp_down,out_f,up_f=forward(mix,triple_full,qm,km,out_cotangent.reshape(blocks),down_weight,zps)
    lay,gmid,gatt,g_out,z_up,z_down,g_kffn,sums=ffn(
        tok.reshape(cells,features),attended,cot.reshape(cells,features),jnp.pad(mod6,((0,2),(0,0))),
        full2(out_f),full2(up_f),zp_down,jnp.pad(kernel_ffn,((0,7),(0,0))),ml,mr,rl,side,cols)
    sp=lambda g:g.reshape(NZ,NC,NR,g.shape[0]//NDEV,g.shape[1])
    gproj,lay_o,o_o,zq,lastq,u_o,d_o=backward(proj,gatt,attended,qm,km,lse_t,mix,lay.reshape(blocks),sp(g_out),[z_up,z_down])
    tg,ctx,adag,gmsum,q_a,q_b,t_o=tail(gproj,triple_full,m1.reshape(cells,features),tok.reshape(cells,features),gmid,jnp.pad(mod6,((0,2),(0,0))),
        jnp.pad(kernel_attn,((0,7),(0,0))),ml,mr,rl,sums,g_kffn,low_all,ada_weight,zq,lastq,side,cols,ta,tf)
    w=features//3
    q_o=jnp.concatenate([part for s in range(3) for part in (q_a[:,2*s*w:2*(s+1)*w],q_b[:,s*w:(s+1)*w])],axis=1)
    shape4=(NR,rows_here,cols,features)
    feats=ada_weight.shape[0]
    dsilu=ctx[:,:NR,:feats].transpose(1,0,2).reshape(NR,features)
    cv=conditioning.astype(F32)
    _,sback=jax.vjp(jax.nn.silu,cv)
    dctx=sback(dsilu)[0]
    gbias=lax.dynamic_slice_in_dim(gmsum.reshape(mod_cols),me*bshard,bshard,0)
    return (lay_o.reshape(shape4),tg.reshape(shape4),dctx,adag,gbias,t_o[:9,:ta],q_o,o_o,u_o,t_o[:9,ta:ta+tf],d_o)


def solution(mesh):
    quick=dict(mesh.shape)=={"dp":NZ*NC,"rows":NR}
    return jax.shard_map(
        fast if quick else local,
        mesh=mesh,
        in_specs=(
            P("dp", "rows", None, None),
            P("dp", None),
            P("dp", None, None),
            P(("dp", "rows"), None),
            P(("dp", "rows")),
            P(None, ("dp", "rows")),
            P(("dp", "rows"), None),
            P(("dp", "rows"), None),
            P(("dp", "rows"), None),
            P(None, ("dp", "rows")),
            P(("dp", "rows"), None),
            P("dp", "rows", None, None),
        ),
        out_specs=(
            P("dp", "rows", None, None),
            P("dp", "rows", None, None),
            P("dp", None),
            P(("dp", "rows"), None),
            P(("dp", "rows")),
            P(None, ("dp", "rows")),
            P(("dp", "rows"), None),
            P(("dp", "rows"), None),
            P(("dp", "rows"), None),
            P(None, ("dp", "rows")),
            P(("dp", "rows"), None),
        ),
        check_vma=False,
    )
```

```python
import functools

import jax
import jax.numpy as jnp
from jax import lax
from jax.experimental import pallas as pl
from jax.experimental.pallas import tpu as pltpu
from jax.sharding import PartitionSpec as P

PER_GROUP_WIDTH = 64


EPSILON = 1e-06


def padded(block, sides, width):
    for axis, dim in sides:
        count = lax.axis_size(axis)
        forward = [(i, i + 1) for i in range(count - 1)]
        backward = [(target, source) for source, target in forward]
        low = lax.ppermute(
            lax.slice_in_dim(block, block.shape[dim] - width, None, axis=dim), axis, forward
        )
        high = lax.ppermute(lax.slice_in_dim(block, 0, width, axis=dim), axis, backward)
        block = jnp.concatenate([low, block, high], axis=dim)
    return block


def normalize(attended_content_array):
    average = jnp.mean(attended_content_array, axis=-1, keepdims=True)
    centred = attended_content_array - average
    inverse = lax.rsqrt(jnp.mean(centred * centred, axis=-1, keepdims=True) + EPSILON)
    return (centred * inverse, inverse)


def normalize_back(incoming, normalized_rows, inverse):
    return inverse * (
        incoming
        - jnp.mean(incoming, axis=-1, keepdims=True)
        - normalized_rows * jnp.mean(incoming * normalized_rows, axis=-1, keepdims=True)
    )


def widen_cols(rimmed):
    return jnp.pad(rimmed, ((0, 0), (0, 0), (1, 1), (0, 0)))


def tap_mask(labels_pad, centre, row_off, col_off):
    rows_here = centre.shape[1]
    cols_here = centre.shape[2]
    return (labels_pad[:, row_off : row_off + rows_here, col_off : col_off + cols_here] == centre)[
        ..., None
    ]


def conv_forward(padded_rows, labels_pad, centre, kernel):
    rows_here = centre.shape[1]
    cols_here = centre.shape[2]
    summed = jnp.zeros(centre.shape + (kernel.shape[1],), jnp.float32)
    for row_off in range(3):
        for col_off in range(3):
            window = padded_rows[
                :, row_off : row_off + rows_here, col_off : col_off + cols_here
            ].astype(jnp.float32)
            tapped = kernel[3 * row_off + col_off].astype(jnp.float32) * window
            summed = summed + jnp.where(tap_mask(labels_pad, centre, row_off, col_off), tapped, 0.0)
    return summed


def conv_mirror(padded_rows, labels_pad, centre, kernel):
    rows_here = centre.shape[1]
    cols_here = centre.shape[2]
    summed = jnp.zeros(centre.shape + (kernel.shape[1],), jnp.float32)
    for row_off in range(3):
        for col_off in range(3):
            row_from = 2 - row_off
            col_from = 2 - col_off
            window = padded_rows[
                :, row_from : row_from + rows_here, col_from : col_from + cols_here
            ].astype(jnp.float32)
            tapped = kernel[3 * row_off + col_off].astype(jnp.float32) * window
            summed = summed + jnp.where(
                tap_mask(labels_pad, centre, row_from, col_from), tapped, 0.0
            )
    return summed


def kernel_grad(incoming, padded_rows, labels_pad, centre):
    rows_here = centre.shape[1]
    cols_here = centre.shape[2]
    incoming_values = incoming.astype(jnp.float32)
    tap_sums = []
    for row_off in range(3):
        for col_off in range(3):
            window = padded_rows[
                :, row_off : row_off + rows_here, col_off : col_off + cols_here
            ].astype(jnp.float32)
            product = jnp.where(
                tap_mask(labels_pad, centre, row_off, col_off), incoming_values * window, 0.0
            )
            tap_sums.append(jnp.sum(product, axis=(0, 1, 2)))
    return jnp.stack(tap_sums, axis=0)


def contract_rows(left, right):
    return lax.dot_general(
        left, right, (((0,), (0,)), ((), ())), preferred_element_type=jnp.float32
    )


def contract_cols(left, right):
    return lax.dot_general(
        left, right, (((1,), (1,)), ((), ())), preferred_element_type=jnp.float32
    )


def local(
    tokens,
    conditioning,
    item_map,
    ada_weight,
    ada_bias,
    attn_kernel,
    qkv_weight,
    out_weight,
    up_weight,
    ffn_kernel,
    down_weight,
    out_cotangent,
):
    canvases, rows_here, cols_here, features = tokens.shape
    cell_count = canvases * rows_here * cols_here
    position = lax.axis_index("rows")
    gathered = (
        lax.all_gather(ada_weight, ("dp", "rows"), axis=0, tiled=True),
        lax.all_gather(ada_bias, ("dp", "rows"), axis=0, tiled=True),
        lax.all_gather(attn_kernel, ("dp", "rows"), axis=1, tiled=True),
        lax.all_gather(qkv_weight, ("dp", "rows"), axis=0, tiled=True),
        lax.all_gather(out_weight, ("dp", "rows"), axis=0, tiled=True),
        lax.all_gather(up_weight, ("dp", "rows"), axis=0, tiled=True),
        lax.all_gather(ffn_kernel, ("dp", "rows"), axis=1, tiled=True),
        lax.all_gather(down_weight, ("dp", "rows"), axis=0, tiled=True),
    )
    ada_full, bias_full, kernel_attn, triple_full, out_full, up_full, kernel_ffn, down_full = (
        gathered
    )
    hidden_units = up_full.shape[1]
    head_count = features // PER_GROUP_WIDTH
    logit_divisor = PER_GROUP_WIDTH ** (-0.5)
    labels_pad = jnp.pad(item_map, ((0, 0), (1, 1), (1, 1)), constant_values=-1)
    labels_here = lax.dynamic_slice_in_dim(labels_pad, position * rows_here, rows_here + 2, 1)
    centre = labels_here[:, 1:-1, 1:-1]
    cond_values = conditioning.astype(jnp.float32)
    silu_low = jax.nn.silu(cond_values).astype(jnp.bfloat16)
    modulation = jnp.dot(silu_low, ada_full, preferred_element_type=jnp.float32) + bias_full.astype(
        jnp.float32
    )
    layer_stack = modulation.reshape(canvases, 6, 1, 1, features)
    shift_one, scale_one, gate_one, shift_two, scale_two, gate_two = (
        layer_stack[:, index] for index in range(6)
    )
    token_values = tokens.astype(jnp.float32)
    normed_one, inverse_one = normalize(token_values)
    modulated_one = (normed_one * (1.0 + scale_one) + shift_one).astype(jnp.bfloat16)
    modulated_padded = widen_cols(padded(modulated_one, (("rows", 1),), 1))
    local_mix = conv_forward(modulated_padded, labels_here, centre, kernel_attn).astype(
        jnp.bfloat16
    )
    mix_rows = local_mix.reshape(cell_count, features)
    projected = jnp.dot(mix_rows, triple_full, preferred_element_type=jnp.float32).astype(
        jnp.bfloat16
    )
    projected = projected.reshape(canvases, rows_here * cols_here, 3 * features)
    queries = projected[..., :features]
    key_rows = projected[..., features : 2 * features]
    value_rows = projected[..., 2 * features :]
    keys_all, values_all = (
        lax.all_gather(key_rows, "rows", axis=1, tiled=True),
        lax.all_gather(value_rows, "rows", axis=1, tiled=True),
    )
    query_heads = queries.reshape(canvases, -1, head_count, PER_GROUP_WIDTH)
    key_heads = keys_all.reshape(canvases, -1, head_count, PER_GROUP_WIDTH)
    value_heads = values_all.reshape(canvases, -1, head_count, PER_GROUP_WIDTH)
    scores = (
        jnp.einsum("bqhd,bkhd->bhqk", query_heads, key_heads, preferred_element_type=jnp.float32)
        * logit_divisor
    )
    label_rows = centre.reshape(canvases, -1)
    label_keys = item_map.reshape(canvases, -1)
    linked = label_rows[:, None, :, None] == label_keys[:, None, None, :]
    masked = jnp.where(linked, scores, -1e30)
    row_peak = jnp.max(masked, axis=-1, keepdims=True)
    raised = jnp.exp(masked - row_peak)
    row_total = jnp.sum(raised, axis=-1, keepdims=True)
    attention = raised / row_total
    attention_low = attention.astype(jnp.bfloat16)
    attended = jnp.einsum(
        "bhqk,bkhd->bqhd", attention_low, value_heads, preferred_element_type=jnp.float32
    ).astype(jnp.bfloat16)
    attended = attended.reshape(cell_count, features)
    attn_branch = jnp.dot(attended, out_full, preferred_element_type=jnp.float32).reshape(
        tokens.shape
    )
    middle = token_values + gate_one * attn_branch
    normed_two, inverse_two = normalize(middle)
    modulated_two = (normed_two * (1.0 + scale_two) + shift_two).astype(jnp.bfloat16)
    modulated_rows = modulated_two.reshape(cell_count, features)
    hidden_up_projection = jnp.dot(
        modulated_rows, up_full, preferred_element_type=jnp.float32
    ).astype(jnp.bfloat16)
    hidden_up_projection = hidden_up_projection.reshape(
        canvases, rows_here, cols_here, hidden_units
    )
    up_padded = widen_cols(padded(hidden_up_projection, (("rows", 1),), 1))
    pre_gelu = conv_forward(up_padded, labels_here, centre, kernel_ffn)
    activated, gelu_back = jax.vjp(jax.nn.gelu, pre_gelu)
    gelu_low = activated.astype(jnp.bfloat16).reshape(cell_count, hidden_units)
    ffn_branch = jnp.dot(gelu_low, down_full, preferred_element_type=jnp.float32).reshape(
        tokens.shape
    )
    layer_out = (middle + gate_two * ffn_branch).astype(jnp.bfloat16)
    weights_back = (
        lax.all_gather(ada_weight, ("dp", "rows"), axis=0, tiled=True),
        lax.all_gather(ada_bias, ("dp", "rows"), axis=0, tiled=True),
        lax.all_gather(attn_kernel, ("dp", "rows"), axis=1, tiled=True),
        lax.all_gather(qkv_weight, ("dp", "rows"), axis=0, tiled=True),
        lax.all_gather(out_weight, ("dp", "rows"), axis=0, tiled=True),
        lax.all_gather(up_weight, ("dp", "rows"), axis=0, tiled=True),
        lax.all_gather(ffn_kernel, ("dp", "rows"), axis=1, tiled=True),
        lax.all_gather(down_weight, ("dp", "rows"), axis=0, tiled=True),
    )
    (
        ada_back,
        bias_back,
        kernel_attn_back,
        triple_back,
        out_back,
        up_back,
        kernel_ffn_back,
        down_projection_back,
    ) = weights_back
    incoming = out_cotangent.astype(jnp.float32)
    grad_gate_two = jnp.sum(incoming * ffn_branch, axis=(1, 2))
    grad_ffn = (gate_two * incoming).astype(jnp.bfloat16).reshape(cell_count, features)
    grad_down = contract_rows(gelu_low, grad_ffn)
    grad_gelu = contract_cols(grad_ffn, down_projection_back).reshape(
        canvases, rows_here, cols_here, hidden_units
    )
    grad_pre = gelu_back(grad_gelu)[0].astype(jnp.bfloat16)
    grad_pre_padded = widen_cols(padded(grad_pre, (("rows", 1),), 1))
    grad_kernel_ffn = kernel_grad(grad_pre, up_padded, labels_here, centre)
    grad_up = (
        conv_mirror(grad_pre_padded, labels_here, centre, kernel_ffn_back)
        .astype(jnp.bfloat16)
        .reshape(cell_count, hidden_units)
    )
    grad_up_weight = contract_rows(modulated_rows, grad_up)
    grad_mod_two = contract_cols(grad_up, up_back).reshape(tokens.shape)
    grad_scale_two = jnp.sum(grad_mod_two * normed_two, axis=(1, 2))
    grad_shift_two = jnp.sum(grad_mod_two, axis=(1, 2))
    grad_middle = incoming + normalize_back(
        grad_mod_two * (1.0 + scale_two), normed_two, inverse_two
    )
    grad_gate_one = jnp.sum(grad_middle * attn_branch, axis=(1, 2))
    grad_attn = (gate_one * grad_middle).astype(jnp.bfloat16).reshape(cell_count, features)
    grad_out_weight = contract_rows(attended, grad_attn)
    grad_attended = (
        contract_cols(grad_attn, out_back)
        .astype(jnp.bfloat16)
        .reshape(canvases, -1, head_count, PER_GROUP_WIDTH)
    )
    grad_weights = jnp.einsum(
        "bqhd,bkhd->bhqk", grad_attended, value_heads, preferred_element_type=jnp.float32
    )
    row_delta = jnp.sum(attention * grad_weights, axis=-1, keepdims=True)
    grad_scores = (attention * (grad_weights - row_delta)).astype(jnp.bfloat16)
    grad_query = (
        jnp.einsum("bhqk,bkhd->bqhd", grad_scores, key_heads, preferred_element_type=jnp.float32)
        * logit_divisor
    )
    grad_key_all = (
        jnp.einsum("bhqk,bqhd->bkhd", grad_scores, query_heads, preferred_element_type=jnp.float32)
        * logit_divisor
    )
    value_gradient_full = jnp.einsum(
        "bhqk,bqhd->bkhd", attention_low, grad_attended, preferred_element_type=jnp.float32
    )
    grad_key, grad_value = (
        lax.psum_scatter(
            grad_key_all.reshape(canvases, -1, features).astype(jnp.bfloat16),
            "rows",
            scatter_dimension=1,
            tiled=True,
        ).astype(jnp.float32),
        lax.psum_scatter(
            value_gradient_full.reshape(canvases, -1, features).astype(jnp.bfloat16),
            "rows",
            scatter_dimension=1,
            tiled=True,
        ).astype(jnp.float32),
    )
    grad_projected = jnp.concatenate(
        [
            grad_query.reshape(cell_count, features),
            grad_key.reshape(cell_count, features),
            grad_value.reshape(cell_count, features),
        ],
        axis=-1,
    ).astype(jnp.bfloat16)
    grad_qkv_weight = contract_rows(mix_rows, grad_projected)
    grad_mix = contract_cols(grad_projected, triple_back).astype(jnp.bfloat16).reshape(tokens.shape)
    grad_mix_padded = widen_cols(padded(grad_mix, (("rows", 1),), 1))
    grad_kernel_attn = kernel_grad(grad_mix, modulated_padded, labels_here, centre)
    grad_mod_one = conv_mirror(grad_mix_padded, labels_here, centre, kernel_attn_back)
    grad_scale_one = jnp.sum(grad_mod_one * normed_one, axis=(1, 2))
    grad_shift_one = jnp.sum(grad_mod_one, axis=(1, 2))
    token_grad = grad_middle + normalize_back(
        grad_mod_one * (1.0 + scale_one), normed_one, inverse_one
    )
    grad_parts = jnp.concatenate(
        [
            grad_shift_one,
            grad_scale_one,
            grad_gate_one,
            grad_shift_two,
            grad_scale_two,
            grad_gate_two,
        ],
        axis=-1,
    )
    grad_modulation = lax.psum(grad_parts.astype(jnp.bfloat16), "rows")
    leader = (position == 0).astype(jnp.float32)
    grad_ada_weight = contract_rows(silu_low, grad_modulation) * leader
    grad_ada_bias = jnp.sum(grad_modulation.astype(jnp.float32), axis=0) * leader
    silu_values, silu_back = jax.vjp(jax.nn.silu, cond_values)
    derivative_of_context = silu_back(contract_cols(grad_modulation, ada_back))[0]
    summed_grads = (
        lax.psum_scatter(grad_ada_weight, ("dp", "rows"), scatter_dimension=0, tiled=True),
        lax.psum_scatter(grad_ada_bias, ("dp", "rows"), scatter_dimension=0, tiled=True),
        lax.psum_scatter(grad_kernel_attn, ("dp", "rows"), scatter_dimension=1, tiled=True),
        lax.psum_scatter(grad_qkv_weight, ("dp", "rows"), scatter_dimension=0, tiled=True),
        lax.psum_scatter(grad_out_weight, ("dp", "rows"), scatter_dimension=0, tiled=True),
        lax.psum_scatter(grad_up_weight, ("dp", "rows"), scatter_dimension=0, tiled=True),
        lax.psum_scatter(grad_kernel_ffn, ("dp", "rows"), scatter_dimension=1, tiled=True),
        lax.psum_scatter(grad_down, ("dp", "rows"), scatter_dimension=0, tiled=True),
    )
    return (layer_out, token_grad, derivative_of_context) + tuple(summed_grads)


F32=jnp.float32; BF=jnp.bfloat16
NT=(((1,),(1,)),((),()))
TN=(((0,),(0,)),((),()))

def head_masks(labels):
    cells=labels.shape[0]
    lane=lax.broadcasted_iota(jnp.int32,(cells,128),1)%64
    lab=labels[:,None]
    qm=(lane==lab).astype(BF)
    km=jnp.where((lane!=lab)&(lane<4),-1e30,0.0).astype(BF)
    return qm,km

MESH=pl.DeviceIdType.MESH
NZ,NC,NR=4,2,4


def here():
    dp=lax.axis_index("dp"); rows=lax.axis_index("rows")
    return dp//NC, lax.rem(dp,NC), rows


def dev(z,core,rows):
    return (z*NC+core, rows)


def partner_xy(rows,t):
    x=lax.rem(rows,2); y=rows//2
    tx=t%2; ty=t//2
    nx=1-x if tx else x
    ny=1-y if ty else y
    return ny*2+nx


def rcopy(src,dst,ssem,rsem,target):
    return pltpu.make_async_remote_copy(src_ref=src,dst_ref=dst,send_sem=ssem,recv_sem=rsem,device_id=target,device_id_type=MESH)


def barrier_all():
    dp=lax.axis_index("dp"); rows=lax.axis_index("rows")
    me=dp*NR+rows
    total=NZ*NC*NR
    bar=pltpu.get_barrier_semaphore()
    def body(k,c):
        other=lax.rem(me+k,total)
        pl.semaphore_signal(bar,inc=1,device_id=(other//NR,lax.rem(other,NR)),device_id_type=MESH)
        return c
    lax.fori_loop(1,total,body,0)
    pl.semaphore_wait(bar,total-1)


def zmod(v):
    return lax.rem(v+NZ,NZ)


class Gather:
    SEMS=[(NZ,),(NZ,),(NZ,NR),(NZ,NR),(NZ,NR),(NZ,NR),(1,)]

    def __init__(self,shard,full,sems):
        self.shard,self.full=shard,full
        self.sz,self.rz,self.sx,self.rx,self.sc,self.rc,self.lo=sems
        self.z,self.core,self.rows=here()

    def slot(self,dz,t,core):
        rows=self.rows if t==0 else partner_xy(self.rows,t)
        return self.full.at[zmod(self.z-dz),core,rows]

    def zcopy(self,dz,receive=False):
        dst=self.slot(dz if receive else 0,0,self.core)
        return rcopy(self.shard,dst,self.sz.at[dz],self.rz.at[dz],dev(zmod(self.z+dz),self.core,self.rows))

    def piece(self,dz):
        return self.shard if dz==0 else self.slot(dz,0,self.core)

    def xcopy(self,dz,t,receive=False):
        dst=self.slot(dz,t if receive else 0,self.core)
        return rcopy(self.piece(dz),dst,self.sx.at[dz,t],self.rx.at[dz,t],dev(self.z,self.core,partner_xy(self.rows,t)))

    def ccopy(self,dz,t,receive=False):
        src=self.piece(dz) if t==0 else self.slot(dz,t,self.core)
        dst=self.slot(dz,t,1-self.core if receive else self.core)
        return rcopy(src,dst,self.sc.at[dz,t],self.rc.at[dz,t],dev(self.z,1-self.core,self.rows))

    def local(self):
        return pltpu.make_async_copy(self.shard,self.slot(0,0,self.core),self.lo.at[0])

    def start(self):
        for dz in range(1,NZ):
            self.zcopy(dz).start()
        for t in range(1,NR):
            self.xcopy(0,t).start()
        self.ccopy(0,0).start()
        self.local().start()

    def zstep(self,dz):
        self.zcopy(dz,True).wait_recv()
        for t in range(1,NR):
            self.xcopy(dz,t).start()
        self.ccopy(dz,0).start()

    def xstep(self,dz,t):
        self.xcopy(dz,t,True).wait_recv()
        self.ccopy(dz,t).start()

    def finish(self):
        for dz in range(NZ):
            for t in range(NR):
                self.ccopy(dz,t,True).wait_recv()
        for dz in range(1,NZ):
            self.zcopy(dz).wait_send()
        for dz in range(NZ):
            for t in range(NR):
                if t: self.xcopy(dz,t).wait_send()
                self.ccopy(dz,t).wait_send()
        self.local().wait()

    def run_z(self):
        for dz in range(1,NZ): self.zstep(dz)

    def run_x(self):
        for dz in range(NZ):
            for t in range(1,NR): self.xstep(dz,t)


class Scatter:
    SEMS=[(1,),(1,),(1,),(NR,),(NR,),(NZ,),(NZ,)]

    @staticmethod
    def scratch(r,c,dt):
        return [pltpu.VMEM((NZ,NR,r,c),dt),pltpu.VMEM((NZ,NR,r,c),dt),pltpu.VMEM((NR,NZ,r,c),dt),pltpu.VMEM((NZ,r,c),dt),pltpu.VMEM((NZ,r,c),dt)]

    def __init__(self,part,out,bufs,sems):
        self.part,self.out=part,out
        self.own,self.sib,self.xin,self.zout,self.zin=bufs
        self.lo,self.sc,self.rc,self.sx,self.rx,self.sz,self.rz=sems
        self.z,self.core,self.rows=here()
        self.dt=self.own.dtype

    def lcopy(self):
        return pltpu.make_async_copy(self.part.at[:,self.core],self.own,self.lo.at[0])

    def ccopy(self):
        return rcopy(self.part.at[:,1-self.core],self.sib,self.sc.at[0],self.rc.at[0],dev(self.z,1-self.core,self.rows))

    def xcopy(self,t):
        to=partner_xy(self.rows,t)
        return rcopy(self.own.at[:,to],self.xin.at[t],self.sx.at[t],self.rx.at[t],dev(self.z,self.core,to))

    def zcopy(self,dz):
        to=zmod(self.z+dz)
        return rcopy(self.zout.at[to],self.zin.at[dz],self.sz.at[dz],self.rz.at[dz],dev(to,self.core,self.rows))

    def start(self):
        self.ccopy().start(); self.lcopy().start()

    def cstep(self):
        self.lcopy().wait(); self.ccopy().wait_recv()
        def body(i,c):
            a,b=i//NR,lax.rem(i,NR)
            self.own[a,b]=(self.own[a,b].astype(F32)+self.sib[a,b].astype(F32)).astype(self.dt)
            return c
        lax.fori_loop(0,NZ*NR,body,0)
        for t in range(1,NR): self.xcopy(t).start()

    def xstep(self):
        for t in range(1,NR): self.xcopy(t).wait_recv()
        def body(a,c):
            s=self.own[a,self.rows].astype(F32)
            for t in range(1,NR): s=s+self.xin[t,a].astype(F32)
            self.zout[a]=s.astype(self.dt)
            return c
        lax.fori_loop(0,NZ,body,0)
        for dz in range(1,NZ): self.zcopy(dz).start()

    def zstep(self):
        for dz in range(1,NZ): self.zcopy(dz).wait_recv()
        s=self.zout[self.z].astype(F32)
        for dz in range(1,NZ): s=s+self.zin[dz].astype(F32)
        if callable(self.out): self.out(s)
        else: self.out[...]=s

    def finish(self):
        self.ccopy().wait_send()
        for t in range(1,NR): self.xcopy(t).wait_send()
        for dz in range(1,NZ): self.zcopy(dz).wait_send()


class Swap:
    SEMS=[(NR,),(NR,),(1,)]
    def __init__(self,src,dst,sems):
        self.src,self.dst=src,dst
        self.s,self.r,self.lo=sems
        self.z,self.core,self.rows=here()
    def copy(self,t,receive=False):
        to=partner_xy(self.rows,t)
        return rcopy(self.src.at[to],self.dst.at[to if receive else self.rows],self.s.at[t],self.r.at[t],dev(self.z,self.core,to))
    def local(self):
        return pltpu.make_async_copy(self.src.at[self.rows],self.dst.at[self.rows],self.lo.at[0])
    def start(self):
        for t in range(1,NR): self.copy(t).start()
        self.local().start()
    def wait(self):
        for t in range(1,NR): self.copy(t,True).wait_recv()
        self.local().wait()
    def finish(self):
        for t in range(1,NR): self.copy(t).wait_send()


class AllToAll:
    N=NZ*NC*NR
    SEMS=[(N,),(N,),(1,)]
    def __init__(self,src,dst,sems,one=False):
        self.src,self.dst,self.one=src,dst,one
        self.s,self.r,self.lo=sems
        self.me=lax.axis_index("dp")*NR+lax.axis_index("rows")
    def piece(self,n):
        return self.src if self.one else self.src.at[n]
    def copy(self,k,receive=False):
        to=lax.rem(self.me+k,self.N)
        frm=lax.rem(self.me-k+self.N,self.N)
        return rcopy(self.piece(to),self.dst.at[frm if receive else self.me],self.s.at[k],self.r.at[k],(to//NR,lax.rem(to,NR)))
    def local(self):
        return pltpu.make_async_copy(self.piece(self.me),self.dst.at[self.me],self.lo.at[0])
    def each(self,fn):
        def body(k,c):
            fn(k); return c
        lax.fori_loop(1,self.N,body,0)
    def start(self):
        self.each(lambda k:self.copy(k).start())
        self.local().start()
    def wait(self):
        self.each(lambda k:self.copy(k,True).wait_recv())
        self.local().wait()
    def finish(self):
        self.each(lambda k:self.copy(k).wait_send())


def sem_types(shapes):
    return [pltpu.SemaphoreType.DMA(s) for s in shapes]
class GatherZ:
    SEMS=[(NZ,),(NZ,),(1,)]
    def __init__(self,shard,zp,sems):
        self.shard,self.zp=shard,zp
        self.s,self.r,self.lo=sems
        self.z,self.core,self.rows=here()
    def copy(self,dz,receive=False):
        to=zmod(self.z+dz)
        frm=zmod(self.z-dz)
        return rcopy(self.shard,self.zp.at[frm if receive else self.z],self.s.at[dz],self.r.at[dz],dev(to,self.core,self.rows))
    def local(self):
        return pltpu.make_async_copy(self.shard,self.zp.at[self.z],self.lo.at[0])
    def start(self):
        for dz in range(1,NZ): self.copy(dz).start()
        self.local().start()
    def wait(self):
        for dz in range(1,NZ): self.copy(dz,True).wait_recv()
    def finish(self):
        for dz in range(1,NZ): self.copy(dz).wait_send()
        self.local().wait()


class GatherXY:
    SEMS=[(NZ,NR),(NZ,NR),(NZ,NR),(NZ,NR),(1,)]
    def __init__(self,zp,full,sems):
        self.zp,self.full=zp,full
        self.sx,self.rx,self.sc,self.rc,self.lo=sems
        self.z,self.core,self.rows=here()
        self.half=full.shape[-1]//2
    def place(self,t):
        return self.rows if t==0 else partner_xy(self.rows,t)
    def to(self,t):
        return dev(self.z,self.core,self.place(t))
    def xcopy(self,k,t,receive=False):
        return rcopy(self.zp.at[k],self.full.at[k,self.core,self.place(t) if receive else self.rows],self.sx.at[k,t],self.rx.at[k,t],self.to(t))
    def fcopy(self,k,t,receive=False):
        q={1:3,2:0}[t]
        part=pl.ds(0 if t==1 else self.half,self.half)
        ref=self.full.at[k,self.core,self.place(3 if receive else t),:,part]
        return rcopy(ref,ref,self.sx.at[k,q],self.rx.at[k,q],self.to(3-t))
    def ccopy(self,k,t,receive=False):
        src=self.zp.at[k] if t==0 else self.full.at[k,self.core,self.place(t)]
        dst=self.full.at[k,1-self.core if receive else self.core,self.place(t)]
        return rcopy(src,dst,self.sc.at[k,t],self.rc.at[k,t],dev(self.z,1-self.core,self.rows))
    def local(self):
        return pltpu.make_async_copy(self.zp,self.full.at[:,self.core,self.rows],self.lo.at[0])
    def start(self,ks=range(NZ)):
        for k in ks:
            for t in (1,2): self.xcopy(k,t).start()
            self.ccopy(k,0).start()
    def start_local(self):
        self.local().start()
    def step(self,k):
        for t in (1,2):
            self.xcopy(k,t,True).wait_recv()
            self.fcopy(k,t).start()
            self.ccopy(k,t).start()
    def step2(self,k):
        for t in (1,2): self.fcopy(k,t,True).wait_recv()
        self.ccopy(k,3).start()
    def arrive(self,k):
        for t in range(NR): self.ccopy(k,t,True).wait_recv()
    def finish_remote(self):
        for k in range(NZ):
            for t in (1,2):
                self.xcopy(k,t).wait_send()
                self.fcopy(k,t).wait_send()
            for t in range(NR): self.ccopy(k,t).wait_send()
    def finish(self):
        self.finish_remote()
        self.local().wait()


class ScatterZ:
    SEMS=[(NZ,),(NZ,)]
    @staticmethod
    def scratch(r,c,dt):
        return [pltpu.VMEM((NZ,r,c),dt)]
    def __init__(self,zout,out,bufs,sems):
        self.zout,self.out=zout,out
        self.zin,=bufs
        self.s,self.r=sems
        self.z,self.core,self.rows=here()
    def copy(self,dz):
        to=zmod(self.z+dz)
        return rcopy(self.zout.at[to],self.zin.at[dz],self.s.at[dz],self.r.at[dz],dev(to,self.core,self.rows))
    def start(self):
        for dz in range(1,NZ): self.copy(dz).start()
    def step(self):
        for dz in range(1,NZ): self.copy(dz).wait_recv()
        v=self.zout[self.z].astype(F32)
        for dz in range(1,NZ): v=v+self.zin[dz].astype(F32)
        if callable(self.out): self.out(v)
        else: self.out[...]=v
    def finish(self):
        for dz in range(1,NZ): self.copy(dz).wait_send()


class Events:
    def __init__(self): self.at={}
    def add(self,slot,fn): self.at.setdefault(slot,[]).append(fn)
    def run(self,outer,inner,width):
        for slot,fns in self.at.items():
            if slot%width==inner:
                @pl.when(outer==slot//width)
                def _(fns=fns):
                    for fn in fns: fn()
NN=(((1,),(0,)),((),()))
C0=0.7978845608028654
C1=0.044715


def dotf(a,b,dims=NN):
    return lax.dot_general(a,b,dims,preferred_element_type=F32)


def loop(n,fn,unroll=1):
    def body(i,c):
        fn(i); return c
    lax.fori_loop(0,n,body,0,unroll=unroll)


def rows_of(i,n):
    return pl.ds(pl.multiple_of(i*n,n),n)


def normal_rows(v):
    d=1.0/v.shape[1]
    c=v-jnp.sum(v,axis=1,keepdims=True)*d
    inv=lax.rsqrt(jnp.sum(c*c,axis=1,keepdims=True)*d+EPSILON)
    return c*inv,inv


def normal_back_rows(g,n,inv):
    d=1.0/g.shape[1]
    return inv*(g-jnp.sum(g,axis=1,keepdims=True)*d-n*(jnp.sum(g*n,axis=1,keepdims=True)*d))


def fold8(v):
    s=v[0:8]
    for k in range(1,v.shape[0]//8): s=s+v[8*k:8*k+8]
    return s


def conv_loops(side,lanes_n,width,forward,finish):
    pass


def shifts(f,ml,mr):
    n=f.shape[0]
    return pltpu.roll(f,1,0)*ml, pltpu.roll(f,n-1,0)*mr


def conv_rows(src,dst_fn,taps,ml_ref,mr_ref,rl_ref,ls,side,cols):
    k=[taps[q:q+1,:] for q in range(9)]
    zero=jnp.zeros((cols,128),F32)
    def body(i,c):
        hm,part=c
        f=src[rows_of(i,cols),ls]
        fm,fp=shifts(f,ml_ref[rows_of(i,cols),:],mr_ref[rows_of(i,cols),:])
        h=[k[3*a]*fm+k[3*a+1]*f+k[3*a+2]*fp for a in range(3)]
        done=part+rl_ref[i]*h[2]
        @pl.when(i>0)
        def _(): dst_fn(i-1,done)
        return h[0],h[1]+rl_ref[i]*hm
    hm,part=lax.fori_loop(0,side,body,(zero,zero),unroll=8)
    dst_fn(side-1,part)


def back_rows(g_ref,f_ref,dst_fn,taps,ml_ref,mr_ref,rl_ref,ls,first,count,side,cols):
    k=[taps[q:q+1,:] for q in range(9)]
    z8=jnp.zeros((8,128),F32)
    def at(i): return rows_of(i,cols)
    def load(i):
        g=g_ref[at(i),ls]
        gm,gp=shifts(g,ml_ref[at(i),:],mr_ref[at(i),:])
        return gp,g,gm
    def mix3(gs,a): return k[3*a]*gs[0]+k[3*a+1]*gs[1]+k[3*a+2]*gs[2]
    whole=isinstance(first,int) and count==side
    zero=jnp.zeros((cols,128),F32)
    before=jnp.maximum(first-1,0)
    hp=zero if whole else mix3(load(before),2)
    fprev=zero if whole else f_ref[at(before),ls].astype(F32)
    def body(n,c):
        hp,part,fprev,acc=c
        i=first+n
        gs=load(i)
        done=part+rl_ref[i]*mix3(gs,0)
        @pl.when(n>0)
        def _(): dst_fn(i-1,done)
        f=f_ref[at(i),ls].astype(F32)
        nxt=f_ref[at(jnp.minimum(i+1,side-1)),ls].astype(F32)
        fs=(fprev*rl_ref[i],f,nxt*rl_ref[i+1])
        acc=tuple(acc[3*a+b]+fold8(fs[a]*gs[b]) for a in range(3) for b in range(3))
        return mix3(gs,2),mix3(gs,1)+rl_ref[i]*hp,f,acc
    hp,part,_,acc=lax.fori_loop(0,count,body,(hp,zero,fprev,(z8,)*9),unroll=8)
    end=first+count
    if not whole: part=part+rl_ref[end]*mix3(load(jnp.minimum(end,side-1)),0)
    dst_fn(end-1,part)
    return acc


def link_masks(labels):
    side,cols=labels.shape
    left=jnp.pad(labels[:,1:]==labels[:,:-1],((0,0),(1,0)))
    right=jnp.pad(labels[:,1:]==labels[:,:-1],((0,0),(0,1)))
    wide=lambda m: jnp.broadcast_to(m.reshape(side*cols,1).astype(F32),(side*cols,128))
    top=labels[:,0]//2
    rl=jnp.pad((top[1:]==top[:-1]).astype(F32),(1,1))
    return wide(left),wide(right),rl
HBM=pl.BlockSpec(memory_space=pl.ANY)
VM=pl.BlockSpec(memory_space=pltpu.VMEM)
SM=pl.BlockSpec(memory_space=pltpu.SMEM)
NDEV=NZ*NC*NR
S_=jax.ShapeDtypeStruct


def taker(it):
    return lambda cls:[next(it) for _ in cls.SEMS]


def assemble(dst,src,width,at):
    lane=lax.broadcasted_iota(jnp.int32,(1,128),1)
    tiles=dst.shape[1]//128
    for c in range(tiles):
        v=jnp.zeros((16,128),F32)
        for n in range(NDEV):
            lo=n*width-c*128
            if lo+width<=0 or lo>=128: continue
            p=src[n//(NC*NR),(n//NR)%NC,n%NR].astype(F32)
            sh=(lo-at)%128
            if sh: p=pltpu.roll(p,sh,1)
            v=jnp.where((lane>=lo)&(lane<lo+width),p,v)
        dst[:,c*128:(c+1)*128]=v


def enter_kernel(n_z,side,cols,ta,tf,*refs):
    it=iter(refs)
    nx=lambda n:[next(it) for _ in range(n)]
    tok,cond,ada,bias,qkv,taps,ml_ref,mr_ref,rl_ref=nx(9)
    shards=nx(n_z)
    tok_o,cond_o,mod_o,qkv_o,tap_a,tap_f,m1,mix=nx(8)
    zps=nx(n_z)
    condv,part,zq,taps_o,modw,F=nx(6)
    mbufs=nx(5)
    take=taker(it)
    c_all=AllToAll(cond,condv,take(AllToAll),one=True)
    swap_t=Swap(tok,tok_o,take(Swap))
    m_all=Scatter(part,mod_o,mbufs,take(Scatter))
    g_taps=Gather(taps,taps_o,take(Gather))
    gq_z=GatherZ(qkv,zq,take(GatherZ))
    gq=GatherXY(zq,qkv_o,take(GatherXY))
    gz=[GatherZ(s,z,take(GatherZ)) for s,z in zip(shards,zps)]
    barrier_all()
    c_all.start()
    gq_z.start()
    swap_t.start()
    g_taps.start()
    c_all.wait()
    me=c_all.me
    feats=ada.shape[0]
    cv=condv[:,0,:].astype(F32)
    low=(cv/(1.0+jnp.exp(-cv))).astype(BF)
    width=cv.shape[1]
    pick=(lax.broadcasted_iota(jnp.int32,(width,feats),0)==lax.broadcasted_iota(jnp.int32,(width,feats),1)+feats*me).astype(BF)
    mine=jnp.dot(low,pick,preferred_element_type=F32).astype(BF)
    chunk=768
    for c in range(ada.shape[1]//chunk):
        pr=jnp.dot(mine,ada[:,c*chunk:(c+1)*chunk],preferred_element_type=F32)
        for l in range(chunk//128):
            i=c*(chunk//128)+l
            part[:,:,:,i,:]=(pr[:,l*128:(l+1)*128]+bias[i:i+1,:]).reshape(NZ,NC,NR,128)
    cond_o[...]=low
    m_all.start()
    m_all.cstep()
    g_taps.run_z()
    gq_z.wait(); gq_z.local().wait()
    gq.start(); gq.start_local()
    for g in gz: g.start()
    m_all.xstep()
    m_all.zstep()
    g_taps.run_x()
    cells,feat=mix.shape
    L=feat//128
    for j in range(2):
        for l in range(L): modw[j:j+1,l*128:(l+1)*128]=mod_o[j*L+l:j*L+l+1,:]
    swap_t.wait()
    shift1=modw[0:1,:]; scale1=modw[1:2,:]
    EC=256
    for b in range(NR):
        n,_=normal_rows(tok_o[b].astype(F32))
        v=(n*(1.0+scale1)+shift1).astype(BF)
        m1[b*EC:(b+1)*EC,:]=v
        F[b*EC:(b+1)*EC,:]=v.astype(F32)
    g_taps.finish()
    assemble(tap_a,taps_o,ta,0)
    assemble(tap_f,taps_o,tf,ta)
    def lanes(l):
        ls=pl.ds(pl.multiple_of(l*128,128),128)
        def put(i,u): mix[rows_of(i,cols),ls]=u.astype(BF)
        conv_rows(F,put,tap_a[:,ls],ml_ref,mr_ref,rl_ref,ls,side,cols)
    gq.step(0)
    loop(L//2,lanes)
    gq.step(1)
    loop(L-L//2,lambda l:lanes(l+L//2))
    for k in range(2,NZ): gq.step(k)
    for k in range(NZ): gq.step2(k)
    for g in gz: g.wait()
    for k in range(NZ): gq.arrive(k)
    gq.finish()
    for dz in range(1,NZ): gq_z.copy(dz).wait_send()
    for g in [swap_t,c_all,m_all]+gz: g.finish()


def enter(tok,cond_row,ada,bias_rows,qkv,taps,ml,mr,rl,shards,side,cols,ta,tf):
    n=len(shards)
    V=pltpu.VMEM
    feat=tok.shape[2]; cells=side*cols
    scr=[V((NDEV,)+cond_row.shape,cond_row.dtype),V((NZ,NC,NR)+bias_rows.shape,F32),V((NZ,)+qkv.shape,BF),V((NZ,NC,NR)+taps.shape,BF),V((8,feat),F32),V((cells,feat),F32)]+Scatter.scratch(bias_rows.shape[0],128,F32)
    sems=sem_types(AllToAll.SEMS)+sem_types(Swap.SEMS)+sem_types(Scatter.SEMS)+sem_types(Gather.SEMS)+sem_types(GatherZ.SEMS)+sem_types(GatherXY.SEMS)+sem_types(GatherZ.SEMS)*n
    outs=[S_(tok.shape,tok.dtype),S_((NDEV,cond_row.shape[1]),BF),S_(bias_rows.shape,F32),S_((NZ,NC,NR)+qkv.shape,qkv.dtype),
          S_((16,NDEV*ta),F32),S_((16,NDEV*tf),F32),S_((cells,feat),BF),S_((cells,feat),BF)]
    outs+=[S_((NZ,)+s.shape,s.dtype) for s in shards]
    return pl.pallas_call(
        functools.partial(enter_kernel,n,side,cols,ta,tf),
        in_specs=[VM,HBM,VM,VM,VM,VM,VM,VM,SM]+[VM]*n,
        out_specs=[VM,VM,VM,HBM,VM,VM,VM,VM]+[HBM]*n,
        out_shape=outs,
        scratch_shapes=scr+sems,
        compiler_params=pltpu.CompilerParams(collective_id=0,has_side_effects=True,vmem_limit_bytes=63<<20),
        name="enter",
    )(tok,cond_row,ada,bias_rows,qkv,taps,ml,mr,rl,*shards)


def forward_kernel(n_w,qb,*refs):
    it=iter(refs)
    mix,qkv,qm,km,cot,late=[next(it) for _ in range(6)]
    zps=[next(it) for _ in range(n_w)]
    proj,att,lse_t,cot_o,late_o=[next(it) for _ in range(5)]
    fulls=[next(it) for _ in range(n_w)]
    lse=next(it)
    take=taker(it)
    barrier_all()
    swap_c=Swap(cot,cot_o,take(Swap))
    gs=[GatherXY(a,b,take(GatherXY)) for a,b in zip(zps,fulls)]
    gl=GatherZ(late,late_o,take(GatherZ))
    gl.start()
    gs[0].start(); swap_c.start(); gs[1].start()
    for g in gs: g.start_local()
    ev=Events()
    for k in range(NZ):
        ev.add(2,lambda k=k: gs[0].step(k))
        ev.add(6,lambda k=k: gs[0].step2(k))
        ev.add(6+k,lambda k=k: gs[1].step(k))
        if k<3: ev.add(9+k,lambda k=k: gs[1].step2(k))
    cells,feat=att.shape
    CH=256
    def pr(i):
        proj[rows_of(i,CH),:]=dotf(mix[rows_of(i,CH),:],qkv[...]).astype(BF)
    loop(cells//CH,pr)
    pairs=feat//128
    lane=lax.broadcasted_iota(jnp.int32,(1,128),1)
    lse[...]=jnp.zeros_like(lse)
    def pair(p):
        cq=pl.ds(pl.multiple_of(p*128,128),128)
        ck=pl.ds(pl.multiple_of(feat+p*128,128),128)
        cv=pl.ds(pl.multiple_of(2*feat+p*128,128),128)
        for h in range(2):
            ev.run(p,h,2)
            mine=(lane//64)==h
            k=jnp.where(mine,proj[:,ck],km[...])
            def body(i):
                r=rows_of(i,qb)
                q=jnp.where(mine,proj[r,cq]*jnp.asarray(0.125,BF),qm[r,:])
                s=dotf(q,k,NT)
                m=jnp.max(s,axis=1,keepdims=True)
                e=jnp.exp(s-m)
                l=jnp.sum(e,axis=1,keepdims=True)
                a=(e*(1.0/l)).astype(BF)
                o=dotf(a,proj[:,cv]).astype(BF)
                if h==0:
                    att[r,cq]=o
                else:
                    att[r,cq]=jnp.where(mine,o,att[r,cq])
                lse[r,:]=jnp.where(lane==2*p+h,m+jnp.log(l),lse[r,:])
            loop(cells//qb,body,2)
    loop(pairs,pair)
    lse_t[...]=jnp.transpose(lse[...])
    gs[1].step2(NZ-1)
    for g in gs:
        for k in range(NZ): g.arrive(k)
    swap_c.wait()
    gl.wait()
    for g in gs+[swap_c,gl]: g.finish()


def forward(mix,qkv,qm,km,cot,late,zps):
    n=len(zps)
    cells,feat=mix.shape
    outs=[S_((cells,3*feat),BF),S_((cells,feat),BF),S_((128,cells),F32),S_(cot.shape,cot.dtype),S_((NZ,)+late.shape,late.dtype)]
    outs+=[S_((NZ,NC,NR)+z.shape[1:],z.dtype) for z in zps]
    return pl.pallas_call(
        functools.partial(forward_kernel,n,512),
        in_specs=[VM,VM,VM,VM,VM,VM]+[VM]*n,
        out_specs=[VM,VM,VM,HBM,HBM]+[HBM]*n,
        out_shape=outs,
        scratch_shapes=[pltpu.VMEM((cells,128),F32)]+sem_types(Swap.SEMS)+sem_types(GatherXY.SEMS)*n+sem_types(GatherZ.SEMS),
        compiler_params=pltpu.CompilerParams(collective_id=1,has_side_effects=True,vmem_limit_bytes=63<<20),
        name="attn_fwd",
    )(mix,qkv,qm,km,cot,late,*zps)


def backward_kernel(n_g,kb,*refs):
    it=iter(refs)
    nx=lambda n:[next(it) for _ in range(n)]
    proj,do,o,qm,km,lse_t,mix,lay,gout=nx(9)
    parts=nx(n_g)
    gp,lay_o,gout_o,zq,lastq=nx(5)
    gouts=nx(n_g)
    qs,dqt,mixt=nx(3)
    obufs=nx(5)
    qbufs=nx(4)
    bufs=[nx(1) for _ in range(n_g)]
    take=taker(it)
    barrier_all()
    sl=Swap(lay,lay_o,take(Swap))
    so=Scatter(gout,gout_o,obufs,take(Scatter))
    uq=PipeScatter(qbufs,take(PipeScatter))
    sc=[ScatterZ(p,g,b,take(ScatterZ)) for p,g,b in zip(parts,gouts,bufs)]
    cells,feat=do.shape
    pairs=feat//128
    W=256
    tiles=pairs//2
    r_=feat//NDEV
    def put_q(m):
        def put(a,v):
            for s in range(3):
                zq[a,:,(s*(tiles-1)+m)*W:(s*(tiles-1)+m+1)*W]=v[:,s*W:(s+1)*W]
        return put
    ev=Events()
    so.start()
    for s in sc: s.start()
    ev.add(1,so.cstep)
    ev.add(2,sl.start)
    ev.add(5,lambda: uq.send_square(0))
    ev.add(6,so.xstep)
    for s in sc: ev.add(7,s.step)
    ev.add(8,lambda: uq.collect(0,put_q(0)))
    ev.add(9,lambda: uq.send_square(1))
    ev.add(11,so.zstep)
    lane=lax.broadcasted_iota(jnp.int32,(1,128),1)
    srow=lax.broadcasted_iota(jnp.int32,(8,128),0)
    slane=lax.broadcasted_iota(jnp.int32,(8,128),1)
    sel=(slane//64==srow).astype(BF)
    def tr(i):
        mixt[:,pl.ds(pl.multiple_of(i*256,256),256)]=jnp.transpose(mix[rows_of(i,256),:])
    loop(cells//256,tr)
    def pair(p):
        cq=pl.ds(pl.multiple_of(p*128,128),128)
        ck=pl.ds(pl.multiple_of(feat+p*128,128),128)
        cv=pl.ds(pl.multiple_of(2*feat+p*128,128),128)
        prod=do[:,cq].astype(F32)*o[:,cq].astype(F32)
        hi=prod.astype(BF); lo=(prod-hi.astype(F32)).astype(BF)
        delta=dotf(sel,hi,NT)+dotf(sel,lo,NT)
        qs[...]=proj[:,cq]*jnp.asarray(0.125,BF)
        for h in range(2):
            ev.run(p,h,2)
            mine=(lane//64)==h
            q=jnp.where(mine,qs[...],qm[...])
            ls=lse_t[pl.ds(2*p+h,1),:]
            dl=delta[h:h+1,:]
            dqt[...]=jnp.zeros_like(dqt)
            def body(i):
                r=rows_of(i,kb)
                kr=proj[r,ck]
                k=jnp.where(mine,kr,km[r,:])
                v=jnp.where(mine,proj[r,cv],jnp.zeros((),BF))
                st=dotf(k,q,NT)
                pt=jnp.exp(st-ls)
                dpt=dotf(v,do[:,cq],NT)
                ds=(pt*(dpt-dl)).astype(BF)
                dv=dotf(pt.astype(BF),do[:,cq]).astype(BF)
                dk=dotf(ds,qs[...]).astype(BF)
                dqt[...]+=dotf(kr,ds,TN)
                if h==0:
                    gp[r,cv]=dv
                    gp[r,ck]=dk
                else:
                    gp[r,cv]=jnp.where(mine,dv,gp[r,cv])
                    gp[r,ck]=jnp.where(mine,dk,gp[r,ck])
            loop(cells//kb,body,2)
            dq=(jnp.transpose(dqt[...])*0.125).astype(BF)
            if h==0:
                gp[:,cq]=dq
            else:
                gp[:,cq]=jnp.where(mine,dq,gp[:,cq])
        @pl.when(lax.rem(p,2)==1)
        def _():
            m=p//2
            s=lax.rem(m,2)
            n=NC*NR*r_
            def tile(i):
                for c in range(3):
                    cols=pl.ds(pl.multiple_of(c*feat+m*W,W),W)
                    uq.part[s,i,:,:,:,c*W:(c+1)*W]=dotf(mixt[rows_of(i,n),:],gp[:,cols]).astype(BF).reshape(NC,NR,r_,W)
            loop(NZ,tile)
            @pl.when(m<tiles-1)
            def _(): uq.send_core(s)
    loop(pairs,pair)
    uq.collect(1,put_q(1))
    lastq[...]=uq.part[0]
    sl.wait()
    for s in sc+[sl,so]: s.finish()


def backward(proj,do,o,qm,km,lse_t,mix,lay,gout,parts):
    n=len(parts)
    cells,feat=do.shape
    r_=feat//NDEV
    outs=[S_((cells,3*feat),BF),S_(lay.shape,lay.dtype),S_(gout.shape[3:],F32),S_((NZ,r_,2*feat),BF),S_((NZ,NC,NR,r_,feat),BF)]+[S_(p.shape[1:],F32) for p in parts]
    scr=[pltpu.VMEM((cells,128),BF),pltpu.VMEM((128,cells),F32),pltpu.VMEM((feat,cells),BF)]
    scr+=Scatter.scratch(gout.shape[3],gout.shape[4],gout.dtype)+PipeScatter.scratch(r_,feat)
    for p in parts: scr+=ScatterZ.scratch(p.shape[1],p.shape[2],p.dtype)
    return pl.pallas_call(
        functools.partial(backward_kernel,n,512),
        in_specs=[VM,VM,VM,VM,VM,VM,VM,VM,HBM]+[VM]*n,
        out_specs=[VM,HBM,VM,VM,VM]+[VM]*n,
        out_shape=outs,
        scratch_shapes=scr+sem_types(Swap.SEMS)+sem_types(Scatter.SEMS)+sem_types(PipeScatter.SEMS)+sem_types(ScatterZ.SEMS)*n,
        compiler_params=pltpu.CompilerParams(collective_id=2,has_side_effects=True,vmem_limit_bytes=63<<20),
        name="attn_bwd",
    )(proj,do,o,qm,km,lse_t,mix,lay,gout,*parts)


def spread(dst,src_ref,width,at):
    lane=lax.broadcasted_iota(jnp.int32,(1,128),1)
    for n in range(NDEV):
        lo=n*width
        c,off=lo//128,lo%128
        sh=(at-off)%128
        v=src_ref[:,c*128:(c+1)*128]
        v=pltpu.roll(v,sh,1) if sh else v
        if off+width>128:
            w=src_ref[:,(c+1)*128:(c+2)*128]
            w=pltpu.roll(w,sh,1) if sh else w
            v=jnp.where(lane<at+128-off,v,w)
        keep=(lane>=at)&(lane<at+width)
        i=(n//(NC*NR),(n//NR)%NC,n%NR)
        if at==0: dst[i]=jnp.where(keep,v,0.0)
        else: dst[i]=jnp.where(keep,v,dst[i])


def tail_kernel(side,cols,ta,tf,*refs):
    it=iter(refs)
    nx=lambda n:[next(it) for _ in range(n)]
    gproj,qkv,m1,x_ref,gmid,mod,tap_ref,ml_ref,mr_ref,rl_ref,sums,gkf,low,ada,zq,lastq=nx(16)
    tg_o,ctx_o,adag_o,gm_o,q_o,ka_o,kf_o=nx(7)
    G,gm1,tgb,tgin,ktap,gme,gml,gmev,gmlv,ctxs,ctxv,tpart=nx(12)
    zbufs=nx(1); lbufs=nx(5); tbufs=nx(5)
    take=taker(it)
    barrier_all()
    def put_z(v):
        n=v.shape[1]//3
        for s in range(3): q_o[:,s*n*3//2:s*n*3//2+n]=v[:,s*n:(s+1)*n]
    def put_l(v):
        n=v.shape[1]//3
        for s in range(3): q_o[:,(3*s+2)*n:(3*s+3)*n]=v[:,s*n:(s+1)*n]
    def put_t(v):
        ka_o[...]=v[0:9,0:ta]
        kf_o[...]=pltpu.roll(v,128-ta,1)[0:9,0:tf]
    sz=ScatterZ(zq,put_z,zbufs,take(ScatterZ))
    slq=Scatter(lastq,put_l,lbufs,take(Scatter))
    stp=Scatter(tpart,put_t,tbufs,take(Scatter))
    st=Swap(tgb,tgin,take(Swap))
    ge=AllToAll(gme,gmev,take(AllToAll),one=True)
    gl=AllToAll(gml,gmlv,take(AllToAll),one=True)
    xa=AllToAll(ctxs,ctxv,take(AllToAll))
    slq.start(); sz.start()
    cells,feat=x_ref.shape
    L=feat//128
    for i,q in enumerate((3,1,2,0)):
        for l in range(L):
            gme[i*L+l:i*L+l+1,:]=sums[q:q+1,l*128:(l+1)*128].astype(BF)
    ge.start()
    CH=1024; EC=256
    def a(i):
        r=rows_of(i,CH)
        G[r,:]=dotf(gproj[r,:],qkv[...],NT).astype(BF).astype(F32)
    loop(cells//CH,a)
    slq.cstep()
    ktap[...]=jnp.zeros_like(ktap)
    shift1=mod[0:1,:]; scale1=mod[1:2,:]
    z8=jnp.zeros((8,feat),F32)
    block=cells//NR
    c=(z8,z8)
    per=side//NR
    for t in (3,1,2,0):
        to=partner_xy(st.rows,t) if t else st.rows
        def lanes(l):
            ls=pl.ds(pl.multiple_of(l*128,128),128)
            def put(i,u): gm1[rows_of(i,cols),ls]=u
            acc=back_rows(G,m1,put,tap_ref[:,ls],ml_ref,mr_ref,rl_ref,ls,to*per,per,side,cols)
            for q in range(9): ktap[q:q+1,ls]+=jnp.sum(acc[q],axis=0,keepdims=True)
        loop(L,lanes)
        r=rows_of(to,block)
        n,inv=normal_rows(x_ref[r,:].astype(F32))
        g=gm1[r,:]
        tgb[to]=(gmid[r,:]+normal_back_rows(g*(1.0+scale1),n,inv)).astype(BF)
        c=(c[0]+fold8(g),c[1]+fold8(g*n))
        if t: st.copy(t).start()
        else: st.local().start()
        if t==1: slq.xstep()
    spread(tpart,ktap,ta,0)
    spread(tpart,gkf,tf,ta)
    stp.start()
    for i,v in enumerate(c):
        v=jnp.sum(v,axis=0,keepdims=True)
        for l in range(L): gml[i*L+l:i*L+l+1,:]=v[:,l*128:(l+1)*128].astype(BF)
    gml[2*L:16,:]=jnp.zeros((16-2*L,128),BF)
    gl.start()
    me=gl.me
    feats=ada.shape[0]
    width=low.shape[1]
    pick=(lax.broadcasted_iota(jnp.int32,(width,feats),0)==lax.broadcasted_iota(jnp.int32,(width,feats),1)+feats*me).astype(BF)
    mine=jnp.dot(low[...],pick,preferred_element_type=F32).astype(BF)
    acc=jnp.zeros((NDEV,feats),F32)
    ge.wait()
    def use(src,n,base,acc):
        for i in range(n):
            g=src[:,i,:]
            j=base+i
            adag_o[:,j*128:(j+1)*128]=lax.dot_general(mine,g,TN,preferred_element_type=F32)
            gm_o[j:j+1,:]=jnp.sum(g.astype(F32),axis=0,keepdims=True)
            acc=acc+lax.dot_general(g,ada[:,j*128:(j+1)*128],NT,preferred_element_type=F32)
        return acc
    acc=use(gmev,4*L,2*L,acc)
    stp.cstep()
    gl.wait()
    acc=use(gmlv,2*L,0,acc)
    for n in range(NDEV):
        g0=(n//NR)*NR
        ctxs[n,0:NR,0:feats]=acc[g0:g0+NR,:]
    xa.start()
    stp.xstep()
    sz.step()
    slq.zstep()
    stp.zstep()
    st.wait()
    def up(i):
        for b in range(NR):
            tg_o[b,rows_of(i,EC),:]=tgin[b,rows_of(i,EC),:].astype(F32)
    loop(block//EC,up)
    xa.wait()
    ctx_o[...]=ctxv[...]
    for s in (sz,slq,stp,st,ge,gl,xa): s.finish()


def tail(gproj,qkv,m1,x,gmid,mod,taps,ml,mr,rl,sums,gkf,low,ada,zq,lastq,side,cols,ta,tf):
    cells,feat=x.shape
    block=cells//NR
    r_=feat//NDEV
    V=pltpu.VMEM
    L=feat//128
    outs=[S_((NR,block,feat),F32),S_((NDEV,8,128),F32),S_(ada.shape,F32),S_((6*L,128),F32),S_((r_,3*feat),F32),S_((9,ta),F32),S_((9,tf),F32)]
    scr=[V((cells,feat),F32),V((cells,feat),F32),V((NR,block,feat),BF),V((NR,block,feat),BF),V((16,feat),F32),
         V((4*L,128),BF),V((16,128),BF),V((NDEV,4*L,128),BF),V((NDEV,16,128),BF),V((NDEV,8,128),F32),V((NDEV,8,128),F32),V((NZ,NC,NR,16,128),F32)]
    scr+=ScatterZ.scratch(r_,zq.shape[2],BF)+Scatter.scratch(r_,feat,BF)+Scatter.scratch(16,128,F32)
    sems=sem_types(ScatterZ.SEMS)+sem_types(Scatter.SEMS)*2+sem_types(Swap.SEMS)+sem_types(AllToAll.SEMS)*3
    return pl.pallas_call(
        functools.partial(tail_kernel,side,cols,ta,tf),
        in_specs=[VM]*9+[SM]+[VM]*6,
        out_specs=[VM]*7,
        out_shape=outs,
        scratch_shapes=scr+sems,
        compiler_params=pltpu.CompilerParams(collective_id=3,has_side_effects=True,vmem_limit_bytes=63<<20),
        name="tail",
    )(gproj,qkv,m1,x,gmid,mod,taps,ml,mr,rl,sums,gkf,low,ada,zq,lastq)


def greet(targets):
    bar=pltpu.get_barrier_semaphore()
    for d in targets:
        pl.semaphore_signal(bar,inc=1,device_id=d,device_id_type=MESH)
    pl.semaphore_wait(bar,len(targets))


def near():
    z,core,rows=here()
    return [dev(z,1-core,rows)]+[dev(z,core,partner_xy(rows,t)) for t in range(1,NR)]


class PipeScatter:
    SEMS=[(2,),(2,),(2,NR),(2,NR)]
    @staticmethod
    def scratch(r,c):
        return [pltpu.VMEM((2,NZ,NC,NR,r,c),BF),pltpu.VMEM((2,NZ,NR,r,c),BF),pltpu.VMEM((2,NZ,NR,r,c),BF),pltpu.VMEM((2,NR,NZ,r,c),BF)]
    def __init__(self,bufs,sems):
        self.part,self.sib,self.own,self.xin=bufs
        self.sc,self.rc,self.sx,self.rx=sems
        self.z,self.core,self.rows=here()
    def ccopy(self,s):
        return rcopy(self.part.at[s,:,1-self.core],self.sib.at[s],self.sc.at[s],self.rc.at[s],dev(self.z,1-self.core,self.rows))
    def xcopy(self,s,t):
        to=partner_xy(self.rows,t)
        return rcopy(self.own.at[s,:,to],self.xin.at[s,t],self.sx.at[s,t],self.rx.at[s,t],dev(self.z,self.core,to))
    def send_core(self,s):
        self.ccopy(s).start()
    def send_square(self,s):
        self.ccopy(s).wait()
        def body(i):
            a,b=i//NR,lax.rem(i,NR)
            self.own[s,a,b]=(self.part[s,a,self.core,b].astype(F32)+self.sib[s,a,b].astype(F32)).astype(BF)
        loop(NZ*NR,body)
        for t in range(1,NR): self.xcopy(s,t).start()
    def collect(self,s,put):
        for t in range(1,NR): self.xcopy(s,t).wait()
        def body(a):
            v=self.own[s,a,self.rows].astype(F32)
            for t in range(1,NR): v=v+self.xin[s,t,a].astype(F32)
            put(a,v.astype(BF))
        loop(NZ,body)


class RowScatter:
    SEMS=[(2,),(2,),(2,NR),(2,NR)]
    @staticmethod
    def scratch(r,c):
        return [pltpu.VMEM((2,NR,r,c),BF),pltpu.VMEM((2,NR,r,c),BF),pltpu.VMEM((2,NR,r,c),BF)]
    def __init__(self,part,zout,bufs,sems):
        self.part,self.zout=part,zout
        self.sib,self.own,self.xin=bufs
        self.sc,self.rc,self.sx,self.rx=sems
        self.z,self.core,self.rows=here()
    def ccopy(self,k):
        s=k%2
        return rcopy(self.part.at[k,1-self.core],self.sib.at[s],self.sc.at[s],self.rc.at[s],dev(self.z,1-self.core,self.rows))
    def xcopy(self,k,t):
        s=k%2
        to=partner_xy(self.rows,t)
        return rcopy(self.own.at[s,to],self.xin.at[s,t],self.sx.at[s,t],self.rx.at[s,t],dev(self.z,self.core,to))
    def send_core(self,k):
        self.ccopy(k).start()
    def send_square(self,k):
        self.ccopy(k).wait()
        s=k%2
        def body(b):
            self.own[s,b]=(self.part[k,self.core,b].astype(F32)+self.sib[s,b].astype(F32)).astype(BF)
        loop(NR,body)
        for t in range(1,NR): self.xcopy(k,t).start()
    def collect(self,k):
        s=k%2
        for t in range(1,NR): self.xcopy(k,t).wait()
        v=self.own[s,self.rows].astype(F32)
        for t in range(1,NR): v=v+self.xin[s,t].astype(F32)
        self.zout[k]=v.astype(BF)


def ffn_kernel_body(*refs,side,cols):
    it=iter(refs)
    nx=lambda n:[next(it) for _ in range(n)]
    x_ref,att_ref,cot_ref,mod_ref,outw_ref,up_ref,zpd,tap_ref,ml_ref,mr_ref,rl_ref=nx(11)
    lay_ref,gmid_ref,gatt_ref,gout_ref,zup,zdown,gtap_ref,sums_ref=nx(8)
    m2,m2t,gffn,branch,middle,fb,gm2,F,G,glow,gub,dfull,gd=nx(13)
    ubufs=nx(4); dbufs=nx(3)
    take=taker(it)
    ga=GatherXY(zpd,dfull,take(GatherXY))
    us=PipeScatter(ubufs,take(PipeScatter))
    ds=RowScatter(gd,zdown,dbufs,take(RowScatter))
    t=pl.program_id(0)
    cells,feat=x_ref.shape
    T=up_ref.shape[1]
    hidden=NDEV*zpd.shape[1]
    steps=hidden//T; last=steps-1
    block=hidden//NZ
    CH=1024; EC=256
    shift2=mod_ref[3:4,:]; scale2=mod_ref[4:5,:]; gate2=mod_ref[5:6,:]; gate1=mod_ref[2:3,:]
    slot=lax.rem(t,2); other=lax.rem(t+1,2)
    ready={}
    for k in range(NZ): ready[k]=-(-((k+1)*block)//T)-1
    need={}
    for k in range(NZ): need[k]=(k*block)//T
    def put_up(tile):
        def put(a,v): zup[a,:,pl.ds(pl.multiple_of(tile*T,128),T)]=v
        return put

    @pl.when(t==0)
    def _():
        greet(near())
        ga.start(); ga.start_local()
        def a(i):
            branch[rows_of(i,CH),:]=dotf(att_ref[rows_of(i,CH),:],outw_ref[...])
        loop(cells//CH,a)
        def b(i):
            r=rows_of(i,EC)
            mid=x_ref[r,:].astype(F32)+gate1*branch[r,:]
            middle[r,:]=mid
            n,_=normal_rows(mid)
            m2[r,:]=(n*(1.0+scale2)+shift2).astype(BF)
            gffn[r,:]=(gate2*cot_ref[r,:].astype(F32)).astype(BF)
        loop(cells//EC,b)
        ga.step(0)
        def c(i):
            r=rows_of(i,CH)
            m2t[:,pl.ds(pl.multiple_of(i*CH,CH),CH)]=jnp.transpose(m2[r,:])
            fb[r,:]=jnp.zeros((CH,feat),F32)
            gm2[r,:]=jnp.zeros((CH,feat),F32)
        loop(cells//CH,c)
        ga.local().wait()
    for k in range(NZ):
        @pl.when(t==need[k])
        def _(k=k):
            if k: ga.step(k)
            ga.step2(k)
            ga.arrive(k)
    @pl.when(t>=2)
    def _():
        us.collect(slot,put_up(t-2))
    for k in range(NZ):
        if ready[k]+2<=last:
            @pl.when(t==ready[k]+2)
            def _(k=k): ds.collect(k)

    dw=dfull.reshape(hidden,feat)
    gdw=gd.reshape(hidden,feat)
    tr=pl.ds(pl.multiple_of(t*T,T),T)
    def first(i):
        r=rows_of(i,CH)
        F[r,:]=dotf(m2[r,:],up_ref[...]).astype(BF).astype(F32)
        G[r,:]=dotf(gffn[r,:],dw[tr,:],NT)
    loop(cells//CH,first)

    def forward_lanes(l):
        ls=pl.ds(pl.multiple_of(l*128,128),128)
        def put(i,u):
            r=rows_of(i,cols)
            u2=u*u
            th=jnp.tanh(C0*(u+C1*(u2*u)))
            half=0.5*(1.0+th)
            glow[r,ls]=(u*half).astype(BF)
            d=half+(0.5*u)*(1.0-th*th)*(C0*(1.0+(3.0*C1)*u2))
            G[r,ls]=(G[r,ls]*d).astype(BF).astype(F32)
        conv_rows(F,put,tap_ref[:,ls],ml_ref,mr_ref,rl_ref,ls,side,cols)
    loop(T//128,forward_lanes)
    @pl.when(t>=1)
    def _():
        us.send_square(other)
    for k in range(NZ):
        if ready[k]+1<=last:
            @pl.when(t==ready[k]+1)
            def _(k=k): ds.send_square(k)
    def back_lanes(l):
        ls=pl.ds(pl.multiple_of(l*128,128),128)
        def put2(i,u):
            gub[rows_of(i,cols),ls]=u.astype(BF)
        acc=back_rows(G,F,put2,tap_ref[:,ls],ml_ref,mr_ref,rl_ref,ls,0,side,side,cols)
        for q in range(9):
            gtap_ref[q:q+1,ls]=jnp.sum(acc[q],axis=0,keepdims=True)
    loop(T//128,back_lanes)
    gtap_ref[9:16,:]=jnp.zeros((7,T),F32)

    r_=feat//NDEV
    def third(i):
        n=NC*NR*r_
        us.part[slot,i]=dotf(m2t[rows_of(i,n),:],gub[...]).astype(BF).reshape(NC,NR,r_,T)
    loop(NZ,third)
    us.send_core(slot)
    for i in range(T//256):
        gdw[pl.ds(pl.multiple_of(t*T+i*256,256),256),:]=dotf(glow[:,i*256:(i+1)*256],gffn[...],TN).astype(BF)
    for k in range(NZ):
        @pl.when(t==ready[k])
        def _(k=k): ds.send_core(k)
    def second(i):
        r=rows_of(i,CH)
        fb[r,:]+=dotf(glow[r,:],dw[tr,:])
        gm2[r,:]+=dotf(gub[r,:],up_ref[...],NT)
    loop(cells//CH,second)

    @pl.when(t==last)
    def _():
        us.collect(other,put_up(last-1))
        late=[k for k in range(NZ) if ready[k]+1>last]
        mid_=[k for k in range(NZ) if ready[k]+1==last]
        for k in mid_: ds.collect(k)
        us.send_square(slot)
        for k in late: ds.send_square(k)
        z=jnp.zeros((8,feat),F32)
        def body(i,c):
            sg2,ss2,sc2,sg1=c
            r=rows_of(i,EC)
            inc=cot_ref[r,:].astype(F32)
            mid=middle[r,:]
            n,inv=normal_rows(mid)
            lay_ref[r,:]=(mid+gate2*fb[r,:]).astype(BF)
            gm=gm2[r,:]
            gmid=inc+normal_back_rows(gm*(1.0+scale2),n,inv)
            gmid_ref[r,:]=gmid
            gffn[r,:]=(gate1*gmid).astype(BF)
            return (sg2+fold8(inc*fb[r,:]),ss2+fold8(gm),sc2+fold8(gm*n),sg1+fold8(gmid*branch[r,:]))
        res=lax.fori_loop(0,cells//EC,body,(z,z,z,z))
        for q in range(4):
            sums_ref[q:q+1,:]=jnp.sum(res[q],axis=0,keepdims=True)
        sums_ref[4:8,:]=jnp.zeros((4,feat),F32)
        def b(i):
            r=rows_of(i,CH)
            gatt_ref[r,:]=dotf(gffn[r,:],outw_ref[...],NT).astype(BF)
        loop(cells//CH,b)
        for i in range(feat//256):
            gout_ref[i*256:(i+1)*256,:]=dotf(att_ref[:,i*256:(i+1)*256],gffn[...],TN).astype(BF)
        us.collect(slot,put_up(last))
        for k in late: ds.collect(k)
        ga.finish_remote()


def ffn(x,att,cot,mod6,outw,up,zpd,taps,ml,mr,rl,side,cols,T=512):
    cells,feat=x.shape
    hidden=up.shape[1]
    vm=lambda shape: pl.BlockSpec(shape,lambda t:(0,)*len(shape),pipeline_mode=pl.Buffered(1))
    r_,d_=feat//NDEV,hidden//NDEV
    return pl.pallas_call(
        functools.partial(ffn_kernel_body,side=side,cols=cols),
        grid=(hidden//T,),
        in_specs=[vm((cells,feat)),vm((cells,feat)),vm((cells,feat)),vm((8,feat)),vm((feat,feat)),
                  pl.BlockSpec((feat,T),lambda t:(0,t)),HBM,pl.BlockSpec((16,T),lambda t:(0,t)),
                  vm((cells,128)),vm((cells,128)),SM],
        out_specs=[vm((cells,feat)),vm((cells,feat)),vm((cells,feat)),vm((feat,feat)),
                   vm((NZ,r_,hidden)),vm((NZ,d_,feat)),pl.BlockSpec((16,T),lambda t:(0,t)),vm((8,feat))],
        out_shape=[S_((cells,feat),BF),S_((cells,feat),F32),S_((cells,feat),BF),S_((feat,feat),BF),S_((NZ,r_,hidden),BF),S_((NZ,d_,feat),BF),S_((16,hidden),F32),S_((8,feat),F32)],
        scratch_shapes=[pltpu.VMEM((cells,feat),BF),pltpu.VMEM((feat,cells),BF),pltpu.VMEM((cells,feat),BF),
                        pltpu.VMEM((cells,feat),F32),pltpu.VMEM((cells,feat),F32),pltpu.VMEM((cells,feat),F32),pltpu.VMEM((cells,feat),F32),
                        pltpu.VMEM((cells,T),F32),pltpu.VMEM((cells,T),F32),pltpu.VMEM((cells,T),BF),pltpu.VMEM((cells,T),BF),
                        pltpu.VMEM((NZ,NC,NR,d_,feat),BF),pltpu.VMEM((NZ,NC,NR,d_,feat),BF)]
                       +PipeScatter.scratch(r_,T)+RowScatter.scratch(d_,feat)
                       +sem_types(GatherXY.SEMS)+sem_types(PipeScatter.SEMS)+sem_types(RowScatter.SEMS),
        compiler_params=pltpu.CompilerParams(dimension_semantics=("arbitrary",),vmem_limit_bytes=63<<20,collective_id=4,has_side_effects=True),
        name="ffn",
    )(x,att,cot,mod6,outw,up,zpd,taps,ml,mr,rl)
def own_rows(padded_cells):
    return jnp.pad(padded_cells,((0,0),(1,1),(1,1),(0,0)))


def fast(tokens,conditioning,item_map,ada_weight,ada_bias,attn_kernel,qkv_weight,out_weight,up_weight,ffn_kernel,down_weight,out_cotangent):
    canvases,rows_here,cols,features=tokens.shape
    side=rows_here*NR
    cells=side*cols
    rows=lax.axis_index("rows"); dp=lax.axis_index("dp"); me=dp*NR+rows
    hidden=up_weight.shape[1]
    cond_row=jnp.pad(lax.dynamic_slice_in_dim(conditioning,rows,1,0),((0,7),(0,0)))
    mod_cols=ada_weight.shape[1]
    bshard=ada_bias.shape[0]
    bias_rows=lax.dynamic_update_slice_in_dim(jnp.zeros((mod_cols,),F32),ada_bias.astype(F32),me*bshard,0).reshape(mod_cols//128,128)
    ta,tf=attn_kernel.shape[1],ffn_kernel.shape[1]
    taps=jnp.pad(jnp.concatenate([attn_kernel,ffn_kernel],axis=1),((0,7),(0,128-ta-tf)))
    blocks=(NR,rows_here*cols,features)
    labels=lax.dynamic_index_in_dim(item_map,rows,0,keepdims=False)
    qm,km=head_masks(labels.reshape(cells))
    ml,mr,rl=link_masks(labels)
    tok,low_all,mod,qkv_f,tap_a,tap_f,m1,mix,*zps=enter(tokens.reshape(blocks),cond_row,ada_weight,bias_rows,qkv_weight,taps,ml,mr,rl,[out_weight,up_weight],side,cols,ta,tf)
    full2=lambda a:a.reshape(-1,a.shape[-1])
    triple_full=full2(qkv_f)
    mod6=jnp.pad(mod.reshape(6,features),((0,2),(0,0)))
    proj,attended,lse_t,cot,zp_down,out_f,up_f=forward(mix,triple_full,qm,km,out_cotangent.reshape(blocks),down_weight,zps)
    lay,gmid,gatt,g_out,z_up,z_down,g_kffn,sums=ffn(
        tok.reshape(cells,features),attended,cot.reshape(cells,features),mod6,
        full2(out_f),full2(up_f),zp_down,tap_f,ml,mr,rl,side,cols)
    sp=lambda g:g.reshape(NZ,NC,NR,g.shape[0]//NDEV,g.shape[1])
    gproj,lay_o,o_o,zq,lastq,u_o,d_o=backward(proj,gatt,attended,qm,km,lse_t,mix,lay.reshape(blocks),sp(g_out),[z_up,z_down])
    tg,ctx,adag,gmsum,q_o,ka_o,kf_o=tail(gproj,triple_full,m1,tok.reshape(cells,features),gmid,mod6,
        tap_a,ml,mr,rl,sums,g_kffn,low_all,ada_weight,zq,lastq,side,cols,ta,tf)
    shape4=(NR,rows_here,cols,features)
    feats=ada_weight.shape[0]
    dsilu=ctx[:,:NR,:feats].transpose(1,0,2).reshape(NR,features)
    cv=conditioning.astype(F32)
    _,sback=jax.vjp(jax.nn.silu,cv)
    dctx=sback(dsilu)[0]
    gbias=lax.dynamic_slice_in_dim(gmsum.reshape(mod_cols),me*bshard,bshard,0)
    return (lay_o.reshape(shape4),tg.reshape(shape4),dctx,adag,gbias,ka_o,q_o,o_o,u_o,kf_o,d_o)


def solution(mesh):
    quick=dict(mesh.shape)=={"dp":NZ*NC,"rows":NR}
    return jax.shard_map(
        fast if quick else local,
        mesh=mesh,
        in_specs=(
            P("dp", "rows", None, None),
            P("dp", None),
            P("dp", None, None),
            P(("dp", "rows"), None),
            P(("dp", "rows")),
            P(None, ("dp", "rows")),
            P(("dp", "rows"), None),
            P(("dp", "rows"), None),
            P(("dp", "rows"), None),
            P(None, ("dp", "rows")),
            P(("dp", "rows"), None),
            P("dp", "rows", None, None),
        ),
        out_specs=(
            P("dp", "rows", None, None),
            P("dp", "rows", None, None),
            P("dp", None),
            P(("dp", "rows"), None),
            P(("dp", "rows")),
            P(None, ("dp", "rows")),
            P(("dp", "rows"), None),
            P(("dp", "rows"), None),
            P(("dp", "rows"), None),
            P(None, ("dp", "rows")),
            P(("dp", "rows"), None),
        ),
        check_vma=False,
    )
```

```python
import functools

import jax
import jax.numpy as jnp
from jax import lax
from jax.experimental import pallas as pl
from jax.experimental.pallas import tpu as pltpu
from jax.sharding import PartitionSpec as P

PER_GROUP_WIDTH = 64


EPSILON = 1e-06


def padded(block, sides, width):
    for axis, dim in sides:
        count = lax.axis_size(axis)
        forward = [(i, i + 1) for i in range(count - 1)]
        backward = [(target, source) for source, target in forward]
        low = lax.ppermute(
            lax.slice_in_dim(block, block.shape[dim] - width, None, axis=dim), axis, forward
        )
        high = lax.ppermute(lax.slice_in_dim(block, 0, width, axis=dim), axis, backward)
        block = jnp.concatenate([low, block, high], axis=dim)
    return block


def normalize(attended_content_array):
    average = jnp.mean(attended_content_array, axis=-1, keepdims=True)
    centred = attended_content_array - average
    inverse = lax.rsqrt(jnp.mean(centred * centred, axis=-1, keepdims=True) + EPSILON)
    return (centred * inverse, inverse)


def normalize_back(incoming, normalized_rows, inverse):
    return inverse * (
        incoming
        - jnp.mean(incoming, axis=-1, keepdims=True)
        - normalized_rows * jnp.mean(incoming * normalized_rows, axis=-1, keepdims=True)
    )


def widen_cols(rimmed):
    return jnp.pad(rimmed, ((0, 0), (0, 0), (1, 1), (0, 0)))


def tap_mask(labels_pad, centre, row_off, col_off):
    rows_here = centre.shape[1]
    cols_here = centre.shape[2]
    return (labels_pad[:, row_off : row_off + rows_here, col_off : col_off + cols_here] == centre)[
        ..., None
    ]


def conv_forward(padded_rows, labels_pad, centre, kernel):
    rows_here = centre.shape[1]
    cols_here = centre.shape[2]
    summed = jnp.zeros(centre.shape + (kernel.shape[1],), jnp.float32)
    for row_off in range(3):
        for col_off in range(3):
            window = padded_rows[
                :, row_off : row_off + rows_here, col_off : col_off + cols_here
            ].astype(jnp.float32)
            tapped = kernel[3 * row_off + col_off].astype(jnp.float32) * window
            summed = summed + jnp.where(tap_mask(labels_pad, centre, row_off, col_off), tapped, 0.0)
    return summed


def conv_mirror(padded_rows, labels_pad, centre, kernel):
    rows_here = centre.shape[1]
    cols_here = centre.shape[2]
    summed = jnp.zeros(centre.shape + (kernel.shape[1],), jnp.float32)
    for row_off in range(3):
        for col_off in range(3):
            row_from = 2 - row_off
            col_from = 2 - col_off
            window = padded_rows[
                :, row_from : row_from + rows_here, col_from : col_from + cols_here
            ].astype(jnp.float32)
            tapped = kernel[3 * row_off + col_off].astype(jnp.float32) * window
            summed = summed + jnp.where(
                tap_mask(labels_pad, centre, row_from, col_from), tapped, 0.0
            )
    return summed


def kernel_grad(incoming, padded_rows, labels_pad, centre):
    rows_here = centre.shape[1]
    cols_here = centre.shape[2]
    incoming_values = incoming.astype(jnp.float32)
    tap_sums = []
    for row_off in range(3):
        for col_off in range(3):
            window = padded_rows[
                :, row_off : row_off + rows_here, col_off : col_off + cols_here
            ].astype(jnp.float32)
            product = jnp.where(
                tap_mask(labels_pad, centre, row_off, col_off), incoming_values * window, 0.0
            )
            tap_sums.append(jnp.sum(product, axis=(0, 1, 2)))
    return jnp.stack(tap_sums, axis=0)


def contract_rows(left, right):
    return lax.dot_general(
        left, right, (((0,), (0,)), ((), ())), preferred_element_type=jnp.float32
    )


def contract_cols(left, right):
    return lax.dot_general(
        left, right, (((1,), (1,)), ((), ())), preferred_element_type=jnp.float32
    )


def local(
    tokens,
    conditioning,
    item_map,
    ada_weight,
    ada_bias,
    attn_kernel,
    qkv_weight,
    out_weight,
    up_weight,
    ffn_kernel,
    down_weight,
    out_cotangent,
):
    canvases, rows_here, cols_here, features = tokens.shape
    cell_count = canvases * rows_here * cols_here
    position = lax.axis_index("rows")
    gathered = (
        lax.all_gather(ada_weight, ("dp", "rows"), axis=0, tiled=True),
        lax.all_gather(ada_bias, ("dp", "rows"), axis=0, tiled=True),
        lax.all_gather(attn_kernel, ("dp", "rows"), axis=1, tiled=True),
        lax.all_gather(qkv_weight, ("dp", "rows"), axis=0, tiled=True),
        lax.all_gather(out_weight, ("dp", "rows"), axis=0, tiled=True),
        lax.all_gather(up_weight, ("dp", "rows"), axis=0, tiled=True),
        lax.all_gather(ffn_kernel, ("dp", "rows"), axis=1, tiled=True),
        lax.all_gather(down_weight, ("dp", "rows"), axis=0, tiled=True),
    )
    ada_full, bias_full, kernel_attn, triple_full, out_full, up_full, kernel_ffn, down_full = (
        gathered
    )
    hidden_units = up_full.shape[1]
    head_count = features // PER_GROUP_WIDTH
    logit_divisor = PER_GROUP_WIDTH ** (-0.5)
    labels_pad = jnp.pad(item_map, ((0, 0), (1, 1), (1, 1)), constant_values=-1)
    labels_here = lax.dynamic_slice_in_dim(labels_pad, position * rows_here, rows_here + 2, 1)
    centre = labels_here[:, 1:-1, 1:-1]
    cond_values = conditioning.astype(jnp.float32)
    silu_low = jax.nn.silu(cond_values).astype(jnp.bfloat16)
    modulation = jnp.dot(silu_low, ada_full, preferred_element_type=jnp.float32) + bias_full.astype(
        jnp.float32
    )
    layer_stack = modulation.reshape(canvases, 6, 1, 1, features)
    shift_one, scale_one, gate_one, shift_two, scale_two, gate_two = (
        layer_stack[:, index] for index in range(6)
    )
    token_values = tokens.astype(jnp.float32)
    normed_one, inverse_one = normalize(token_values)
    modulated_one = (normed_one * (1.0 + scale_one) + shift_one).astype(jnp.bfloat16)
    modulated_padded = widen_cols(padded(modulated_one, (("rows", 1),), 1))
    local_mix = conv_forward(modulated_padded, labels_here, centre, kernel_attn).astype(
        jnp.bfloat16
    )
    mix_rows = local_mix.reshape(cell_count, features)
    projected = jnp.dot(mix_rows, triple_full, preferred_element_type=jnp.float32).astype(
        jnp.bfloat16
    )
    projected = projected.reshape(canvases, rows_here * cols_here, 3 * features)
    queries = projected[..., :features]
    key_rows = projected[..., features : 2 * features]
    value_rows = projected[..., 2 * features :]
    keys_all, values_all = (
        lax.all_gather(key_rows, "rows", axis=1, tiled=True),
        lax.all_gather(value_rows, "rows", axis=1, tiled=True),
    )
    query_heads = queries.reshape(canvases, -1, head_count, PER_GROUP_WIDTH)
    key_heads = keys_all.reshape(canvases, -1, head_count, PER_GROUP_WIDTH)
    value_heads = values_all.reshape(canvases, -1, head_count, PER_GROUP_WIDTH)
    scores = (
        jnp.einsum("bqhd,bkhd->bhqk", query_heads, key_heads, preferred_element_type=jnp.float32)
        * logit_divisor
    )
    label_rows = centre.reshape(canvases, -1)
    label_keys = item_map.reshape(canvases, -1)
    linked = label_rows[:, None, :, None] == label_keys[:, None, None, :]
    masked = jnp.where(linked, scores, -1e30)
    row_peak = jnp.max(masked, axis=-1, keepdims=True)
    raised = jnp.exp(masked - row_peak)
    row_total = jnp.sum(raised, axis=-1, keepdims=True)
    attention = raised / row_total
    attention_low = attention.astype(jnp.bfloat16)
    attended = jnp.einsum(
        "bhqk,bkhd->bqhd", attention_low, value_heads, preferred_element_type=jnp.float32
    ).astype(jnp.bfloat16)
    attended = attended.reshape(cell_count, features)
    attn_branch = jnp.dot(attended, out_full, preferred_element_type=jnp.float32).reshape(
        tokens.shape
    )
    middle = token_values + gate_one * attn_branch
    normed_two, inverse_two = normalize(middle)
    modulated_two = (normed_two * (1.0 + scale_two) + shift_two).astype(jnp.bfloat16)
    modulated_rows = modulated_two.reshape(cell_count, features)
    hidden_up_projection = jnp.dot(
        modulated_rows, up_full, preferred_element_type=jnp.float32
    ).astype(jnp.bfloat16)
    hidden_up_projection = hidden_up_projection.reshape(
        canvases, rows_here, cols_here, hidden_units
    )
    up_padded = widen_cols(padded(hidden_up_projection, (("rows", 1),), 1))
    pre_gelu = conv_forward(up_padded, labels_here, centre, kernel_ffn)
    activated, gelu_back = jax.vjp(jax.nn.gelu, pre_gelu)
    gelu_low = activated.astype(jnp.bfloat16).reshape(cell_count, hidden_units)
    ffn_branch = jnp.dot(gelu_low, down_full, preferred_element_type=jnp.float32).reshape(
        tokens.shape
    )
    layer_out = (middle + gate_two * ffn_branch).astype(jnp.bfloat16)
    weights_back = (
        lax.all_gather(ada_weight, ("dp", "rows"), axis=0, tiled=True),
        lax.all_gather(ada_bias, ("dp", "rows"), axis=0, tiled=True),
        lax.all_gather(attn_kernel, ("dp", "rows"), axis=1, tiled=True),
        lax.all_gather(qkv_weight, ("dp", "rows"), axis=0, tiled=True),
        lax.all_gather(out_weight, ("dp", "rows"), axis=0, tiled=True),
        lax.all_gather(up_weight, ("dp", "rows"), axis=0, tiled=True),
        lax.all_gather(ffn_kernel, ("dp", "rows"), axis=1, tiled=True),
        lax.all_gather(down_weight, ("dp", "rows"), axis=0, tiled=True),
    )
    (
        ada_back,
        bias_back,
        kernel_attn_back,
        triple_back,
        out_back,
        up_back,
        kernel_ffn_back,
        down_projection_back,
    ) = weights_back
    incoming = out_cotangent.astype(jnp.float32)
    grad_gate_two = jnp.sum(incoming * ffn_branch, axis=(1, 2))
    grad_ffn = (gate_two * incoming).astype(jnp.bfloat16).reshape(cell_count, features)
    grad_down = contract_rows(gelu_low, grad_ffn)
    grad_gelu = contract_cols(grad_ffn, down_projection_back).reshape(
        canvases, rows_here, cols_here, hidden_units
    )
    grad_pre = gelu_back(grad_gelu)[0].astype(jnp.bfloat16)
    grad_pre_padded = widen_cols(padded(grad_pre, (("rows", 1),), 1))
    grad_kernel_ffn = kernel_grad(grad_pre, up_padded, labels_here, centre)
    grad_up = (
        conv_mirror(grad_pre_padded, labels_here, centre, kernel_ffn_back)
        .astype(jnp.bfloat16)
        .reshape(cell_count, hidden_units)
    )
    grad_up_weight = contract_rows(modulated_rows, grad_up)
    grad_mod_two = contract_cols(grad_up, up_back).reshape(tokens.shape)
    grad_scale_two = jnp.sum(grad_mod_two * normed_two, axis=(1, 2))
    grad_shift_two = jnp.sum(grad_mod_two, axis=(1, 2))
    grad_middle = incoming + normalize_back(
        grad_mod_two * (1.0 + scale_two), normed_two, inverse_two
    )
    grad_gate_one = jnp.sum(grad_middle * attn_branch, axis=(1, 2))
    grad_attn = (gate_one * grad_middle).astype(jnp.bfloat16).reshape(cell_count, features)
    grad_out_weight = contract_rows(attended, grad_attn)
    grad_attended = (
        contract_cols(grad_attn, out_back)
        .astype(jnp.bfloat16)
        .reshape(canvases, -1, head_count, PER_GROUP_WIDTH)
    )
    grad_weights = jnp.einsum(
        "bqhd,bkhd->bhqk", grad_attended, value_heads, preferred_element_type=jnp.float32
    )
    row_delta = jnp.sum(attention * grad_weights, axis=-1, keepdims=True)
    grad_scores = (attention * (grad_weights - row_delta)).astype(jnp.bfloat16)
    grad_query = (
        jnp.einsum("bhqk,bkhd->bqhd", grad_scores, key_heads, preferred_element_type=jnp.float32)
        * logit_divisor
    )
    grad_key_all = (
        jnp.einsum("bhqk,bqhd->bkhd", grad_scores, query_heads, preferred_element_type=jnp.float32)
        * logit_divisor
    )
    value_gradient_full = jnp.einsum(
        "bhqk,bqhd->bkhd", attention_low, grad_attended, preferred_element_type=jnp.float32
    )
    grad_key, grad_value = (
        lax.psum_scatter(
            grad_key_all.reshape(canvases, -1, features).astype(jnp.bfloat16),
            "rows",
            scatter_dimension=1,
            tiled=True,
        ).astype(jnp.float32),
        lax.psum_scatter(
            value_gradient_full.reshape(canvases, -1, features).astype(jnp.bfloat16),
            "rows",
            scatter_dimension=1,
            tiled=True,
        ).astype(jnp.float32),
    )
    grad_projected = jnp.concatenate(
        [
            grad_query.reshape(cell_count, features),
            grad_key.reshape(cell_count, features),
            grad_value.reshape(cell_count, features),
        ],
        axis=-1,
    ).astype(jnp.bfloat16)
    grad_qkv_weight = contract_rows(mix_rows, grad_projected)
    grad_mix = contract_cols(grad_projected, triple_back).astype(jnp.bfloat16).reshape(tokens.shape)
    grad_mix_padded = widen_cols(padded(grad_mix, (("rows", 1),), 1))
    grad_kernel_attn = kernel_grad(grad_mix, modulated_padded, labels_here, centre)
    grad_mod_one = conv_mirror(grad_mix_padded, labels_here, centre, kernel_attn_back)
    grad_scale_one = jnp.sum(grad_mod_one * normed_one, axis=(1, 2))
    grad_shift_one = jnp.sum(grad_mod_one, axis=(1, 2))
    token_grad = grad_middle + normalize_back(
        grad_mod_one * (1.0 + scale_one), normed_one, inverse_one
    )
    grad_parts = jnp.concatenate(
        [
            grad_shift_one,
            grad_scale_one,
            grad_gate_one,
            grad_shift_two,
            grad_scale_two,
            grad_gate_two,
        ],
        axis=-1,
    )
    grad_modulation = lax.psum(grad_parts.astype(jnp.bfloat16), "rows")
    leader = (position == 0).astype(jnp.float32)
    grad_ada_weight = contract_rows(silu_low, grad_modulation) * leader
    grad_ada_bias = jnp.sum(grad_modulation.astype(jnp.float32), axis=0) * leader
    silu_values, silu_back = jax.vjp(jax.nn.silu, cond_values)
    derivative_of_context = silu_back(contract_cols(grad_modulation, ada_back))[0]
    summed_grads = (
        lax.psum_scatter(grad_ada_weight, ("dp", "rows"), scatter_dimension=0, tiled=True),
        lax.psum_scatter(grad_ada_bias, ("dp", "rows"), scatter_dimension=0, tiled=True),
        lax.psum_scatter(grad_kernel_attn, ("dp", "rows"), scatter_dimension=1, tiled=True),
        lax.psum_scatter(grad_qkv_weight, ("dp", "rows"), scatter_dimension=0, tiled=True),
        lax.psum_scatter(grad_out_weight, ("dp", "rows"), scatter_dimension=0, tiled=True),
        lax.psum_scatter(grad_up_weight, ("dp", "rows"), scatter_dimension=0, tiled=True),
        lax.psum_scatter(grad_kernel_ffn, ("dp", "rows"), scatter_dimension=1, tiled=True),
        lax.psum_scatter(grad_down, ("dp", "rows"), scatter_dimension=0, tiled=True),
    )
    return (layer_out, token_grad, derivative_of_context) + tuple(summed_grads)


F32=jnp.float32; BF=jnp.bfloat16
NT=(((1,),(1,)),((),()))
TN=(((0,),(0,)),((),()))

def head_masks(labels):
    cells=labels.shape[0]
    lane=lax.broadcasted_iota(jnp.int32,(cells,128),1)%64
    lab=labels[:,None]
    qm=(lane==lab).astype(BF)
    km=jnp.where((lane!=lab)&(lane<4),-1e30,0.0).astype(BF)
    return qm,km

MESH=pl.DeviceIdType.MESH
NZ,NC,NR=4,2,4


def here():
    dp=lax.axis_index("dp"); rows=lax.axis_index("rows")
    return dp//NC, lax.rem(dp,NC), rows


def dev(z,core,rows):
    return (z*NC+core, rows)


def partner_xy(rows,t):
    x=lax.rem(rows,2); y=rows//2
    tx=t%2; ty=t//2
    nx=1-x if tx else x
    ny=1-y if ty else y
    return ny*2+nx


def rcopy(src,dst,ssem,rsem,target):
    return pltpu.make_async_remote_copy(src_ref=src,dst_ref=dst,send_sem=ssem,recv_sem=rsem,device_id=target,device_id_type=MESH)


def barrier_all():
    dp=lax.axis_index("dp"); rows=lax.axis_index("rows")
    me=dp*NR+rows
    total=NZ*NC*NR
    bar=pltpu.get_barrier_semaphore()
    def body(k,c):
        other=lax.rem(me+k,total)
        pl.semaphore_signal(bar,inc=1,device_id=(other//NR,lax.rem(other,NR)),device_id_type=MESH)
        return c
    lax.fori_loop(1,total,body,0)
    pl.semaphore_wait(bar,total-1)


def zmod(v):
    return lax.rem(v+NZ,NZ)


class Gather:
    SEMS=[(NZ,),(NZ,),(NZ,NR),(NZ,NR),(NZ,NR),(NZ,NR),(1,)]

    def __init__(self,shard,full,sems):
        self.shard,self.full=shard,full
        self.sz,self.rz,self.sx,self.rx,self.sc,self.rc,self.lo=sems
        self.z,self.core,self.rows=here()

    def slot(self,dz,t,core):
        rows=self.rows if t==0 else partner_xy(self.rows,t)
        return self.full.at[zmod(self.z-dz),core,rows]

    def zcopy(self,dz,receive=False):
        dst=self.slot(dz if receive else 0,0,self.core)
        return rcopy(self.shard,dst,self.sz.at[dz],self.rz.at[dz],dev(zmod(self.z+dz),self.core,self.rows))

    def piece(self,dz):
        return self.shard if dz==0 else self.slot(dz,0,self.core)

    def xcopy(self,dz,t,receive=False):
        dst=self.slot(dz,t if receive else 0,self.core)
        return rcopy(self.piece(dz),dst,self.sx.at[dz,t],self.rx.at[dz,t],dev(self.z,self.core,partner_xy(self.rows,t)))

    def ccopy(self,dz,t,receive=False):
        src=self.piece(dz) if t==0 else self.slot(dz,t,self.core)
        dst=self.slot(dz,t,1-self.core if receive else self.core)
        return rcopy(src,dst,self.sc.at[dz,t],self.rc.at[dz,t],dev(self.z,1-self.core,self.rows))

    def local(self):
        return pltpu.make_async_copy(self.shard,self.slot(0,0,self.core),self.lo.at[0])

    def start(self):
        for dz in range(1,NZ):
            self.zcopy(dz).start()
        for t in range(1,NR):
            self.xcopy(0,t).start()
        self.ccopy(0,0).start()
        self.local().start()

    def zstep(self,dz):
        self.zcopy(dz,True).wait_recv()
        for t in range(1,NR):
            self.xcopy(dz,t).start()
        self.ccopy(dz,0).start()

    def xstep(self,dz,t):
        self.xcopy(dz,t,True).wait_recv()
        self.ccopy(dz,t).start()

    def finish(self):
        for dz in range(NZ):
            for t in range(NR):
                self.ccopy(dz,t,True).wait_recv()
        for dz in range(1,NZ):
            self.zcopy(dz).wait_send()
        for dz in range(NZ):
            for t in range(NR):
                if t: self.xcopy(dz,t).wait_send()
                self.ccopy(dz,t).wait_send()
        self.local().wait()

    def run_z(self):
        for dz in range(1,NZ): self.zstep(dz)

    def run_x(self):
        for dz in range(NZ):
            for t in range(1,NR): self.xstep(dz,t)


class Scatter:
    SEMS=[(1,),(1,),(1,),(NR,),(NR,),(NZ,),(NZ,)]

    @staticmethod
    def scratch(r,c,dt):
        return [pltpu.VMEM((NZ,NR,r,c),dt),pltpu.VMEM((NZ,NR,r,c),dt),pltpu.VMEM((NR,NZ,r,c),dt),pltpu.VMEM((NZ,r,c),dt),pltpu.VMEM((NZ,r,c),dt)]

    def __init__(self,part,out,bufs,sems):
        self.part,self.out=part,out
        self.own,self.sib,self.xin,self.zout,self.zin=bufs
        self.lo,self.sc,self.rc,self.sx,self.rx,self.sz,self.rz=sems
        self.z,self.core,self.rows=here()
        self.dt=self.own.dtype

    def lcopy(self):
        return pltpu.make_async_copy(self.part.at[:,self.core],self.own,self.lo.at[0])

    def ccopy(self):
        return rcopy(self.part.at[:,1-self.core],self.sib,self.sc.at[0],self.rc.at[0],dev(self.z,1-self.core,self.rows))

    def xcopy(self,t):
        to=partner_xy(self.rows,t)
        return rcopy(self.own.at[:,to],self.xin.at[t],self.sx.at[t],self.rx.at[t],dev(self.z,self.core,to))

    def zcopy(self,dz):
        to=zmod(self.z+dz)
        return rcopy(self.zout.at[to],self.zin.at[dz],self.sz.at[dz],self.rz.at[dz],dev(to,self.core,self.rows))

    def start(self):
        self.ccopy().start(); self.lcopy().start()

    def cstep(self):
        self.lcopy().wait(); self.ccopy().wait_recv()
        def body(i,c):
            a,b=i//NR,lax.rem(i,NR)
            self.own[a,b]=(self.own[a,b].astype(F32)+self.sib[a,b].astype(F32)).astype(self.dt)
            return c
        lax.fori_loop(0,NZ*NR,body,0)
        for t in range(1,NR): self.xcopy(t).start()

    def xstep(self):
        for t in range(1,NR): self.xcopy(t).wait_recv()
        def body(a,c):
            s=self.own[a,self.rows].astype(F32)
            for t in range(1,NR): s=s+self.xin[t,a].astype(F32)
            self.zout[a]=s.astype(self.dt)
            return c
        lax.fori_loop(0,NZ,body,0)
        for dz in range(1,NZ): self.zcopy(dz).start()

    def zstep(self):
        for dz in range(1,NZ): self.zcopy(dz).wait_recv()
        s=self.zout[self.z].astype(F32)
        for dz in range(1,NZ): s=s+self.zin[dz].astype(F32)
        if callable(self.out): self.out(s)
        else: self.out[...]=s

    def finish(self):
        self.ccopy().wait_send()
        for t in range(1,NR): self.xcopy(t).wait_send()
        for dz in range(1,NZ): self.zcopy(dz).wait_send()


class Swap:
    SEMS=[(NR,),(NR,),(1,)]
    def __init__(self,src,dst,sems):
        self.src,self.dst=src,dst
        self.s,self.r,self.lo=sems
        self.z,self.core,self.rows=here()
    def copy(self,t,receive=False):
        to=partner_xy(self.rows,t)
        return rcopy(self.src.at[to],self.dst.at[to if receive else self.rows],self.s.at[t],self.r.at[t],dev(self.z,self.core,to))
    def local(self):
        return pltpu.make_async_copy(self.src.at[self.rows],self.dst.at[self.rows],self.lo.at[0])
    def start(self):
        for t in range(1,NR): self.copy(t).start()
        self.local().start()
    def wait(self):
        for t in range(1,NR): self.copy(t,True).wait_recv()
        self.local().wait()
    def finish(self):
        for t in range(1,NR): self.copy(t).wait_send()


class AllToAll:
    N=NZ*NC*NR
    SEMS=[(N,),(N,),(1,)]
    def __init__(self,src,dst,sems,one=False):
        self.src,self.dst,self.one=src,dst,one
        self.s,self.r,self.lo=sems
        self.me=lax.axis_index("dp")*NR+lax.axis_index("rows")
    def piece(self,n):
        return self.src if self.one else self.src.at[n]
    def copy(self,k,receive=False):
        to=lax.rem(self.me+k,self.N)
        frm=lax.rem(self.me-k+self.N,self.N)
        return rcopy(self.piece(to),self.dst.at[frm if receive else self.me],self.s.at[k],self.r.at[k],(to//NR,lax.rem(to,NR)))
    def local(self):
        return pltpu.make_async_copy(self.piece(self.me),self.dst.at[self.me],self.lo.at[0])
    def each(self,fn):
        def body(k,c):
            fn(k); return c
        lax.fori_loop(1,self.N,body,0)
    def start(self):
        self.each(lambda k:self.copy(k).start())
        self.local().start()
    def wait(self):
        self.each(lambda k:self.copy(k,True).wait_recv())
        self.local().wait()
    def finish(self):
        self.each(lambda k:self.copy(k).wait_send())


def sem_types(shapes):
    return [pltpu.SemaphoreType.DMA(s) for s in shapes]
class GatherZ:
    SEMS=[(NZ,),(NZ,),(1,)]
    def __init__(self,shard,zp,sems):
        self.shard,self.zp=shard,zp
        self.s,self.r,self.lo=sems
        self.z,self.core,self.rows=here()
    def copy(self,dz,receive=False):
        to=zmod(self.z+dz)
        frm=zmod(self.z-dz)
        return rcopy(self.shard,self.zp.at[frm if receive else self.z],self.s.at[dz],self.r.at[dz],dev(to,self.core,self.rows))
    def local(self):
        return pltpu.make_async_copy(self.shard,self.zp.at[self.z],self.lo.at[0])
    def start(self):
        for dz in range(1,NZ): self.copy(dz).start()
        self.local().start()
    def wait(self):
        for dz in range(1,NZ): self.copy(dz,True).wait_recv()
    def finish(self):
        for dz in range(1,NZ): self.copy(dz).wait_send()
        self.local().wait()


class GatherXY:
    SEMS=[(NZ,NR),(NZ,NR),(NZ,NR),(NZ,NR),(1,)]
    def __init__(self,zp,full,sems):
        self.zp,self.full=zp,full
        self.sx,self.rx,self.sc,self.rc,self.lo=sems
        self.z,self.core,self.rows=here()
    def place(self,t):
        return self.rows if t==0 else partner_xy(self.rows,t)
    def to(self,t):
        return dev(self.z,self.core,self.place(t))
    def xcopy(self,k,t,receive=False):
        return rcopy(self.zp.at[k],self.full.at[k,self.core,self.place(t) if receive else self.rows],self.sx.at[k,t],self.rx.at[k,t],self.to(t))
    def fcopy(self,k,receive=False):
        t=1 if k<NZ//2 else 2
        ref=self.full.at[k,self.core,self.place(3 if receive else t)]
        return rcopy(ref,ref,self.sx.at[k,3],self.rx.at[k,3],self.to(3-t))
    def ccopy(self,k,t,receive=False):
        src=self.zp.at[k] if t==0 else self.full.at[k,self.core,self.place(t)]
        dst=self.full.at[k,1-self.core if receive else self.core,self.place(t)]
        return rcopy(src,dst,self.sc.at[k,t],self.rc.at[k,t],dev(self.z,1-self.core,self.rows))
    def local(self):
        return pltpu.make_async_copy(self.zp,self.full.at[:,self.core,self.rows],self.lo.at[0])
    def start(self,ks=range(NZ)):
        for k in ks:
            for t in (1,2): self.xcopy(k,t).start()
            self.ccopy(k,0).start()
    def start_local(self):
        self.local().start()
    def step(self,k):
        order=(1,2) if k<NZ//2 else (2,1)
        self.xcopy(k,order[0],True).wait_recv()
        self.fcopy(k).start()
        self.ccopy(k,order[0]).start()
        self.xcopy(k,order[1],True).wait_recv()
        self.ccopy(k,order[1]).start()
    def step2(self,k):
        self.fcopy(k,True).wait_recv()
        self.ccopy(k,3).start()
    def arrive(self,k):
        for t in range(NR): self.ccopy(k,t,True).wait_recv()
    def finish_remote(self):
        for k in range(NZ):
            for t in (1,2): self.xcopy(k,t).wait_send()
            self.fcopy(k).wait_send()
            for t in range(NR): self.ccopy(k,t).wait_send()
    def finish(self):
        self.finish_remote()
        self.local().wait()


class GatherTile:
    def __init__(self,zp,full,width,sems):
        self.zp,self.full,self.width=zp,full,width
        self.sx,self.rx,self.sc,self.rc,self.lo=sems
        self.z,self.core,self.rows=here()
    @staticmethod
    def sems(tiles):
        return [(tiles,NR),(tiles,NR),(tiles,NR),(tiles,NR),(1,)]
    def cols(self,i): return pl.ds(pl.multiple_of(i*self.width,128),self.width)
    def place(self,t):
        return self.rows if t==0 else partner_xy(self.rows,t)
    def to(self,t):
        return dev(self.z,self.core,self.place(t))
    def xcopy(self,i,t,receive=False):
        return rcopy(self.zp.at[:,:,self.cols(i)],self.full.at[:,self.core,self.place(t) if receive else self.rows,:,self.cols(i)],self.sx.at[i,t],self.rx.at[i,t],self.to(t))
    def fcopy(self,i,t,receive=False):
        h=NZ//2
        ref=self.full.at[pl.ds(0 if t==1 else h,h),self.core,self.place(3 if receive else t),:,self.cols(i)]
        q=3 if t==1 else 0
        return rcopy(ref,ref,self.sx.at[i,q],self.rx.at[i,q],self.to(3-t))
    def ccopy(self,i,t,receive=False):
        src=self.zp.at[:,:,self.cols(i)] if t==0 else self.full.at[:,self.core,self.place(t),:,self.cols(i)]
        dst=self.full.at[:,1-self.core if receive else self.core,self.place(t),:,self.cols(i)]
        return rcopy(src,dst,self.sc.at[i,t],self.rc.at[i,t],dev(self.z,1-self.core,self.rows))
    def local(self):
        return pltpu.make_async_copy(self.zp,self.full.at[:,self.core,self.rows],self.lo.at[0])
    def start(self,i):
        for t in (1,2): self.xcopy(i,t).start()
        self.ccopy(i,0).start()
    def step(self,i):
        for t in (1,2):
            self.xcopy(i,t,True).wait_recv()
            self.fcopy(i,t).start()
            self.ccopy(i,t).start()
    def step2(self,i):
        for t in (1,2): self.fcopy(i,t,True).wait_recv()
        self.ccopy(i,3).start()
    def arrive(self,i):
        for t in range(NR): self.ccopy(i,t,True).wait_recv()
    def finish_remote(self,i):
        for t in (1,2):
            self.xcopy(i,t).wait_send()
            self.fcopy(i,t).wait_send()
        for t in range(NR): self.ccopy(i,t).wait_send()


class ScatterZ:
    SEMS=[(NZ,),(NZ,)]
    @staticmethod
    def scratch(r,c,dt):
        return [pltpu.VMEM((NZ,r,c),dt)]
    def __init__(self,zout,out,bufs,sems):
        self.zout,self.out=zout,out
        self.zin,=bufs
        self.s,self.r=sems
        self.z,self.core,self.rows=here()
    def copy(self,dz):
        to=zmod(self.z+dz)
        return rcopy(self.zout.at[to],self.zin.at[dz],self.s.at[dz],self.r.at[dz],dev(to,self.core,self.rows))
    def start(self):
        for dz in range(1,NZ): self.copy(dz).start()
    def step(self):
        for dz in range(1,NZ): self.copy(dz).wait_recv()
        v=self.zout[self.z].astype(F32)
        for dz in range(1,NZ): v=v+self.zin[dz].astype(F32)
        if callable(self.out): self.out(v)
        else: self.out[...]=v
    def finish(self):
        for dz in range(1,NZ): self.copy(dz).wait_send()


class Events:
    def __init__(self): self.at={}
    def add(self,slot,fn): self.at.setdefault(slot,[]).append(fn)
    def run(self,outer,inner,width):
        for slot,fns in self.at.items():
            if slot%width==inner:
                @pl.when(outer==slot//width)
                def _(fns=fns):
                    for fn in fns: fn()
NN=(((1,),(0,)),((),()))
C0=0.7978845608028654
C1=0.044715


def dotf(a,b,dims=NN):
    return lax.dot_general(a,b,dims,preferred_element_type=F32)


def loop(n,fn,unroll=1):
    def body(i,c):
        fn(i); return c
    lax.fori_loop(0,n,body,0,unroll=unroll)


def rows_of(i,n):
    return pl.ds(pl.multiple_of(i*n,n),n)


def normal_rows(v):
    d=1.0/v.shape[1]
    c=v-jnp.sum(v,axis=1,keepdims=True)*d
    inv=lax.rsqrt(jnp.sum(c*c,axis=1,keepdims=True)*d+EPSILON)
    return c*inv,inv


def normal_back_rows(g,n,inv):
    d=1.0/g.shape[1]
    return inv*(g-jnp.sum(g,axis=1,keepdims=True)*d-n*(jnp.sum(g*n,axis=1,keepdims=True)*d))


def fold8(v):
    s=v[0:8]
    for k in range(1,v.shape[0]//8): s=s+v[8*k:8*k+8]
    return s


def conv_loops(side,lanes_n,width,forward,finish):
    pass


def shifts(f,ml,mr):
    n=f.shape[0]
    return pltpu.roll(f,1,0)*ml, pltpu.roll(f,n-1,0)*mr


def conv_rows(src,dst_fn,taps,ml_ref,mr_ref,rl_ref,ls,side,cols):
    k=[taps[q:q+1,:] for q in range(9)]
    zero=jnp.zeros((cols,128),F32)
    def body(i,c):
        hm,part=c
        f=src[rows_of(i,cols),ls]
        fm,fp=shifts(f,ml_ref[rows_of(i,cols),:],mr_ref[rows_of(i,cols),:])
        h=[k[3*a]*fm+k[3*a+1]*f+k[3*a+2]*fp for a in range(3)]
        done=part+rl_ref[i]*h[2]
        @pl.when(i>0)
        def _(): dst_fn(i-1,done)
        return h[0],h[1]+rl_ref[i]*hm
    hm,part=lax.fori_loop(0,side,body,(zero,zero),unroll=8)
    dst_fn(side-1,part)


def back_rows(g_ref,f_ref,dst_fn,taps,ml_ref,mr_ref,rl_ref,ls,first,count,side,cols):
    k=[taps[q:q+1,:] for q in range(9)]
    z8=jnp.zeros((8,128),F32)
    def at(i): return rows_of(i,cols)
    def load(i):
        g=g_ref[at(i),ls]
        gm,gp=shifts(g,ml_ref[at(i),:],mr_ref[at(i),:])
        return gp,g,gm
    def mix3(gs,a): return k[3*a]*gs[0]+k[3*a+1]*gs[1]+k[3*a+2]*gs[2]
    whole=isinstance(first,int) and count==side
    zero=jnp.zeros((cols,128),F32)
    before=jnp.maximum(first-1,0)
    hp=zero if whole else mix3(load(before),2)
    fprev=zero if whole else f_ref[at(before),ls].astype(F32)
    def body(n,c):
        hp,part,fprev,acc=c
        i=first+n
        gs=load(i)
        done=part+rl_ref[i]*mix3(gs,0)
        @pl.when(n>0)
        def _(): dst_fn(i-1,done)
        f=f_ref[at(i),ls].astype(F32)
        nxt=f_ref[at(jnp.minimum(i+1,side-1)),ls].astype(F32)
        fs=(fprev*rl_ref[i],f,nxt*rl_ref[i+1])
        acc=tuple(acc[3*a+b]+fold8(fs[a]*gs[b]) for a in range(3) for b in range(3))
        return mix3(gs,2),mix3(gs,1)+rl_ref[i]*hp,f,acc
    hp,part,_,acc=lax.fori_loop(0,count,body,(hp,zero,fprev,(z8,)*9),unroll=8)
    end=first+count
    if not whole: part=part+rl_ref[end]*mix3(load(jnp.minimum(end,side-1)),0)
    dst_fn(end-1,part)
    return acc


def link_masks(labels):
    side,cols=labels.shape
    left=jnp.pad(labels[:,1:]==labels[:,:-1],((0,0),(1,0)))
    right=jnp.pad(labels[:,1:]==labels[:,:-1],((0,0),(0,1)))
    wide=lambda m: jnp.broadcast_to(m.reshape(side*cols,1).astype(F32),(side*cols,128))
    top=labels[:,0]//2
    rl=jnp.pad((top[1:]==top[:-1]).astype(F32),(1,1))
    return wide(left),wide(right),rl
HBM=pl.BlockSpec(memory_space=pl.ANY)
VM=pl.BlockSpec(memory_space=pltpu.VMEM)
SM=pl.BlockSpec(memory_space=pltpu.SMEM)
NDEV=NZ*NC*NR
S_=jax.ShapeDtypeStruct


def taker(it):
    return lambda cls:[next(it) for _ in cls.SEMS]


def assemble(dst,src,width,at):
    lane=lax.broadcasted_iota(jnp.int32,(1,128),1)
    tiles=dst.shape[1]//128
    for c in range(tiles):
        v=jnp.zeros((16,128),F32)
        for n in range(NDEV):
            lo=n*width-c*128
            if lo+width<=0 or lo>=128: continue
            p=src[n//(NC*NR),(n//NR)%NC,n%NR].astype(F32)
            sh=(lo-at)%128
            if sh: p=pltpu.roll(p,sh,1)
            v=jnp.where((lane>=lo)&(lane<lo+width),p,v)
        dst[:,c*128:(c+1)*128]=v


def enter_kernel(n_z,side,cols,ta,tf,*refs):
    it=iter(refs)
    nx=lambda n:[next(it) for _ in range(n)]
    tok,cond,ada,bias,qkv,taps,ml_ref,mr_ref,rl_ref=nx(9)
    shards=nx(n_z)
    tok_o,cond_o,mod_o,qkv_o,tap_a,tap_f,m1,mix=nx(8)
    zps=nx(n_z)
    condv,part,zq,taps_o,modw,F=nx(6)
    mbufs=nx(5)
    take=taker(it)
    c_all=AllToAll(cond,condv,take(AllToAll),one=True)
    swap_t=Swap(tok,tok_o,take(Swap))
    m_all=Scatter(part,mod_o,mbufs,take(Scatter))
    g_taps=Gather(taps,taps_o,take(Gather))
    gq_z=GatherZ(qkv,zq,take(GatherZ))
    gq=GatherXY(zq,qkv_o,take(GatherXY))
    gz=[GatherZ(s,z,take(GatherZ)) for s,z in zip(shards,zps)]
    barrier_all()
    c_all.start()
    gq_z.start()
    swap_t.copy(1).start(); swap_t.copy(2).start(); swap_t.local().start()
    c_all.wait()
    me=c_all.me
    feats=ada.shape[0]
    cv=condv[:,0,:].astype(F32)
    low=(cv/(1.0+jnp.exp(-cv))).astype(BF)
    width=cv.shape[1]
    pick=(lax.broadcasted_iota(jnp.int32,(width,feats),0)==lax.broadcasted_iota(jnp.int32,(width,feats),1)+feats*me).astype(BF)
    mine=jnp.dot(low,pick,preferred_element_type=F32).astype(BF)
    chunk=768
    for c in range(ada.shape[1]//chunk):
        pr=jnp.dot(mine,ada[:,c*chunk:(c+1)*chunk],preferred_element_type=F32)
        for l in range(chunk//128):
            i=c*(chunk//128)+l
            part[:,:,:,i,:]=(pr[:,l*128:(l+1)*128]+bias[i:i+1,:]).reshape(NZ,NC,NR,128)
    cond_o[...]=low
    m_all.start()
    m_all.cstep()
    g_taps.start()
    swap_t.copy(3).start()
    g_taps.run_z()
    gq_z.wait(); gq_z.local().wait()
    gq.start(); gq.start_local()
    m_all.xstep()
    for g in gz: g.start()
    m_all.zstep()
    g_taps.run_x()
    cells,feat=mix.shape
    L=feat//128
    for j in range(2):
        for l in range(L): modw[j:j+1,l*128:(l+1)*128]=mod_o[j*L+l:j*L+l+1,:]
    swap_t.wait()
    shift1=modw[0:1,:]; scale1=modw[1:2,:]
    EC=256
    for b in range(NR):
        n,_=normal_rows(tok_o[b].astype(F32))
        v=(n*(1.0+scale1)+shift1).astype(BF)
        m1[b*EC:(b+1)*EC,:]=v
        F[b*EC:(b+1)*EC,:]=v.astype(F32)
    g_taps.finish()
    assemble(tap_a,taps_o,ta,0)
    assemble(tap_f,taps_o,tf,ta)
    def lanes(l):
        ls=pl.ds(pl.multiple_of(l*128,128),128)
        def put(i,u): mix[rows_of(i,cols),ls]=u.astype(BF)
        conv_rows(F,put,tap_a[:,ls],ml_ref,mr_ref,rl_ref,ls,side,cols)
    for i in range(L):
        if i>=1 and i-1<NZ: gq.step(i-1)
        if i>=L-2: gq.step2(i-L+2)
        lanes(i)
    for k in range(2,NZ): gq.step2(k)
    for g in gz: g.wait()
    for k in range(NZ): gq.arrive(k)
    gq.finish()
    for dz in range(1,NZ): gq_z.copy(dz).wait_send()
    for g in [swap_t,c_all,m_all]+gz: g.finish()


def enter(tok,cond_row,ada,bias_rows,qkv,taps,ml,mr,rl,shards,side,cols,ta,tf):
    n=len(shards)
    V=pltpu.VMEM
    feat=tok.shape[2]; cells=side*cols
    scr=[V((NDEV,)+cond_row.shape,cond_row.dtype),V((NZ,NC,NR)+bias_rows.shape,F32),V((NZ,)+qkv.shape,BF),V((NZ,NC,NR)+taps.shape,BF),V((8,feat),F32),V((cells,feat),F32)]+Scatter.scratch(bias_rows.shape[0],128,F32)
    sems=sem_types(AllToAll.SEMS)+sem_types(Swap.SEMS)+sem_types(Scatter.SEMS)+sem_types(Gather.SEMS)+sem_types(GatherZ.SEMS)+sem_types(GatherXY.SEMS)+sem_types(GatherZ.SEMS)*n
    outs=[S_(tok.shape,tok.dtype),S_((NDEV,cond_row.shape[1]),BF),S_(bias_rows.shape,F32),S_((NZ,NC,NR)+qkv.shape,qkv.dtype),
          S_((16,NDEV*ta),F32),S_((16,NDEV*tf),F32),S_((cells,feat),BF),S_((cells,feat),BF)]
    outs+=[S_((NZ,)+s.shape,s.dtype) for s in shards]
    return pl.pallas_call(
        functools.partial(enter_kernel,n,side,cols,ta,tf),
        in_specs=[VM,HBM,VM,VM,VM,VM,VM,VM,SM]+[VM]*n,
        out_specs=[VM,VM,VM,HBM,VM,VM,VM,VM]+[HBM]*n,
        out_shape=outs,
        scratch_shapes=scr+sems,
        compiler_params=pltpu.CompilerParams(collective_id=0,has_side_effects=True,vmem_limit_bytes=63<<20),
        name="enter",
    )(tok,cond_row,ada,bias_rows,qkv,taps,ml,mr,rl,*shards)


def forward_kernel(n_w,qb,*refs):
    it=iter(refs)
    mix,qkv,qm,km,cot,late,late2=[next(it) for _ in range(7)]
    zps=[next(it) for _ in range(n_w)]
    proj,att,lse_t,cot_o,late_o,late2_o=[next(it) for _ in range(6)]
    fulls=[next(it) for _ in range(n_w)]
    lse=next(it)
    take=taker(it)
    barrier_all()
    swap_c=Swap(cot,cot_o,take(Swap))
    gs=[GatherXY(a,b,take(GatherXY)) for a,b in zip(zps,fulls)]
    gl=GatherZ(late,late_o,take(GatherZ))
    gl2=GatherZ(late2,late2_o,take(GatherZ))
    gs[0].start(); gs[0].start_local()
    gl2.start(); gl.start()
    swap_c.start()
    ev=Events()
    for k in range(NZ):
        ev.add(2,lambda k=k: gs[0].step(k))
        ev.add(9,lambda k=k: gs[0].step2(k))
    cells,feat=att.shape
    CH=512
    def pr(i):
        proj[rows_of(i,CH),:]=dotf(mix[rows_of(i,CH),:],qkv[...]).astype(BF)
    loop(cells//CH,pr)
    pairs=feat//128
    lane=lax.broadcasted_iota(jnp.int32,(1,128),1)
    lse[...]=jnp.zeros_like(lse)
    def pair(p):
        cq=pl.ds(pl.multiple_of(p*128,128),128)
        ck=pl.ds(pl.multiple_of(feat+p*128,128),128)
        cv=pl.ds(pl.multiple_of(2*feat+p*128,128),128)
        for h in range(2):
            ev.run(p,h,2)
            mine=(lane//64)==h
            k=jnp.where(mine,proj[:,ck],km[...])
            def body(i):
                r=rows_of(i,qb)
                q=jnp.where(mine,proj[r,cq]*jnp.asarray(0.125,BF),qm[r,:])
                s=dotf(q,k,NT)
                m=jnp.max(s,axis=1,keepdims=True)
                e=jnp.exp(s-m)
                l=jnp.sum(e,axis=1,keepdims=True)
                a=(e*(1.0/l)).astype(BF)
                o=dotf(a,proj[:,cv]).astype(BF)
                if h==0:
                    att[r,cq]=o
                else:
                    att[r,cq]=jnp.where(mine,o,att[r,cq])
                lse[r,:]=jnp.where(lane==2*p+h,m+jnp.log(l),lse[r,:])
            loop(cells//qb,body,2)
    loop(pairs,pair)
    lse_t[...]=jnp.transpose(lse[...])
    for g in gs:
        for k in range(NZ): g.arrive(k)
    swap_c.wait()
    gl.wait(); gl2.wait()
    for g in gs+[swap_c,gl,gl2]: g.finish()


def forward(mix,qkv,qm,km,cot,late,late2,zps):
    n=len(zps)
    cells,feat=mix.shape
    outs=[S_((cells,3*feat),BF),S_((cells,feat),BF),S_((128,cells),F32),S_(cot.shape,cot.dtype),S_((NZ,)+late.shape,late.dtype),S_((NZ,)+late2.shape,late2.dtype)]
    outs+=[S_((NZ,NC,NR)+z.shape[1:],z.dtype) for z in zps]
    return pl.pallas_call(
        functools.partial(forward_kernel,n,512),
        in_specs=[VM,VM,VM,VM,VM,VM,VM]+[VM]*n,
        out_specs=[VM,VM,VM,HBM,HBM,HBM]+[HBM]*n,
        out_shape=outs,
        scratch_shapes=[pltpu.VMEM((cells,128),F32)]+sem_types(Swap.SEMS)+sem_types(GatherXY.SEMS)*n+sem_types(GatherZ.SEMS)*2,
        compiler_params=pltpu.CompilerParams(collective_id=1,has_side_effects=True,vmem_limit_bytes=63<<20),
        name="attn_fwd",
    )(mix,qkv,qm,km,cot,late,late2,*zps)


def backward_kernel(n_g,kb,*refs):
    it=iter(refs)
    nx=lambda n:[next(it) for _ in range(n)]
    proj,do,o,qm,km,lse_t,mix,lay,gout=nx(9)
    parts=nx(n_g)
    gp,lay_o,gout_o,zq,lastq=nx(5)
    gouts=nx(n_g)
    qs,dqt,mixt=nx(3)
    obufs=nx(5)
    qbufs=nx(4)
    bufs=[nx(1) for _ in range(n_g)]
    take=taker(it)
    barrier_all()
    sl=Swap(lay,lay_o,take(Swap))
    so=Scatter(gout,gout_o,obufs,take(Scatter))
    uq=PipeScatter(qbufs,take(PipeScatter))
    sc=[ScatterZ(p,g,b,take(ScatterZ)) for p,g,b in zip(parts,gouts,bufs)]
    cells,feat=do.shape
    pairs=feat//128
    W=256
    tiles=pairs//2
    r_=feat//NDEV
    def put_q(m):
        def put(a,v):
            for s in range(3):
                zq[a,:,(s*(tiles-1)+m)*W:(s*(tiles-1)+m+1)*W]=v[:,s*W:(s+1)*W]
        return put
    ev=Events()
    so.start()
    for s in sc: s.start()
    ev.add(1,so.cstep)
    ev.add(2,sl.start)
    ev.add(5,lambda: uq.send_square(0))
    ev.add(6,so.xstep)
    for s in sc: ev.add(7,s.step)
    ev.add(8,lambda: uq.collect(0,put_q(0)))
    ev.add(9,lambda: uq.send_square(1))
    ev.add(11,so.zstep)
    lane=lax.broadcasted_iota(jnp.int32,(1,128),1)
    srow=lax.broadcasted_iota(jnp.int32,(8,128),0)
    slane=lax.broadcasted_iota(jnp.int32,(8,128),1)
    sel=(slane//64==srow).astype(BF)
    def tr(i):
        mixt[:,pl.ds(pl.multiple_of(i*256,256),256)]=jnp.transpose(mix[rows_of(i,256),:])
    loop(cells//256,tr)
    def pair(p):
        cq=pl.ds(pl.multiple_of(p*128,128),128)
        ck=pl.ds(pl.multiple_of(feat+p*128,128),128)
        cv=pl.ds(pl.multiple_of(2*feat+p*128,128),128)
        prod=do[:,cq].astype(F32)*o[:,cq].astype(F32)
        hi=prod.astype(BF); lo=(prod-hi.astype(F32)).astype(BF)
        delta=dotf(sel,hi,NT)+dotf(sel,lo,NT)
        qs[...]=proj[:,cq]*jnp.asarray(0.125,BF)
        for h in range(2):
            ev.run(p,h,2)
            mine=(lane//64)==h
            q=jnp.where(mine,qs[...],qm[...])
            ls=lse_t[pl.ds(2*p+h,1),:]
            dl=delta[h:h+1,:]
            dqt[...]=jnp.zeros_like(dqt)
            def body(i):
                r=rows_of(i,kb)
                kr=proj[r,ck]
                k=jnp.where(mine,kr,km[r,:])
                v=jnp.where(mine,proj[r,cv],jnp.zeros((),BF))
                st=dotf(k,q,NT)
                pt=jnp.exp(st-ls)
                dpt=dotf(v,do[:,cq],NT)
                ds=(pt*(dpt-dl)).astype(BF)
                dv=dotf(pt.astype(BF),do[:,cq]).astype(BF)
                dk=dotf(ds,qs[...]).astype(BF)
                dqt[...]+=dotf(kr,ds,TN)
                if h==0:
                    gp[r,cv]=dv
                    gp[r,ck]=dk
                else:
                    gp[r,cv]=jnp.where(mine,dv,gp[r,cv])
                    gp[r,ck]=jnp.where(mine,dk,gp[r,ck])
            loop(cells//kb,body,2)
            dq=(jnp.transpose(dqt[...])*0.125).astype(BF)
            if h==0:
                gp[:,cq]=dq
            else:
                gp[:,cq]=jnp.where(mine,dq,gp[:,cq])
        @pl.when(lax.rem(p,2)==1)
        def _():
            m=p//2
            s=lax.rem(m,2)
            n=NC*NR*r_
            def tile(i):
                for c in range(3):
                    cols=pl.ds(pl.multiple_of(c*feat+m*W,W),W)
                    uq.part[s,i,:,:,:,c*W:(c+1)*W]=dotf(mixt[rows_of(i,n),:],gp[:,cols]).astype(BF).reshape(NC,NR,r_,W)
            loop(NZ,tile)
            @pl.when(m<tiles-1)
            def _(): uq.send_core(s)
    loop(pairs,pair)
    uq.collect(1,put_q(1))
    lastq[...]=uq.part[0]
    sl.wait()
    for s in sc+[sl,so]: s.finish()


def backward(proj,do,o,qm,km,lse_t,mix,lay,gout,parts):
    n=len(parts)
    cells,feat=do.shape
    r_=feat//NDEV
    outs=[S_((cells,3*feat),BF),S_(lay.shape,lay.dtype),S_(gout.shape[3:],F32),S_((NZ,r_,2*feat),BF),S_((NZ,NC,NR,r_,feat),BF)]+[S_(p.shape[1:],F32) for p in parts]
    scr=[pltpu.VMEM((cells,128),BF),pltpu.VMEM((128,cells),F32),pltpu.VMEM((feat,cells),BF)]
    scr+=Scatter.scratch(gout.shape[3],gout.shape[4],gout.dtype)+PipeScatter.scratch(r_,feat)
    for p in parts: scr+=ScatterZ.scratch(p.shape[1],p.shape[2],p.dtype)
    return pl.pallas_call(
        functools.partial(backward_kernel,n,512),
        in_specs=[VM,VM,VM,VM,VM,VM,VM,VM,HBM]+[VM]*n,
        out_specs=[VM,HBM,VM,VM,VM]+[VM]*n,
        out_shape=outs,
        scratch_shapes=scr+sem_types(Swap.SEMS)+sem_types(Scatter.SEMS)+sem_types(PipeScatter.SEMS)+sem_types(ScatterZ.SEMS)*n,
        compiler_params=pltpu.CompilerParams(collective_id=2,has_side_effects=True,vmem_limit_bytes=63<<20),
        name="attn_bwd",
    )(proj,do,o,qm,km,lse_t,mix,lay,gout,*parts)


def spread(dst,src_ref,width,at):
    lane=lax.broadcasted_iota(jnp.int32,(1,128),1)
    for n in range(NDEV):
        lo=n*width
        c,off=lo//128,lo%128
        sh=(at-off)%128
        v=src_ref[:,c*128:(c+1)*128]
        v=pltpu.roll(v,sh,1) if sh else v
        if off+width>128:
            w=src_ref[:,(c+1)*128:(c+2)*128]
            w=pltpu.roll(w,sh,1) if sh else w
            v=jnp.where(lane<at+128-off,v,w)
        keep=(lane>=at)&(lane<at+width)
        i=(n//(NC*NR),(n//NR)%NC,n%NR)
        if at==0: dst[i]=jnp.where(keep,v,0.0)
        else: dst[i]=jnp.where(keep,v,dst[i])


def tail_kernel(side,cols,ta,tf,*refs):
    it=iter(refs)
    nx=lambda n:[next(it) for _ in range(n)]
    gproj,qkv,m1,x_ref,gmid,mod,tap_ref,ml_ref,mr_ref,rl_ref,sums,gkf,low,ada,zq,lastq=nx(16)
    tg_o,ctx_o,adag_o,gm_o,q_o,ka_o,kf_o=nx(7)
    G,gm1,tgb,tgin,ktap,gme,gml,gmev,gmlv,ctxs,ctxv,tpart=nx(12)
    zbufs=nx(1); lbufs=nx(5); tbufs=nx(5)
    take=taker(it)
    barrier_all()
    def put_z(v):
        n=v.shape[1]//3
        for s in range(3): q_o[:,s*n*3//2:s*n*3//2+n]=v[:,s*n:(s+1)*n]
    def put_l(v):
        n=v.shape[1]//3
        for s in range(3): q_o[:,(3*s+2)*n:(3*s+3)*n]=v[:,s*n:(s+1)*n]
    def put_t(v):
        ka_o[...]=v[0:9,0:ta]
        kf_o[...]=pltpu.roll(v,128-ta,1)[0:9,0:tf]
    sz=ScatterZ(zq,put_z,zbufs,take(ScatterZ))
    slq=Scatter(lastq,put_l,lbufs,take(Scatter))
    stp=Scatter(tpart,put_t,tbufs,take(Scatter))
    st=Swap(tgb,tgin,take(Swap))
    ge=AllToAll(gme,gmev,take(AllToAll),one=True)
    gl=AllToAll(gml,gmlv,take(AllToAll),one=True)
    xa=AllToAll(ctxs,ctxv,take(AllToAll))
    slq.start(); sz.start()
    cells,feat=x_ref.shape
    L=feat//128
    for i,q in enumerate((3,1,2,0)):
        for l in range(L):
            gme[i*L+l:i*L+l+1,:]=sums[q:q+1,l*128:(l+1)*128].astype(BF)
    ge.start()
    CH=1024; EC=256
    def a(i):
        r=rows_of(i,CH)
        G[r,:]=dotf(gproj[r,:],qkv[...],NT).astype(BF).astype(F32)
    loop(cells//CH,a)
    slq.cstep()
    ktap[...]=jnp.zeros_like(ktap)
    shift1=mod[0:1,:]; scale1=mod[1:2,:]
    z8=jnp.zeros((8,feat),F32)
    block=cells//NR
    c=(z8,z8)
    per=side//NR
    for t in (3,1,2,0):
        to=partner_xy(st.rows,t) if t else st.rows
        def lanes(l):
            ls=pl.ds(pl.multiple_of(l*128,128),128)
            def put(i,u): gm1[rows_of(i,cols),ls]=u
            acc=back_rows(G,m1,put,tap_ref[:,ls],ml_ref,mr_ref,rl_ref,ls,to*per,per,side,cols)
            for q in range(9): ktap[q:q+1,ls]+=jnp.sum(acc[q],axis=0,keepdims=True)
        loop(L,lanes)
        r=rows_of(to,block)
        n,inv=normal_rows(x_ref[r,:].astype(F32))
        g=gm1[r,:]
        tgb[to]=(gmid[r,:]+normal_back_rows(g*(1.0+scale1),n,inv)).astype(BF)
        c=(c[0]+fold8(g),c[1]+fold8(g*n))
        if t: st.copy(t).start()
        else: st.local().start()
        if t==1: slq.xstep()
    spread(tpart,ktap,ta,0)
    spread(tpart,gkf,tf,ta)
    stp.start()
    for i,v in enumerate(c):
        v=jnp.sum(v,axis=0,keepdims=True)
        for l in range(L): gml[i*L+l:i*L+l+1,:]=v[:,l*128:(l+1)*128].astype(BF)
    gml[2*L:16,:]=jnp.zeros((16-2*L,128),BF)
    gl.start()
    me=gl.me
    feats=ada.shape[0]
    width=low.shape[1]
    pick=(lax.broadcasted_iota(jnp.int32,(width,feats),0)==lax.broadcasted_iota(jnp.int32,(width,feats),1)+feats*me).astype(BF)
    mine=jnp.dot(low[...],pick,preferred_element_type=F32).astype(BF)
    acc=jnp.zeros((NDEV,feats),F32)
    ge.wait()
    def use(src,n,base,acc):
        for i in range(n):
            g=src[:,i,:]
            j=base+i
            adag_o[:,j*128:(j+1)*128]=lax.dot_general(mine,g,TN,preferred_element_type=F32)
            gm_o[j:j+1,:]=jnp.sum(g.astype(F32),axis=0,keepdims=True)
            acc=acc+lax.dot_general(g,ada[:,j*128:(j+1)*128],NT,preferred_element_type=F32)
        return acc
    acc=use(gmev,4*L,2*L,acc)
    stp.cstep()
    gl.wait()
    acc=use(gmlv,2*L,0,acc)
    for n in range(NDEV):
        g0=(n//NR)*NR
        ctxs[n,0:NR,0:feats]=acc[g0:g0+NR,:]
    xa.start()
    stp.xstep()
    sz.step()
    slq.zstep()
    stp.zstep()
    st.wait()
    def up(i):
        for b in range(NR):
            tg_o[b,rows_of(i,EC),:]=tgin[b,rows_of(i,EC),:].astype(F32)
    loop(block//EC,up)
    xa.wait()
    ctx_o[...]=ctxv[...]
    for s in (sz,slq,stp,st,ge,gl,xa): s.finish()


def tail(gproj,qkv,m1,x,gmid,mod,taps,ml,mr,rl,sums,gkf,low,ada,zq,lastq,side,cols,ta,tf):
    cells,feat=x.shape
    block=cells//NR
    r_=feat//NDEV
    V=pltpu.VMEM
    L=feat//128
    outs=[S_((NR,block,feat),F32),S_((NDEV,8,128),F32),S_(ada.shape,F32),S_((6*L,128),F32),S_((r_,3*feat),F32),S_((9,ta),F32),S_((9,tf),F32)]
    scr=[V((cells,feat),F32),V((cells,feat),F32),V((NR,block,feat),BF),V((NR,block,feat),BF),V((16,feat),F32),
         V((4*L,128),BF),V((16,128),BF),V((NDEV,4*L,128),BF),V((NDEV,16,128),BF),V((NDEV,8,128),F32),V((NDEV,8,128),F32),V((NZ,NC,NR,16,128),F32)]
    scr+=ScatterZ.scratch(r_,zq.shape[2],BF)+Scatter.scratch(r_,feat,BF)+Scatter.scratch(16,128,F32)
    sems=sem_types(ScatterZ.SEMS)+sem_types(Scatter.SEMS)*2+sem_types(Swap.SEMS)+sem_types(AllToAll.SEMS)*3
    return pl.pallas_call(
        functools.partial(tail_kernel,side,cols,ta,tf),
        in_specs=[VM]*9+[SM]+[VM]*6,
        out_specs=[VM]*7,
        out_shape=outs,
        scratch_shapes=scr+sems,
        compiler_params=pltpu.CompilerParams(collective_id=3,has_side_effects=True,vmem_limit_bytes=63<<20),
        name="tail",
    )(gproj,qkv,m1,x,gmid,mod,taps,ml,mr,rl,sums,gkf,low,ada,zq,lastq)


def greet(targets):
    bar=pltpu.get_barrier_semaphore()
    for d in targets:
        pl.semaphore_signal(bar,inc=1,device_id=d,device_id_type=MESH)
    pl.semaphore_wait(bar,len(targets))


def near():
    z,core,rows=here()
    return [dev(z,1-core,rows)]+[dev(z,core,partner_xy(rows,t)) for t in range(1,NR)]


class PipeScatter:
    SEMS=[(2,),(2,),(2,NR),(2,NR)]
    @staticmethod
    def scratch(r,c):
        return [pltpu.VMEM((2,NZ,NC,NR,r,c),BF),pltpu.VMEM((2,NZ,NR,r,c),BF),pltpu.VMEM((2,NZ,NR,r,c),BF),pltpu.VMEM((2,NR,NZ,r,c),BF)]
    def __init__(self,bufs,sems):
        self.part,self.sib,self.own,self.xin=bufs
        self.sc,self.rc,self.sx,self.rx=sems
        self.z,self.core,self.rows=here()
    def ccopy(self,s):
        return rcopy(self.part.at[s,:,1-self.core],self.sib.at[s],self.sc.at[s],self.rc.at[s],dev(self.z,1-self.core,self.rows))
    def xcopy(self,s,t):
        to=partner_xy(self.rows,t)
        return rcopy(self.own.at[s,:,to],self.xin.at[s,t],self.sx.at[s,t],self.rx.at[s,t],dev(self.z,self.core,to))
    def send_core(self,s):
        self.ccopy(s).start()
    def send_square(self,s):
        self.ccopy(s).wait()
        def body(i):
            a,b=i//NR,lax.rem(i,NR)
            self.own[s,a,b]=(self.part[s,a,self.core,b].astype(F32)+self.sib[s,a,b].astype(F32)).astype(BF)
        loop(NZ*NR,body)
        for t in range(1,NR): self.xcopy(s,t).start()
    def collect(self,s,put):
        for t in range(1,NR): self.xcopy(s,t).wait()
        def body(a):
            v=self.own[s,a,self.rows].astype(F32)
            for t in range(1,NR): v=v+self.xin[s,t,a].astype(F32)
            put(a,v.astype(BF))
        loop(NZ,body)


class RowScatter:
    SEMS=[(2,),(2,),(2,NR),(2,NR)]
    @staticmethod
    def scratch(r,c):
        return [pltpu.VMEM((2,NR,r,c),BF),pltpu.VMEM((2,NR,r,c),BF),pltpu.VMEM((2,NR,r,c),BF)]
    def __init__(self,part,zout,bufs,sems):
        self.part,self.zout=part,zout
        self.sib,self.own,self.xin=bufs
        self.sc,self.rc,self.sx,self.rx=sems
        self.z,self.core,self.rows=here()
    def ccopy(self,k):
        s=k%2
        return rcopy(self.part.at[k,1-self.core],self.sib.at[s],self.sc.at[s],self.rc.at[s],dev(self.z,1-self.core,self.rows))
    def xcopy(self,k,t):
        s=k%2
        to=partner_xy(self.rows,t)
        return rcopy(self.own.at[s,to],self.xin.at[s,t],self.sx.at[s,t],self.rx.at[s,t],dev(self.z,self.core,to))
    def send_core(self,k):
        self.ccopy(k).start()
    def send_square(self,k):
        self.ccopy(k).wait()
        s=k%2
        def body(b):
            self.own[s,b]=(self.part[k,self.core,b].astype(F32)+self.sib[s,b].astype(F32)).astype(BF)
        loop(NR,body)
        for t in range(1,NR): self.xcopy(k,t).start()
    def collect(self,k):
        s=k%2
        for t in range(1,NR): self.xcopy(k,t).wait()
        v=self.own[s,self.rows].astype(F32)
        for t in range(1,NR): v=v+self.xin[s,t].astype(F32)
        self.zout[k]=v.astype(BF)


def ffn_kernel_body(*refs,side,cols):
    it=iter(refs)
    nx=lambda n:[next(it) for _ in range(n)]
    x_ref,att_ref,cot_ref,mod_ref,outw_ref,zpu,zpd,tap_ref,ml_ref,mr_ref,rl_ref=nx(11)
    lay_ref,gmid_ref,gatt_ref,gout_ref,zup,zdown,gtap_ref,sums_ref=nx(8)
    m2,m2t,gffn,branch,fb,gm2,F,G,glow,gub,dfull,ufull,gd,ucur=nx(14)
    ubufs=nx(4); dbufs=nx(3)
    take=taker(it)
    ga=GatherXY(zpd,dfull,take(GatherXY))
    T=F.shape[1]
    gu=GatherTile(zpu,ufull,T,nx(5))
    middle=gmid_ref
    us=PipeScatter(ubufs,take(PipeScatter))
    ds=RowScatter(gd,zdown,dbufs,take(RowScatter))
    t=pl.program_id(0)
    cells,feat=x_ref.shape
    hidden=NDEV*zpd.shape[1]
    steps=hidden//T; last=steps-1
    block=hidden//NZ
    CH=1024; EC=256
    shift2=mod_ref[3:4,:]; scale2=mod_ref[4:5,:]; gate2=mod_ref[5:6,:]; gate1=mod_ref[2:3,:]
    slot=lax.rem(t,2); other=lax.rem(t+1,2)
    ready={}
    for k in range(NZ): ready[k]=-(-((k+1)*block)//T)-1
    need={}
    for k in range(NZ): need[k]=(k*block)//T
    def put_up(tile):
        def put(a,v): zup[a,:,pl.ds(pl.multiple_of(tile*T,128),T)]=v
        return put

    @pl.when(t==0)
    def _():
        greet(near())
        gu.local().start(); ga.start_local()
        gu.start(0); ga.start([0]); gu.start(1); ga.start([1])
        def a(i):
            branch[rows_of(i,CH),:]=dotf(att_ref[rows_of(i,CH),:],outw_ref[...])
        loop(cells//CH,a)
        def b(i):
            r=rows_of(i,EC)
            mid=x_ref[r,:].astype(F32)+gate1*branch[r,:]
            middle[r,:]=mid
            n,_=normal_rows(mid)
            m2[r,:]=(n*(1.0+scale2)+shift2).astype(BF)
            gffn[r,:]=(gate2*cot_ref[r,:].astype(F32)).astype(BF)
        loop(cells//EC,b)
        gu.step(0); ga.step(0)
        def c(i):
            r=rows_of(i,CH)
            m2t[:,pl.ds(pl.multiple_of(i*CH,CH),CH)]=jnp.transpose(m2[r,:])
            fb[r,:]=jnp.zeros((CH,feat),F32)
            gm2[r,:]=jnp.zeros((CH,feat),F32)
        loop(cells//CH,c)
        gu.step2(0); ga.step2(0)
        ga.local().wait(); gu.local().wait()
    gu.arrive(t)
    for k in range(NZ):
        @pl.when(t==need[k])
        def _(k=k): ga.arrive(k)
    @pl.when(t>=2)
    def _():
        us.collect(slot,put_up(t-2))
    for k in range(NZ):
        if ready[k]+2<=last:
            @pl.when(t==ready[k]+2)
            def _(k=k): ds.collect(k)

    dw=dfull.reshape(hidden,feat)
    tc=pl.ds(pl.multiple_of(t*T,T),T)
    def flat(i):
        n=feat//NZ
        ucur[rows_of(i,n),:]=ufull[i,:,:,:,tc].reshape(n,T)
    loop(NZ,flat)
    gdw=gd.reshape(hidden,feat)
    tr=pl.ds(pl.multiple_of(t*T,T),T)
    def first(i):
        r=rows_of(i,CH)
        F[r,:]=dotf(m2[r,:],ucur[...]).astype(BF).astype(F32)
        G[r,:]=dotf(gffn[r,:],dw[tr,:],NT)
    loop(cells//CH,first)
    @pl.when(t<last)
    def _(): gu.step(t+1)
    @pl.when(t<last-1)
    def _(): gu.start(t+2)
    for k in range(1,NZ):
        @pl.when(t==k-1)
        def _(k=k):
            ga.step(k)
            if k+1<NZ: ga.start([k+1])

    def forward_lanes(l):
        ls=pl.ds(pl.multiple_of(l*128,128),128)
        def put(i,u):
            r=rows_of(i,cols)
            u2=u*u
            th=jnp.tanh(C0*(u+C1*(u2*u)))
            half=0.5*(1.0+th)
            glow[r,ls]=(u*half).astype(BF)
            d=half+(0.5*u)*(1.0-th*th)*(C0*(1.0+(3.0*C1)*u2))
            G[r,ls]=(G[r,ls]*d).astype(BF).astype(F32)
        conv_rows(F,put,tap_ref[:,ls],ml_ref,mr_ref,rl_ref,ls,side,cols)
    loop(T//128,forward_lanes)
    @pl.when(t<last)
    def _(): gu.step2(t+1)
    for k in range(1,NZ):
        @pl.when(t==k-1)
        def _(k=k): ga.step2(k)
    @pl.when(t>=1)
    def _():
        us.send_square(other)
    for k in range(NZ):
        if ready[k]+1<=last:
            @pl.when(t==ready[k]+1)
            def _(k=k): ds.send_square(k)
    def back_lanes(l):
        ls=pl.ds(pl.multiple_of(l*128,128),128)
        def put2(i,u):
            gub[rows_of(i,cols),ls]=u.astype(BF)
        acc=back_rows(G,F,put2,tap_ref[:,ls],ml_ref,mr_ref,rl_ref,ls,0,side,side,cols)
        for q in range(9):
            gtap_ref[q:q+1,ls]=jnp.sum(acc[q],axis=0,keepdims=True)
    loop(T//128,back_lanes)
    gtap_ref[9:16,:]=jnp.zeros((7,T),F32)

    r_=feat//NDEV
    def third(i):
        n=NC*NR*r_
        us.part[slot,i]=dotf(m2t[rows_of(i,n),:],gub[...]).astype(BF).reshape(NC,NR,r_,T)
    loop(NZ,third)
    us.send_core(slot)
    for i in range(T//256):
        gdw[pl.ds(pl.multiple_of(t*T+i*256,256),256),:]=dotf(glow[:,i*256:(i+1)*256],gffn[...],TN).astype(BF)
    for k in range(NZ):
        @pl.when(t==ready[k])
        def _(k=k): ds.send_core(k)
    def second(i):
        r=rows_of(i,CH)
        fb[r,:]+=dotf(glow[r,:],dw[tr,:])
        gm2[r,:]+=dotf(gub[r,:],ucur[...],NT)
    loop(cells//CH,second)

    @pl.when(t==last)
    def _():
        us.collect(other,put_up(last-1))
        late=[k for k in range(NZ) if ready[k]+1>last]
        mid_=[k for k in range(NZ) if ready[k]+1==last]
        for k in mid_: ds.collect(k)
        us.send_square(slot)
        for k in late: ds.send_square(k)
        z=jnp.zeros((8,feat),F32)
        def body(i,c):
            sg2,ss2,sc2,sg1=c
            r=rows_of(i,EC)
            inc=cot_ref[r,:].astype(F32)
            mid=middle[r,:]
            n,inv=normal_rows(mid)
            lay_ref[r,:]=(mid+gate2*fb[r,:]).astype(BF)
            gm=gm2[r,:]
            gmid=inc+normal_back_rows(gm*(1.0+scale2),n,inv)
            gmid_ref[r,:]=gmid
            gffn[r,:]=(gate1*gmid).astype(BF)
            return (sg2+fold8(inc*fb[r,:]),ss2+fold8(gm),sc2+fold8(gm*n),sg1+fold8(gmid*branch[r,:]))
        res=lax.fori_loop(0,cells//EC,body,(z,z,z,z))
        for q in range(4):
            sums_ref[q:q+1,:]=jnp.sum(res[q],axis=0,keepdims=True)
        sums_ref[4:8,:]=jnp.zeros((4,feat),F32)
        def b(i):
            r=rows_of(i,CH)
            gatt_ref[r,:]=dotf(gffn[r,:],outw_ref[...],NT).astype(BF)
        loop(cells//CH,b)
        for i in range(feat//256):
            gout_ref[i*256:(i+1)*256,:]=dotf(att_ref[:,i*256:(i+1)*256],gffn[...],TN).astype(BF)
        us.collect(slot,put_up(last))
        for k in late: ds.collect(k)
        ga.finish_remote()
        loop(steps,gu.finish_remote)


def ffn(x,att,cot,mod6,outw,zpu,zpd,taps,ml,mr,rl,side,cols,T=512):
    cells,feat=x.shape
    hidden=zpu.shape[2]
    vm=lambda shape: pl.BlockSpec(shape,lambda t:(0,)*len(shape),pipeline_mode=pl.Buffered(1))
    r_,d_=feat//NDEV,hidden//NDEV
    return pl.pallas_call(
        functools.partial(ffn_kernel_body,side=side,cols=cols),
        grid=(hidden//T,),
        in_specs=[vm((cells,feat)),vm((cells,feat)),vm((cells,feat)),vm((8,feat)),vm((feat,feat)),
                  HBM,HBM,pl.BlockSpec((16,T),lambda t:(0,t)),
                  vm((cells,128)),vm((cells,128)),SM],
        out_specs=[vm((cells,feat)),vm((cells,feat)),vm((cells,feat)),vm((feat,feat)),
                   vm((NZ,r_,hidden)),vm((NZ,d_,feat)),pl.BlockSpec((16,T),lambda t:(0,t)),vm((8,feat))],
        out_shape=[S_((cells,feat),BF),S_((cells,feat),F32),S_((cells,feat),BF),S_((feat,feat),BF),S_((NZ,r_,hidden),BF),S_((NZ,d_,feat),BF),S_((16,hidden),F32),S_((8,feat),F32)],
        scratch_shapes=[pltpu.VMEM((cells,feat),BF),pltpu.VMEM((feat,cells),BF),pltpu.VMEM((cells,feat),BF),
                        pltpu.VMEM((cells,feat),F32),pltpu.VMEM((cells,feat),F32),pltpu.VMEM((cells,feat),F32),
                        pltpu.VMEM((cells,T),F32),pltpu.VMEM((cells,T),F32),pltpu.VMEM((cells,T),BF),pltpu.VMEM((cells,T),BF),
                        pltpu.VMEM((NZ,NC,NR,d_,feat),BF),pltpu.VMEM((NZ,NC,NR,r_,hidden),BF),pltpu.VMEM((NZ,NC,NR,d_,feat),BF),pltpu.VMEM((feat,T),BF)]
                       +PipeScatter.scratch(r_,T)+RowScatter.scratch(d_,feat)
                       +sem_types(GatherXY.SEMS)+sem_types(GatherTile.sems(hidden//T))+sem_types(PipeScatter.SEMS)+sem_types(RowScatter.SEMS),
        compiler_params=pltpu.CompilerParams(dimension_semantics=("arbitrary",),vmem_limit_bytes=63<<20,collective_id=4,has_side_effects=True),
        name="ffn",
    )(x,att,cot,mod6,outw,zpu,zpd,taps,ml,mr,rl)
def own_rows(padded_cells):
    return jnp.pad(padded_cells,((0,0),(1,1),(1,1),(0,0)))


def fast(tokens,conditioning,item_map,ada_weight,ada_bias,attn_kernel,qkv_weight,out_weight,up_weight,ffn_kernel,down_weight,out_cotangent):
    canvases,rows_here,cols,features=tokens.shape
    side=rows_here*NR
    cells=side*cols
    rows=lax.axis_index("rows"); dp=lax.axis_index("dp"); me=dp*NR+rows
    hidden=up_weight.shape[1]
    cond_row=jnp.pad(lax.dynamic_slice_in_dim(conditioning,rows,1,0),((0,7),(0,0)))
    mod_cols=ada_weight.shape[1]
    bshard=ada_bias.shape[0]
    bias_rows=lax.dynamic_update_slice_in_dim(jnp.zeros((mod_cols,),F32),ada_bias.astype(F32),me*bshard,0).reshape(mod_cols//128,128)
    ta,tf=attn_kernel.shape[1],ffn_kernel.shape[1]
    taps=jnp.pad(jnp.concatenate([attn_kernel,ffn_kernel],axis=1),((0,7),(0,128-ta-tf)))
    blocks=(NR,rows_here*cols,features)
    labels=lax.dynamic_index_in_dim(item_map,rows,0,keepdims=False)
    qm,km=head_masks(labels.reshape(cells))
    ml,mr,rl=link_masks(labels)
    tok,low_all,mod,qkv_f,tap_a,tap_f,m1,mix,*zps=enter(tokens.reshape(blocks),cond_row,ada_weight,bias_rows,qkv_weight,taps,ml,mr,rl,[out_weight],side,cols,ta,tf)
    full2=lambda a:a.reshape(-1,a.shape[-1])
    triple_full=full2(qkv_f)
    mod6=jnp.pad(mod.reshape(6,features),((0,2),(0,0)))
    proj,attended,lse_t,cot,zp_down,zp_up,out_f=forward(mix,triple_full,qm,km,out_cotangent.reshape(blocks),down_weight,up_weight,zps)
    lay,gmid,gatt,g_out,z_up,z_down,g_kffn,sums=ffn(
        tok.reshape(cells,features),attended,cot.reshape(cells,features),mod6,
        full2(out_f),zp_up,zp_down,tap_f,ml,mr,rl,side,cols)
    sp=lambda g:g.reshape(NZ,NC,NR,g.shape[0]//NDEV,g.shape[1])
    gproj,lay_o,o_o,zq,lastq,u_o,d_o=backward(proj,gatt,attended,qm,km,lse_t,mix,lay.reshape(blocks),sp(g_out),[z_up,z_down])
    tg,ctx,adag,gmsum,q_o,ka_o,kf_o=tail(gproj,triple_full,m1,tok.reshape(cells,features),gmid,mod6,
        tap_a,ml,mr,rl,sums,g_kffn,low_all,ada_weight,zq,lastq,side,cols,ta,tf)
    shape4=(NR,rows_here,cols,features)
    feats=ada_weight.shape[0]
    dsilu=ctx[:,:NR,:feats].transpose(1,0,2).reshape(NR,features)
    cv=conditioning.astype(F32)
    _,sback=jax.vjp(jax.nn.silu,cv)
    dctx=sback(dsilu)[0]
    gbias=lax.dynamic_slice_in_dim(gmsum.reshape(mod_cols),me*bshard,bshard,0)
    return (lay_o.reshape(shape4),tg.reshape(shape4),dctx,adag,gbias,ka_o,q_o,o_o,u_o,kf_o,d_o)


def solution(mesh):
    quick=dict(mesh.shape)=={"dp":NZ*NC,"rows":NR}
    return jax.shard_map(
        fast if quick else local,
        mesh=mesh,
        in_specs=(
            P("dp", "rows", None, None),
            P("dp", None),
            P("dp", None, None),
            P(("dp", "rows"), None),
            P(("dp", "rows")),
            P(None, ("dp", "rows")),
            P(("dp", "rows"), None),
            P(("dp", "rows"), None),
            P(("dp", "rows"), None),
            P(None, ("dp", "rows")),
            P(("dp", "rows"), None),
            P("dp", "rows", None, None),
        ),
        out_specs=(
            P("dp", "rows", None, None),
            P("dp", "rows", None, None),
            P("dp", None),
            P(("dp", "rows"), None),
            P(("dp", "rows")),
            P(None, ("dp", "rows")),
            P(("dp", "rows"), None),
            P(("dp", "rows"), None),
            P(("dp", "rows"), None),
            P(None, ("dp", "rows")),
            P(("dp", "rows"), None),
        ),
        check_vma=False,
    )
```

```python
import functools

import jax
import jax.numpy as jnp
from jax import lax
from jax.experimental import pallas as pl
from jax.experimental.pallas import tpu as pltpu
from jax.sharding import PartitionSpec as P

PER_GROUP_WIDTH = 64


EPSILON = 1e-06


def padded(block, sides, width):
    for axis, dim in sides:
        count = lax.axis_size(axis)
        forward = [(i, i + 1) for i in range(count - 1)]
        backward = [(target, source) for source, target in forward]
        low = lax.ppermute(
            lax.slice_in_dim(block, block.shape[dim] - width, None, axis=dim), axis, forward
        )
        high = lax.ppermute(lax.slice_in_dim(block, 0, width, axis=dim), axis, backward)
        block = jnp.concatenate([low, block, high], axis=dim)
    return block


def normalize(attended_content_array):
    average = jnp.mean(attended_content_array, axis=-1, keepdims=True)
    centred = attended_content_array - average
    inverse = lax.rsqrt(jnp.mean(centred * centred, axis=-1, keepdims=True) + EPSILON)
    return (centred * inverse, inverse)


def normalize_back(incoming, normalized_rows, inverse):
    return inverse * (
        incoming
        - jnp.mean(incoming, axis=-1, keepdims=True)
        - normalized_rows * jnp.mean(incoming * normalized_rows, axis=-1, keepdims=True)
    )


def widen_cols(rimmed):
    return jnp.pad(rimmed, ((0, 0), (0, 0), (1, 1), (0, 0)))


def tap_mask(labels_pad, centre, row_off, col_off):
    rows_here = centre.shape[1]
    cols_here = centre.shape[2]
    return (labels_pad[:, row_off : row_off + rows_here, col_off : col_off + cols_here] == centre)[
        ..., None
    ]


def conv_forward(padded_rows, labels_pad, centre, kernel):
    rows_here = centre.shape[1]
    cols_here = centre.shape[2]
    summed = jnp.zeros(centre.shape + (kernel.shape[1],), jnp.float32)
    for row_off in range(3):
        for col_off in range(3):
            window = padded_rows[
                :, row_off : row_off + rows_here, col_off : col_off + cols_here
            ].astype(jnp.float32)
            tapped = kernel[3 * row_off + col_off].astype(jnp.float32) * window
            summed = summed + jnp.where(tap_mask(labels_pad, centre, row_off, col_off), tapped, 0.0)
    return summed


def conv_mirror(padded_rows, labels_pad, centre, kernel):
    rows_here = centre.shape[1]
    cols_here = centre.shape[2]
    summed = jnp.zeros(centre.shape + (kernel.shape[1],), jnp.float32)
    for row_off in range(3):
        for col_off in range(3):
            row_from = 2 - row_off
            col_from = 2 - col_off
            window = padded_rows[
                :, row_from : row_from + rows_here, col_from : col_from + cols_here
            ].astype(jnp.float32)
            tapped = kernel[3 * row_off + col_off].astype(jnp.float32) * window
            summed = summed + jnp.where(
                tap_mask(labels_pad, centre, row_from, col_from), tapped, 0.0
            )
    return summed


def kernel_grad(incoming, padded_rows, labels_pad, centre):
    rows_here = centre.shape[1]
    cols_here = centre.shape[2]
    incoming_values = incoming.astype(jnp.float32)
    tap_sums = []
    for row_off in range(3):
        for col_off in range(3):
            window = padded_rows[
                :, row_off : row_off + rows_here, col_off : col_off + cols_here
            ].astype(jnp.float32)
            product = jnp.where(
                tap_mask(labels_pad, centre, row_off, col_off), incoming_values * window, 0.0
            )
            tap_sums.append(jnp.sum(product, axis=(0, 1, 2)))
    return jnp.stack(tap_sums, axis=0)


def contract_rows(left, right):
    return lax.dot_general(
        left, right, (((0,), (0,)), ((), ())), preferred_element_type=jnp.float32
    )


def contract_cols(left, right):
    return lax.dot_general(
        left, right, (((1,), (1,)), ((), ())), preferred_element_type=jnp.float32
    )


def local(
    tokens,
    conditioning,
    item_map,
    ada_weight,
    ada_bias,
    attn_kernel,
    qkv_weight,
    out_weight,
    up_weight,
    ffn_kernel,
    down_weight,
    out_cotangent,
):
    canvases, rows_here, cols_here, features = tokens.shape
    cell_count = canvases * rows_here * cols_here
    position = lax.axis_index("rows")
    gathered = (
        lax.all_gather(ada_weight, ("dp", "rows"), axis=0, tiled=True),
        lax.all_gather(ada_bias, ("dp", "rows"), axis=0, tiled=True),
        lax.all_gather(attn_kernel, ("dp", "rows"), axis=1, tiled=True),
        lax.all_gather(qkv_weight, ("dp", "rows"), axis=0, tiled=True),
        lax.all_gather(out_weight, ("dp", "rows"), axis=0, tiled=True),
        lax.all_gather(up_weight, ("dp", "rows"), axis=0, tiled=True),
        lax.all_gather(ffn_kernel, ("dp", "rows"), axis=1, tiled=True),
        lax.all_gather(down_weight, ("dp", "rows"), axis=0, tiled=True),
    )
    ada_full, bias_full, kernel_attn, triple_full, out_full, up_full, kernel_ffn, down_full = (
        gathered
    )
    hidden_units = up_full.shape[1]
    head_count = features // PER_GROUP_WIDTH
    logit_divisor = PER_GROUP_WIDTH ** (-0.5)
    labels_pad = jnp.pad(item_map, ((0, 0), (1, 1), (1, 1)), constant_values=-1)
    labels_here = lax.dynamic_slice_in_dim(labels_pad, position * rows_here, rows_here + 2, 1)
    centre = labels_here[:, 1:-1, 1:-1]
    cond_values = conditioning.astype(jnp.float32)
    silu_low = jax.nn.silu(cond_values).astype(jnp.bfloat16)
    modulation = jnp.dot(silu_low, ada_full, preferred_element_type=jnp.float32) + bias_full.astype(
        jnp.float32
    )
    layer_stack = modulation.reshape(canvases, 6, 1, 1, features)
    shift_one, scale_one, gate_one, shift_two, scale_two, gate_two = (
        layer_stack[:, index] for index in range(6)
    )
    token_values = tokens.astype(jnp.float32)
    normed_one, inverse_one = normalize(token_values)
    modulated_one = (normed_one * (1.0 + scale_one) + shift_one).astype(jnp.bfloat16)
    modulated_padded = widen_cols(padded(modulated_one, (("rows", 1),), 1))
    local_mix = conv_forward(modulated_padded, labels_here, centre, kernel_attn).astype(
        jnp.bfloat16
    )
    mix_rows = local_mix.reshape(cell_count, features)
    projected = jnp.dot(mix_rows, triple_full, preferred_element_type=jnp.float32).astype(
        jnp.bfloat16
    )
    projected = projected.reshape(canvases, rows_here * cols_here, 3 * features)
    queries = projected[..., :features]
    key_rows = projected[..., features : 2 * features]
    value_rows = projected[..., 2 * features :]
    keys_all, values_all = (
        lax.all_gather(key_rows, "rows", axis=1, tiled=True),
        lax.all_gather(value_rows, "rows", axis=1, tiled=True),
    )
    query_heads = queries.reshape(canvases, -1, head_count, PER_GROUP_WIDTH)
    key_heads = keys_all.reshape(canvases, -1, head_count, PER_GROUP_WIDTH)
    value_heads = values_all.reshape(canvases, -1, head_count, PER_GROUP_WIDTH)
    scores = (
        jnp.einsum("bqhd,bkhd->bhqk", query_heads, key_heads, preferred_element_type=jnp.float32)
        * logit_divisor
    )
    label_rows = centre.reshape(canvases, -1)
    label_keys = item_map.reshape(canvases, -1)
    linked = label_rows[:, None, :, None] == label_keys[:, None, None, :]
    masked = jnp.where(linked, scores, -1e30)
    row_peak = jnp.max(masked, axis=-1, keepdims=True)
    raised = jnp.exp(masked - row_peak)
    row_total = jnp.sum(raised, axis=-1, keepdims=True)
    attention = raised / row_total
    attention_low = attention.astype(jnp.bfloat16)
    attended = jnp.einsum(
        "bhqk,bkhd->bqhd", attention_low, value_heads, preferred_element_type=jnp.float32
    ).astype(jnp.bfloat16)
    attended = attended.reshape(cell_count, features)
    attn_branch = jnp.dot(attended, out_full, preferred_element_type=jnp.float32).reshape(
        tokens.shape
    )
    middle = token_values + gate_one * attn_branch
    normed_two, inverse_two = normalize(middle)
    modulated_two = (normed_two * (1.0 + scale_two) + shift_two).astype(jnp.bfloat16)
    modulated_rows = modulated_two.reshape(cell_count, features)
    hidden_up_projection = jnp.dot(
        modulated_rows, up_full, preferred_element_type=jnp.float32
    ).astype(jnp.bfloat16)
    hidden_up_projection = hidden_up_projection.reshape(
        canvases, rows_here, cols_here, hidden_units
    )
    up_padded = widen_cols(padded(hidden_up_projection, (("rows", 1),), 1))
    pre_gelu = conv_forward(up_padded, labels_here, centre, kernel_ffn)
    activated, gelu_back = jax.vjp(jax.nn.gelu, pre_gelu)
    gelu_low = activated.astype(jnp.bfloat16).reshape(cell_count, hidden_units)
    ffn_branch = jnp.dot(gelu_low, down_full, preferred_element_type=jnp.float32).reshape(
        tokens.shape
    )
    layer_out = (middle + gate_two * ffn_branch).astype(jnp.bfloat16)
    weights_back = (
        lax.all_gather(ada_weight, ("dp", "rows"), axis=0, tiled=True),
        lax.all_gather(ada_bias, ("dp", "rows"), axis=0, tiled=True),
        lax.all_gather(attn_kernel, ("dp", "rows"), axis=1, tiled=True),
        lax.all_gather(qkv_weight, ("dp", "rows"), axis=0, tiled=True),
        lax.all_gather(out_weight, ("dp", "rows"), axis=0, tiled=True),
        lax.all_gather(up_weight, ("dp", "rows"), axis=0, tiled=True),
        lax.all_gather(ffn_kernel, ("dp", "rows"), axis=1, tiled=True),
        lax.all_gather(down_weight, ("dp", "rows"), axis=0, tiled=True),
    )
    (
        ada_back,
        bias_back,
        kernel_attn_back,
        triple_back,
        out_back,
        up_back,
        kernel_ffn_back,
        down_projection_back,
    ) = weights_back
    incoming = out_cotangent.astype(jnp.float32)
    grad_gate_two = jnp.sum(incoming * ffn_branch, axis=(1, 2))
    grad_ffn = (gate_two * incoming).astype(jnp.bfloat16).reshape(cell_count, features)
    grad_down = contract_rows(gelu_low, grad_ffn)
    grad_gelu = contract_cols(grad_ffn, down_projection_back).reshape(
        canvases, rows_here, cols_here, hidden_units
    )
    grad_pre = gelu_back(grad_gelu)[0].astype(jnp.bfloat16)
    grad_pre_padded = widen_cols(padded(grad_pre, (("rows", 1),), 1))
    grad_kernel_ffn = kernel_grad(grad_pre, up_padded, labels_here, centre)
    grad_up = (
        conv_mirror(grad_pre_padded, labels_here, centre, kernel_ffn_back)
        .astype(jnp.bfloat16)
        .reshape(cell_count, hidden_units)
    )
    grad_up_weight = contract_rows(modulated_rows, grad_up)
    grad_mod_two = contract_cols(grad_up, up_back).reshape(tokens.shape)
    grad_scale_two = jnp.sum(grad_mod_two * normed_two, axis=(1, 2))
    grad_shift_two = jnp.sum(grad_mod_two, axis=(1, 2))
    grad_middle = incoming + normalize_back(
        grad_mod_two * (1.0 + scale_two), normed_two, inverse_two
    )
    grad_gate_one = jnp.sum(grad_middle * attn_branch, axis=(1, 2))
    grad_attn = (gate_one * grad_middle).astype(jnp.bfloat16).reshape(cell_count, features)
    grad_out_weight = contract_rows(attended, grad_attn)
    grad_attended = (
        contract_cols(grad_attn, out_back)
        .astype(jnp.bfloat16)
        .reshape(canvases, -1, head_count, PER_GROUP_WIDTH)
    )
    grad_weights = jnp.einsum(
        "bqhd,bkhd->bhqk", grad_attended, value_heads, preferred_element_type=jnp.float32
    )
    row_delta = jnp.sum(attention * grad_weights, axis=-1, keepdims=True)
    grad_scores = (attention * (grad_weights - row_delta)).astype(jnp.bfloat16)
    grad_query = (
        jnp.einsum("bhqk,bkhd->bqhd", grad_scores, key_heads, preferred_element_type=jnp.float32)
        * logit_divisor
    )
    grad_key_all = (
        jnp.einsum("bhqk,bqhd->bkhd", grad_scores, query_heads, preferred_element_type=jnp.float32)
        * logit_divisor
    )
    value_gradient_full = jnp.einsum(
        "bhqk,bqhd->bkhd", attention_low, grad_attended, preferred_element_type=jnp.float32
    )
    grad_key, grad_value = (
        lax.psum_scatter(
            grad_key_all.reshape(canvases, -1, features).astype(jnp.bfloat16),
            "rows",
            scatter_dimension=1,
            tiled=True,
        ).astype(jnp.float32),
        lax.psum_scatter(
            value_gradient_full.reshape(canvases, -1, features).astype(jnp.bfloat16),
            "rows",
            scatter_dimension=1,
            tiled=True,
        ).astype(jnp.float32),
    )
    grad_projected = jnp.concatenate(
        [
            grad_query.reshape(cell_count, features),
            grad_key.reshape(cell_count, features),
            grad_value.reshape(cell_count, features),
        ],
        axis=-1,
    ).astype(jnp.bfloat16)
    grad_qkv_weight = contract_rows(mix_rows, grad_projected)
    grad_mix = contract_cols(grad_projected, triple_back).astype(jnp.bfloat16).reshape(tokens.shape)
    grad_mix_padded = widen_cols(padded(grad_mix, (("rows", 1),), 1))
    grad_kernel_attn = kernel_grad(grad_mix, modulated_padded, labels_here, centre)
    grad_mod_one = conv_mirror(grad_mix_padded, labels_here, centre, kernel_attn_back)
    grad_scale_one = jnp.sum(grad_mod_one * normed_one, axis=(1, 2))
    grad_shift_one = jnp.sum(grad_mod_one, axis=(1, 2))
    token_grad = grad_middle + normalize_back(
        grad_mod_one * (1.0 + scale_one), normed_one, inverse_one
    )
    grad_parts = jnp.concatenate(
        [
            grad_shift_one,
            grad_scale_one,
            grad_gate_one,
            grad_shift_two,
            grad_scale_two,
            grad_gate_two,
        ],
        axis=-1,
    )
    grad_modulation = lax.psum(grad_parts.astype(jnp.bfloat16), "rows")
    leader = (position == 0).astype(jnp.float32)
    grad_ada_weight = contract_rows(silu_low, grad_modulation) * leader
    grad_ada_bias = jnp.sum(grad_modulation.astype(jnp.float32), axis=0) * leader
    silu_values, silu_back = jax.vjp(jax.nn.silu, cond_values)
    derivative_of_context = silu_back(contract_cols(grad_modulation, ada_back))[0]
    summed_grads = (
        lax.psum_scatter(grad_ada_weight, ("dp", "rows"), scatter_dimension=0, tiled=True),
        lax.psum_scatter(grad_ada_bias, ("dp", "rows"), scatter_dimension=0, tiled=True),
        lax.psum_scatter(grad_kernel_attn, ("dp", "rows"), scatter_dimension=1, tiled=True),
        lax.psum_scatter(grad_qkv_weight, ("dp", "rows"), scatter_dimension=0, tiled=True),
        lax.psum_scatter(grad_out_weight, ("dp", "rows"), scatter_dimension=0, tiled=True),
        lax.psum_scatter(grad_up_weight, ("dp", "rows"), scatter_dimension=0, tiled=True),
        lax.psum_scatter(grad_kernel_ffn, ("dp", "rows"), scatter_dimension=1, tiled=True),
        lax.psum_scatter(grad_down, ("dp", "rows"), scatter_dimension=0, tiled=True),
    )
    return (layer_out, token_grad, derivative_of_context) + tuple(summed_grads)


F32=jnp.float32; BF=jnp.bfloat16
NT=(((1,),(1,)),((),()))
TN=(((0,),(0,)),((),()))

def head_masks(labels):
    cells=labels.shape[0]
    lane=lax.broadcasted_iota(jnp.int32,(cells,128),1)%64
    lab=labels[:,None]
    qm=(lane==lab).astype(BF)
    km=jnp.where((lane!=lab)&(lane<4),-1e30,0.0).astype(BF)
    return qm,km

MESH=pl.DeviceIdType.MESH
NZ,NC,NR=4,2,4


def here():
    dp=lax.axis_index("dp"); rows=lax.axis_index("rows")
    return dp//NC, lax.rem(dp,NC), rows


def dev(z,core,rows):
    return (z*NC+core, rows)


def partner_xy(rows,t):
    x=lax.rem(rows,2); y=rows//2
    tx=t%2; ty=t//2
    nx=1-x if tx else x
    ny=1-y if ty else y
    return ny*2+nx


def rcopy(src,dst,ssem,rsem,target):
    return pltpu.make_async_remote_copy(src_ref=src,dst_ref=dst,send_sem=ssem,recv_sem=rsem,device_id=target,device_id_type=MESH)


def barrier_all():
    dp=lax.axis_index("dp"); rows=lax.axis_index("rows")
    me=dp*NR+rows
    total=NZ*NC*NR
    bar=pltpu.get_barrier_semaphore()
    def body(k,c):
        other=lax.rem(me+k,total)
        pl.semaphore_signal(bar,inc=1,device_id=(other//NR,lax.rem(other,NR)),device_id_type=MESH)
        return c
    lax.fori_loop(1,total,body,0)
    pl.semaphore_wait(bar,total-1)


def zmod(v):
    return lax.rem(v+NZ,NZ)


class Gather:
    SEMS=[(NZ,),(NZ,),(NZ,NR),(NZ,NR),(NZ,NR),(NZ,NR),(1,)]

    def __init__(self,shard,full,sems):
        self.shard,self.full=shard,full
        self.sz,self.rz,self.sx,self.rx,self.sc,self.rc,self.lo=sems
        self.z,self.core,self.rows=here()

    def slot(self,dz,t,core):
        rows=self.rows if t==0 else partner_xy(self.rows,t)
        return self.full.at[zmod(self.z-dz),core,rows]

    def zcopy(self,dz,receive=False):
        dst=self.slot(dz if receive else 0,0,self.core)
        return rcopy(self.shard,dst,self.sz.at[dz],self.rz.at[dz],dev(zmod(self.z+dz),self.core,self.rows))

    def piece(self,dz):
        return self.shard if dz==0 else self.slot(dz,0,self.core)

    def xcopy(self,dz,t,receive=False):
        dst=self.slot(dz,t if receive else 0,self.core)
        return rcopy(self.piece(dz),dst,self.sx.at[dz,t],self.rx.at[dz,t],dev(self.z,self.core,partner_xy(self.rows,t)))

    def ccopy(self,dz,t,receive=False):
        src=self.piece(dz) if t==0 else self.slot(dz,t,self.core)
        dst=self.slot(dz,t,1-self.core if receive else self.core)
        return rcopy(src,dst,self.sc.at[dz,t],self.rc.at[dz,t],dev(self.z,1-self.core,self.rows))

    def local(self):
        return pltpu.make_async_copy(self.shard,self.slot(0,0,self.core),self.lo.at[0])

    def start(self):
        for dz in range(1,NZ):
            self.zcopy(dz).start()
        for t in range(1,NR):
            self.xcopy(0,t).start()
        self.ccopy(0,0).start()
        self.local().start()

    def zstep(self,dz):
        self.zcopy(dz,True).wait_recv()
        for t in range(1,NR):
            self.xcopy(dz,t).start()
        self.ccopy(dz,0).start()

    def xstep(self,dz,t):
        self.xcopy(dz,t,True).wait_recv()
        self.ccopy(dz,t).start()

    def finish(self):
        for dz in range(NZ):
            for t in range(NR):
                self.ccopy(dz,t,True).wait_recv()
        for dz in range(1,NZ):
            self.zcopy(dz).wait_send()
        for dz in range(NZ):
            for t in range(NR):
                if t: self.xcopy(dz,t).wait_send()
                self.ccopy(dz,t).wait_send()
        self.local().wait()

    def run_z(self):
        for dz in range(1,NZ): self.zstep(dz)

    def run_x(self):
        for dz in range(NZ):
            for t in range(1,NR): self.xstep(dz,t)


class Scatter:
    SEMS=[(1,),(1,),(1,),(NR,),(NR,),(NZ,),(NZ,)]

    @staticmethod
    def scratch(r,c,dt):
        return [pltpu.VMEM((NZ,NR,r,c),dt),pltpu.VMEM((NZ,NR,r,c),dt),pltpu.VMEM((NR,NZ,r,c),dt),pltpu.VMEM((NZ,r,c),dt),pltpu.VMEM((NZ,r,c),dt)]

    def __init__(self,part,out,bufs,sems):
        self.part,self.out=part,out
        self.own,self.sib,self.xin,self.zout,self.zin=bufs
        self.lo,self.sc,self.rc,self.sx,self.rx,self.sz,self.rz=sems
        self.z,self.core,self.rows=here()
        self.dt=self.own.dtype

    def lcopy(self):
        return pltpu.make_async_copy(self.part.at[:,self.core],self.own,self.lo.at[0])

    def ccopy(self):
        return rcopy(self.part.at[:,1-self.core],self.sib,self.sc.at[0],self.rc.at[0],dev(self.z,1-self.core,self.rows))

    def xcopy(self,t):
        to=partner_xy(self.rows,t)
        return rcopy(self.own.at[:,to],self.xin.at[t],self.sx.at[t],self.rx.at[t],dev(self.z,self.core,to))

    def zcopy(self,dz):
        to=zmod(self.z+dz)
        return rcopy(self.zout.at[to],self.zin.at[dz],self.sz.at[dz],self.rz.at[dz],dev(to,self.core,self.rows))

    def start(self):
        self.ccopy().start(); self.lcopy().start()

    def cstep(self):
        self.lcopy().wait(); self.ccopy().wait_recv()
        def body(i,c):
            a,b=i//NR,lax.rem(i,NR)
            self.own[a,b]=(self.own[a,b].astype(F32)+self.sib[a,b].astype(F32)).astype(self.dt)
            return c
        lax.fori_loop(0,NZ*NR,body,0)
        for t in range(1,NR): self.xcopy(t).start()

    def xstep(self):
        for t in range(1,NR): self.xcopy(t).wait_recv()
        def body(a,c):
            s=self.own[a,self.rows].astype(F32)
            for t in range(1,NR): s=s+self.xin[t,a].astype(F32)
            self.zout[a]=s.astype(self.dt)
            return c
        lax.fori_loop(0,NZ,body,0)
        for dz in range(1,NZ): self.zcopy(dz).start()

    def zstep(self):
        for dz in range(1,NZ): self.zcopy(dz).wait_recv()
        s=self.zout[self.z].astype(F32)
        for dz in range(1,NZ): s=s+self.zin[dz].astype(F32)
        if callable(self.out): self.out(s)
        else: self.out[...]=s

    def finish(self):
        self.ccopy().wait_send()
        for t in range(1,NR): self.xcopy(t).wait_send()
        for dz in range(1,NZ): self.zcopy(dz).wait_send()


class Swap:
    SEMS=[(NR,),(NR,),(1,)]
    def __init__(self,src,dst,sems):
        self.src,self.dst=src,dst
        self.s,self.r,self.lo=sems
        self.z,self.core,self.rows=here()
    def copy(self,t,receive=False):
        to=partner_xy(self.rows,t)
        return rcopy(self.src.at[to],self.dst.at[to if receive else self.rows],self.s.at[t],self.r.at[t],dev(self.z,self.core,to))
    def local(self):
        return pltpu.make_async_copy(self.src.at[self.rows],self.dst.at[self.rows],self.lo.at[0])
    def start(self):
        for t in range(1,NR): self.copy(t).start()
        self.local().start()
    def wait(self):
        for t in range(1,NR): self.copy(t,True).wait_recv()
        self.local().wait()
    def finish(self):
        for t in range(1,NR): self.copy(t).wait_send()


class AllToAll:
    N=NZ*NC*NR
    SEMS=[(N,),(N,),(1,)]
    def __init__(self,src,dst,sems,one=False):
        self.src,self.dst,self.one=src,dst,one
        self.s,self.r,self.lo=sems
        self.me=lax.axis_index("dp")*NR+lax.axis_index("rows")
    def piece(self,n):
        return self.src if self.one else self.src.at[n]
    def copy(self,k,receive=False):
        to=lax.rem(self.me+k,self.N)
        frm=lax.rem(self.me-k+self.N,self.N)
        return rcopy(self.piece(to),self.dst.at[frm if receive else self.me],self.s.at[k],self.r.at[k],(to//NR,lax.rem(to,NR)))
    def local(self):
        return pltpu.make_async_copy(self.piece(self.me),self.dst.at[self.me],self.lo.at[0])
    def each(self,fn):
        def body(k,c):
            fn(k); return c
        lax.fori_loop(1,self.N,body,0)
    def start(self):
        self.each(lambda k:self.copy(k).start())
        self.local().start()
    def wait(self):
        self.each(lambda k:self.copy(k,True).wait_recv())
        self.local().wait()
    def finish(self):
        self.each(lambda k:self.copy(k).wait_send())


def sem_types(shapes):
    return [pltpu.SemaphoreType.DMA(s) for s in shapes]
class GatherZ:
    SEMS=[(NZ,),(NZ,),(1,)]
    def __init__(self,shard,zp,sems):
        self.shard,self.zp=shard,zp
        self.s,self.r,self.lo=sems
        self.z,self.core,self.rows=here()
    def copy(self,dz,receive=False):
        to=zmod(self.z+dz)
        frm=zmod(self.z-dz)
        return rcopy(self.shard,self.zp.at[frm if receive else self.z],self.s.at[dz],self.r.at[dz],dev(to,self.core,self.rows))
    def local(self):
        return pltpu.make_async_copy(self.shard,self.zp.at[self.z],self.lo.at[0])
    def start(self):
        for dz in range(1,NZ): self.copy(dz).start()
        self.local().start()
    def wait(self):
        for dz in range(1,NZ): self.copy(dz,True).wait_recv()
    def finish(self):
        for dz in range(1,NZ): self.copy(dz).wait_send()
        self.local().wait()


class GatherXY:
    SEMS=[(NZ,NR),(NZ,NR),(NZ,NR),(NZ,NR),(1,)]
    def __init__(self,zp,full,sems):
        self.zp,self.full=zp,full
        self.sx,self.rx,self.sc,self.rc,self.lo=sems
        self.z,self.core,self.rows=here()
    def place(self,t):
        return self.rows if t==0 else partner_xy(self.rows,t)
    def to(self,t):
        return dev(self.z,self.core,self.place(t))
    def xcopy(self,k,t,receive=False):
        return rcopy(self.zp.at[k],self.full.at[k,self.core,self.place(t) if receive else self.rows],self.sx.at[k,t],self.rx.at[k,t],self.to(t))
    def fcopy(self,k,receive=False):
        t=1 if k<NZ//2 else 2
        ref=self.full.at[k,self.core,self.place(3 if receive else t)]
        return rcopy(ref,ref,self.sx.at[k,3],self.rx.at[k,3],self.to(3-t))
    def ccopy(self,k,t,receive=False):
        src=self.zp.at[k] if t==0 else self.full.at[k,self.core,self.place(t)]
        dst=self.full.at[k,1-self.core if receive else self.core,self.place(t)]
        return rcopy(src,dst,self.sc.at[k,t],self.rc.at[k,t],dev(self.z,1-self.core,self.rows))
    def local(self):
        return pltpu.make_async_copy(self.zp,self.full.at[:,self.core,self.rows],self.lo.at[0])
    def start(self,ks=range(NZ)):
        for k in ks:
            for t in (1,2): self.xcopy(k,t).start()
            self.ccopy(k,0).start()
    def start_local(self):
        self.local().start()
    def step(self,k):
        order=(1,2) if k<NZ//2 else (2,1)
        self.xcopy(k,order[0],True).wait_recv()
        self.fcopy(k).start()
        self.ccopy(k,order[0]).start()
        self.xcopy(k,order[1],True).wait_recv()
        self.ccopy(k,order[1]).start()
    def step2(self,k):
        self.fcopy(k,True).wait_recv()
        self.ccopy(k,3).start()
    def arrive(self,k):
        for t in range(NR): self.ccopy(k,t,True).wait_recv()
    def finish_remote(self):
        for k in range(NZ):
            for t in (1,2): self.xcopy(k,t).wait_send()
            self.fcopy(k).wait_send()
            for t in range(NR): self.ccopy(k,t).wait_send()
    def finish(self):
        self.finish_remote()
        self.local().wait()


class GatherTile:
    def __init__(self,zp,full,width,sems):
        self.zp,self.full,self.width=zp,full,width
        self.sx,self.rx,self.sc,self.rc,self.lo=sems
        self.z,self.core,self.rows=here()
    @staticmethod
    def sems(tiles):
        return [(tiles,NR),(tiles,NR),(tiles,NR),(tiles,NR),(1,)]
    def cols(self,i): return pl.ds(pl.multiple_of(i*self.width,128),self.width)
    def place(self,t):
        return self.rows if t==0 else partner_xy(self.rows,t)
    def to(self,t):
        return dev(self.z,self.core,self.place(t))
    def xcopy(self,i,t,receive=False):
        return rcopy(self.zp.at[:,:,self.cols(i)],self.full.at[:,self.core,self.place(t) if receive else self.rows,:,self.cols(i)],self.sx.at[i,t],self.rx.at[i,t],self.to(t))
    def fcopy(self,i,t,receive=False):
        h=NZ//2
        ref=self.full.at[pl.ds(0 if t==1 else h,h),self.core,self.place(3 if receive else t),:,self.cols(i)]
        q=3 if t==1 else 0
        return rcopy(ref,ref,self.sx.at[i,q],self.rx.at[i,q],self.to(3-t))
    def ccopy(self,i,t,receive=False):
        src=self.zp.at[:,:,self.cols(i)] if t==0 else self.full.at[:,self.core,self.place(t),:,self.cols(i)]
        dst=self.full.at[:,1-self.core if receive else self.core,self.place(t),:,self.cols(i)]
        return rcopy(src,dst,self.sc.at[i,t],self.rc.at[i,t],dev(self.z,1-self.core,self.rows))
    def local(self):
        return pltpu.make_async_copy(self.zp,self.full.at[:,self.core,self.rows],self.lo.at[0])
    def start(self,i):
        for t in (1,2): self.xcopy(i,t).start()
        self.ccopy(i,0).start()
    def step(self,i):
        for t in (1,2):
            self.xcopy(i,t,True).wait_recv()
            self.fcopy(i,t).start()
            self.ccopy(i,t).start()
    def step2(self,i):
        for t in (1,2): self.fcopy(i,t,True).wait_recv()
        self.ccopy(i,3).start()
    def arrive(self,i):
        for t in range(NR): self.ccopy(i,t,True).wait_recv()
    def finish_remote(self,i):
        for t in (1,2):
            self.xcopy(i,t).wait_send()
            self.fcopy(i,t).wait_send()
        for t in range(NR): self.ccopy(i,t).wait_send()


class ScatterZ:
    SEMS=[(NZ,),(NZ,)]
    @staticmethod
    def scratch(r,c,dt):
        return [pltpu.VMEM((NZ,r,c),dt)]
    def __init__(self,zout,out,bufs,sems):
        self.zout,self.out=zout,out
        self.zin,=bufs
        self.s,self.r=sems
        self.z,self.core,self.rows=here()
    def copy(self,dz):
        to=zmod(self.z+dz)
        return rcopy(self.zout.at[to],self.zin.at[dz],self.s.at[dz],self.r.at[dz],dev(to,self.core,self.rows))
    def start(self):
        for dz in range(1,NZ): self.copy(dz).start()
    def step(self):
        for dz in range(1,NZ): self.copy(dz).wait_recv()
        v=self.zout[self.z].astype(F32)
        for dz in range(1,NZ): v=v+self.zin[dz].astype(F32)
        if callable(self.out): self.out(v)
        else: self.out[...]=v
    def finish(self):
        for dz in range(1,NZ): self.copy(dz).wait_send()


class GroupAll:
    N=NZ*NC
    SEMS=[(N,),(N,),(1,)]
    def __init__(self,src,dst,sems):
        self.src,self.dst=src,dst
        self.s,self.r,self.lo=sems
        self.dp=lax.axis_index("dp"); self.rows=lax.axis_index("rows")
    def copy(self,k,receive=False):
        to=lax.rem(self.dp+k,self.N)
        frm=lax.rem(self.dp-k+self.N,self.N)
        return rcopy(self.src,self.dst.at[frm if receive else self.dp],self.s.at[k],self.r.at[k],(to,self.rows))
    def local(self):
        return pltpu.make_async_copy(self.src,self.dst.at[self.dp],self.lo.at[0])
    def start(self):
        for k in range(1,self.N): self.copy(k).start()
        self.local().start()
    def wait(self):
        for k in range(1,self.N): self.copy(k,True).wait_recv()
        self.local().wait()
    def finish(self):
        for k in range(1,self.N): self.copy(k).wait_send()


class Events:
    def __init__(self): self.at={}
    def add(self,slot,fn): self.at.setdefault(slot,[]).append(fn)
    def run(self,outer,inner,width):
        for slot,fns in self.at.items():
            if slot%width==inner:
                @pl.when(outer==slot//width)
                def _(fns=fns):
                    for fn in fns: fn()
NN=(((1,),(0,)),((),()))
C0=0.7978845608028654
C1=0.044715


def dotf(a,b,dims=NN):
    return lax.dot_general(a,b,dims,preferred_element_type=F32)


def loop(n,fn,unroll=1):
    def body(i,c):
        fn(i); return c
    lax.fori_loop(0,n,body,0,unroll=unroll)


def rows_of(i,n):
    return pl.ds(pl.multiple_of(i*n,n),n)


def normal_rows(v):
    d=1.0/v.shape[1]
    c=v-jnp.sum(v,axis=1,keepdims=True)*d
    inv=lax.rsqrt(jnp.sum(c*c,axis=1,keepdims=True)*d+EPSILON)
    return c*inv,inv


def normal_back_rows(g,n,inv):
    d=1.0/g.shape[1]
    return inv*(g-jnp.sum(g,axis=1,keepdims=True)*d-n*(jnp.sum(g*n,axis=1,keepdims=True)*d))


def fold8(v):
    s=v[0:8]
    for k in range(1,v.shape[0]//8): s=s+v[8*k:8*k+8]
    return s


def conv_loops(side,lanes_n,width,forward,finish):
    pass


def shifts(f,ml,mr):
    n=f.shape[0]
    return pltpu.roll(f,1,0)*ml, pltpu.roll(f,n-1,0)*mr


def conv_rows(src,dst_fn,taps,ml_ref,mr_ref,rl_ref,ls,side,cols,unroll=8):
    k=[taps[q:q+1,:] for q in range(9)]
    zero=jnp.zeros((cols,128),F32)
    def body(i,c):
        hm,part=c
        f=src[rows_of(i,cols),ls]
        fm,fp=shifts(f,ml_ref[rows_of(i,cols),:],mr_ref[rows_of(i,cols),:])
        h=[k[3*a]*fm+k[3*a+1]*f+k[3*a+2]*fp for a in range(3)]
        done=part+rl_ref[i]*h[2]
        @pl.when(i>0)
        def _(): dst_fn(i-1,done)
        return h[0],h[1]+rl_ref[i]*hm
    hm,part=lax.fori_loop(0,side,body,(zero,zero),unroll=unroll)
    dst_fn(side-1,part)


def back_rows(g_ref,f_ref,dst_fn,taps,ml_ref,mr_ref,rl_ref,ls,first,count,side,cols,unroll=8):
    k=[taps[q:q+1,:] for q in range(9)]
    z8=jnp.zeros((8,128),F32)
    def at(i): return rows_of(i,cols)
    def load(i):
        g=g_ref[at(i),ls]
        gm,gp=shifts(g,ml_ref[at(i),:],mr_ref[at(i),:])
        return gp,g,gm
    def mix3(gs,a): return k[3*a]*gs[0]+k[3*a+1]*gs[1]+k[3*a+2]*gs[2]
    whole=isinstance(first,int) and count==side
    zero=jnp.zeros((cols,128),F32)
    before=jnp.maximum(first-1,0)
    hp=zero if whole else mix3(load(before),2)
    fprev=zero if whole else f_ref[at(before),ls].astype(F32)
    def body(n,c):
        hp,part,fprev,acc=c
        i=first+n
        gs=load(i)
        done=part+rl_ref[i]*mix3(gs,0)
        @pl.when(n>0)
        def _(): dst_fn(i-1,done)
        f=f_ref[at(i),ls].astype(F32)
        nxt=f_ref[at(jnp.minimum(i+1,side-1)),ls].astype(F32)
        fs=(fprev*rl_ref[i],f,nxt*rl_ref[i+1])
        acc=tuple(acc[3*a+b]+fold8(fs[a]*gs[b]) for a in range(3) for b in range(3))
        return mix3(gs,2),mix3(gs,1)+rl_ref[i]*hp,f,acc
    hp,part,_,acc=lax.fori_loop(0,count,body,(hp,zero,fprev,(z8,)*9),unroll=unroll)
    end=first+count
    if not whole: part=part+rl_ref[end]*mix3(load(jnp.minimum(end,side-1)),0)
    dst_fn(end-1,part)
    return acc


def link_masks(labels):
    side,cols=labels.shape
    left=jnp.pad(labels[:,1:]==labels[:,:-1],((0,0),(1,0)))
    right=jnp.pad(labels[:,1:]==labels[:,:-1],((0,0),(0,1)))
    wide=lambda m: jnp.broadcast_to(m.reshape(side*cols,1).astype(F32),(side*cols,128))
    top=labels[:,0]//2
    rl=jnp.pad((top[1:]==top[:-1]).astype(F32),(1,1))
    return wide(left),wide(right),rl
HBM=pl.BlockSpec(memory_space=pl.ANY)
VM=pl.BlockSpec(memory_space=pltpu.VMEM)
SM=pl.BlockSpec(memory_space=pltpu.SMEM)
NDEV=NZ*NC*NR
S_=jax.ShapeDtypeStruct


def taker(it):
    return lambda cls:[next(it) for _ in cls.SEMS]


def assemble(dst,src,width,at):
    lane=lax.broadcasted_iota(jnp.int32,(1,128),1)
    tiles=dst.shape[1]//128
    for c in range(tiles):
        v=jnp.zeros((16,128),F32)
        for n in range(NDEV):
            lo=n*width-c*128
            if lo+width<=0 or lo>=128: continue
            p=src[n//(NC*NR),(n//NR)%NC,n%NR].astype(F32)
            sh=(lo-at)%128
            if sh: p=pltpu.roll(p,sh,1)
            v=jnp.where((lane>=lo)&(lane<lo+width),p,v)
        dst[:,c*128:(c+1)*128]=v


def enter_kernel(n_z,side,cols,ta,tf,*refs):
    it=iter(refs)
    nx=lambda n:[next(it) for _ in range(n)]
    tok,cond,ada,bias,qkv,taps,ml_ref,mr_ref,rl_ref=nx(9)
    shards=nx(n_z)
    tok_o,cond_o,mod_o,qkv_o,tap_a,tap_f,m1,mix=nx(8)
    zps=nx(n_z)
    condv,condf,part,zq,taps_o,modw,F=nx(7)
    mbufs=nx(5)
    take=taker(it)
    c_all=GroupAll(cond,condv,take(GroupAll))
    swap_t=Swap(tok,tok_o,take(Swap))
    m_all=Scatter(part,mod_o,mbufs,take(Scatter))
    g_taps=Gather(taps,taps_o,take(Gather))
    gq_z=GatherZ(qkv,zq,take(GatherZ))
    gq=GatherXY(zq,qkv_o,take(GatherXY))
    gz=[GatherZ(s,z,take(GatherZ)) for s,z in zip(shards,zps)]
    barrier_all()
    c_all.start()
    gq_z.start()
    swap_t.copy(1).start(); swap_t.copy(2).start(); swap_t.local().start()
    c_all.wait()
    me=lax.axis_index("dp")*NR+lax.axis_index("rows")
    feats=ada.shape[0]
    for d in range(NZ*NC): condf[d*NR:(d+1)*NR,:]=condv[d,0:NR,:].astype(F32)
    cv=condf[...]
    low=(cv/(1.0+jnp.exp(-cv))).astype(BF)
    width=cv.shape[1]
    pick=(lax.broadcasted_iota(jnp.int32,(width,feats),0)==lax.broadcasted_iota(jnp.int32,(width,feats),1)+feats*me).astype(BF)
    mine=jnp.dot(low,pick,preferred_element_type=F32).astype(BF)
    chunk=768
    for c in range(ada.shape[1]//chunk):
        pr=jnp.dot(mine,ada[:,c*chunk:(c+1)*chunk],preferred_element_type=F32)
        for l in range(chunk//128):
            i=c*(chunk//128)+l
            part[:,:,:,i,:]=(pr[:,l*128:(l+1)*128]+bias[i:i+1,:]).reshape(NZ,NC,NR,128)
    cond_o[...]=low
    m_all.start()
    m_all.cstep()
    g_taps.start()
    swap_t.copy(3).start()
    g_taps.run_z()
    gq_z.wait(); gq_z.local().wait()
    gq.start(); gq.start_local()
    m_all.xstep()
    for g in gz: g.start()
    m_all.zstep()
    g_taps.run_x()
    cells,feat=mix.shape
    L=feat//128
    for j in range(2):
        for l in range(L): modw[j:j+1,l*128:(l+1)*128]=mod_o[j*L+l:j*L+l+1,:]
    swap_t.wait()
    shift1=modw[0:1,:]; scale1=modw[1:2,:]
    EC=256
    for b in range(NR):
        n,_=normal_rows(tok_o[b].astype(F32))
        v=(n*(1.0+scale1)+shift1).astype(BF)
        m1[b*EC:(b+1)*EC,:]=v
        F[b*EC:(b+1)*EC,:]=v.astype(F32)
    g_taps.finish()
    assemble(tap_a,taps_o,ta,0)
    assemble(tap_f,taps_o,tf,ta)
    def lanes(l):
        ls=pl.ds(pl.multiple_of(l*128,128),128)
        def put(i,u): mix[rows_of(i,cols),ls]=u.astype(BF)
        conv_rows(F,put,tap_a[:,ls],ml_ref,mr_ref,rl_ref,ls,side,cols,4)
    def some(i):
        for k in range(NZ):
            @pl.when(i==k+1)
            def _(k=k): gq.step(k)
        for k in range(2):
            @pl.when(i==L-2+k)
            def _(k=k): gq.step2(k)
        lanes(i)
    loop(L,some)
    for k in range(2,NZ): gq.step2(k)
    for g in gz: g.wait()
    for k in range(NZ): gq.arrive(k)
    gq.finish()
    for dz in range(1,NZ): gq_z.copy(dz).wait_send()
    for g in [swap_t,c_all,m_all]+gz: g.finish()


def enter(tok,cond_row,ada,bias_rows,qkv,taps,ml,mr,rl,shards,side,cols,ta,tf):
    n=len(shards)
    V=pltpu.VMEM
    feat=tok.shape[2]; cells=side*cols
    scr=[V((NZ*NC,)+cond_row.shape,cond_row.dtype),V((NDEV,cond_row.shape[1]),F32),V((NZ,NC,NR)+bias_rows.shape,F32),V((NZ,)+qkv.shape,BF),V((NZ,NC,NR)+taps.shape,BF),V((8,feat),F32),V((cells,feat),F32)]+Scatter.scratch(bias_rows.shape[0],128,F32)
    sems=sem_types(GroupAll.SEMS)+sem_types(Swap.SEMS)+sem_types(Scatter.SEMS)+sem_types(Gather.SEMS)+sem_types(GatherZ.SEMS)+sem_types(GatherXY.SEMS)+sem_types(GatherZ.SEMS)*n
    outs=[S_(tok.shape,tok.dtype),S_((NDEV,cond_row.shape[1]),BF),S_(bias_rows.shape,F32),S_((NZ,NC,NR)+qkv.shape,qkv.dtype),
          S_((16,NDEV*ta),F32),S_((16,NDEV*tf),F32),S_((cells,feat),BF),S_((cells,feat),BF)]
    outs+=[S_((NZ,)+s.shape,s.dtype) for s in shards]
    return pl.pallas_call(
        functools.partial(enter_kernel,n,side,cols,ta,tf),
        in_specs=[VM,HBM,VM,VM,VM,VM,VM,VM,SM]+[VM]*n,
        out_specs=[VM,VM,VM,HBM,VM,VM,VM,VM]+[HBM]*n,
        out_shape=outs,
        scratch_shapes=scr+sems,
        compiler_params=pltpu.CompilerParams(collective_id=0,has_side_effects=True,vmem_limit_bytes=63<<20),
        name="enter",
    )(tok,cond_row,ada,bias_rows,qkv,taps,ml,mr,rl,*shards)


def forward_kernel(n_w,qb,*refs):
    it=iter(refs)
    mix,qkv,qm,km,cot,late,late2=[next(it) for _ in range(7)]
    zps=[next(it) for _ in range(n_w)]
    proj,att,lse_t,cot_o,late_o,late2_o=[next(it) for _ in range(6)]
    fulls=[next(it) for _ in range(n_w)]
    lse=next(it)
    take=taker(it)
    barrier_all()
    swap_c=Swap(cot,cot_o,take(Swap))
    gs=[GatherXY(a,b,take(GatherXY)) for a,b in zip(zps,fulls)]
    gl=GatherZ(late,late_o,take(GatherZ))
    gl2=GatherZ(late2,late2_o,take(GatherZ))
    gs[0].start(); gs[0].start_local()
    gl2.start(); gl.start()
    swap_c.start()
    ev=Events()
    for k in range(NZ):
        ev.add(2,lambda k=k: gs[0].step(k))
        ev.add(9,lambda k=k: gs[0].step2(k))
    cells,feat=att.shape
    CH=512
    def pr(i):
        proj[rows_of(i,CH),:]=dotf(mix[rows_of(i,CH),:],qkv[...]).astype(BF)
    loop(cells//CH,pr)
    pairs=feat//128
    lane=lax.broadcasted_iota(jnp.int32,(1,128),1)
    lse[...]=jnp.zeros_like(lse)
    def pair(p):
        cq=pl.ds(pl.multiple_of(p*128,128),128)
        ck=pl.ds(pl.multiple_of(feat+p*128,128),128)
        cv=pl.ds(pl.multiple_of(2*feat+p*128,128),128)
        for h in range(2):
            ev.run(p,h,2)
            mine=(lane//64)==h
            k=jnp.where(mine,proj[:,ck],km[...])
            def body(i):
                r=rows_of(i,qb)
                q=jnp.where(mine,proj[r,cq]*jnp.asarray(0.125,BF),qm[r,:])
                s=dotf(q,k,NT)
                m=jnp.max(s,axis=1,keepdims=True)
                e=jnp.exp(s-m)
                l=jnp.sum(e,axis=1,keepdims=True)
                a=(e*(1.0/l)).astype(BF)
                o=dotf(a,proj[:,cv]).astype(BF)
                if h==0:
                    att[r,cq]=o
                else:
                    att[r,cq]=jnp.where(mine,o,att[r,cq])
                lse[r,:]=jnp.where(lane==2*p+h,m+jnp.log(l),lse[r,:])
            loop(cells//qb,body,2)
    loop(pairs,pair)
    lse_t[...]=jnp.transpose(lse[...])
    for g in gs:
        for k in range(NZ): g.arrive(k)
    swap_c.wait()
    gl.wait(); gl2.wait()
    for g in gs+[swap_c,gl,gl2]: g.finish()


def forward(mix,qkv,qm,km,cot,late,late2,zps):
    n=len(zps)
    cells,feat=mix.shape
    outs=[S_((cells,3*feat),BF),S_((cells,feat),BF),S_((128,cells),F32),S_(cot.shape,cot.dtype),S_((NZ,)+late.shape,late.dtype),S_((NZ,)+late2.shape,late2.dtype)]
    outs+=[S_((NZ,NC,NR)+z.shape[1:],z.dtype) for z in zps]
    return pl.pallas_call(
        functools.partial(forward_kernel,n,512),
        in_specs=[VM,VM,VM,VM,VM,VM,VM]+[VM]*n,
        out_specs=[VM,VM,VM,HBM,HBM,HBM]+[HBM]*n,
        out_shape=outs,
        scratch_shapes=[pltpu.VMEM((cells,128),F32)]+sem_types(Swap.SEMS)+sem_types(GatherXY.SEMS)*n+sem_types(GatherZ.SEMS)*2,
        compiler_params=pltpu.CompilerParams(collective_id=1,has_side_effects=True,vmem_limit_bytes=63<<20),
        name="attn_fwd",
    )(mix,qkv,qm,km,cot,late,late2,*zps)


def backward_kernel(n_g,kb,*refs):
    it=iter(refs)
    nx=lambda n:[next(it) for _ in range(n)]
    proj,do,o,qm,km,lse_t,mix,lay,gout=nx(9)
    parts=nx(n_g)
    gp,lay_o,gout_o,zq,lastq=nx(5)
    gouts=nx(n_g)
    qs,dqt,mixt=nx(3)
    obufs=nx(5)
    qbufs=nx(4)
    bufs=[nx(1) for _ in range(n_g)]
    take=taker(it)
    barrier_all()
    sl=Swap(lay,lay_o,take(Swap))
    so=Scatter(gout,gout_o,obufs,take(Scatter))
    uq=PipeScatter(qbufs,take(PipeScatter))
    sc=[ScatterZ(p,g,b,take(ScatterZ)) for p,g,b in zip(parts,gouts,bufs)]
    cells,feat=do.shape
    pairs=feat//128
    W=256
    tiles=pairs//2
    r_=feat//NDEV
    def put_q(m):
        def put(a,v):
            for s in range(3):
                zq[a,:,(s*(tiles-1)+m)*W:(s*(tiles-1)+m+1)*W]=v[:,s*W:(s+1)*W]
        return put
    ev=Events()
    so.start()
    for s in sc: s.start()
    ev.add(1,so.cstep)
    ev.add(2,sl.start)
    ev.add(5,lambda: uq.send_square(0))
    ev.add(6,so.xstep)
    for s in sc: ev.add(7,s.step)
    ev.add(8,lambda: uq.collect(0,put_q(0)))
    ev.add(9,lambda: uq.send_square(1))
    ev.add(11,so.zstep)
    lane=lax.broadcasted_iota(jnp.int32,(1,128),1)
    srow=lax.broadcasted_iota(jnp.int32,(8,128),0)
    slane=lax.broadcasted_iota(jnp.int32,(8,128),1)
    sel=(slane//64==srow).astype(BF)
    def tr(i):
        mixt[:,pl.ds(pl.multiple_of(i*256,256),256)]=jnp.transpose(mix[rows_of(i,256),:])
    loop(cells//256,tr)
    def pair(p):
        cq=pl.ds(pl.multiple_of(p*128,128),128)
        ck=pl.ds(pl.multiple_of(feat+p*128,128),128)
        cv=pl.ds(pl.multiple_of(2*feat+p*128,128),128)
        prod=do[:,cq].astype(F32)*o[:,cq].astype(F32)
        hi=prod.astype(BF); lo=(prod-hi.astype(F32)).astype(BF)
        delta=dotf(sel,hi,NT)+dotf(sel,lo,NT)
        qs[...]=proj[:,cq]*jnp.asarray(0.125,BF)
        for h in range(2):
            ev.run(p,h,2)
            mine=(lane//64)==h
            q=jnp.where(mine,qs[...],qm[...])
            ls=lse_t[pl.ds(2*p+h,1),:]
            dl=delta[h:h+1,:]
            dqt[...]=jnp.zeros_like(dqt)
            def body(i):
                r=rows_of(i,kb)
                kr=proj[r,ck]
                k=jnp.where(mine,kr,km[r,:])
                v=jnp.where(mine,proj[r,cv],jnp.zeros((),BF))
                st=dotf(k,q,NT)
                pt=jnp.exp(st-ls)
                dpt=dotf(v,do[:,cq],NT)
                ds=(pt*(dpt-dl)).astype(BF)
                dv=dotf(pt.astype(BF),do[:,cq]).astype(BF)
                dk=dotf(ds,qs[...]).astype(BF)
                dqt[...]+=dotf(kr,ds,TN)
                if h==0:
                    gp[r,cv]=dv
                    gp[r,ck]=dk
                else:
                    gp[r,cv]=jnp.where(mine,dv,gp[r,cv])
                    gp[r,ck]=jnp.where(mine,dk,gp[r,ck])
            loop(cells//kb,body,2)
            dq=(jnp.transpose(dqt[...])*0.125).astype(BF)
            if h==0:
                gp[:,cq]=dq
            else:
                gp[:,cq]=jnp.where(mine,dq,gp[:,cq])
        @pl.when(lax.rem(p,2)==1)
        def _():
            m=p//2
            s=lax.rem(m,2)
            n=NC*NR*r_
            def tile(i):
                for c in range(3):
                    cols=pl.ds(pl.multiple_of(c*feat+m*W,W),W)
                    uq.part[s,i,:,:,:,c*W:(c+1)*W]=dotf(mixt[rows_of(i,n),:],gp[:,cols]).astype(BF).reshape(NC,NR,r_,W)
            loop(NZ,tile)
            @pl.when(m<tiles-1)
            def _(): uq.send_core(s)
    loop(pairs,pair)
    uq.collect(1,put_q(1))
    lastq[...]=uq.part[0]
    sl.wait()
    for s in sc+[sl,so]: s.finish()


def backward(proj,do,o,qm,km,lse_t,mix,lay,gout,parts):
    n=len(parts)
    cells,feat=do.shape
    r_=feat//NDEV
    outs=[S_((cells,3*feat),BF),S_(lay.shape,lay.dtype),S_(gout.shape[3:],F32),S_((NZ,r_,2*feat),BF),S_((NZ,NC,NR,r_,feat),BF)]+[S_(p.shape[1:],F32) for p in parts]
    scr=[pltpu.VMEM((cells,128),BF),pltpu.VMEM((128,cells),F32),pltpu.VMEM((feat,cells),BF)]
    scr+=Scatter.scratch(gout.shape[3],gout.shape[4],gout.dtype)+PipeScatter.scratch(r_,feat)
    for p in parts: scr+=ScatterZ.scratch(p.shape[1],p.shape[2],p.dtype)
    return pl.pallas_call(
        functools.partial(backward_kernel,n,512),
        in_specs=[VM,VM,VM,VM,VM,VM,VM,VM,HBM]+[VM]*n,
        out_specs=[VM,HBM,VM,VM,VM]+[VM]*n,
        out_shape=outs,
        scratch_shapes=scr+sem_types(Swap.SEMS)+sem_types(Scatter.SEMS)+sem_types(PipeScatter.SEMS)+sem_types(ScatterZ.SEMS)*n,
        compiler_params=pltpu.CompilerParams(collective_id=2,has_side_effects=True,vmem_limit_bytes=63<<20),
        name="attn_bwd",
    )(proj,do,o,qm,km,lse_t,mix,lay,gout,*parts)


def spread(dst,src_ref,width,at):
    lane=lax.broadcasted_iota(jnp.int32,(1,128),1)
    for n in range(NDEV):
        lo=n*width
        c,off=lo//128,lo%128
        sh=(at-off)%128
        v=src_ref[:,c*128:(c+1)*128]
        v=pltpu.roll(v,sh,1) if sh else v
        if off+width>128:
            w=src_ref[:,(c+1)*128:(c+2)*128]
            w=pltpu.roll(w,sh,1) if sh else w
            v=jnp.where(lane<at+128-off,v,w)
        keep=(lane>=at)&(lane<at+width)
        i=(n//(NC*NR),(n//NR)%NC,n%NR)
        if at==0: dst[i]=jnp.where(keep,v,0.0)
        else: dst[i]=jnp.where(keep,v,dst[i])


def tail_kernel(side,cols,ta,tf,*refs):
    it=iter(refs)
    nx=lambda n:[next(it) for _ in range(n)]
    gproj_h,qkv_h,m1,x_ref,gmid_h,mod,tap_ref,ml_ref,mr_ref,rl_ref,sums,gkf,low,ada,zq,lastq=nx(16)
    tg_o,ctx_o,adag_o,gm_o,q_o,ka_o,kf_o=nx(7)
    G,gm1,tgb,tgin,ktap,gme,gml,gmev,gmlv,ctxs,ctxv,tpart,gproj,qkv,gmid,lsem=nx(16)
    zbufs=nx(1); lbufs=nx(5); tbufs=nx(5)
    take=taker(it)
    loads=[pltpu.make_async_copy(a,b,lsem.at[i]) for i,(a,b) in enumerate(((gproj_h,gproj),(qkv_h,qkv),(gmid_h,gmid)))]
    for l in loads: l.start()
    barrier_all()
    def put_z(v):
        n=v.shape[1]//3
        for s in range(3): q_o[:,s*n*3//2:s*n*3//2+n]=v[:,s*n:(s+1)*n]
    def put_l(v):
        n=v.shape[1]//3
        for s in range(3): q_o[:,(3*s+2)*n:(3*s+3)*n]=v[:,s*n:(s+1)*n]
    def put_t(v):
        ka_o[...]=v[0:9,0:ta]
        kf_o[...]=pltpu.roll(v,128-ta,1)[0:9,0:tf]
    sz=ScatterZ(zq,put_z,zbufs,take(ScatterZ))
    slq=Scatter(lastq,put_l,lbufs,take(Scatter))
    stp=Scatter(tpart,put_t,tbufs,take(Scatter))
    st=Swap(tgb,tgin,take(Swap))
    ge=AllToAll(gme,gmev,take(AllToAll),one=True)
    gl=AllToAll(gml,gmlv,take(AllToAll),one=True)
    xa=AllToAll(ctxs,ctxv,take(AllToAll))
    slq.start(); sz.start()
    cells,feat=x_ref.shape
    L=feat//128
    for i,q in enumerate((3,1,2,0)):
        for l in range(L):
            gme[i*L+l:i*L+l+1,:]=sums[q:q+1,l*128:(l+1)*128].astype(BF)
    ge.start()
    CH=1024; EC=256
    for l in loads: l.wait()
    def a(i):
        r=rows_of(i,CH)
        G[r,:]=dotf(gproj[r,:],qkv[...],NT).astype(BF).astype(F32)
    loop(cells//CH,a)
    slq.cstep()
    ktap[...]=jnp.zeros_like(ktap)
    shift1=mod[0:1,:]; scale1=mod[1:2,:]
    z8=jnp.zeros((8,feat),F32)
    block=cells//NR
    c=(z8,z8)
    per=side//NR
    for t in (3,1,2,0):
        to=partner_xy(st.rows,t) if t else st.rows
        def lanes(l):
            ls=pl.ds(pl.multiple_of(l*128,128),128)
            def put(i,u): gm1[rows_of(i,cols),ls]=u
            acc=back_rows(G,m1,put,tap_ref[:,ls],ml_ref,mr_ref,rl_ref,ls,to*per,per,side,cols,4)
            for q in range(9): ktap[q:q+1,ls]+=jnp.sum(acc[q],axis=0,keepdims=True)
        loop(L,lanes)
        r=rows_of(to,block)
        n,inv=normal_rows(x_ref[r,:].astype(F32))
        g=gm1[r,:]
        tgb[to]=(gmid[r,:]+normal_back_rows(g*(1.0+scale1),n,inv)).astype(BF)
        c=(c[0]+fold8(g),c[1]+fold8(g*n))
        if t: st.copy(t).start()
        else: st.local().start()
        if t==1: slq.xstep()
    spread(tpart,ktap,ta,0)
    spread(tpart,gkf,tf,ta)
    stp.start()
    for i,v in enumerate(c):
        v=jnp.sum(v,axis=0,keepdims=True)
        for l in range(L): gml[i*L+l:i*L+l+1,:]=v[:,l*128:(l+1)*128].astype(BF)
    gml[2*L:16,:]=jnp.zeros((16-2*L,128),BF)
    gl.start()
    me=gl.me
    feats=ada.shape[0]
    width=low.shape[1]
    pick=(lax.broadcasted_iota(jnp.int32,(width,feats),0)==lax.broadcasted_iota(jnp.int32,(width,feats),1)+feats*me).astype(BF)
    mine=jnp.dot(low[...],pick,preferred_element_type=F32).astype(BF)
    acc=jnp.zeros((NDEV,feats),F32)
    ge.wait()
    def use(src,n,base,acc):
        for i in range(n):
            g=src[:,i,:]
            j=base+i
            adag_o[:,j*128:(j+1)*128]=lax.dot_general(mine,g,TN,preferred_element_type=F32)
            gm_o[j:j+1,:]=jnp.sum(g.astype(F32),axis=0,keepdims=True)
            acc=acc+lax.dot_general(g,ada[:,j*128:(j+1)*128],NT,preferred_element_type=F32)
        return acc
    acc=use(gmev,4*L,2*L,acc)
    stp.cstep()
    gl.wait()
    acc=use(gmlv,2*L,0,acc)
    for n in range(NDEV):
        g0=(n//NR)*NR
        ctxs[n,0:NR,0:feats]=acc[g0:g0+NR,:]
    xa.start()
    sz.step()
    slq.zstep()
    stp.xstep()
    st.wait()
    def up(i):
        for b in range(NR):
            tg_o[b,rows_of(i,EC),:]=tgin[b,rows_of(i,EC),:].astype(F32)
    loop(block//EC,up)
    stp.zstep()
    xa.wait()
    ctx_o[...]=ctxv[...]
    for s in (sz,slq,stp,st,ge,gl,xa): s.finish()


def tail(gproj,qkv,m1,x,gmid,mod,taps,ml,mr,rl,sums,gkf,low,ada,zq,lastq,side,cols,ta,tf):
    cells,feat=x.shape
    block=cells//NR
    r_=feat//NDEV
    V=pltpu.VMEM
    L=feat//128
    outs=[S_((NR,block,feat),F32),S_((NDEV,8,128),F32),S_(ada.shape,F32),S_((6*L,128),F32),S_((r_,3*feat),F32),S_((9,ta),F32),S_((9,tf),F32)]
    scr=[V((cells,feat),F32),V((cells,feat),F32),V((NR,block,feat),BF),V((NR,block,feat),BF),V((16,feat),F32),
         V((4*L,128),BF),V((16,128),BF),V((NDEV,4*L,128),BF),V((NDEV,16,128),BF),V((NDEV,8,128),F32),V((NDEV,8,128),F32),V((NZ,NC,NR,16,128),F32),V(gproj.shape,BF),V(qkv.shape,BF),V(gmid.shape,F32),pltpu.SemaphoreType.DMA((3,))]
    scr+=ScatterZ.scratch(r_,zq.shape[2],BF)+Scatter.scratch(r_,feat,BF)+Scatter.scratch(16,128,F32)
    sems=sem_types(ScatterZ.SEMS)+sem_types(Scatter.SEMS)*2+sem_types(Swap.SEMS)+sem_types(AllToAll.SEMS)*3
    return pl.pallas_call(
        functools.partial(tail_kernel,side,cols,ta,tf),
        in_specs=[HBM,HBM,VM,VM,HBM]+[VM]*4+[SM]+[VM]*6,
        out_specs=[VM]*7,
        out_shape=outs,
        scratch_shapes=scr+sems,
        compiler_params=pltpu.CompilerParams(collective_id=3,has_side_effects=True,vmem_limit_bytes=63<<20),
        name="tail",
    )(gproj,qkv,m1,x,gmid,mod,taps,ml,mr,rl,sums,gkf,low,ada,zq,lastq)


def greet(targets):
    bar=pltpu.get_barrier_semaphore()
    for d in targets:
        pl.semaphore_signal(bar,inc=1,device_id=d,device_id_type=MESH)
    pl.semaphore_wait(bar,len(targets))


def near():
    z,core,rows=here()
    return [dev(z,1-core,rows)]+[dev(z,core,partner_xy(rows,t)) for t in range(1,NR)]


class PipeScatter:
    SEMS=[(2,),(2,),(2,NR),(2,NR)]
    @staticmethod
    def scratch(r,c):
        return [pltpu.VMEM((2,NZ,NC,NR,r,c),BF),pltpu.VMEM((2,NZ,NR,r,c),BF),pltpu.VMEM((2,NZ,NR,r,c),BF),pltpu.VMEM((2,NR,NZ,r,c),BF)]
    def __init__(self,bufs,sems):
        self.part,self.sib,self.own,self.xin=bufs
        self.sc,self.rc,self.sx,self.rx=sems
        self.z,self.core,self.rows=here()
    def ccopy(self,s):
        return rcopy(self.part.at[s,:,1-self.core],self.sib.at[s],self.sc.at[s],self.rc.at[s],dev(self.z,1-self.core,self.rows))
    def xcopy(self,s,t):
        to=partner_xy(self.rows,t)
        return rcopy(self.own.at[s,:,to],self.xin.at[s,t],self.sx.at[s,t],self.rx.at[s,t],dev(self.z,self.core,to))
    def send_core(self,s):
        self.ccopy(s).start()
    def send_square(self,s):
        self.ccopy(s).wait()
        def body(i):
            a,b=i//NR,lax.rem(i,NR)
            self.own[s,a,b]=(self.part[s,a,self.core,b].astype(F32)+self.sib[s,a,b].astype(F32)).astype(BF)
        loop(NZ*NR,body)
        for t in range(1,NR): self.xcopy(s,t).start()
    def collect(self,s,put):
        for t in range(1,NR): self.xcopy(s,t).wait()
        def body(a):
            v=self.own[s,a,self.rows].astype(F32)
            for t in range(1,NR): v=v+self.xin[s,t,a].astype(F32)
            put(a,v.astype(BF))
        loop(NZ,body)


class RowScatter:
    SEMS=[(2,),(2,),(2,NR),(2,NR)]
    @staticmethod
    def scratch(r,c):
        return [pltpu.VMEM((2,NR,r,c),BF),pltpu.VMEM((2,NR,r,c),BF),pltpu.VMEM((2,NR,r,c),BF)]
    def __init__(self,part,zout,bufs,sems):
        self.part,self.zout=part,zout
        self.sib,self.own,self.xin=bufs
        self.sc,self.rc,self.sx,self.rx=sems
        self.z,self.core,self.rows=here()
    def ccopy(self,k):
        s=k%2
        return rcopy(self.part.at[k,1-self.core],self.sib.at[s],self.sc.at[s],self.rc.at[s],dev(self.z,1-self.core,self.rows))
    def xcopy(self,k,t):
        s=k%2
        to=partner_xy(self.rows,t)
        return rcopy(self.own.at[s,to],self.xin.at[s,t],self.sx.at[s,t],self.rx.at[s,t],dev(self.z,self.core,to))
    def send_core(self,k):
        self.ccopy(k).start()
    def send_square(self,k):
        self.ccopy(k).wait()
        s=k%2
        def body(b):
            self.own[s,b]=(self.part[k,self.core,b].astype(F32)+self.sib[s,b].astype(F32)).astype(BF)
        loop(NR,body)
        for t in range(1,NR): self.xcopy(k,t).start()
    def collect(self,k):
        s=k%2
        for t in range(1,NR): self.xcopy(k,t).wait()
        v=self.own[s,self.rows].astype(F32)
        for t in range(1,NR): v=v+self.xin[s,t].astype(F32)
        self.zout[k]=v.astype(BF)


def ffn_kernel_body(*refs,side,cols):
    it=iter(refs)
    nx=lambda n:[next(it) for _ in range(n)]
    x_ref,att_ref,cot_ref,mod_ref,outw_ref,zpu,zpd,tap_ref,ml_ref,mr_ref,rl_ref=nx(11)
    lay_ref,gmid_ref,gatt_ref,gout_ref,zup,zdown,gtap_ref,sums_ref=nx(8)
    m2,m2t,gffn,branch,fb,gm2,F,G,glow,gub,dfull,ufull,gd,ucur=nx(14)
    ubufs=nx(4); dbufs=nx(3)
    take=taker(it)
    ga=GatherXY(zpd,dfull,take(GatherXY))
    T=F.shape[1]
    gu=GatherTile(zpu,ufull,T,nx(5))
    middle=gmid_ref
    us=PipeScatter(ubufs,take(PipeScatter))
    ds=RowScatter(gd,zdown,dbufs,take(RowScatter))
    t=pl.program_id(0)
    cells,feat=x_ref.shape
    hidden=NDEV*zpd.shape[1]
    steps=hidden//T; last=steps-1
    block=hidden//NZ
    CH=1024; EC=256
    shift2=mod_ref[3:4,:]; scale2=mod_ref[4:5,:]; gate2=mod_ref[5:6,:]; gate1=mod_ref[2:3,:]
    slot=lax.rem(t,2); other=lax.rem(t+1,2)
    ready={}
    for k in range(NZ): ready[k]=-(-((k+1)*block)//T)-1
    need={}
    for k in range(NZ): need[k]=(k*block)//T
    def put_up(tile):
        def put(a,v): zup[a,:,pl.ds(pl.multiple_of(tile*T,128),T)]=v
        return put

    @pl.when(t==0)
    def _():
        greet(near())
        gu.local().start(); ga.start_local()
        gu.start(0); ga.start([0])
        def a(i):
            branch[rows_of(i,CH),:]=dotf(att_ref[rows_of(i,CH),:],outw_ref[...])
        loop(cells//CH,a)
        def b(i):
            r=rows_of(i,EC)
            mid=x_ref[r,:].astype(F32)+gate1*branch[r,:]
            middle[r,:]=mid
            n,_=normal_rows(mid)
            m2[r,:]=(n*(1.0+scale2)+shift2).astype(BF)
            gffn[r,:]=(gate2*cot_ref[r,:].astype(F32)).astype(BF)
        loop(cells//EC,b)
        gu.step(0); ga.step(0)
        gu.start(1); ga.start([1])
        def c(i):
            r=rows_of(i,CH)
            m2t[:,pl.ds(pl.multiple_of(i*CH,CH),CH)]=jnp.transpose(m2[r,:])
            fb[r,:]=jnp.zeros((CH,feat),F32)
            gm2[r,:]=jnp.zeros((CH,feat),F32)
        loop(cells//CH,c)
        gu.step2(0); ga.step2(0)
        ga.local().wait(); gu.local().wait()
    gu.arrive(t)
    for k in range(NZ):
        @pl.when(t==need[k])
        def _(k=k): ga.arrive(k)
    dw=dfull.reshape(hidden,feat)
    tc=pl.ds(pl.multiple_of(t*T,T),T)
    def flat(i):
        n=feat//NZ
        ucur[rows_of(i,n),:]=ufull[i,:,:,:,tc].reshape(n,T)
    loop(NZ,flat)
    gdw=gd.reshape(hidden,feat)
    tr=pl.ds(pl.multiple_of(t*T,T),T)
    def first(i):
        r=rows_of(i,CH)
        F[r,:]=dotf(m2[r,:],ucur[...]).astype(BF).astype(F32)
        G[r,:]=dotf(gffn[r,:],dw[tr,:],NT)
    loop(cells//CH,first)
    @pl.when(t<last)
    def _(): gu.step(t+1)
    for k in range(1,NZ):
        @pl.when(t==k-1)
        def _(k=k): ga.step(k)
    @pl.when(t<last-1)
    def _(): gu.start(t+2)
    for k in range(2,NZ):
        @pl.when(t==k-2)
        def _(k=k): ga.start([k])

    def forward_lanes(l):
        ls=pl.ds(pl.multiple_of(l*128,128),128)
        def put(i,u):
            r=rows_of(i,cols)
            u2=u*u
            th=jnp.tanh(C0*(u+C1*(u2*u)))
            half=0.5*(1.0+th)
            glow[r,ls]=(u*half).astype(BF)
            d=half+(0.5*u)*(1.0-th*th)*(C0*(1.0+(3.0*C1)*u2))
            G[r,ls]=(G[r,ls]*d).astype(BF).astype(F32)
        conv_rows(F,put,tap_ref[:,ls],ml_ref,mr_ref,rl_ref,ls,side,cols)
    loop(T//128,forward_lanes)
    @pl.when(t<last)
    def _(): gu.step2(t+1)
    @pl.when(t>=2)
    def _(): us.collect(slot,put_up(t-2))
    for k in range(NZ):
        if ready[k]+2<=last:
            @pl.when(t==ready[k]+2)
            def _(k=k): ds.collect(k)
    @pl.when(t>=1)
    def _():
        us.send_square(other)
    for k in range(NZ):
        if ready[k]+1<=last:
            @pl.when(t==ready[k]+1)
            def _(k=k): ds.send_square(k)
    def back_lanes(l):
        ls=pl.ds(pl.multiple_of(l*128,128),128)
        def put2(i,u):
            gub[rows_of(i,cols),ls]=u.astype(BF)
        acc=back_rows(G,F,put2,tap_ref[:,ls],ml_ref,mr_ref,rl_ref,ls,0,side,side,cols)
        for q in range(9):
            gtap_ref[q:q+1,ls]=jnp.sum(acc[q],axis=0,keepdims=True)
    loop(T//128,back_lanes)
    for k in range(1,NZ):
        @pl.when(t==k-1)
        def _(k=k): ga.step2(k)
    gtap_ref[9:16,:]=jnp.zeros((7,T),F32)

    r_=feat//NDEV
    def third(i):
        n=NC*NR*r_
        us.part[slot,i]=dotf(m2t[rows_of(i,n),:],gub[...]).astype(BF).reshape(NC,NR,r_,T)
    loop(NZ,third)
    us.send_core(slot)
    for i in range(T//256):
        gdw[pl.ds(pl.multiple_of(t*T+i*256,256),256),:]=dotf(glow[:,i*256:(i+1)*256],gffn[...],TN).astype(BF)
    for k in range(NZ):
        @pl.when(t==ready[k])
        def _(k=k): ds.send_core(k)
    def second(i):
        r=rows_of(i,CH)
        fb[r,:]+=dotf(glow[r,:],dw[tr,:])
        gm2[r,:]+=dotf(gub[r,:],ucur[...],NT)
    loop(cells//CH,second)

    @pl.when(t==last)
    def _():
        us.collect(other,put_up(last-1))
        late=[k for k in range(NZ) if ready[k]+1>last]
        mid_=[k for k in range(NZ) if ready[k]+1==last]
        for k in mid_: ds.collect(k)
        us.send_square(slot)
        for k in late: ds.send_square(k)
        z=jnp.zeros((8,feat),F32)
        def body(i,c):
            sg2,ss2,sc2,sg1=c
            r=rows_of(i,EC)
            inc=cot_ref[r,:].astype(F32)
            mid=middle[r,:]
            n,inv=normal_rows(mid)
            lay_ref[r,:]=(mid+gate2*fb[r,:]).astype(BF)
            gm=gm2[r,:]
            gmid=inc+normal_back_rows(gm*(1.0+scale2),n,inv)
            gmid_ref[r,:]=gmid
            gffn[r,:]=(gate1*gmid).astype(BF)
            return (sg2+fold8(inc*fb[r,:]),ss2+fold8(gm),sc2+fold8(gm*n),sg1+fold8(gmid*branch[r,:]))
        res=lax.fori_loop(0,cells//EC,body,(z,z,z,z))
        for q in range(4):
            sums_ref[q:q+1,:]=jnp.sum(res[q],axis=0,keepdims=True)
        sums_ref[4:8,:]=jnp.zeros((4,feat),F32)
        def b(i):
            r=rows_of(i,CH)
            gatt_ref[r,:]=dotf(gffn[r,:],outw_ref[...],NT).astype(BF)
        loop(cells//CH,b)
        for i in range(feat//256):
            gout_ref[i*256:(i+1)*256,:]=dotf(att_ref[:,i*256:(i+1)*256],gffn[...],TN).astype(BF)
        us.collect(slot,put_up(last))
        for k in late: ds.collect(k)
        ga.finish_remote()
        loop(steps,gu.finish_remote)


def ffn(x,att,cot,mod6,outw,zpu,zpd,taps,ml,mr,rl,side,cols,T=512):
    cells,feat=x.shape
    hidden=zpu.shape[2]
    vm=lambda shape: pl.BlockSpec(shape,lambda t:(0,)*len(shape),pipeline_mode=pl.Buffered(1))
    r_,d_=feat//NDEV,hidden//NDEV
    return pl.pallas_call(
        functools.partial(ffn_kernel_body,side=side,cols=cols),
        grid=(hidden//T,),
        in_specs=[vm((cells,feat)),vm((cells,feat)),vm((cells,feat)),vm((8,feat)),vm((feat,feat)),
                  HBM,HBM,pl.BlockSpec((16,T),lambda t:(0,t)),
                  vm((cells,128)),vm((cells,128)),SM],
        out_specs=[vm((cells,feat)),vm((cells,feat)),vm((cells,feat)),vm((feat,feat)),
                   vm((NZ,r_,hidden)),vm((NZ,d_,feat)),pl.BlockSpec((16,T),lambda t:(0,t)),vm((8,feat))],
        out_shape=[S_((cells,feat),BF),S_((cells,feat),F32),S_((cells,feat),BF),S_((feat,feat),BF),S_((NZ,r_,hidden),BF),S_((NZ,d_,feat),BF),S_((16,hidden),F32),S_((8,feat),F32)],
        scratch_shapes=[pltpu.VMEM((cells,feat),BF),pltpu.VMEM((feat,cells),BF),pltpu.VMEM((cells,feat),BF),
                        pltpu.VMEM((cells,feat),F32),pltpu.VMEM((cells,feat),F32),pltpu.VMEM((cells,feat),F32),
                        pltpu.VMEM((cells,T),F32),pltpu.VMEM((cells,T),F32),pltpu.VMEM((cells,T),BF),pltpu.VMEM((cells,T),BF),
                        pltpu.VMEM((NZ,NC,NR,d_,feat),BF),pltpu.VMEM((NZ,NC,NR,r_,hidden),BF),pltpu.VMEM((NZ,NC,NR,d_,feat),BF),pltpu.VMEM((feat,T),BF)]
                       +PipeScatter.scratch(r_,T)+RowScatter.scratch(d_,feat)
                       +sem_types(GatherXY.SEMS)+sem_types(GatherTile.sems(hidden//T))+sem_types(PipeScatter.SEMS)+sem_types(RowScatter.SEMS),
        compiler_params=pltpu.CompilerParams(dimension_semantics=("arbitrary",),vmem_limit_bytes=63<<20,collective_id=4,has_side_effects=True),
        name="ffn",
    )(x,att,cot,mod6,outw,zpu,zpd,taps,ml,mr,rl)
def own_rows(padded_cells):
    return jnp.pad(padded_cells,((0,0),(1,1),(1,1),(0,0)))


def fast(tokens,conditioning,item_map,ada_weight,ada_bias,attn_kernel,qkv_weight,out_weight,up_weight,ffn_kernel,down_weight,out_cotangent):
    canvases,rows_here,cols,features=tokens.shape
    side=rows_here*NR
    cells=side*cols
    rows=lax.axis_index("rows"); dp=lax.axis_index("dp"); me=dp*NR+rows
    hidden=up_weight.shape[1]
    cond_row=jnp.pad(conditioning,((0,8-NR),(0,0)))
    mod_cols=ada_weight.shape[1]
    bshard=ada_bias.shape[0]
    bias_rows=lax.dynamic_update_slice_in_dim(jnp.zeros((mod_cols,),F32),ada_bias.astype(F32),me*bshard,0).reshape(mod_cols//128,128)
    ta,tf=attn_kernel.shape[1],ffn_kernel.shape[1]
    taps=jnp.pad(jnp.concatenate([attn_kernel,ffn_kernel],axis=1),((0,7),(0,128-ta-tf)))
    blocks=(NR,rows_here*cols,features)
    labels=lax.dynamic_index_in_dim(item_map,rows,0,keepdims=False)
    qm,km=head_masks(labels.reshape(cells))
    ml,mr,rl=link_masks(labels)
    tok,low_all,mod,qkv_f,tap_a,tap_f,m1,mix,*zps=enter(tokens.reshape(blocks),cond_row,ada_weight,bias_rows,qkv_weight,taps,ml,mr,rl,[out_weight],side,cols,ta,tf)
    full2=lambda a:a.reshape(-1,a.shape[-1])
    triple_full=full2(qkv_f)
    mod6=jnp.pad(mod.reshape(6,features),((0,2),(0,0)))
    proj,attended,lse_t,cot,zp_down,zp_up,out_f=forward(mix,triple_full,qm,km,out_cotangent.reshape(blocks),down_weight,up_weight,zps)
    lay,gmid,gatt,g_out,z_up,z_down,g_kffn,sums=ffn(
        tok.reshape(cells,features),attended,cot.reshape(cells,features),mod6,
        full2(out_f),zp_up,zp_down,tap_f,ml,mr,rl,side,cols)
    sp=lambda g:g.reshape(NZ,NC,NR,g.shape[0]//NDEV,g.shape[1])
    gproj,lay_o,o_o,zq,lastq,u_o,d_o=backward(proj,gatt,attended,qm,km,lse_t,mix,lay.reshape(blocks),sp(g_out),[z_up,z_down])
    tg,ctx,adag,gmsum,q_o,ka_o,kf_o=tail(gproj,triple_full,m1,tok.reshape(cells,features),gmid,mod6,
        tap_a,ml,mr,rl,sums,g_kffn,low_all,ada_weight,zq,lastq,side,cols,ta,tf)
    shape4=(NR,rows_here,cols,features)
    feats=ada_weight.shape[0]
    dsilu=ctx[:,:NR,:feats].transpose(1,0,2).reshape(NR,features)
    cv=conditioning.astype(F32)
    _,sback=jax.vjp(jax.nn.silu,cv)
    dctx=sback(dsilu)[0]
    gbias=lax.dynamic_slice_in_dim(gmsum.reshape(mod_cols),me*bshard,bshard,0)
    return (lay_o.reshape(shape4),tg.reshape(shape4),dctx,adag,gbias,ka_o,q_o,o_o,u_o,kf_o,d_o)


def solution(mesh):
    quick=dict(mesh.shape)=={"dp":NZ*NC,"rows":NR}
    return jax.shard_map(
        fast if quick else local,
        mesh=mesh,
        in_specs=(
            P("dp", "rows", None, None),
            P("dp", None),
            P("dp", None, None),
            P(("dp", "rows"), None),
            P(("dp", "rows")),
            P(None, ("dp", "rows")),
            P(("dp", "rows"), None),
            P(("dp", "rows"), None),
            P(("dp", "rows"), None),
            P(None, ("dp", "rows")),
            P(("dp", "rows"), None),
            P("dp", "rows", None, None),
        ),
        out_specs=(
            P("dp", "rows", None, None),
            P("dp", "rows", None, None),
            P("dp", None),
            P(("dp", "rows"), None),
            P(("dp", "rows")),
            P(None, ("dp", "rows")),
            P(("dp", "rows"), None),
            P(("dp", "rows"), None),
            P(("dp", "rows"), None),
            P(None, ("dp", "rows")),
            P(("dp", "rows"), None),
        ),
        check_vma=False,
    )
```

```python
import functools

import jax
import jax.numpy as jnp
from jax import lax
from jax.experimental import pallas as pl
from jax.experimental.pallas import tpu as pltpu
from jax.sharding import PartitionSpec as P

PER_GROUP_WIDTH = 64


EPSILON = 1e-06


def padded(block, sides, width):
    for axis, dim in sides:
        count = lax.axis_size(axis)
        forward = [(i, i + 1) for i in range(count - 1)]
        backward = [(target, source) for source, target in forward]
        low = lax.ppermute(
            lax.slice_in_dim(block, block.shape[dim] - width, None, axis=dim), axis, forward
        )
        high = lax.ppermute(lax.slice_in_dim(block, 0, width, axis=dim), axis, backward)
        block = jnp.concatenate([low, block, high], axis=dim)
    return block


def normalize(attended_content_array):
    average = jnp.mean(attended_content_array, axis=-1, keepdims=True)
    centred = attended_content_array - average
    inverse = lax.rsqrt(jnp.mean(centred * centred, axis=-1, keepdims=True) + EPSILON)
    return (centred * inverse, inverse)


def normalize_back(incoming, normalized_rows, inverse):
    return inverse * (
        incoming
        - jnp.mean(incoming, axis=-1, keepdims=True)
        - normalized_rows * jnp.mean(incoming * normalized_rows, axis=-1, keepdims=True)
    )


def widen_cols(rimmed):
    return jnp.pad(rimmed, ((0, 0), (0, 0), (1, 1), (0, 0)))


def tap_mask(labels_pad, centre, row_off, col_off):
    rows_here = centre.shape[1]
    cols_here = centre.shape[2]
    return (labels_pad[:, row_off : row_off + rows_here, col_off : col_off + cols_here] == centre)[
        ..., None
    ]


def conv_forward(padded_rows, labels_pad, centre, kernel):
    rows_here = centre.shape[1]
    cols_here = centre.shape[2]
    summed = jnp.zeros(centre.shape + (kernel.shape[1],), jnp.float32)
    for row_off in range(3):
        for col_off in range(3):
            window = padded_rows[
                :, row_off : row_off + rows_here, col_off : col_off + cols_here
            ].astype(jnp.float32)
            tapped = kernel[3 * row_off + col_off].astype(jnp.float32) * window
            summed = summed + jnp.where(tap_mask(labels_pad, centre, row_off, col_off), tapped, 0.0)
    return summed


def conv_mirror(padded_rows, labels_pad, centre, kernel):
    rows_here = centre.shape[1]
    cols_here = centre.shape[2]
    summed = jnp.zeros(centre.shape + (kernel.shape[1],), jnp.float32)
    for row_off in range(3):
        for col_off in range(3):
            row_from = 2 - row_off
            col_from = 2 - col_off
            window = padded_rows[
                :, row_from : row_from + rows_here, col_from : col_from + cols_here
            ].astype(jnp.float32)
            tapped = kernel[3 * row_off + col_off].astype(jnp.float32) * window
            summed = summed + jnp.where(
                tap_mask(labels_pad, centre, row_from, col_from), tapped, 0.0
            )
    return summed


def kernel_grad(incoming, padded_rows, labels_pad, centre):
    rows_here = centre.shape[1]
    cols_here = centre.shape[2]
    incoming_values = incoming.astype(jnp.float32)
    tap_sums = []
    for row_off in range(3):
        for col_off in range(3):
            window = padded_rows[
                :, row_off : row_off + rows_here, col_off : col_off + cols_here
            ].astype(jnp.float32)
            product = jnp.where(
                tap_mask(labels_pad, centre, row_off, col_off), incoming_values * window, 0.0
            )
            tap_sums.append(jnp.sum(product, axis=(0, 1, 2)))
    return jnp.stack(tap_sums, axis=0)


def contract_rows(left, right):
    return lax.dot_general(
        left, right, (((0,), (0,)), ((), ())), preferred_element_type=jnp.float32
    )


def contract_cols(left, right):
    return lax.dot_general(
        left, right, (((1,), (1,)), ((), ())), preferred_element_type=jnp.float32
    )


def local(
    tokens,
    conditioning,
    item_map,
    ada_weight,
    ada_bias,
    attn_kernel,
    qkv_weight,
    out_weight,
    up_weight,
    ffn_kernel,
    down_weight,
    out_cotangent,
):
    canvases, rows_here, cols_here, features = tokens.shape
    cell_count = canvases * rows_here * cols_here
    position = lax.axis_index("rows")
    gathered = (
        lax.all_gather(ada_weight, ("dp", "rows"), axis=0, tiled=True),
        lax.all_gather(ada_bias, ("dp", "rows"), axis=0, tiled=True),
        lax.all_gather(attn_kernel, ("dp", "rows"), axis=1, tiled=True),
        lax.all_gather(qkv_weight, ("dp", "rows"), axis=0, tiled=True),
        lax.all_gather(out_weight, ("dp", "rows"), axis=0, tiled=True),
        lax.all_gather(up_weight, ("dp", "rows"), axis=0, tiled=True),
        lax.all_gather(ffn_kernel, ("dp", "rows"), axis=1, tiled=True),
        lax.all_gather(down_weight, ("dp", "rows"), axis=0, tiled=True),
    )
    ada_full, bias_full, kernel_attn, triple_full, out_full, up_full, kernel_ffn, down_full = (
        gathered
    )
    hidden_units = up_full.shape[1]
    head_count = features // PER_GROUP_WIDTH
    logit_divisor = PER_GROUP_WIDTH ** (-0.5)
    labels_pad = jnp.pad(item_map, ((0, 0), (1, 1), (1, 1)), constant_values=-1)
    labels_here = lax.dynamic_slice_in_dim(labels_pad, position * rows_here, rows_here + 2, 1)
    centre = labels_here[:, 1:-1, 1:-1]
    cond_values = conditioning.astype(jnp.float32)
    silu_low = jax.nn.silu(cond_values).astype(jnp.bfloat16)
    modulation = jnp.dot(silu_low, ada_full, preferred_element_type=jnp.float32) + bias_full.astype(
        jnp.float32
    )
    layer_stack = modulation.reshape(canvases, 6, 1, 1, features)
    shift_one, scale_one, gate_one, shift_two, scale_two, gate_two = (
        layer_stack[:, index] for index in range(6)
    )
    token_values = tokens.astype(jnp.float32)
    normed_one, inverse_one = normalize(token_values)
    modulated_one = (normed_one * (1.0 + scale_one) + shift_one).astype(jnp.bfloat16)
    modulated_padded = widen_cols(padded(modulated_one, (("rows", 1),), 1))
    local_mix = conv_forward(modulated_padded, labels_here, centre, kernel_attn).astype(
        jnp.bfloat16
    )
    mix_rows = local_mix.reshape(cell_count, features)
    projected = jnp.dot(mix_rows, triple_full, preferred_element_type=jnp.float32).astype(
        jnp.bfloat16
    )
    projected = projected.reshape(canvases, rows_here * cols_here, 3 * features)
    queries = projected[..., :features]
    key_rows = projected[..., features : 2 * features]
    value_rows = projected[..., 2 * features :]
    keys_all, values_all = (
        lax.all_gather(key_rows, "rows", axis=1, tiled=True),
        lax.all_gather(value_rows, "rows", axis=1, tiled=True),
    )
    query_heads = queries.reshape(canvases, -1, head_count, PER_GROUP_WIDTH)
    key_heads = keys_all.reshape(canvases, -1, head_count, PER_GROUP_WIDTH)
    value_heads = values_all.reshape(canvases, -1, head_count, PER_GROUP_WIDTH)
    scores = (
        jnp.einsum("bqhd,bkhd->bhqk", query_heads, key_heads, preferred_element_type=jnp.float32)
        * logit_divisor
    )
    label_rows = centre.reshape(canvases, -1)
    label_keys = item_map.reshape(canvases, -1)
    linked = label_rows[:, None, :, None] == label_keys[:, None, None, :]
    masked = jnp.where(linked, scores, -1e30)
    row_peak = jnp.max(masked, axis=-1, keepdims=True)
    raised = jnp.exp(masked - row_peak)
    row_total = jnp.sum(raised, axis=-1, keepdims=True)
    attention = raised / row_total
    attention_low = attention.astype(jnp.bfloat16)
    attended = jnp.einsum(
        "bhqk,bkhd->bqhd", attention_low, value_heads, preferred_element_type=jnp.float32
    ).astype(jnp.bfloat16)
    attended = attended.reshape(cell_count, features)
    attn_branch = jnp.dot(attended, out_full, preferred_element_type=jnp.float32).reshape(
        tokens.shape
    )
    middle = token_values + gate_one * attn_branch
    normed_two, inverse_two = normalize(middle)
    modulated_two = (normed_two * (1.0 + scale_two) + shift_two).astype(jnp.bfloat16)
    modulated_rows = modulated_two.reshape(cell_count, features)
    hidden_up_projection = jnp.dot(
        modulated_rows, up_full, preferred_element_type=jnp.float32
    ).astype(jnp.bfloat16)
    hidden_up_projection = hidden_up_projection.reshape(
        canvases, rows_here, cols_here, hidden_units
    )
    up_padded = widen_cols(padded(hidden_up_projection, (("rows", 1),), 1))
    pre_gelu = conv_forward(up_padded, labels_here, centre, kernel_ffn)
    activated, gelu_back = jax.vjp(jax.nn.gelu, pre_gelu)
    gelu_low = activated.astype(jnp.bfloat16).reshape(cell_count, hidden_units)
    ffn_branch = jnp.dot(gelu_low, down_full, preferred_element_type=jnp.float32).reshape(
        tokens.shape
    )
    layer_out = (middle + gate_two * ffn_branch).astype(jnp.bfloat16)
    weights_back = (
        lax.all_gather(ada_weight, ("dp", "rows"), axis=0, tiled=True),
        lax.all_gather(ada_bias, ("dp", "rows"), axis=0, tiled=True),
        lax.all_gather(attn_kernel, ("dp", "rows"), axis=1, tiled=True),
        lax.all_gather(qkv_weight, ("dp", "rows"), axis=0, tiled=True),
        lax.all_gather(out_weight, ("dp", "rows"), axis=0, tiled=True),
        lax.all_gather(up_weight, ("dp", "rows"), axis=0, tiled=True),
        lax.all_gather(ffn_kernel, ("dp", "rows"), axis=1, tiled=True),
        lax.all_gather(down_weight, ("dp", "rows"), axis=0, tiled=True),
    )
    (
        ada_back,
        bias_back,
        kernel_attn_back,
        triple_back,
        out_back,
        up_back,
        kernel_ffn_back,
        down_projection_back,
    ) = weights_back
    incoming = out_cotangent.astype(jnp.float32)
    grad_gate_two = jnp.sum(incoming * ffn_branch, axis=(1, 2))
    grad_ffn = (gate_two * incoming).astype(jnp.bfloat16).reshape(cell_count, features)
    grad_down = contract_rows(gelu_low, grad_ffn)
    grad_gelu = contract_cols(grad_ffn, down_projection_back).reshape(
        canvases, rows_here, cols_here, hidden_units
    )
    grad_pre = gelu_back(grad_gelu)[0].astype(jnp.bfloat16)
    grad_pre_padded = widen_cols(padded(grad_pre, (("rows", 1),), 1))
    grad_kernel_ffn = kernel_grad(grad_pre, up_padded, labels_here, centre)
    grad_up = (
        conv_mirror(grad_pre_padded, labels_here, centre, kernel_ffn_back)
        .astype(jnp.bfloat16)
        .reshape(cell_count, hidden_units)
    )
    grad_up_weight = contract_rows(modulated_rows, grad_up)
    grad_mod_two = contract_cols(grad_up, up_back).reshape(tokens.shape)
    grad_scale_two = jnp.sum(grad_mod_two * normed_two, axis=(1, 2))
    grad_shift_two = jnp.sum(grad_mod_two, axis=(1, 2))
    grad_middle = incoming + normalize_back(
        grad_mod_two * (1.0 + scale_two), normed_two, inverse_two
    )
    grad_gate_one = jnp.sum(grad_middle * attn_branch, axis=(1, 2))
    grad_attn = (gate_one * grad_middle).astype(jnp.bfloat16).reshape(cell_count, features)
    grad_out_weight = contract_rows(attended, grad_attn)
    grad_attended = (
        contract_cols(grad_attn, out_back)
        .astype(jnp.bfloat16)
        .reshape(canvases, -1, head_count, PER_GROUP_WIDTH)
    )
    grad_weights = jnp.einsum(
        "bqhd,bkhd->bhqk", grad_attended, value_heads, preferred_element_type=jnp.float32
    )
    row_delta = jnp.sum(attention * grad_weights, axis=-1, keepdims=True)
    grad_scores = (attention * (grad_weights - row_delta)).astype(jnp.bfloat16)
    grad_query = (
        jnp.einsum("bhqk,bkhd->bqhd", grad_scores, key_heads, preferred_element_type=jnp.float32)
        * logit_divisor
    )
    grad_key_all = (
        jnp.einsum("bhqk,bqhd->bkhd", grad_scores, query_heads, preferred_element_type=jnp.float32)
        * logit_divisor
    )
    value_gradient_full = jnp.einsum(
        "bhqk,bqhd->bkhd", attention_low, grad_attended, preferred_element_type=jnp.float32
    )
    grad_key, grad_value = (
        lax.psum_scatter(
            grad_key_all.reshape(canvases, -1, features).astype(jnp.bfloat16),
            "rows",
            scatter_dimension=1,
            tiled=True,
        ).astype(jnp.float32),
        lax.psum_scatter(
            value_gradient_full.reshape(canvases, -1, features).astype(jnp.bfloat16),
            "rows",
            scatter_dimension=1,
            tiled=True,
        ).astype(jnp.float32),
    )
    grad_projected = jnp.concatenate(
        [
            grad_query.reshape(cell_count, features),
            grad_key.reshape(cell_count, features),
            grad_value.reshape(cell_count, features),
        ],
        axis=-1,
    ).astype(jnp.bfloat16)
    grad_qkv_weight = contract_rows(mix_rows, grad_projected)
    grad_mix = contract_cols(grad_projected, triple_back).astype(jnp.bfloat16).reshape(tokens.shape)
    grad_mix_padded = widen_cols(padded(grad_mix, (("rows", 1),), 1))
    grad_kernel_attn = kernel_grad(grad_mix, modulated_padded, labels_here, centre)
    grad_mod_one = conv_mirror(grad_mix_padded, labels_here, centre, kernel_attn_back)
    grad_scale_one = jnp.sum(grad_mod_one * normed_one, axis=(1, 2))
    grad_shift_one = jnp.sum(grad_mod_one, axis=(1, 2))
    token_grad = grad_middle + normalize_back(
        grad_mod_one * (1.0 + scale_one), normed_one, inverse_one
    )
    grad_parts = jnp.concatenate(
        [
            grad_shift_one,
            grad_scale_one,
            grad_gate_one,
            grad_shift_two,
            grad_scale_two,
            grad_gate_two,
        ],
        axis=-1,
    )
    grad_modulation = lax.psum(grad_parts.astype(jnp.bfloat16), "rows")
    leader = (position == 0).astype(jnp.float32)
    grad_ada_weight = contract_rows(silu_low, grad_modulation) * leader
    grad_ada_bias = jnp.sum(grad_modulation.astype(jnp.float32), axis=0) * leader
    silu_values, silu_back = jax.vjp(jax.nn.silu, cond_values)
    derivative_of_context = silu_back(contract_cols(grad_modulation, ada_back))[0]
    summed_grads = (
        lax.psum_scatter(grad_ada_weight, ("dp", "rows"), scatter_dimension=0, tiled=True),
        lax.psum_scatter(grad_ada_bias, ("dp", "rows"), scatter_dimension=0, tiled=True),
        lax.psum_scatter(grad_kernel_attn, ("dp", "rows"), scatter_dimension=1, tiled=True),
        lax.psum_scatter(grad_qkv_weight, ("dp", "rows"), scatter_dimension=0, tiled=True),
        lax.psum_scatter(grad_out_weight, ("dp", "rows"), scatter_dimension=0, tiled=True),
        lax.psum_scatter(grad_up_weight, ("dp", "rows"), scatter_dimension=0, tiled=True),
        lax.psum_scatter(grad_kernel_ffn, ("dp", "rows"), scatter_dimension=1, tiled=True),
        lax.psum_scatter(grad_down, ("dp", "rows"), scatter_dimension=0, tiled=True),
    )
    return (layer_out, token_grad, derivative_of_context) + tuple(summed_grads)


F32=jnp.float32; BF=jnp.bfloat16
NT=(((1,),(1,)),((),()))
TN=(((0,),(0,)),((),()))

def head_masks(labels):
    cells=labels.shape[0]
    lane=lax.broadcasted_iota(jnp.int32,(cells,128),1)%64
    lab=labels[:,None]
    qm=(lane==lab).astype(BF)
    km=jnp.where((lane!=lab)&(lane<4),-1e30,0.0).astype(BF)
    return qm,km

MESH=pl.DeviceIdType.MESH
NZ,NC,NR=4,2,4


def here():
    dp=lax.axis_index("dp"); rows=lax.axis_index("rows")
    return dp//NC, lax.rem(dp,NC), rows


def dev(z,core,rows):
    return (z*NC+core, rows)


def partner_xy(rows,t):
    x=lax.rem(rows,2); y=rows//2
    tx=t%2; ty=t//2
    nx=1-x if tx else x
    ny=1-y if ty else y
    return ny*2+nx


def rcopy(src,dst,ssem,rsem,target):
    return pltpu.make_async_remote_copy(src_ref=src,dst_ref=dst,send_sem=ssem,recv_sem=rsem,device_id=target,device_id_type=MESH)


def barrier_all():
    dp=lax.axis_index("dp"); rows=lax.axis_index("rows")
    me=dp*NR+rows
    total=NZ*NC*NR
    bar=pltpu.get_barrier_semaphore()
    def body(k,c):
        other=lax.rem(me+k,total)
        pl.semaphore_signal(bar,inc=1,device_id=(other//NR,lax.rem(other,NR)),device_id_type=MESH)
        return c
    lax.fori_loop(1,total,body,0)
    pl.semaphore_wait(bar,total-1)


def zmod(v):
    return lax.rem(v+NZ,NZ)


class Gather:
    SEMS=[(NZ,),(NZ,),(NZ,NR),(NZ,NR),(NZ,NR),(NZ,NR),(1,)]

    def __init__(self,shard,full,sems):
        self.shard,self.full=shard,full
        self.sz,self.rz,self.sx,self.rx,self.sc,self.rc,self.lo=sems
        self.z,self.core,self.rows=here()

    def slot(self,dz,t,core):
        rows=self.rows if t==0 else partner_xy(self.rows,t)
        return self.full.at[zmod(self.z-dz),core,rows]

    def zcopy(self,dz,receive=False):
        dst=self.slot(dz if receive else 0,0,self.core)
        return rcopy(self.shard,dst,self.sz.at[dz],self.rz.at[dz],dev(zmod(self.z+dz),self.core,self.rows))

    def piece(self,dz):
        return self.shard if dz==0 else self.slot(dz,0,self.core)

    def xcopy(self,dz,t,receive=False):
        dst=self.slot(dz,t if receive else 0,self.core)
        return rcopy(self.piece(dz),dst,self.sx.at[dz,t],self.rx.at[dz,t],dev(self.z,self.core,partner_xy(self.rows,t)))

    def ccopy(self,dz,t,receive=False):
        src=self.piece(dz) if t==0 else self.slot(dz,t,self.core)
        dst=self.slot(dz,t,1-self.core if receive else self.core)
        return rcopy(src,dst,self.sc.at[dz,t],self.rc.at[dz,t],dev(self.z,1-self.core,self.rows))

    def local(self):
        return pltpu.make_async_copy(self.shard,self.slot(0,0,self.core),self.lo.at[0])

    def start(self):
        for dz in range(1,NZ):
            self.zcopy(dz).start()
        for t in range(1,NR):
            self.xcopy(0,t).start()
        self.ccopy(0,0).start()
        self.local().start()

    def zstep(self,dz):
        self.zcopy(dz,True).wait_recv()
        for t in range(1,NR):
            self.xcopy(dz,t).start()
        self.ccopy(dz,0).start()

    def xstep(self,dz,t):
        self.xcopy(dz,t,True).wait_recv()
        self.ccopy(dz,t).start()

    def finish(self):
        for dz in range(NZ):
            for t in range(NR):
                self.ccopy(dz,t,True).wait_recv()
        for dz in range(1,NZ):
            self.zcopy(dz).wait_send()
        for dz in range(NZ):
            for t in range(NR):
                if t: self.xcopy(dz,t).wait_send()
                self.ccopy(dz,t).wait_send()
        self.local().wait()

    def run_z(self):
        for dz in range(1,NZ): self.zstep(dz)

    def run_x(self):
        for dz in range(NZ):
            for t in range(1,NR): self.xstep(dz,t)


class Scatter:
    SEMS=[(1,),(1,),(1,),(NR,),(NR,),(NZ,),(NZ,)]

    @staticmethod
    def scratch(r,c,dt):
        return [pltpu.VMEM((NZ,NR,r,c),dt),pltpu.VMEM((NZ,NR,r,c),dt),pltpu.VMEM((NR,NZ,r,c),dt),pltpu.VMEM((NZ,r,c),dt),pltpu.VMEM((NZ,r,c),dt)]

    def __init__(self,part,out,bufs,sems):
        self.part,self.out=part,out
        self.own,self.sib,self.xin,self.zout,self.zin=bufs
        self.lo,self.sc,self.rc,self.sx,self.rx,self.sz,self.rz=sems
        self.z,self.core,self.rows=here()
        self.dt=self.own.dtype

    def lcopy(self):
        return pltpu.make_async_copy(self.part.at[:,self.core],self.own,self.lo.at[0])

    def ccopy(self):
        return rcopy(self.part.at[:,1-self.core],self.sib,self.sc.at[0],self.rc.at[0],dev(self.z,1-self.core,self.rows))

    def xcopy(self,t):
        to=partner_xy(self.rows,t)
        return rcopy(self.own.at[:,to],self.xin.at[t],self.sx.at[t],self.rx.at[t],dev(self.z,self.core,to))

    def zcopy(self,dz):
        to=zmod(self.z+dz)
        return rcopy(self.zout.at[to],self.zin.at[dz],self.sz.at[dz],self.rz.at[dz],dev(to,self.core,self.rows))

    def start(self):
        self.ccopy().start(); self.lcopy().start()

    def cstep(self):
        self.lcopy().wait(); self.ccopy().wait_recv()
        def body(i,c):
            a,b=i//NR,lax.rem(i,NR)
            self.own[a,b]=(self.own[a,b].astype(F32)+self.sib[a,b].astype(F32)).astype(self.dt)
            return c
        lax.fori_loop(0,NZ*NR,body,0)
        for t in range(1,NR): self.xcopy(t).start()

    def xstep(self):
        for t in range(1,NR): self.xcopy(t).wait_recv()
        def body(a,c):
            s=self.own[a,self.rows].astype(F32)
            for t in range(1,NR): s=s+self.xin[t,a].astype(F32)
            self.zout[a]=s.astype(self.dt)
            return c
        lax.fori_loop(0,NZ,body,0)
        for dz in range(1,NZ): self.zcopy(dz).start()

    def zstep(self):
        for dz in range(1,NZ): self.zcopy(dz).wait_recv()
        s=self.zout[self.z].astype(F32)
        for dz in range(1,NZ): s=s+self.zin[dz].astype(F32)
        if callable(self.out): self.out(s)
        else: self.out[...]=s

    def finish(self):
        self.ccopy().wait_send()
        for t in range(1,NR): self.xcopy(t).wait_send()
        for dz in range(1,NZ): self.zcopy(dz).wait_send()


class Swap:
    SEMS=[(NR,),(NR,),(1,)]
    def __init__(self,src,dst,sems):
        self.src,self.dst=src,dst
        self.s,self.r,self.lo=sems
        self.z,self.core,self.rows=here()
    def copy(self,t,receive=False):
        to=partner_xy(self.rows,t)
        return rcopy(self.src.at[to],self.dst.at[to if receive else self.rows],self.s.at[t],self.r.at[t],dev(self.z,self.core,to))
    def local(self):
        return pltpu.make_async_copy(self.src.at[self.rows],self.dst.at[self.rows],self.lo.at[0])
    def start(self):
        for t in range(1,NR): self.copy(t).start()
        self.local().start()
    def wait(self):
        for t in range(1,NR): self.copy(t,True).wait_recv()
        self.local().wait()
    def finish(self):
        for t in range(1,NR): self.copy(t).wait_send()


class AllToAll:
    N=NZ*NC*NR
    SEMS=[(N,),(N,),(1,)]
    def __init__(self,src,dst,sems,one=False):
        self.src,self.dst,self.one=src,dst,one
        self.s,self.r,self.lo=sems
        self.me=lax.axis_index("dp")*NR+lax.axis_index("rows")
    def piece(self,n):
        return self.src if self.one else self.src.at[n]
    def copy(self,k,receive=False):
        to=lax.rem(self.me+k,self.N)
        frm=lax.rem(self.me-k+self.N,self.N)
        return rcopy(self.piece(to),self.dst.at[frm if receive else self.me],self.s.at[k],self.r.at[k],(to//NR,lax.rem(to,NR)))
    def local(self):
        return pltpu.make_async_copy(self.piece(self.me),self.dst.at[self.me],self.lo.at[0])
    def each(self,fn):
        def body(k,c):
            fn(k); return c
        lax.fori_loop(1,self.N,body,0)
    def start(self):
        self.each(lambda k:self.copy(k).start())
        self.local().start()
    def wait(self):
        self.each(lambda k:self.copy(k,True).wait_recv())
        self.local().wait()
    def finish(self):
        self.each(lambda k:self.copy(k).wait_send())


def sem_types(shapes):
    return [pltpu.SemaphoreType.DMA(s) for s in shapes]
class GatherZ:
    SEMS=[(NZ,),(NZ,),(1,)]
    def __init__(self,shard,zp,sems):
        self.shard,self.zp=shard,zp
        self.s,self.r,self.lo=sems
        self.z,self.core,self.rows=here()
    def copy(self,dz,receive=False):
        to=zmod(self.z+dz)
        frm=zmod(self.z-dz)
        return rcopy(self.shard,self.zp.at[frm if receive else self.z],self.s.at[dz],self.r.at[dz],dev(to,self.core,self.rows))
    def local(self):
        return pltpu.make_async_copy(self.shard,self.zp.at[self.z],self.lo.at[0])
    def start(self):
        for dz in range(1,NZ): self.copy(dz).start()
        self.local().start()
    def wait(self):
        for dz in range(1,NZ): self.copy(dz,True).wait_recv()
    def finish(self):
        for dz in range(1,NZ): self.copy(dz).wait_send()
        self.local().wait()


class GatherXY:
    SEMS=[(NZ,NR),(NZ,NR),(NZ,NR),(NZ,NR),(1,)]
    def __init__(self,zp,full,sems):
        self.zp,self.full=zp,full
        self.sx,self.rx,self.sc,self.rc,self.lo=sems
        self.z,self.core,self.rows=here()
    def place(self,t):
        return self.rows if t==0 else partner_xy(self.rows,t)
    def to(self,t):
        return dev(self.z,self.core,self.place(t))
    def xcopy(self,k,t,receive=False):
        return rcopy(self.zp.at[k],self.full.at[k,self.core,self.place(t) if receive else self.rows],self.sx.at[k,t],self.rx.at[k,t],self.to(t))
    def fcopy(self,k,receive=False):
        t=1 if k<NZ//2 else 2
        ref=self.full.at[k,self.core,self.place(3 if receive else t)]
        return rcopy(ref,ref,self.sx.at[k,3],self.rx.at[k,3],self.to(3-t))
    def ccopy(self,k,t,receive=False):
        src=self.zp.at[k] if t==0 else self.full.at[k,self.core,self.place(t)]
        dst=self.full.at[k,1-self.core if receive else self.core,self.place(t)]
        return rcopy(src,dst,self.sc.at[k,t],self.rc.at[k,t],dev(self.z,1-self.core,self.rows))
    def local(self):
        return pltpu.make_async_copy(self.zp,self.full.at[:,self.core,self.rows],self.lo.at[0])
    def start(self,ks=range(NZ)):
        for k in ks:
            for t in (1,2): self.xcopy(k,t).start()
            self.ccopy(k,0).start()
    def start_local(self):
        self.local().start()
    def step(self,k):
        order=(1,2) if k<NZ//2 else (2,1)
        self.xcopy(k,order[0],True).wait_recv()
        self.fcopy(k).start()
        self.ccopy(k,order[0]).start()
        self.xcopy(k,order[1],True).wait_recv()
        self.ccopy(k,order[1]).start()
    def step2(self,k):
        self.fcopy(k,True).wait_recv()
        self.ccopy(k,3).start()
    def arrive(self,k):
        for t in range(NR): self.ccopy(k,t,True).wait_recv()
    def finish_remote(self):
        for k in range(NZ):
            for t in (1,2): self.xcopy(k,t).wait_send()
            self.fcopy(k).wait_send()
            for t in range(NR): self.ccopy(k,t).wait_send()
    def finish(self):
        self.finish_remote()
        self.local().wait()


class GatherTile:
    def __init__(self,zp,full,width,sems):
        self.zp,self.full,self.width=zp,full,width
        self.sx,self.rx,self.sc,self.rc,self.lo=sems
        self.z,self.core,self.rows=here()
    @staticmethod
    def sems(tiles):
        return [(tiles,NR),(tiles,NR),(tiles,NR),(tiles,NR),(1,)]
    def cols(self,i): return pl.ds(pl.multiple_of(i*self.width,128),self.width)
    def place(self,t):
        return self.rows if t==0 else partner_xy(self.rows,t)
    def to(self,t):
        return dev(self.z,self.core,self.place(t))
    def xcopy(self,i,t,receive=False):
        return rcopy(self.zp.at[:,:,self.cols(i)],self.full.at[:,self.core,self.place(t) if receive else self.rows,:,self.cols(i)],self.sx.at[i,t],self.rx.at[i,t],self.to(t))
    def fcopy(self,i,t,receive=False):
        h=NZ//2
        ref=self.full.at[pl.ds(0 if t==1 else h,h),self.core,self.place(3 if receive else t),:,self.cols(i)]
        q=3 if t==1 else 0
        return rcopy(ref,ref,self.sx.at[i,q],self.rx.at[i,q],self.to(3-t))
    def ccopy(self,i,t,receive=False):
        src=self.zp.at[:,:,self.cols(i)] if t==0 else self.full.at[:,self.core,self.place(t),:,self.cols(i)]
        dst=self.full.at[:,1-self.core if receive else self.core,self.place(t),:,self.cols(i)]
        return rcopy(src,dst,self.sc.at[i,t],self.rc.at[i,t],dev(self.z,1-self.core,self.rows))
    def local(self):
        return pltpu.make_async_copy(self.zp,self.full.at[:,self.core,self.rows],self.lo.at[0])
    def start(self,i):
        for t in (1,2): self.xcopy(i,t).start()
        self.ccopy(i,0).start()
    def step(self,i):
        for t in (1,2):
            self.xcopy(i,t,True).wait_recv()
            self.fcopy(i,t).start()
            self.ccopy(i,t).start()
    def step2(self,i):
        for t in (1,2): self.fcopy(i,t,True).wait_recv()
        self.ccopy(i,3).start()
    def arrive(self,i):
        for t in range(NR): self.ccopy(i,t,True).wait_recv()
    def finish_remote(self,i):
        for t in (1,2):
            self.xcopy(i,t).wait_send()
            self.fcopy(i,t).wait_send()
        for t in range(NR): self.ccopy(i,t).wait_send()


class ScatterZ:
    SEMS=[(NZ,),(NZ,)]
    @staticmethod
    def scratch(r,c,dt):
        return [pltpu.VMEM((NZ,r,c),dt)]
    def __init__(self,zout,out,bufs,sems):
        self.zout,self.out=zout,out
        self.zin,=bufs
        self.s,self.r=sems
        self.z,self.core,self.rows=here()
    def copy(self,dz):
        to=zmod(self.z+dz)
        return rcopy(self.zout.at[to],self.zin.at[dz],self.s.at[dz],self.r.at[dz],dev(to,self.core,self.rows))
    def start(self):
        for dz in range(1,NZ): self.copy(dz).start()
    def step(self):
        for dz in range(1,NZ): self.copy(dz).wait_recv()
        v=self.zout[self.z].astype(F32)
        for dz in range(1,NZ): v=v+self.zin[dz].astype(F32)
        if callable(self.out): self.out(v)
        else: self.out[...]=v
    def finish(self):
        for dz in range(1,NZ): self.copy(dz).wait_send()


class GroupAll:
    N=NZ*NC
    SEMS=[(N,),(N,),(1,)]
    def __init__(self,src,dst,sems):
        self.src,self.dst=src,dst
        self.s,self.r,self.lo=sems
        self.dp=lax.axis_index("dp"); self.rows=lax.axis_index("rows")
    def copy(self,k,receive=False):
        to=lax.rem(self.dp+k,self.N)
        frm=lax.rem(self.dp-k+self.N,self.N)
        return rcopy(self.src,self.dst.at[frm if receive else self.dp],self.s.at[k],self.r.at[k],(to,self.rows))
    def local(self):
        return pltpu.make_async_copy(self.src,self.dst.at[self.dp],self.lo.at[0])
    def start(self):
        for k in range(1,self.N): self.copy(k).start()
        self.local().start()
    def wait(self):
        for k in range(1,self.N): self.copy(k,True).wait_recv()
        self.local().wait()
    def finish(self):
        for k in range(1,self.N): self.copy(k).wait_send()


class Events:
    def __init__(self): self.at={}
    def add(self,slot,fn): self.at.setdefault(slot,[]).append(fn)
    def run(self,outer,inner,width):
        for slot,fns in self.at.items():
            if slot%width==inner:
                @pl.when(outer==slot//width)
                def _(fns=fns):
                    for fn in fns: fn()
NN=(((1,),(0,)),((),()))
C0=0.7978845608028654
C1=0.044715


def dotf(a,b,dims=NN):
    return lax.dot_general(a,b,dims,preferred_element_type=F32)


def loop(n,fn,unroll=1):
    def body(i,c):
        fn(i); return c
    lax.fori_loop(0,n,body,0,unroll=unroll)


def rows_of(i,n):
    return pl.ds(pl.multiple_of(i*n,n),n)


def normal_rows(v):
    d=1.0/v.shape[1]
    c=v-jnp.sum(v,axis=1,keepdims=True)*d
    inv=lax.rsqrt(jnp.sum(c*c,axis=1,keepdims=True)*d+EPSILON)
    return c*inv,inv


def normal_back_rows(g,n,inv):
    d=1.0/g.shape[1]
    return inv*(g-jnp.sum(g,axis=1,keepdims=True)*d-n*(jnp.sum(g*n,axis=1,keepdims=True)*d))


def fold8(v):
    s=v[0:8]
    for k in range(1,v.shape[0]//8): s=s+v[8*k:8*k+8]
    return s


def conv_loops(side,lanes_n,width,forward,finish):
    pass


def shifts(f,ml,mr):
    n=f.shape[0]
    return pltpu.roll(f,1,0)*ml, pltpu.roll(f,n-1,0)*mr


def conv_rows(src,dst_fn,taps,ml_ref,mr_ref,rl_ref,ls,side,cols,unroll=8):
    k=[taps[q:q+1,:] for q in range(9)]
    zero=jnp.zeros((cols,128),F32)
    def body(i,c):
        hm,part=c
        f=src[rows_of(i,cols),ls]
        fm,fp=shifts(f,ml_ref[rows_of(i,cols),:],mr_ref[rows_of(i,cols),:])
        h=[k[3*a]*fm+k[3*a+1]*f+k[3*a+2]*fp for a in range(3)]
        done=part+rl_ref[i]*h[2]
        @pl.when(i>0)
        def _(): dst_fn(i-1,done)
        return h[0],h[1]+rl_ref[i]*hm
    hm,part=lax.fori_loop(0,side,body,(zero,zero),unroll=unroll)
    dst_fn(side-1,part)


def back_rows(g_ref,f_ref,dst_fn,taps,ml_ref,mr_ref,rl_ref,ls,first,count,side,cols,unroll=8):
    k=[taps[q:q+1,:] for q in range(9)]
    z8=jnp.zeros((8,128),F32)
    def at(i): return rows_of(i,cols)
    def load(i):
        g=g_ref[at(i),ls]
        gm,gp=shifts(g,ml_ref[at(i),:],mr_ref[at(i),:])
        return gp,g,gm
    def mix3(gs,a): return k[3*a]*gs[0]+k[3*a+1]*gs[1]+k[3*a+2]*gs[2]
    whole=isinstance(first,int) and count==side
    zero=jnp.zeros((cols,128),F32)
    before=jnp.maximum(first-1,0)
    hp=zero if whole else mix3(load(before),2)
    fprev=zero if whole else f_ref[at(before),ls].astype(F32)
    def body(n,c):
        hp,part,fprev,acc=c
        i=first+n
        gs=load(i)
        done=part+rl_ref[i]*mix3(gs,0)
        @pl.when(n>0)
        def _(): dst_fn(i-1,done)
        f=f_ref[at(i),ls].astype(F32)
        nxt=f_ref[at(jnp.minimum(i+1,side-1)),ls].astype(F32)
        fs=(fprev*rl_ref[i],f,nxt*rl_ref[i+1])
        acc=tuple(acc[3*a+b]+fold8(fs[a]*gs[b]) for a in range(3) for b in range(3))
        return mix3(gs,2),mix3(gs,1)+rl_ref[i]*hp,f,acc
    hp,part,_,acc=lax.fori_loop(0,count,body,(hp,zero,fprev,(z8,)*9),unroll=unroll)
    end=first+count
    if not whole: part=part+rl_ref[end]*mix3(load(jnp.minimum(end,side-1)),0)
    dst_fn(end-1,part)
    return acc


def link_masks(labels):
    side,cols=labels.shape
    left=jnp.pad(labels[:,1:]==labels[:,:-1],((0,0),(1,0)))
    right=jnp.pad(labels[:,1:]==labels[:,:-1],((0,0),(0,1)))
    wide=lambda m: jnp.broadcast_to(m.reshape(side*cols,1).astype(F32),(side*cols,128))
    top=labels[:,0]//2
    rl=jnp.pad((top[1:]==top[:-1]).astype(F32),(1,1))
    return wide(left),wide(right),rl
HBM=pl.BlockSpec(memory_space=pl.ANY)
VM=pl.BlockSpec(memory_space=pltpu.VMEM)
SM=pl.BlockSpec(memory_space=pltpu.SMEM)
NDEV=NZ*NC*NR
S_=jax.ShapeDtypeStruct


def taker(it):
    return lambda cls:[next(it) for _ in cls.SEMS]


def assemble(dst,src,width,at):
    lane=lax.broadcasted_iota(jnp.int32,(1,128),1)
    tiles=dst.shape[1]//128
    for c in range(tiles):
        v=jnp.zeros((16,128),F32)
        for n in range(NDEV):
            lo=n*width-c*128
            if lo+width<=0 or lo>=128: continue
            p=src[n//(NC*NR),(n//NR)%NC,n%NR].astype(F32)
            sh=(lo-at)%128
            if sh: p=pltpu.roll(p,sh,1)
            v=jnp.where((lane>=lo)&(lane<lo+width),p,v)
        dst[:,c*128:(c+1)*128]=v


def enter_kernel(n_z,side,cols,ta,tf,*refs):
    it=iter(refs)
    nx=lambda n:[next(it) for _ in range(n)]
    tok,cond,ada,bias,qkv,taps,lab,rl_ref=nx(8)
    shards=nx(n_z)
    tok_o,cond_o,mod_o,qkv_o,tap_a,tap_f,m1,mix,ml_ref,mr_ref,qm,km=nx(12)
    zps=nx(n_z)
    condv,condf,part,zq,taps_o,modw,F=nx(7)
    mbufs=nx(5)
    take=taker(it)
    c_all=GroupAll(cond,condv,take(GroupAll))
    swap_t=Swap(tok,tok_o,take(Swap))
    m_all=Scatter(part,mod_o,mbufs,take(Scatter))
    g_taps=Gather(taps,taps_o,take(Gather))
    gq_z=GatherZ(qkv,zq,take(GatherZ))
    gq=GatherXY(zq,qkv_o,take(GatherXY))
    gz=[GatherZ(s,z,take(GatherZ)) for s,z in zip(shards,zps)]
    barrier_all()
    c_all.start()
    gq_z.start()
    swap_t.copy(1).start(); swap_t.copy(2).start(); swap_t.local().start()
    c_all.wait()
    me=lax.axis_index("dp")*NR+lax.axis_index("rows")
    feats=ada.shape[0]
    for d in range(NZ*NC): condf[d*NR:(d+1)*NR,:]=condv[d,0:NR,:].astype(F32)
    cv=condf[...]
    low=(cv/(1.0+jnp.exp(-cv))).astype(BF)
    width=cv.shape[1]
    pick=(lax.broadcasted_iota(jnp.int32,(width,feats),0)==lax.broadcasted_iota(jnp.int32,(width,feats),1)+feats*me).astype(BF)
    mine=jnp.dot(low,pick,preferred_element_type=F32).astype(BF)
    chunk=768
    for c in range(ada.shape[1]//chunk):
        pr=jnp.dot(mine,ada[:,c*chunk:(c+1)*chunk],preferred_element_type=F32)
        for l in range(chunk//128):
            i=c*(chunk//128)+l
            part[:,:,:,i,:]=(pr[:,l*128:(l+1)*128]+bias[i:i+1,:]).reshape(NZ,NC,NR,128)
    cond_o[...]=low
    m_all.start()
    m_all.cstep()
    g_taps.start()
    lv=lab[...]
    total=lv.shape[0]
    col=lax.rem(lax.broadcasted_iota(jnp.int32,lv.shape,0),cols)
    ml_ref[...]=jnp.where((pltpu.roll(lv,1,0)==lv)&(col>0),1.0,0.0)
    mr_ref[...]=jnp.where((pltpu.roll(lv,total-1,0)==lv)&(col<cols-1),1.0,0.0)
    which=lax.rem(lax.broadcasted_iota(jnp.int32,lv.shape,1),64)
    qm[...]=jnp.where(which==lv,1.0,0.0).astype(BF)
    km[...]=jnp.where((which!=lv)&(which<4),-1e30,0.0).astype(BF)
    swap_t.copy(3).start()
    g_taps.run_z()
    gq_z.wait(); gq_z.local().wait()
    gq.start(); gq.start_local()
    m_all.xstep()
    for g in gz: g.start()
    m_all.zstep()
    g_taps.run_x()
    cells,feat=mix.shape
    L=feat//128
    for j in range(2):
        for l in range(L): modw[j:j+1,l*128:(l+1)*128]=mod_o[j*L+l:j*L+l+1,:]
    swap_t.wait()
    shift1=modw[0:1,:]; scale1=modw[1:2,:]
    EC=256
    for b in range(NR):
        n,_=normal_rows(tok_o[b].astype(F32))
        v=(n*(1.0+scale1)+shift1).astype(BF)
        m1[b*EC:(b+1)*EC,:]=v
        F[b*EC:(b+1)*EC,:]=v.astype(F32)
    g_taps.finish()
    assemble(tap_a,taps_o,ta,0)
    assemble(tap_f,taps_o,tf,ta)
    def lanes(l):
        ls=pl.ds(pl.multiple_of(l*128,128),128)
        def put(i,u): mix[rows_of(i,cols),ls]=u.astype(BF)
        conv_rows(F,put,tap_a[:,ls],ml_ref,mr_ref,rl_ref,ls,side,cols,4)
    def some(i):
        for k in range(NZ):
            @pl.when(i==k+1)
            def _(k=k): gq.step(k)
        for k in range(2):
            @pl.when(i==L-2+k)
            def _(k=k): gq.step2(k)
        lanes(i)
    loop(L,some)
    for k in range(2,NZ): gq.step2(k)
    for g in gz: g.wait()
    for k in range(NZ): gq.arrive(k)
    gq.finish()
    for dz in range(1,NZ): gq_z.copy(dz).wait_send()
    for g in [swap_t,c_all,m_all]+gz: g.finish()


def enter(tok,cond_row,ada,bias_rows,qkv,taps,lab,rl,shards,side,cols,ta,tf):
    n=len(shards)
    V=pltpu.VMEM
    feat=tok.shape[2]; cells=side*cols
    scr=[V((NZ*NC,)+cond_row.shape,cond_row.dtype),V((NDEV,cond_row.shape[1]),F32),V((NZ,NC,NR)+bias_rows.shape,F32),V((NZ,)+qkv.shape,BF),V((NZ,NC,NR)+taps.shape,BF),V((8,feat),F32),V((cells,feat),F32)]+Scatter.scratch(bias_rows.shape[0],128,F32)
    sems=sem_types(GroupAll.SEMS)+sem_types(Swap.SEMS)+sem_types(Scatter.SEMS)+sem_types(Gather.SEMS)+sem_types(GatherZ.SEMS)+sem_types(GatherXY.SEMS)+sem_types(GatherZ.SEMS)*n
    outs=[S_(tok.shape,tok.dtype),S_((NDEV,cond_row.shape[1]),BF),S_(bias_rows.shape,F32),S_((NZ,NC,NR)+qkv.shape,qkv.dtype),
          S_((16,NDEV*ta),F32),S_((16,NDEV*tf),F32),S_((cells,feat),BF),S_((cells,feat),BF)]+[S_((cells,128),d) for d in (F32,F32,BF,BF)]
    outs+=[S_((NZ,)+s.shape,s.dtype) for s in shards]
    return pl.pallas_call(
        functools.partial(enter_kernel,n,side,cols,ta,tf),
        in_specs=[VM,HBM,VM,VM,VM,VM,VM,SM]+[VM]*n,
        out_specs=[VM,VM,VM,HBM]+[VM]*8+[HBM]*n,
        out_shape=outs,
        scratch_shapes=scr+sems,
        compiler_params=pltpu.CompilerParams(collective_id=0,has_side_effects=True,vmem_limit_bytes=63<<20),
        name="enter",
    )(tok,cond_row,ada,bias_rows,qkv,taps,lab,rl,*shards)


def forward_kernel(n_w,qb,*refs):
    it=iter(refs)
    mix,qkv,qm,km,cot,late,late2=[next(it) for _ in range(7)]
    zps=[next(it) for _ in range(n_w)]
    proj,att,lse_t,cot_o,late_o,late2_o=[next(it) for _ in range(6)]
    fulls=[next(it) for _ in range(n_w)]
    lse=next(it)
    take=taker(it)
    barrier_all()
    swap_c=Swap(cot,cot_o,take(Swap))
    gs=[GatherXY(a,b,take(GatherXY)) for a,b in zip(zps,fulls)]
    gl=GatherZ(late,late_o,take(GatherZ))
    gl2=GatherZ(late2,late2_o,take(GatherZ))
    gs[0].start(); gs[0].start_local()
    gl2.start(); gl.start()
    swap_c.start()
    ev=Events()
    for k in range(NZ):
        ev.add(2,lambda k=k: gs[0].step(k))
        ev.add(9,lambda k=k: gs[0].step2(k))
    cells,feat=att.shape
    CH=256
    def pr(i):
        proj[rows_of(i,CH),:]=dotf(mix[rows_of(i,CH),:],qkv[...]).astype(BF)
    loop(cells//CH,pr)
    pairs=feat//128
    lane=lax.broadcasted_iota(jnp.int32,(1,128),1)
    lse[...]=jnp.zeros_like(lse)
    def pair(p):
        cq=pl.ds(pl.multiple_of(p*128,128),128)
        ck=pl.ds(pl.multiple_of(feat+p*128,128),128)
        cv=pl.ds(pl.multiple_of(2*feat+p*128,128),128)
        for h in range(2):
            ev.run(p,h,2)
            mine=(lane//64)==h
            k=jnp.where(mine,proj[:,ck],km[...])
            def body(i):
                r=rows_of(i,qb)
                q=jnp.where(mine,proj[r,cq]*jnp.asarray(0.125,BF),qm[r,:])
                s=dotf(q,k,NT)
                m=jnp.max(s,axis=1,keepdims=True)
                e=jnp.exp(s-m)
                l=jnp.sum(e,axis=1,keepdims=True)
                a=(e*(1.0/l)).astype(BF)
                o=dotf(a,proj[:,cv]).astype(BF)
                if h==0:
                    att[r,cq]=o
                else:
                    att[r,cq]=jnp.where(mine,o,att[r,cq])
                lse[r,:]=jnp.where(lane==2*p+h,m+jnp.log(l),lse[r,:])
            loop(cells//qb,body,2)
    loop(pairs,pair)
    lse_t[...]=jnp.transpose(lse[...])
    for g in gs:
        for k in range(NZ): g.arrive(k)
    swap_c.wait()
    gl.wait(); gl2.wait()
    for g in gs+[swap_c,gl,gl2]: g.finish()


def forward(mix,qkv,qm,km,cot,late,late2,zps):
    n=len(zps)
    cells,feat=mix.shape
    outs=[S_((cells,3*feat),BF),S_((cells,feat),BF),S_((128,cells),F32),S_(cot.shape,cot.dtype),S_((NZ,)+late.shape,late.dtype),S_((NZ,)+late2.shape,late2.dtype)]
    outs+=[S_((NZ,NC,NR)+z.shape[1:],z.dtype) for z in zps]
    return pl.pallas_call(
        functools.partial(forward_kernel,n,512),
        in_specs=[VM,VM,VM,VM,VM,VM,VM]+[VM]*n,
        out_specs=[VM,VM,VM,HBM,HBM,HBM]+[HBM]*n,
        out_shape=outs,
        scratch_shapes=[pltpu.VMEM((cells,128),F32)]+sem_types(Swap.SEMS)+sem_types(GatherXY.SEMS)*n+sem_types(GatherZ.SEMS)*2,
        compiler_params=pltpu.CompilerParams(collective_id=1,has_side_effects=True,vmem_limit_bytes=63<<20),
        name="attn_fwd",
    )(mix,qkv,qm,km,cot,late,late2,*zps)


def backward_kernel(n_g,kb,*refs):
    it=iter(refs)
    nx=lambda n:[next(it) for _ in range(n)]
    proj,do,o,qm,km,lse_t,mix,lay,gout=nx(9)
    parts=nx(n_g)
    gp,lay_o,gout_o,zq,lastq=nx(5)
    gouts=nx(n_g)
    qs,dqt,mixt=nx(3)
    obufs=nx(5)
    qbufs=nx(4)
    bufs=[nx(1) for _ in range(n_g)]
    take=taker(it)
    barrier_all()
    sl=Swap(lay,lay_o,take(Swap))
    so=Scatter(gout,gout_o,obufs,take(Scatter))
    uq=PipeScatter(qbufs,take(PipeScatter))
    sc=[ScatterZ(p,g,b,take(ScatterZ)) for p,g,b in zip(parts,gouts,bufs)]
    cells,feat=do.shape
    pairs=feat//128
    W=256
    tiles=pairs//2
    r_=feat//NDEV
    def put_q(m):
        def put(a,v):
            for s in range(3):
                zq[a,:,(s*(tiles-1)+m)*W:(s*(tiles-1)+m+1)*W]=v[:,s*W:(s+1)*W]
        return put
    ev=Events()
    so.start()
    for s in sc: s.start()
    ev.add(1,so.cstep)
    ev.add(2,sl.start)
    ev.add(5,lambda: uq.send_square(0))
    ev.add(6,so.xstep)
    for s in sc: ev.add(7,s.step)
    ev.add(8,lambda: uq.collect(0,put_q(0)))
    ev.add(9,lambda: uq.send_square(1))
    ev.add(11,so.zstep)
    lane=lax.broadcasted_iota(jnp.int32,(1,128),1)
    srow=lax.broadcasted_iota(jnp.int32,(8,128),0)
    slane=lax.broadcasted_iota(jnp.int32,(8,128),1)
    sel=(slane//64==srow).astype(BF)
    def tr(i):
        mixt[:,pl.ds(pl.multiple_of(i*256,256),256)]=jnp.transpose(mix[rows_of(i,256),:])
    loop(cells//256,tr)
    def pair(p):
        cq=pl.ds(pl.multiple_of(p*128,128),128)
        ck=pl.ds(pl.multiple_of(feat+p*128,128),128)
        cv=pl.ds(pl.multiple_of(2*feat+p*128,128),128)
        prod=do[:,cq].astype(F32)*o[:,cq].astype(F32)
        hi=prod.astype(BF); lo=(prod-hi.astype(F32)).astype(BF)
        delta=dotf(sel,hi,NT)+dotf(sel,lo,NT)
        qs[...]=proj[:,cq]*jnp.asarray(0.125,BF)
        for h in range(2):
            ev.run(p,h,2)
            mine=(lane//64)==h
            q=jnp.where(mine,qs[...],qm[...])
            ls=lse_t[pl.ds(2*p+h,1),:]
            dl=delta[h:h+1,:]
            dqt[...]=jnp.zeros_like(dqt)
            def body(i):
                r=rows_of(i,kb)
                kr=proj[r,ck]
                k=jnp.where(mine,kr,km[r,:])
                v=jnp.where(mine,proj[r,cv],jnp.zeros((),BF))
                st=dotf(k,q,NT)
                pt=jnp.exp(st-ls)
                dpt=dotf(v,do[:,cq],NT)
                ds=(pt*(dpt-dl)).astype(BF)
                dv=dotf(pt.astype(BF),do[:,cq]).astype(BF)
                dk=dotf(ds,qs[...]).astype(BF)
                dqt[...]+=dotf(kr,ds,TN)
                if h==0:
                    gp[r,cv]=dv
                    gp[r,ck]=dk
                else:
                    gp[r,cv]=jnp.where(mine,dv,gp[r,cv])
                    gp[r,ck]=jnp.where(mine,dk,gp[r,ck])
            loop(cells//kb,body,2)
            dq=(jnp.transpose(dqt[...])*0.125).astype(BF)
            if h==0:
                gp[:,cq]=dq
            else:
                gp[:,cq]=jnp.where(mine,dq,gp[:,cq])
        @pl.when(lax.rem(p,2)==1)
        def _():
            m=p//2
            s=lax.rem(m,2)
            n=NC*NR*r_
            def tile(i):
                for c in range(3):
                    cols=pl.ds(pl.multiple_of(c*feat+m*W,W),W)
                    uq.part[s,i,:,:,:,c*W:(c+1)*W]=dotf(mixt[rows_of(i,n),:],gp[:,cols]).astype(BF).reshape(NC,NR,r_,W)
            loop(NZ,tile)
            @pl.when(m<tiles-1)
            def _(): uq.send_core(s)
    loop(pairs,pair)
    uq.collect(1,put_q(1))
    lastq[...]=uq.part[0]
    sl.wait()
    for s in sc+[sl,so]: s.finish()


def backward(proj,do,o,qm,km,lse_t,mix,lay,gout,parts):
    n=len(parts)
    cells,feat=do.shape
    r_=feat//NDEV
    outs=[S_((cells,3*feat),BF),S_(lay.shape,lay.dtype),S_(gout.shape[3:],F32),S_((NZ,r_,2*feat),BF),S_((NZ,NC,NR,r_,feat),BF)]+[S_(p.shape[1:],F32) for p in parts]
    scr=[pltpu.VMEM((cells,128),BF),pltpu.VMEM((128,cells),F32),pltpu.VMEM((feat,cells),BF)]
    scr+=Scatter.scratch(gout.shape[3],gout.shape[4],gout.dtype)+PipeScatter.scratch(r_,feat)
    for p in parts: scr+=ScatterZ.scratch(p.shape[1],p.shape[2],p.dtype)
    return pl.pallas_call(
        functools.partial(backward_kernel,n,512),
        in_specs=[VM,VM,VM,VM,VM,VM,VM,VM,HBM]+[VM]*n,
        out_specs=[VM,HBM,VM,VM,VM]+[VM]*n,
        out_shape=outs,
        scratch_shapes=scr+sem_types(Swap.SEMS)+sem_types(Scatter.SEMS)+sem_types(PipeScatter.SEMS)+sem_types(ScatterZ.SEMS)*n,
        compiler_params=pltpu.CompilerParams(collective_id=2,has_side_effects=True,vmem_limit_bytes=63<<20),
        name="attn_bwd",
    )(proj,do,o,qm,km,lse_t,mix,lay,gout,*parts)


def spread(dst,src_ref,width,at):
    lane=lax.broadcasted_iota(jnp.int32,(1,128),1)
    for n in range(NDEV):
        lo=n*width
        c,off=lo//128,lo%128
        sh=(at-off)%128
        v=src_ref[:,c*128:(c+1)*128]
        v=pltpu.roll(v,sh,1) if sh else v
        if off+width>128:
            w=src_ref[:,(c+1)*128:(c+2)*128]
            w=pltpu.roll(w,sh,1) if sh else w
            v=jnp.where(lane<at+128-off,v,w)
        keep=(lane>=at)&(lane<at+width)
        i=(n//(NC*NR),(n//NR)%NC,n%NR)
        if at==0: dst[i]=jnp.where(keep,v,0.0)
        else: dst[i]=jnp.where(keep,v,dst[i])


def tail_kernel(side,cols,ta,tf,*refs):
    it=iter(refs)
    nx=lambda n:[next(it) for _ in range(n)]
    gproj_h,qkv_h,m1,x_ref,gmid_h,mod,tap_ref,ml_ref,mr_ref,rl_ref,sums,gkf,low,ada,zq,lastq=nx(16)
    tg_o,ctx_o,adag_o,gm_o,q_o,ka_o,kf_o=nx(7)
    G,gm1,tgb,tgin,ktap,gme,gml,gmev,gmlv,ctxs,ctxv,tpart,gproj,qkv,gmid,lsem=nx(16)
    zbufs=nx(1); lbufs=nx(5); tbufs=nx(5)
    take=taker(it)
    loads=[pltpu.make_async_copy(a,b,lsem.at[i]) for i,(a,b) in enumerate(((gproj_h,gproj),(qkv_h,qkv),(gmid_h,gmid)))]
    for l in loads: l.start()
    barrier_all()
    def put_z(v):
        n=v.shape[1]//3
        for s in range(3): q_o[:,s*n*3//2:s*n*3//2+n]=v[:,s*n:(s+1)*n]
    def put_l(v):
        n=v.shape[1]//3
        for s in range(3): q_o[:,(3*s+2)*n:(3*s+3)*n]=v[:,s*n:(s+1)*n]
    def put_t(v):
        ka_o[...]=v[0:9,0:ta]
        kf_o[...]=pltpu.roll(v,128-ta,1)[0:9,0:tf]
    sz=ScatterZ(zq,put_z,zbufs,take(ScatterZ))
    slq=Scatter(lastq,put_l,lbufs,take(Scatter))
    stp=Scatter(tpart,put_t,tbufs,take(Scatter))
    st=Swap(tgb,tgin,take(Swap))
    ge=AllToAll(gme,gmev,take(AllToAll),one=True)
    gl=AllToAll(gml,gmlv,take(AllToAll),one=True)
    xa=AllToAll(ctxs,ctxv,take(AllToAll))
    slq.start(); sz.start()
    cells,feat=x_ref.shape
    L=feat//128
    for i,q in enumerate((3,1,2,0)):
        for l in range(L):
            gme[i*L+l:i*L+l+1,:]=sums[q:q+1,l*128:(l+1)*128].astype(BF)
    ge.start()
    CH=512; EC=256
    for l in loads: l.wait()
    def a(i):
        r=rows_of(i,CH)
        G[r,:]=dotf(gproj[r,:],qkv[...],NT).astype(BF).astype(F32)
    loop(cells//CH,a)
    slq.cstep()
    ktap[...]=jnp.zeros_like(ktap)
    shift1=mod[0:1,:]; scale1=mod[1:2,:]
    z8=jnp.zeros((8,feat),F32)
    block=cells//NR
    c=(z8,z8)
    per=side//NR
    for t in (3,1,2,0):
        to=partner_xy(st.rows,t) if t else st.rows
        def lanes(l):
            ls=pl.ds(pl.multiple_of(l*128,128),128)
            def put(i,u): gm1[rows_of(i,cols),ls]=u
            acc=back_rows(G,m1,put,tap_ref[:,ls],ml_ref,mr_ref,rl_ref,ls,to*per,per,side,cols,2)
            for q in range(9): ktap[q:q+1,ls]+=jnp.sum(acc[q],axis=0,keepdims=True)
        loop(L,lanes)
        r=rows_of(to,block)
        n,inv=normal_rows(x_ref[r,:].astype(F32))
        g=gm1[r,:]
        tgb[to]=(gmid[r,:]+normal_back_rows(g*(1.0+scale1),n,inv)).astype(BF)
        c=(c[0]+fold8(g),c[1]+fold8(g*n))
        if t: st.copy(t).start()
        else: st.local().start()
        if t==1: slq.xstep()
    spread(tpart,ktap,ta,0)
    spread(tpart,gkf,tf,ta)
    stp.start()
    for i,v in enumerate(c):
        v=jnp.sum(v,axis=0,keepdims=True)
        for l in range(L): gml[i*L+l:i*L+l+1,:]=v[:,l*128:(l+1)*128].astype(BF)
    gml[2*L:16,:]=jnp.zeros((16-2*L,128),BF)
    gl.start()
    me=gl.me
    feats=ada.shape[0]
    width=low.shape[1]
    pick=(lax.broadcasted_iota(jnp.int32,(width,feats),0)==lax.broadcasted_iota(jnp.int32,(width,feats),1)+feats*me).astype(BF)
    mine=jnp.dot(low[...],pick,preferred_element_type=F32).astype(BF)
    acc=jnp.zeros((NDEV,feats),F32)
    ge.wait()
    def use(src,n,base,acc):
        for i in range(n):
            g=src[:,i,:]
            j=base+i
            adag_o[:,j*128:(j+1)*128]=lax.dot_general(mine,g,TN,preferred_element_type=F32)
            gm_o[j:j+1,:]=jnp.sum(g.astype(F32),axis=0,keepdims=True)
            acc=acc+lax.dot_general(g,ada[:,j*128:(j+1)*128],NT,preferred_element_type=F32)
        return acc
    acc=use(gmev,4*L,2*L,acc)
    stp.cstep()
    gl.wait()
    acc=use(gmlv,2*L,0,acc)
    for n in range(NDEV):
        g0=(n//NR)*NR
        ctxs[n,0:NR,0:feats]=acc[g0:g0+NR,:]
    xa.start()
    sz.step()
    slq.zstep()
    stp.xstep()
    st.wait()
    def up(i):
        for b in range(NR):
            tg_o[b,rows_of(i,EC),:]=tgin[b,rows_of(i,EC),:].astype(F32)
    loop(block//EC,up)
    stp.zstep()
    xa.wait()
    ctx_o[...]=ctxv[...]
    for s in (sz,slq,stp,st,ge,gl,xa): s.finish()


def tail(gproj,qkv,m1,x,gmid,mod,taps,ml,mr,rl,sums,gkf,low,ada,zq,lastq,side,cols,ta,tf):
    cells,feat=x.shape
    block=cells//NR
    r_=feat//NDEV
    V=pltpu.VMEM
    L=feat//128
    outs=[S_((NR,block,feat),F32),S_((NDEV,8,128),F32),S_(ada.shape,F32),S_((6*L,128),F32),S_((r_,3*feat),F32),S_((9,ta),F32),S_((9,tf),F32)]
    scr=[V((cells,feat),F32),V((cells,feat),F32),V((NR,block,feat),BF),V((NR,block,feat),BF),V((16,feat),F32),
         V((4*L,128),BF),V((16,128),BF),V((NDEV,4*L,128),BF),V((NDEV,16,128),BF),V((NDEV,8,128),F32),V((NDEV,8,128),F32),V((NZ,NC,NR,16,128),F32),V(gproj.shape,BF),V(qkv.shape,BF),V(gmid.shape,F32),pltpu.SemaphoreType.DMA((3,))]
    scr+=ScatterZ.scratch(r_,zq.shape[2],BF)+Scatter.scratch(r_,feat,BF)+Scatter.scratch(16,128,F32)
    sems=sem_types(ScatterZ.SEMS)+sem_types(Scatter.SEMS)*2+sem_types(Swap.SEMS)+sem_types(AllToAll.SEMS)*3
    return pl.pallas_call(
        functools.partial(tail_kernel,side,cols,ta,tf),
        in_specs=[HBM,HBM,VM,VM,HBM]+[VM]*4+[SM]+[VM]*6,
        out_specs=[VM]*7,
        out_shape=outs,
        scratch_shapes=scr+sems,
        compiler_params=pltpu.CompilerParams(collective_id=3,has_side_effects=True,vmem_limit_bytes=63<<20),
        name="tail",
    )(gproj,qkv,m1,x,gmid,mod,taps,ml,mr,rl,sums,gkf,low,ada,zq,lastq)


def greet(targets):
    bar=pltpu.get_barrier_semaphore()
    for d in targets:
        pl.semaphore_signal(bar,inc=1,device_id=d,device_id_type=MESH)
    pl.semaphore_wait(bar,len(targets))


def near():
    z,core,rows=here()
    return [dev(z,1-core,rows)]+[dev(z,core,partner_xy(rows,t)) for t in range(1,NR)]


class PipeScatter:
    SEMS=[(2,),(2,),(2,NR),(2,NR)]
    @staticmethod
    def scratch(r,c):
        return [pltpu.VMEM((2,NZ,NC,NR,r,c),BF),pltpu.VMEM((2,NZ,NR,r,c),BF),pltpu.VMEM((2,NZ,NR,r,c),BF),pltpu.VMEM((2,NR,NZ,r,c),BF)]
    def __init__(self,bufs,sems):
        self.part,self.sib,self.own,self.xin=bufs
        self.sc,self.rc,self.sx,self.rx=sems
        self.z,self.core,self.rows=here()
    def ccopy(self,s):
        return rcopy(self.part.at[s,:,1-self.core],self.sib.at[s],self.sc.at[s],self.rc.at[s],dev(self.z,1-self.core,self.rows))
    def xcopy(self,s,t):
        to=partner_xy(self.rows,t)
        return rcopy(self.own.at[s,:,to],self.xin.at[s,t],self.sx.at[s,t],self.rx.at[s,t],dev(self.z,self.core,to))
    def send_core(self,s):
        self.ccopy(s).start()
    def send_square(self,s):
        self.ccopy(s).wait()
        def body(i):
            a,b=i//NR,lax.rem(i,NR)
            self.own[s,a,b]=(self.part[s,a,self.core,b].astype(F32)+self.sib[s,a,b].astype(F32)).astype(BF)
        loop(NZ*NR,body)
        for t in range(1,NR): self.xcopy(s,t).start()
    def collect(self,s,put):
        for t in range(1,NR): self.xcopy(s,t).wait()
        def body(a):
            v=self.own[s,a,self.rows].astype(F32)
            for t in range(1,NR): v=v+self.xin[s,t,a].astype(F32)
            put(a,v.astype(BF))
        loop(NZ,body)


class RowScatter:
    SEMS=[(2,),(2,),(2,NR),(2,NR)]
    @staticmethod
    def scratch(r,c):
        return [pltpu.VMEM((2,NR,r,c),BF),pltpu.VMEM((2,NR,r,c),BF),pltpu.VMEM((2,NR,r,c),BF)]
    def __init__(self,part,zout,bufs,sems):
        self.part,self.zout=part,zout
        self.sib,self.own,self.xin=bufs
        self.sc,self.rc,self.sx,self.rx=sems
        self.z,self.core,self.rows=here()
    def ccopy(self,k):
        s=k%2
        return rcopy(self.part.at[k,1-self.core],self.sib.at[s],self.sc.at[s],self.rc.at[s],dev(self.z,1-self.core,self.rows))
    def xcopy(self,k,t):
        s=k%2
        to=partner_xy(self.rows,t)
        return rcopy(self.own.at[s,to],self.xin.at[s,t],self.sx.at[s,t],self.rx.at[s,t],dev(self.z,self.core,to))
    def send_core(self,k):
        self.ccopy(k).start()
    def send_square(self,k):
        self.ccopy(k).wait()
        s=k%2
        def body(b):
            self.own[s,b]=(self.part[k,self.core,b].astype(F32)+self.sib[s,b].astype(F32)).astype(BF)
        loop(NR,body)
        for t in range(1,NR): self.xcopy(k,t).start()
    def collect(self,k):
        s=k%2
        for t in range(1,NR): self.xcopy(k,t).wait()
        v=self.own[s,self.rows].astype(F32)
        for t in range(1,NR): v=v+self.xin[s,t].astype(F32)
        self.zout[k]=v.astype(BF)


def ffn_kernel_body(*refs,side,cols):
    it=iter(refs)
    nx=lambda n:[next(it) for _ in range(n)]
    x_ref,att_ref,cot_ref,mod_ref,outw_ref,zpu,zpd,tap_ref,ml_ref,mr_ref,rl_ref=nx(11)
    lay_ref,gmid_ref,gatt_ref,gout_ref,zup,zdown,gtap_ref,sums_ref=nx(8)
    m2,m2t,gffn,branch,fb,gm2,F,G,glow,gub,dfull,ufull,gd,ucur=nx(14)
    ubufs=nx(4); dbufs=nx(3)
    take=taker(it)
    ga=GatherXY(zpd,dfull,take(GatherXY))
    T=F.shape[1]
    gu=GatherTile(zpu,ufull,T,nx(5))
    middle=gmid_ref
    us=PipeScatter(ubufs,take(PipeScatter))
    ds=RowScatter(gd,zdown,dbufs,take(RowScatter))
    t=pl.program_id(0)
    cells,feat=x_ref.shape
    hidden=NDEV*zpd.shape[1]
    steps=hidden//T; last=steps-1
    block=hidden//NZ
    CH=1024; EC=256
    shift2=mod_ref[3:4,:]; scale2=mod_ref[4:5,:]; gate2=mod_ref[5:6,:]; gate1=mod_ref[2:3,:]
    slot=lax.rem(t,2); other=lax.rem(t+1,2)
    ready={}
    for k in range(NZ): ready[k]=-(-((k+1)*block)//T)-1
    need={}
    for k in range(NZ): need[k]=(k*block)//T
    def put_up(tile):
        def put(a,v): zup[a,:,pl.ds(pl.multiple_of(tile*T,128),T)]=v
        return put

    @pl.when(t==0)
    def _():
        greet(near())
        gu.local().start(); ga.start_local()
        gu.start(0); ga.start([0])
        def a(i):
            branch[rows_of(i,EC),:]=dotf(att_ref[rows_of(i,EC),:],outw_ref[...])
        loop(cells//EC,a)
        def b(i):
            r=rows_of(i,EC)
            mid=x_ref[r,:].astype(F32)+gate1*branch[r,:]
            middle[r,:]=mid
            n,_=normal_rows(mid)
            m2[r,:]=(n*(1.0+scale2)+shift2).astype(BF)
            gffn[r,:]=(gate2*cot_ref[r,:].astype(F32)).astype(BF)
        loop(cells//EC,b)
        gu.step(0); ga.step(0)
        gu.start(1); ga.start([1])
        def c(i):
            r=rows_of(i,EC)
            m2t[:,pl.ds(pl.multiple_of(i*EC,EC),EC)]=jnp.transpose(m2[r,:])
            fb[r,:]=jnp.zeros((EC,feat),F32)
            gm2[r,:]=jnp.zeros((EC,feat),F32)
        loop(cells//EC,c)
        gu.step2(0); ga.step2(0)
        ga.local().wait(); gu.local().wait()
    gu.arrive(t)
    for k in range(NZ):
        @pl.when(t==need[k])
        def _(k=k): ga.arrive(k)
    dw=dfull.reshape(hidden,feat)
    tc=pl.ds(pl.multiple_of(t*T,T),T)
    def flat(i):
        n=feat//NZ
        ucur[rows_of(i,n),:]=ufull[i,:,:,:,tc].reshape(n,T)
    loop(NZ,flat)
    gdw=gd.reshape(hidden,feat)
    tr=pl.ds(pl.multiple_of(t*T,T),T)
    def first(i):
        r=rows_of(i,CH)
        F[r,:]=dotf(m2[r,:],ucur[...]).astype(BF).astype(F32)
        G[r,:]=dotf(gffn[r,:],dw[tr,:],NT)
    loop(cells//CH,first)
    @pl.when(t<last)
    def _(): gu.step(t+1)
    for k in range(1,NZ):
        @pl.when(t==k-1)
        def _(k=k): ga.step(k)
    @pl.when(t<last-1)
    def _(): gu.start(t+2)
    for k in range(2,NZ):
        @pl.when(t==k-2)
        def _(k=k): ga.start([k])

    def forward_lanes(l):
        ls=pl.ds(pl.multiple_of(l*128,128),128)
        def put(i,u):
            r=rows_of(i,cols)
            u2=u*u
            th=jnp.tanh(C0*(u+C1*(u2*u)))
            half=0.5*(1.0+th)
            glow[r,ls]=(u*half).astype(BF)
            d=half+(0.5*u)*(1.0-th*th)*(C0*(1.0+(3.0*C1)*u2))
            G[r,ls]=(G[r,ls]*d).astype(BF).astype(F32)
        conv_rows(F,put,tap_ref[:,ls],ml_ref,mr_ref,rl_ref,ls,side,cols)
    loop(T//128,forward_lanes)
    @pl.when(t<last)
    def _(): gu.step2(t+1)
    @pl.when(t>=2)
    def _(): us.collect(slot,put_up(t-2))
    for k in range(NZ):
        if ready[k]+2<=last:
            @pl.when(t==ready[k]+2)
            def _(k=k): ds.collect(k)
    @pl.when(t>=1)
    def _():
        us.send_square(other)
    for k in range(NZ):
        if ready[k]+1<=last:
            @pl.when(t==ready[k]+1)
            def _(k=k): ds.send_square(k)
    def back_lanes(l):
        ls=pl.ds(pl.multiple_of(l*128,128),128)
        def put2(i,u):
            gub[rows_of(i,cols),ls]=u.astype(BF)
        acc=back_rows(G,F,put2,tap_ref[:,ls],ml_ref,mr_ref,rl_ref,ls,0,side,side,cols)
        for q in range(9):
            gtap_ref[q:q+1,ls]=jnp.sum(acc[q],axis=0,keepdims=True)
    loop(T//128,back_lanes)
    for k in range(1,NZ):
        @pl.when(t==k-1)
        def _(k=k): ga.step2(k)
    gtap_ref[9:16,:]=jnp.zeros((7,T),F32)

    r_=feat//NDEV
    def third(i):
        n=NC*NR*r_
        us.part[slot,i]=dotf(m2t[rows_of(i,n),:],gub[...]).astype(BF).reshape(NC,NR,r_,T)
    loop(NZ,third)
    us.send_core(slot)
    for i in range(T//256):
        gdw[pl.ds(pl.multiple_of(t*T+i*256,256),256),:]=dotf(glow[:,i*256:(i+1)*256],gffn[...],TN).astype(BF)
    for k in range(NZ):
        @pl.when(t==ready[k])
        def _(k=k): ds.send_core(k)
    def second(i):
        r=rows_of(i,CH)
        fb[r,:]+=dotf(glow[r,:],dw[tr,:])
        gm2[r,:]+=dotf(gub[r,:],ucur[...],NT)
    loop(cells//CH,second)

    @pl.when(t==last)
    def _():
        us.collect(other,put_up(last-1))
        late=[k for k in range(NZ) if ready[k]+1>last]
        mid_=[k for k in range(NZ) if ready[k]+1==last]
        for k in mid_: ds.collect(k)
        us.send_square(slot)
        for k in late: ds.send_square(k)
        z=jnp.zeros((8,feat),F32)
        def body(i,c):
            sg2,ss2,sc2,sg1=c
            r=rows_of(i,EC)
            inc=cot_ref[r,:].astype(F32)
            mid=middle[r,:]
            n,inv=normal_rows(mid)
            lay_ref[r,:]=(mid+gate2*fb[r,:]).astype(BF)
            gm=gm2[r,:]
            gmid=inc+normal_back_rows(gm*(1.0+scale2),n,inv)
            gmid_ref[r,:]=gmid
            gffn[r,:]=(gate1*gmid).astype(BF)
            return (sg2+fold8(inc*fb[r,:]),ss2+fold8(gm),sc2+fold8(gm*n),sg1+fold8(gmid*branch[r,:]))
        res=lax.fori_loop(0,cells//EC,body,(z,z,z,z))
        for q in range(4):
            sums_ref[q:q+1,:]=jnp.sum(res[q],axis=0,keepdims=True)
        sums_ref[4:8,:]=jnp.zeros((4,feat),F32)
        def b(i):
            r=rows_of(i,512)
            gatt_ref[r,:]=dotf(gffn[r,:],outw_ref[...],NT).astype(BF)
        loop(cells//512,b)
        for i in range(feat//256):
            gout_ref[i*256:(i+1)*256,:]=dotf(att_ref[:,i*256:(i+1)*256],gffn[...],TN).astype(BF)
        us.collect(slot,put_up(last))
        for k in late: ds.collect(k)
        ga.finish_remote()
        loop(steps,gu.finish_remote)


def ffn(x,att,cot,mod6,outw,zpu,zpd,taps,ml,mr,rl,side,cols,T=512):
    cells,feat=x.shape
    hidden=zpu.shape[2]
    vm=lambda shape: pl.BlockSpec(shape,lambda t:(0,)*len(shape),pipeline_mode=pl.Buffered(1))
    r_,d_=feat//NDEV,hidden//NDEV
    return pl.pallas_call(
        functools.partial(ffn_kernel_body,side=side,cols=cols),
        grid=(hidden//T,),
        in_specs=[vm((cells,feat)),vm((cells,feat)),vm((cells,feat)),vm((8,feat)),vm((feat,feat)),
                  HBM,HBM,pl.BlockSpec((16,T),lambda t:(0,t)),
                  vm((cells,128)),vm((cells,128)),SM],
        out_specs=[vm((cells,feat)),vm((cells,feat)),vm((cells,feat)),vm((feat,feat)),
                   vm((NZ,r_,hidden)),vm((NZ,d_,feat)),pl.BlockSpec((16,T),lambda t:(0,t)),vm((8,feat))],
        out_shape=[S_((cells,feat),BF),S_((cells,feat),F32),S_((cells,feat),BF),S_((feat,feat),BF),S_((NZ,r_,hidden),BF),S_((NZ,d_,feat),BF),S_((16,hidden),F32),S_((8,feat),F32)],
        scratch_shapes=[pltpu.VMEM((cells,feat),BF),pltpu.VMEM((feat,cells),BF),pltpu.VMEM((cells,feat),BF),
                        pltpu.VMEM((cells,feat),F32),pltpu.VMEM((cells,feat),F32),pltpu.VMEM((cells,feat),F32),
                        pltpu.VMEM((cells,T),F32),pltpu.VMEM((cells,T),F32),pltpu.VMEM((cells,T),BF),pltpu.VMEM((cells,T),BF),
                        pltpu.VMEM((NZ,NC,NR,d_,feat),BF),pltpu.VMEM((NZ,NC,NR,r_,hidden),BF),pltpu.VMEM((NZ,NC,NR,d_,feat),BF),pltpu.VMEM((feat,T),BF)]
                       +PipeScatter.scratch(r_,T)+RowScatter.scratch(d_,feat)
                       +sem_types(GatherXY.SEMS)+sem_types(GatherTile.sems(hidden//T))+sem_types(PipeScatter.SEMS)+sem_types(RowScatter.SEMS),
        compiler_params=pltpu.CompilerParams(dimension_semantics=("arbitrary",),vmem_limit_bytes=63<<20,collective_id=4,has_side_effects=True),
        name="ffn",
    )(x,att,cot,mod6,outw,zpu,zpd,taps,ml,mr,rl)
def own_rows(padded_cells):
    return jnp.pad(padded_cells,((0,0),(1,1),(1,1),(0,0)))


def fast(tokens,conditioning,item_map,ada_weight,ada_bias,attn_kernel,qkv_weight,out_weight,up_weight,ffn_kernel,down_weight,out_cotangent):
    canvases,rows_here,cols,features=tokens.shape
    side=rows_here*NR
    cells=side*cols
    rows=lax.axis_index("rows"); dp=lax.axis_index("dp"); me=dp*NR+rows
    hidden=up_weight.shape[1]
    cond_row=jnp.pad(conditioning,((0,8-NR),(0,0)))
    mod_cols=ada_weight.shape[1]
    bshard=ada_bias.shape[0]
    bias_rows=lax.dynamic_update_slice_in_dim(jnp.zeros((mod_cols,),F32),ada_bias.astype(F32),me*bshard,0).reshape(mod_cols//128,128)
    ta,tf=attn_kernel.shape[1],ffn_kernel.shape[1]
    taps=jnp.pad(jnp.concatenate([attn_kernel,ffn_kernel],axis=1),((0,7),(0,128-ta-tf)))
    blocks=(NR,rows_here*cols,features)
    labels=lax.dynamic_index_in_dim(item_map,rows,0,keepdims=False)
    lab=jnp.broadcast_to(labels.reshape(cells,1),(cells,128))
    top=labels[:,0]//2
    rl=jnp.pad((top[1:]==top[:-1]).astype(F32),(1,1))
    tok,low_all,mod,qkv_f,tap_a,tap_f,m1,mix,ml,mr,qm,km,*zps=enter(tokens.reshape(blocks),cond_row,ada_weight,bias_rows,qkv_weight,taps,lab,rl,[out_weight],side,cols,ta,tf)
    full2=lambda a:a.reshape(-1,a.shape[-1])
    triple_full=full2(qkv_f)
    mod6=jnp.pad(mod.reshape(6,features),((0,2),(0,0)))
    proj,attended,lse_t,cot,zp_down,zp_up,out_f=forward(mix,triple_full,qm,km,out_cotangent.reshape(blocks),down_weight,up_weight,zps)
    lay,gmid,gatt,g_out,z_up,z_down,g_kffn,sums=ffn(
        tok.reshape(cells,features),attended,cot.reshape(cells,features),mod6,
        full2(out_f),zp_up,zp_down,tap_f,ml,mr,rl,side,cols)
    sp=lambda g:g.reshape(NZ,NC,NR,g.shape[0]//NDEV,g.shape[1])
    gproj,lay_o,o_o,zq,lastq,u_o,d_o=backward(proj,gatt,attended,qm,km,lse_t,mix,lay.reshape(blocks),sp(g_out),[z_up,z_down])
    tg,ctx,adag,gmsum,q_o,ka_o,kf_o=tail(gproj,triple_full,m1,tok.reshape(cells,features),gmid,mod6,
        tap_a,ml,mr,rl,sums,g_kffn,low_all,ada_weight,zq,lastq,side,cols,ta,tf)
    shape4=(NR,rows_here,cols,features)
    feats=ada_weight.shape[0]
    dsilu=ctx[:,:NR,:feats].transpose(1,0,2).reshape(NR,features)
    cv=conditioning.astype(F32)
    _,sback=jax.vjp(jax.nn.silu,cv)
    dctx=sback(dsilu)[0]
    gbias=lax.dynamic_slice_in_dim(gmsum.reshape(mod_cols),me*bshard,bshard,0)
    return (lay_o.reshape(shape4),tg.reshape(shape4),dctx,adag,gbias,ka_o,q_o,o_o,u_o,kf_o,d_o)


def solution(mesh):
    quick=dict(mesh.shape)=={"dp":NZ*NC,"rows":NR}
    return jax.shard_map(
        fast if quick else local,
        mesh=mesh,
        in_specs=(
            P("dp", "rows", None, None),
            P("dp", None),
            P("dp", None, None),
            P(("dp", "rows"), None),
            P(("dp", "rows")),
            P(None, ("dp", "rows")),
            P(("dp", "rows"), None),
            P(("dp", "rows"), None),
            P(("dp", "rows"), None),
            P(None, ("dp", "rows")),
            P(("dp", "rows"), None),
            P("dp", "rows", None, None),
        ),
        out_specs=(
            P("dp", "rows", None, None),
            P("dp", "rows", None, None),
            P("dp", None),
            P(("dp", "rows"), None),
            P(("dp", "rows")),
            P(None, ("dp", "rows")),
            P(("dp", "rows"), None),
            P(("dp", "rows"), None),
            P(("dp", "rows"), None),
            P(None, ("dp", "rows")),
            P(("dp", "rows"), None),
        ),
        check_vma=False,
    )
```
